32 devices in a mesh: fsdp: 4 (over z), ctx: 2 (over x), tp: 4 (over y, core).
Axes of the slice: x: 2, y: 2, z: 4, core: 2. Of those that a mesh axis runs over, the one named last changes fastest.
Arguments:
- hidden: bfloat16 [1536, 2048], P(('fsdp', 'ctx')), may hold values from -6 to 6
- embeds: bfloat16 [1536, 2048], P(('fsdp', 'ctx')), may hold values from -6 to 6
- cotangent: bfloat16 [1536, 2048], P(('fsdp', 'ctx')), may hold values from -6 to 6
- lengths: int32 [4, 3], P('fsdp'), may hold values from 1 to 192, 384 in all within a row
- attention_norm_gain: float32 [4096], replicated, may hold values from 0.5 to 1.5
- adapter_down_maps: bfloat16 [3, 4096, 128], replicated, may hold values from -0.09375 to 0.09375
- query_key_value_weight: bfloat16 [3, 4096, 4096], P(None, ('fsdp', 'ctx'), 'tp'), may hold values from -0.09375 to 0.09375
- adapter_up_maps: bfloat16 [3, 128, 4096], P(None, None, 'tp'), may hold values from -0.5 to 0.5
- attention_output_weight: bfloat16 [4096, 2048], P('tp', ('fsdp', 'ctx')), may hold values from -0.375 to 0.375
- feedforward_norm_gain: float32 [2048], replicated, may hold values from 0.5 to 1.5
- gate_up_weight: bfloat16 [2, 2048, 8192], P(None, ('fsdp', 'ctx'), 'tp'), may hold values from -0.125 to 0.125
- down_weight: bfloat16 [8192, 2048], P('tp', ('fsdp', 'ctx')), may hold values from -0.0625 to 0.0625
- mixer_norm_gain: float32 [2048], replicated, may hold values from 0.5 to 1.5
- mixer_gate_input_weight: bfloat16 [2, 2048, 4096], P(None, ('fsdp', 'ctx'), 'tp'), may hold values from -0.125 to 0.125
- state_map_weight: bfloat16 [2048, 256], replicated, may hold values from -0.125 to 0.125
- step_size_weight: bfloat16 [2048, 64], P(None, 'tp'), may hold values from -0.0625 to 0.0625
- mixer_input_taps: float32 [4, 4096], P(None, 'tp'), may hold values from -3 to 3
- mixer_input_tap_bias: float32 [4096], P('tp'), may hold values from -0.5 to 0.5
- state_map_taps: float32 [4, 256], replicated, may hold values from -3 to 3
- state_map_tap_bias: float32 [256], replicated, may hold values from -0.5 to 0.5
- step_size_bias: float32 [64], P('tp'), may hold values from -7 to -2
- log_decay_rate: float32 [64], P('tp'), may hold values from 0 to 2.77
- head_skip_weight: float32 [64], P('tp'), may hold values from 0.5 to 2
- gated_norm_gain: float32 [4096], P('tp'), may hold values from 0.5 to 1.5
- mixer_output_weight: bfloat16 [4096, 2048], P('tp', ('fsdp', 'ctx')), may hold values from -0.09375 to 0.09375
Outputs:
- out: bfloat16 [1536, 2048], P(('fsdp', 'ctx'))
- d_hidden: float32 [1536, 2048], P(('fsdp', 'ctx'))
- d_embeds: float32 [1536, 2048], P(('fsdp', 'ctx'))
- grad_g_attn: float32 [4096], replicated
- adapter_down_gradient: float32 [3, 4096, 128], replicated
- grad_w_qkv: float32 [3, 4096, 4096], P(None, ('fsdp', 'ctx'), 'tp')
- adapter_up_gradient: float32 [3, 128, 4096], P(None, None, 'tp')
- grad_w_o: float32 [4096, 2048], P('tp', ('fsdp', 'ctx'))
- grad_g_mlp: float32 [2048], replicated
- grad_w_gu: float32 [2, 2048, 8192], P(None, ('fsdp', 'ctx'), 'tp')
- grad_w_down: float32 [8192, 2048], P('tp', ('fsdp', 'ctx'))
- grad_g_mamba: float32 [2048], replicated
- grad_w_zx: float32 [2, 2048, 4096], P(None, ('fsdp', 'ctx'), 'tp')
- grad_w_bc: float32 [2048, 256], replicated
- grad_w_dt: float32 [2048, 64], P(None, 'tp')
- grad_conv_x: float32 [4, 4096], P(None, 'tp')
- grad_conv_x_bias: float32 [4096], P('tp')
- grad_conv_bc: float32 [4, 256], replicated
- grad_conv_bc_bias: float32 [256], replicated
- grad_dt_bias: float32 [64], P('tp')
- grad_a_log: float32 [64], P('tp')
- grad_d_skip: float32 [64], P('tp')
- grad_g_gate: float32 [4096], P('tp')
- grad_w_out: float32 [4096, 2048], P('tp', ('fsdp', 'ctx'))
The draws below stay inside these ranges and needn't reach their ends.
Inputs may be any that keep to these rules, and one draw needn't show every extreme that they name: `lengths`: each row lists the 3 sequences of one group of 384 tokens in order; the row sums to 384 and its largest length is exactly 192.
All inputs are finite; a program needn't handle non-finite values.
Results may differ from the reference program's by a relative error of at most 0.035.
Values may be sent and summed in bfloat16 or wider, within the bound.
A program may use at most 384 MiB of HBM per device.

```python
import math
import jax
import jax.numpy as jnp
import numpy as np
from jax import lax

MODEL_WIDTH = 2048
FF = 8192
AHEADS = 32
AHD = 128
MHEADS = 64
INNER = 4096
MIXER_HEAD_SIZE = 64
STATE = 128
ADAPTER_RANK = 128
CONV = 4
SPAN = 128
GROUP = 384
TOKENS = 1536
SEQS = 3
LMAX = 192
QBLK = 384
N_FSDP = 4


def block_scale(rng, extent, shards, low, top_value):
    factor_of, own = 1.0, jax.random.fold_in(rng, 6)
    for dim, blocks in shards:
        heights = jnp.exp(jax.random.uniform(jax.random.fold_in(own, dim), (blocks,), jnp.float32, low / len(shards), top_value / len(shards)))
        factor_of = factor_of * jnp.repeat(heights, extent[dim] // blocks).reshape([-1 if axis == dim else 1 for axis in range(len(extent))])
    return factor_of


def length_profile(count, total, limit, slope):
    portions = [(1 << 20) // math.isqrt(grade ** slope) + 1 for grade in range(2, count + 1)]
    rest, holding = total - limit - (count - 1), [1] * (count - 1)
    while rest > 0:
        candidates = [i for i in range(count - 1) if holding[i] < limit]
        mass, budget = sum([portions[i] for i in candidates]), rest
        for i in candidates:
            more = min(limit - holding[i], max(1, budget * portions[i] // mass), rest)
            holding[i] = holding[i] + more
            rest = rest - more
    return np.array([limit] + holding)


def uneven_parts(stream_key, amount, total, bound, slope):
    if amount == 2:
        one = jax.random.randint(stream_key, (), max(1, total - bound), min(bound, total - 1) + 1)
        return jnp.stack([one, total - one])
    sizes = jnp.asarray(length_profile(amount, total, bound, slope), jnp.int32)
    twos = (amount - 1) // 2
    source_of, taker = sizes[1:1 + 2 * twos:2], sizes[2:2 + 2 * twos:2]
    slack = jnp.minimum(source_of - 1, bound - taker)
    moved = jax.random.randint(jax.random.fold_in(stream_key, 1), (twos,), 0, 1 << 20) % (slack + 1)
    sizes = sizes.at[1:1 + 2 * twos:2].set(source_of - moved).at[2:2 + 2 * twos:2].set(taker + moved)
    return sizes[jax.random.permutation(jax.random.fold_in(stream_key, 2), amount)]


def scatter_about(rng, shape, width, most, cuts=(), held_as=jnp.bfloat16):
    entries = width * jax.random.normal(rng, shape, jnp.float32)
    if cuts:
        entries = entries * block_scale(rng, shape, cuts, -0.22, 0.18)
    return jnp.clip(entries, -most, most).astype(held_as)


def setup_inputs(seed: int = 0) -> dict:
    key_of = jax.random.split(jax.random.key(seed), 26)
    return {
        "hidden": scatter_about(key_of[0], (TOKENS, MODEL_WIDTH), 1.0, 6.0, ((0, 8),)),
        "embeds": scatter_about(key_of[1], (TOKENS, MODEL_WIDTH), 1.0, 6.0, ((0, 8),)),
        "cotangent": scatter_about(key_of[2], (TOKENS, MODEL_WIDTH), 1.0, 6.0, ((0, 8),)),
        "lengths": jax.vmap(lambda own: uneven_parts(own, SEQS, GROUP, LMAX, 2))(jax.random.split(key_of[3], N_FSDP)).reshape((N_FSDP, SEQS)).astype(jnp.int32),
        "attention_norm_gain": jnp.clip(1.0 + 0.1 * jax.random.normal(key_of[4], (2 * MODEL_WIDTH,), jnp.float32), 0.5, 1.5),
        "adapter_down_maps": scatter_about(key_of[5], (3, 2 * MODEL_WIDTH, ADAPTER_RANK), (2 * MODEL_WIDTH) ** -0.5, 0.09375),
        "query_key_value_weight": scatter_about(key_of[6], (3, 2 * MODEL_WIDTH, 2 * MODEL_WIDTH), (2 * MODEL_WIDTH) ** -0.5, 0.09375, ((1, 8), (2, 4))),
        "adapter_up_maps": scatter_about(key_of[7], (3, ADAPTER_RANK, 2 * MODEL_WIDTH), ADAPTER_RANK ** -0.5, 0.5, ((2, 4),)),
        "attention_output_weight": scatter_about(key_of[8], (2 * MODEL_WIDTH, MODEL_WIDTH), (2 * MODEL_WIDTH // 16) ** -0.5, 0.375, ((0, 4), (1, 8))),
        "feedforward_norm_gain": jnp.clip(1.0 + 0.1 * jax.random.normal(key_of[9], (MODEL_WIDTH,), jnp.float32), 0.5, 1.5),
        "gate_up_weight": scatter_about(key_of[10], (2, MODEL_WIDTH, FF), MODEL_WIDTH ** -0.5, 0.125, ((1, 8), (2, 4))),
        "down_weight": scatter_about(key_of[11], (FF, MODEL_WIDTH), FF ** -0.5, 0.0625, ((0, 4), (1, 8))),
        "mixer_norm_gain": jnp.clip(1.0 + 0.1 * jax.random.normal(key_of[12], (MODEL_WIDTH,), jnp.float32), 0.5, 1.5),
        "mixer_gate_input_weight": scatter_about(key_of[13], (2, MODEL_WIDTH, INNER), MODEL_WIDTH ** -0.5, 0.125, ((1, 8), (2, 4))),
        "state_map_weight": scatter_about(key_of[14], (MODEL_WIDTH, 2 * STATE), MODEL_WIDTH ** -0.5, 0.125),
        "step_size_weight": scatter_about(key_of[15], (MODEL_WIDTH, MHEADS), (4 * MODEL_WIDTH) ** -0.5, 0.0625, ((1, 4),)),
        "mixer_input_taps": scatter_about(key_of[16], (CONV, INNER), CONV ** -0.5, 3.0, ((1, 4),), jnp.float32),
        "mixer_input_tap_bias": jnp.clip(jax.random.uniform(key_of[17], (INNER,), jnp.float32, -0.5, 0.5) * block_scale(key_of[17], (INNER,), ((0, 4),), -0.4, 0.0), -0.5, 0.5),
        "state_map_taps": scatter_about(key_of[18], (CONV, 2 * STATE), CONV ** -0.5, 3.0, (), jnp.float32),
        "state_map_tap_bias": jnp.clip(jax.random.uniform(key_of[19], (2 * STATE,), jnp.float32, -0.5, 0.5), -0.5, 0.5),
        "step_size_bias": jnp.clip(-7.0 + 5.0 * jax.random.uniform(key_of[20], (MHEADS,), jnp.float32) ** block_scale(key_of[20], (MHEADS,), ((0, 4),), -0.2, 0.2), -7.0, -2.0),
        "log_decay_rate": jnp.clip(2.77 * jax.random.uniform(key_of[21], (MHEADS,), jnp.float32) ** block_scale(key_of[21], (MHEADS,), ((0, 4),), -0.2, 0.2), 0.0, 2.77),
        "head_skip_weight": jnp.clip(0.5 + 1.5 * jax.random.uniform(key_of[22], (MHEADS,), jnp.float32) ** block_scale(key_of[22], (MHEADS,), ((0, 4),), -0.2, 0.2), 0.5, 2.0),
        "gated_norm_gain": jnp.clip(1.0 + 0.1 * jax.random.normal(key_of[23], (INNER,), jnp.float32), 0.5, 1.5),
        "mixer_output_weight": scatter_about(key_of[24], (INNER, MODEL_WIDTH), INNER ** -0.5, 0.09375, ((0, 4), (1, 8))),
    }


highest = lax.Precision.HIGHEST
epsilon = 1e-05

@jax.custom_vjp
def low(v):
    return lax.optimization_barrier(v.astype(jnp.bfloat16)).astype(jnp.float32)

@jax.custom_vjp
def low_back(v):
    return v

def low_keep(v):
    return (low(v), None)

def low_pass(kept, grad):
    return (grad,)

def back_keep(v):
    return (v, None)

def back_low(kept, grad):
    return (low(grad),)
low.defvjp(low_keep, low_pass)
low_back.defvjp(back_keep, back_low)

def rounded_pair(values):
    return low(low_back(values))

def matrix_product(left, right):
    return jnp.dot(left, right, precision=highest)

def rms_scale(values, gain):
    return values * lax.rsqrt(lax.optimization_barrier(jnp.mean(values * values, axis=-1, keepdims=True)) + epsilon) * gain

def layout(lengths_row, total_rows):
    lengths_row = lengths_row.astype(jnp.int32)
    ends = jnp.cumsum(lengths_row).astype(jnp.int32)
    slot_index = jnp.arange(total_rows, dtype=jnp.int32)
    passed = (slot_index[:, None] >= ends[None, :]).astype(jnp.int32)
    segment = lax.optimization_barrier(jnp.sum(passed, axis=1)).astype(jnp.int32)
    position = (slot_index - lax.optimization_barrier(jnp.sum(passed * lengths_row[None, :], axis=1))).astype(jnp.int32)
    return (segment, position, slot_index)

def causal_conv(values, kernel, bias, position):
    total_rows = values.shape[0]
    total = values * kernel[0][None, :] + bias[None, :]
    for lag in range(1, kernel.shape[0]):
        shifted = jnp.concatenate([jnp.zeros((lag, values.shape[1]), values.dtype), values[:total_rows - lag]], axis=0)
        keep = (position >= lag).astype(values.dtype)[:, None]
        total = total + shifted * keep * kernel[lag][None, :]
    return jax.nn.silu(total)

def rotate(values, position):
    half_dim = values.shape[-1] // 2
    inverse = 10000.0 ** (-jnp.arange(half_dim, dtype=jnp.float32) / half_dim)
    angle = position.astype(jnp.float32)[:, None] * inverse[None, :]
    cosine = jnp.cos(angle)[:, None, :]
    sine_part = jnp.sin(angle)[:, None, :]
    first_half = values[..., :half_dim]
    second_half = values[..., half_dim:]
    return jnp.concatenate([first_half * cosine - second_half * sine_part, second_half * cosine + first_half * sine_part], axis=-1)

def attend_all(queries, keys_all, vals_all, segment, slot_index, block_rows):
    group_row_block, count_of_heads, head_dim = queries.shape
    scaling = head_dim ** (-0.5)
    block_count = group_row_block // block_rows

    def one_block(inputs):
        query_part, query_seg, query_slot = inputs
        scores = jnp.einsum('qhd,khd->hqk', query_part, keys_all, precision=highest) * scaling
        allowed = (query_seg[:, None] == segment[None, :]) & (query_slot[:, None] >= slot_index[None, :])
        scores = jnp.where(allowed[None], scores, -1e+30)
        weights = jnp.exp(scores)
        weights_low = rounded_pair(weights / lax.optimization_barrier(jnp.sum(weights, axis=-1, keepdims=True)))
        return jnp.einsum('hqk,khd->qhd', weights_low, vals_all, precision=highest)
    mapped = lax.map(jax.checkpoint(one_block), (queries.reshape(block_count, block_rows, count_of_heads, head_dim), segment.reshape(block_count, block_rows), slot_index.reshape(block_count, block_rows)))
    return mapped.reshape(group_row_block, count_of_heads * head_dim)

def state_scan(inputs_x, step_size, b_mat, c_mat, decay_rate, segment):
    total_rows, count_of_heads, head_dim = inputs_x.shape
    spans = total_rows // SPAN
    log_decay = step_size * decay_rate[None, :]
    weighted = inputs_x * step_size[:, :, None]
    causal = jnp.arange(SPAN)[:, None] >= jnp.arange(SPAN)[None, :]

    def advance(carried_in, inputs):
        memory, last_segment = carried_in
        decay_part, weighted_part, b_part, c_part, seg_part = inputs
        running = jnp.cumsum(decay_part, axis=0)
        same_seq = (seg_part[:, None] == seg_part[None, :]) & causal
        intersection = jnp.dot(c_part, b_part.T, precision=highest)
        log_gap = jnp.where(same_seq[:, :, None], running[:, None, :] - running[None, :, :], 0.0)
        mixing = jnp.where(same_seq[:, :, None], jnp.exp(log_gap), 0.0) * intersection[:, :, None]
        output = jnp.einsum('tsh,shp->thp', mixing, weighted_part, precision=highest)
        carried = (seg_part == last_segment).astype(jnp.float32)
        reach_back = jnp.exp(running) * carried[:, None]
        output = output + jnp.einsum('tn,hpn->thp', c_part, memory, precision=highest) * reach_back[:, :, None]
        tail_seg = seg_part[-1]
        toward = jnp.exp(running[-1][None, :] - running) * (seg_part == tail_seg).astype(jnp.float32)[:, None]
        next_state = jnp.einsum('sh,shp,sn->hpn', toward, weighted_part, b_part, precision=highest)
        keep_all = jnp.exp(running[-1]) * (tail_seg == last_segment).astype(jnp.float32)
        next_state = next_state + memory * keep_all[:, None, None]
        return ((next_state, tail_seg), output)
    initial = (jnp.zeros((count_of_heads, head_dim, b_mat.shape[1]), jnp.float32), jnp.int32(-1))
    pieces = (log_decay.reshape(spans, SPAN, count_of_heads), weighted.reshape(spans, SPAN, count_of_heads, head_dim), b_mat.reshape(spans, SPAN, -1), c_mat.reshape(spans, SPAN, -1), segment.reshape(spans, SPAN))
    last_state, outputs = lax.scan(jax.checkpoint(advance), initial, pieces)
    return outputs.reshape(total_rows, count_of_heads, head_dim)

def mamba_core(inner_in, step_in, bc_post, bias_in, decay_in, skip_weight_input, kernel_in, conv_bias_in, position, segment):
    group_row_block = inner_in.shape[0]
    count_of_heads = step_in.shape[1]
    mixer_result = causal_conv(inner_in, kernel_in, conv_bias_in, position)
    reshaped_tensor = mixer_result.reshape(group_row_block, count_of_heads, MIXER_HEAD_SIZE)
    step_size = jax.nn.softplus(step_in + bias_in[None, :])
    scan_result = state_scan(reshaped_tensor, step_size, bc_post[:, :STATE], bc_post[:, STATE:], -jnp.exp(decay_in), segment)
    return (scan_result + skip_weight_input[None, :, None] * reshaped_tensor).reshape(group_row_block, count_of_heads * MIXER_HEAD_SIZE)

def forward(hidden_f, embeds_f, parameter_set, segment, position, slot_index, block_rows):
    attention_norm_gain, adapter_down_maps, query_key_value_weight, adapter_up_maps, attention_output_weight, feedforward_norm_gain, gate_up_weight, down_weight, mixer_norm_gain, mixer_gate_input_weight, state_map_weight, step_size_weight, mixer_input_taps, mixer_input_tap_bias, state_map_taps, state_map_tap_bias, step_size_bias, log_decay_rate, head_skip_weight, gated_norm_gain, mixer_output_weight = parameter_set
    group_row_block = hidden_f.shape[0]
    attention_input_reduced = low(rms_scale(jnp.concatenate([hidden_f, embeds_f], axis=1), attention_norm_gain))
    projected_input = []
    for group_member in range(3):
        middle_reduced_precision = rounded_pair(matrix_product(attention_input_reduced, adapter_down_maps[group_member]))
        projected_input.append(rounded_pair(matrix_product(attention_input_reduced, query_key_value_weight[group_member]) + matrix_product(middle_reduced_precision, adapter_up_maps[group_member])))
    reshaped_tensor = [piece_part.reshape(group_row_block, AHEADS, AHD) for piece_part in projected_input]
    queries = rounded_pair(rotate(reshaped_tensor[0], position))
    keys_all = rounded_pair(rotate(reshaped_tensor[1], position))
    attended = rounded_pair(attend_all(queries, keys_all, reshaped_tensor[2], segment, slot_index, block_rows))
    after_attn = hidden_f + low_back(matrix_product(attended, attention_output_weight))
    xm_low = low(rms_scale(after_attn, feedforward_norm_gain))
    gate_pre = low_back(matrix_product(xm_low, gate_up_weight[0]))
    up_pre = low_back(matrix_product(xm_low, gate_up_weight[1]))
    hid_low = low(jax.nn.gelu(gate_pre, approximate=True) * up_pre)
    after_mlp = after_attn + low_back(matrix_product(hid_low, down_weight))
    xn_low = low(rms_scale(after_mlp, mixer_norm_gain))
    gate_z = low_back(matrix_product(xn_low, mixer_gate_input_weight[0]))
    inner_x = rounded_pair(matrix_product(xn_low, mixer_gate_input_weight[1]))
    step_raw = rounded_pair(matrix_product(xn_low, step_size_weight))
    bc_low = rounded_pair(matrix_product(xn_low, state_map_weight))
    bc_post = causal_conv(bc_low, state_map_taps, state_map_tap_bias, position)
    scan_result = rounded_pair(mamba_core(inner_x, step_raw, bc_post, step_size_bias, log_decay_rate, head_skip_weight, mixer_input_taps, mixer_input_tap_bias, position, segment))
    gated = scan_result * jax.nn.silu(gate_z)
    yn_low = low(rms_scale(gated, gated_norm_gain))
    return after_mlp + low_back(matrix_product(yn_low, mixer_output_weight))

def reference(hidden, embeds, cotangent, lengths, attention_norm_gain, adapter_down_maps, query_key_value_weight, adapter_up_maps, attention_output_weight, feedforward_norm_gain, gate_up_weight, down_weight, mixer_norm_gain, mixer_gate_input_weight, state_map_weight, step_size_weight, mixer_input_taps, mixer_input_tap_bias, state_map_taps, state_map_tap_bias, step_size_bias, log_decay_rate, head_skip_weight, gated_norm_gain, mixer_output_weight):
    parameter_set = tuple((tensor_value.astype(jnp.float32) for tensor_value in (attention_norm_gain, adapter_down_maps, query_key_value_weight, adapter_up_maps, attention_output_weight, feedforward_norm_gain, gate_up_weight, down_weight, mixer_norm_gain, mixer_gate_input_weight, state_map_weight, step_size_weight, mixer_input_taps, mixer_input_tap_bias, state_map_taps, state_map_tap_bias, step_size_bias, log_decay_rate, head_skip_weight, gated_norm_gain, mixer_output_weight)))
    group_row_block = hidden.shape[0] // N_FSDP
    block_rows = QBLK

    def one_group(totals, inputs):
        hidden_g, embeds_g, cot_g, lengths_row = inputs
        segment, position, slot_index = layout(lengths_row, group_row_block)
        result, pullback = jax.vjp(lambda hid_in, emb_in, par_in: forward(hid_in, emb_in, par_in, segment, position, slot_index, block_rows), hidden_g, embeds_g, parameter_set)
        d_hid, d_emb, d_par = pullback(cot_g)
        totals = jax.tree.map(lambda acc_in, new_in: acc_in + new_in, totals, d_par)
        return (totals, (result.astype(jnp.bfloat16), d_hid, d_emb))
    shaped_h = hidden.astype(jnp.float32).reshape(N_FSDP, group_row_block, MODEL_WIDTH)
    shaped_e = embeds.astype(jnp.float32).reshape(N_FSDP, group_row_block, MODEL_WIDTH)
    shaped_c = cotangent.astype(jnp.float32).reshape(N_FSDP, group_row_block, MODEL_WIDTH)
    zeros_init = jax.tree.map(jnp.zeros_like, parameter_set)
    grad_totals, (outs_all, d_hidden_all, d_embeds_all) = lax.scan(one_group, zeros_init, (shaped_h, shaped_e, shaped_c, lengths.astype(jnp.int32)))
    return (outs_all.reshape(-1, MODEL_WIDTH), d_hidden_all.reshape(-1, MODEL_WIDTH), d_embeds_all.reshape(-1, MODEL_WIDTH), grad_totals[0], grad_totals[1], grad_totals[2], grad_totals[3], grad_totals[4], grad_totals[5], grad_totals[6], grad_totals[7], grad_totals[8], grad_totals[9], grad_totals[10], grad_totals[11], grad_totals[12], grad_totals[13], grad_totals[14], grad_totals[15], grad_totals[16], grad_totals[17], grad_totals[18], grad_totals[19], grad_totals[20])
```

```python
import jax
import jax.numpy as jnp
from jax import lax
from jax.sharding import PartitionSpec as P

MODEL_WIDTH = 2048
AHEADS = 32
AHD = 128
MHEADS = 64
INNER = 4096
MIXER_HEAD_SIZE = 64
STATE = 128
SPAN = 128


highest = lax.Precision.HIGHEST
epsilon = 1e-05


def matrix_product(left, right):
    return jnp.dot(left, right, preferred_element_type=jnp.float32)


def matrix_product_transposed(left, right):
    return lax.dot_general(
        left, right, (((1,), (1,)), ((), ())), preferred_element_type=jnp.float32
    )


def outer_product_sum(left, right):
    return lax.dot_general(
        left, right, (((0,), (0,)), ((), ())), preferred_element_type=jnp.float32
    )


def rms_scale(values, gain):
    return values * lax.rsqrt(jnp.mean(values * values, axis=-1, keepdims=True) + epsilon) * gain


def gated_gelu(gate_in, up_in):
    return jax.nn.gelu(gate_in, approximate=True) * up_in


def layout(lengths_row, total_rows):
    ends = jnp.cumsum(lengths_row)
    slot_index = jnp.arange(total_rows, dtype=jnp.int32)
    passed = (slot_index[:, None] >= ends[None, :]).astype(jnp.int32)
    segment = jnp.sum(passed, axis=1)
    position = slot_index - jnp.sum(passed * lengths_row[None, :], axis=1)
    return (segment, position, slot_index)


def causal_conv(values, kernel, bias, position):
    total_rows = values.shape[0]
    total = values * kernel[0][None, :] + bias[None, :]
    for lag in range(1, kernel.shape[0]):
        shifted = jnp.concatenate(
            [jnp.zeros((lag, values.shape[1]), values.dtype), values[: total_rows - lag]], axis=0
        )
        keep = (position >= lag).astype(values.dtype)[:, None]
        total = total + shifted * keep * kernel[lag][None, :]
    return jax.nn.silu(total)


def rotate(values, position):
    half_dim = values.shape[-1] // 2
    inverse = 10000.0 ** (-jnp.arange(half_dim, dtype=jnp.float32) / half_dim)
    angle = position.astype(jnp.float32)[:, None] * inverse[None, :]
    cosine = jnp.cos(angle)[:, None, :]
    sine_part = jnp.sin(angle)[:, None, :]
    first_half = values[..., :half_dim]
    second_half = values[..., half_dim:]
    return jnp.concatenate(
        [
            first_half * cosine - second_half * sine_part,
            second_half * cosine + first_half * sine_part,
        ],
        axis=-1,
    )


def attend_core(pair_data, values, segment, slot_index, position, block_rows):
    group_row_block = values.shape[0]
    count_of_heads = values.shape[1] // AHD
    paired = pair_data.reshape(group_row_block, count_of_heads, 2, AHD)
    queries = rotate(paired[:, :, 0], position).astype(jnp.bfloat16)
    keys_all = rotate(paired[:, :, 1], position).astype(jnp.bfloat16)
    vals_all = values.reshape(group_row_block, count_of_heads, AHD).astype(jnp.bfloat16)
    scaling = AHD ** (-0.5)
    block_count = group_row_block // block_rows

    def one_block(inputs):
        query_part, query_seg, query_slot = inputs
        scores = (
            jnp.einsum("qhd,khd->hqk", query_part, keys_all, preferred_element_type=jnp.float32)
            * scaling
        )
        allowed = (query_seg[:, None] == segment[None, :]) & (
            query_slot[:, None] >= slot_index[None, :]
        )
        scores = jnp.where(allowed[None], scores, -1e30)
        weights = jnp.exp(scores)
        weights_low = (weights / jnp.sum(weights, axis=-1, keepdims=True)).astype(jnp.bfloat16)
        return jnp.einsum("hqk,khd->qhd", weights_low, vals_all, preferred_element_type=jnp.float32)

    mapped = lax.map(
        jax.checkpoint(one_block),
        (
            queries.reshape(block_count, block_rows, count_of_heads, AHD),
            segment.reshape(block_count, block_rows),
            slot_index.reshape(block_count, block_rows),
        ),
    )
    return mapped.reshape(group_row_block, count_of_heads * AHD)


def state_scan(inputs_x, step_size, b_mat, c_mat, decay_rate, segment):
    total_rows, count_of_heads, head_dim = inputs_x.shape
    spans = total_rows // SPAN
    log_decay = step_size * decay_rate[None, :]
    weighted = inputs_x * step_size[:, :, None]
    causal = jnp.arange(SPAN)[:, None] >= jnp.arange(SPAN)[None, :]

    def advance(carried_in, inputs):
        memory, last_segment = carried_in
        decay_part, weighted_part, b_part, c_part, seg_part = inputs
        running = jnp.cumsum(decay_part, axis=0)
        same_seq = (seg_part[:, None] == seg_part[None, :]) & causal
        intersection = jnp.dot(c_part, b_part.T, precision=highest)
        log_gap = jnp.where(same_seq[:, :, None], running[:, None, :] - running[None, :, :], 0.0)
        mixing = jnp.where(same_seq[:, :, None], jnp.exp(log_gap), 0.0) * intersection[:, :, None]
        output = jnp.einsum("tsh,shp->thp", mixing, weighted_part, precision=highest)
        carried = (seg_part == last_segment).astype(jnp.float32)
        reach_back = jnp.exp(running) * carried[:, None]
        output = (
            output
            + jnp.einsum("tn,hpn->thp", c_part, memory, precision=highest) * reach_back[:, :, None]
        )
        tail_seg = seg_part[-1]
        toward = (
            jnp.exp(running[-1][None, :] - running)
            * (seg_part == tail_seg).astype(jnp.float32)[:, None]
        )
        next_state = jnp.einsum("sh,shp,sn->hpn", toward, weighted_part, b_part, precision=highest)
        keep_all = jnp.exp(running[-1]) * (tail_seg == last_segment).astype(jnp.float32)
        next_state = next_state + memory * keep_all[:, None, None]
        return ((next_state, tail_seg), output)

    initial = (jnp.zeros((count_of_heads, head_dim, b_mat.shape[1]), jnp.float32), jnp.int32(-1))
    pieces = (
        log_decay.reshape(spans, SPAN, count_of_heads),
        weighted.reshape(spans, SPAN, count_of_heads, head_dim),
        b_mat.reshape(spans, SPAN, -1),
        c_mat.reshape(spans, SPAN, -1),
        segment.reshape(spans, SPAN),
    )
    last_state, outputs = lax.scan(jax.checkpoint(advance), initial, pieces)
    return outputs.reshape(total_rows, count_of_heads, head_dim)


def mamba_core(
    inner_in,
    step_in,
    bc_post,
    bias_in,
    decay_in,
    skip_weight_input,
    kernel_in,
    conv_bias_in,
    position,
    segment,
):
    group_row_block = inner_in.shape[0]
    count_of_heads = step_in.shape[1]
    mixer_result = causal_conv(inner_in, kernel_in, conv_bias_in, position)
    reshaped_tensor = mixer_result.reshape(group_row_block, count_of_heads, MIXER_HEAD_SIZE)
    step_size = jax.nn.softplus(step_in + bias_in[None, :])
    scan_result = state_scan(
        reshaped_tensor,
        step_size,
        bc_post[:, :STATE],
        bc_post[:, STATE:],
        -jnp.exp(decay_in),
        segment,
    )
    return (scan_result + skip_weight_input[None, :, None] * reshaped_tensor).reshape(
        group_row_block, count_of_heads * MIXER_HEAD_SIZE
    )


def collect(first_part, second_part):
    return (
        lax.all_gather(first_part, ("fsdp", "ctx"), axis=1, tiled=True),
        lax.all_gather(second_part, ("fsdp", "ctx"), axis=1, tiled=True),
    )


def collect_again(first_part, second_part):
    return (
        lax.all_gather(first_part, ("fsdp", "ctx"), axis=1, tiled=True),
        lax.all_gather(second_part, ("fsdp", "ctx"), axis=1, tiled=True),
    )


def tensor_sum(partial_sum):
    return lax.psum(partial_sum, "tp")


def tensor_pair(first_part, second_part):
    return (
        lax.psum(first_part.astype(jnp.bfloat16), "tp").astype(jnp.float32),
        lax.psum(second_part.astype(jnp.bfloat16), "tp").astype(jnp.float32),
    )


def heads_pair(first_part, second_part):
    return (
        lax.all_to_all(first_part, "ctx", split_axis=1, concat_axis=0, tiled=True),
        lax.all_to_all(second_part, "ctx", split_axis=1, concat_axis=0, tiled=True),
    )


def heads_one(values):
    return lax.all_to_all(values, "ctx", split_axis=1, concat_axis=0, tiled=True)


def tokens_pair(first_part, second_part):
    return (
        lax.all_to_all(first_part, "ctx", split_axis=0, concat_axis=1, tiled=True),
        lax.all_to_all(second_part, "ctx", split_axis=0, concat_axis=1, tiled=True),
    )


def tokens_one(values):
    return lax.all_to_all(values, "ctx", split_axis=0, concat_axis=1, tiled=True)


def per_device(
    hidden,
    embeds,
    cotangent,
    lengths,
    attention_norm_gain,
    adapter_down_maps,
    query_key_value_weight,
    adapter_up_maps,
    attention_output_weight,
    feedforward_norm_gain,
    gate_up_weight,
    down_weight,
    mixer_norm_gain,
    mixer_gate_input_weight,
    state_map_weight,
    step_size_weight,
    mixer_input_taps,
    mixer_input_tap_bias,
    state_map_taps,
    state_map_tap_bias,
    step_size_bias,
    log_decay_rate,
    head_skip_weight,
    gated_norm_gain,
    mixer_output_weight,
):
    tok_rows = hidden.shape[0]
    ctx_size = lax.axis_size("ctx")
    ctx_index = lax.axis_index("ctx")
    group_row_block = tok_rows * ctx_size
    block_rows = group_row_block // max(1, group_row_block // 1024)
    segment, position, slot_index = layout(lengths[0], group_row_block)
    hidden_f = hidden.astype(jnp.float32)
    embeds_f = embeds.astype(jnp.float32)
    attention_block_full, attn_out = collect(query_key_value_weight, attention_output_weight)
    joined = jnp.concatenate([hidden_f, embeds_f], axis=1)
    normed_a, norm_a_back = jax.vjp(rms_scale, joined, attention_norm_gain)
    attention_input_reduced = normed_a.astype(jnp.bfloat16)
    middle_reduced_precision = [
        matrix_product(attention_input_reduced, adapter_down_maps[group_member]).astype(
            jnp.bfloat16
        )
        for group_member in range(3)
    ]
    projected_input = [
        (
            matrix_product(attention_input_reduced, attention_block_full[group_member])
            + matrix_product(middle_reduced_precision[group_member], adapter_up_maps[group_member])
        ).astype(jnp.bfloat16)
        for group_member in range(3)
    ]
    tp_heads = projected_input[0].shape[1] // AHD
    pair_data = jnp.stack(
        [
            projected_input[0].reshape(tok_rows, tp_heads, AHD),
            projected_input[1].reshape(tok_rows, tp_heads, AHD),
        ],
        axis=2,
    ).reshape(tok_rows, tp_heads * 2 * AHD)
    pair_heads, value_heads = heads_pair(pair_data, projected_input[2])
    attn_core, attn_pull = jax.vjp(
        lambda pairs_in, values_in: attend_core(
            pairs_in, values_in, segment, slot_index, position, block_rows
        ),
        pair_heads.astype(jnp.float32),
        value_heads.astype(jnp.float32),
    )
    attn_tokens = tokens_one(attn_core.astype(jnp.bfloat16))
    after_attn = hidden_f + tensor_sum(matrix_product(attn_tokens, attn_out))
    mlp_big, mlp_down = collect(gate_up_weight, down_weight)
    normed_m, norm_m_back = jax.vjp(rms_scale, after_attn, feedforward_norm_gain)
    xm_low = normed_m.astype(jnp.bfloat16)
    gate_pre = matrix_product(xm_low, mlp_big[0])
    up_pre = matrix_product(xm_low, mlp_big[1])
    activated, act_back = jax.vjp(gated_gelu, gate_pre, up_pre)
    hid_low = activated.astype(jnp.bfloat16)
    after_mlp = after_attn + tensor_sum(matrix_product(hid_low, mlp_down))
    mamba_big, mamba_out = collect(mixer_gate_input_weight, mixer_output_weight)
    normed_n, norm_n_back = jax.vjp(rms_scale, after_mlp, mixer_norm_gain)
    xn_low = normed_n.astype(jnp.bfloat16)
    gate_z = matrix_product(xn_low, mamba_big[0])
    inner_x = matrix_product(xn_low, mamba_big[1]).astype(jnp.bfloat16)
    step_raw = matrix_product(xn_low, step_size_weight).astype(jnp.bfloat16)
    bc_low = matrix_product(xn_low, state_map_weight).astype(jnp.bfloat16)
    x_heads, step_heads = heads_pair(inner_x, step_raw)
    bc_group = lax.all_gather(bc_low, "ctx", axis=0, tiled=True)
    bc_post, bc_conv_pull = jax.vjp(
        lambda values_in, kernel_in, conv_bias_in: causal_conv(
            values_in, kernel_in, conv_bias_in, position
        ),
        bc_group.astype(jnp.float32),
        state_map_taps,
        state_map_tap_bias,
    )
    heads_on_device_share = step_heads.shape[1]
    start_offset = ctx_index * heads_on_device_share
    channel_count_here = heads_on_device_share * MIXER_HEAD_SIZE
    channel_offset_begin = start_offset * MIXER_HEAD_SIZE
    bias_local = lax.dynamic_slice_in_dim(step_size_bias, start_offset, heads_on_device_share)
    decay_local = lax.dynamic_slice_in_dim(log_decay_rate, start_offset, heads_on_device_share)
    skip_local = lax.dynamic_slice_in_dim(head_skip_weight, start_offset, heads_on_device_share)
    kernel_local = lax.dynamic_slice_in_dim(
        mixer_input_taps, channel_offset_begin, channel_count_here, 1
    )
    conv_bias_local = lax.dynamic_slice_in_dim(
        mixer_input_tap_bias, channel_offset_begin, channel_count_here, 0
    )
    scan_out, scan_pull = jax.vjp(
        lambda xs_in, step_in, bcp_in, bias_in, decay_in, skip_weight_input, kernel_in, conv_bias_in: mamba_core(
            xs_in,
            step_in,
            bcp_in,
            bias_in,
            decay_in,
            skip_weight_input,
            kernel_in,
            conv_bias_in,
            position,
            segment,
        ),
        x_heads.astype(jnp.float32),
        step_heads.astype(jnp.float32),
        bc_post,
        bias_local,
        decay_local,
        skip_local,
        kernel_local,
        conv_bias_local,
    )
    y_tokens = tokens_one(scan_out.astype(jnp.bfloat16)).astype(jnp.float32)
    silu_z = jax.nn.silu(gate_z)
    gated = y_tokens * silu_z
    total_sq = tensor_sum(jnp.sum(gated * gated, axis=1))
    inverse = lax.rsqrt(total_sq / INNER + epsilon)[:, None]
    yn_low = (gated * inverse * gated_norm_gain).astype(jnp.bfloat16)
    after_mamba = after_mlp + tensor_sum(matrix_product(yn_low, mamba_out))
    result = after_mamba.astype(jnp.bfloat16)
    grad_out = cotangent.astype(jnp.float32)
    mamba_big, mamba_out = collect_again(mixer_gate_input_weight, mixer_output_weight)
    d_yn = matrix_product_transposed(cotangent, mamba_out)
    grad_w_out = outer_product_sum(yn_low, cotangent)
    gain_part = d_yn * gated_norm_gain
    cross = tensor_sum(jnp.sum(gain_part * gated, axis=1))
    grad_g_gate = jnp.sum(d_yn * gated * inverse, axis=0)
    d_gated = gain_part * inverse - gated * inverse**3 * (cross / INNER)[:, None]
    d_y = (d_gated * silu_z).astype(jnp.bfloat16)
    sigmoid_z = jax.nn.sigmoid(gate_z)
    d_z = (d_gated * y_tokens * sigmoid_z * (1.0 + gate_z * (1.0 - sigmoid_z))).astype(jnp.bfloat16)
    dy_heads = heads_one(d_y)
    (
        d_xs,
        d_step,
        d_bc_post,
        grad_bias_local,
        grad_decay_local,
        grad_skip_local,
        grad_kernel_local,
        grad_conv_bias_local,
    ) = scan_pull(dy_heads.astype(jnp.float32))
    d_xs_tok, d_step_tok = tokens_pair(d_xs.astype(jnp.bfloat16), d_step.astype(jnp.bfloat16))
    d_bc_ctx = lax.psum(d_bc_post.astype(jnp.bfloat16), "ctx").astype(jnp.float32)
    dxn_part = (
        matrix_product_transposed(d_z, mamba_big[0])
        + matrix_product_transposed(d_xs_tok, mamba_big[1])
        + matrix_product_transposed(d_step_tok, step_size_weight)
    )
    grad_w_zx = jnp.stack([outer_product_sum(xn_low, d_z), outer_product_sum(xn_low, d_xs_tok)])
    grad_w_dt = outer_product_sum(xn_low, d_step_tok)
    dxn_sum, d_bc_full = tensor_pair(dxn_part, d_bc_ctx)
    d_bc_pre = bc_conv_pull(d_bc_full)[0]
    d_bc_mine = lax.dynamic_slice_in_dim(d_bc_pre, ctx_index * tok_rows, tok_rows, 0)
    own_rows = (slot_index // tok_rows == ctx_index).astype(jnp.float32)[:, None]
    ignored_part, grad_conv_bc, grad_conv_bc_bias = bc_conv_pull(d_bc_full * own_rows)
    d_bc_low = d_bc_mine.astype(jnp.bfloat16)
    dxn_total = dxn_sum + matrix_product_transposed(d_bc_low, state_map_weight)
    grad_w_bc = outer_product_sum(xn_low, d_bc_low)
    d_norm_n, grad_g_mamba = norm_n_back(dxn_total)
    d_after_mlp = grad_out + d_norm_n
    shard_heads = step_size_bias.shape[0]
    zero_heads = jnp.zeros((shard_heads,), jnp.float32)
    grad_dt_bias = lax.dynamic_update_slice_in_dim(zero_heads, grad_bias_local, start_offset, 0)
    grad_a_log = lax.dynamic_update_slice_in_dim(zero_heads, grad_decay_local, start_offset, 0)
    grad_d_skip = lax.dynamic_update_slice_in_dim(zero_heads, grad_skip_local, start_offset, 0)
    grad_conv_x = lax.dynamic_update_slice_in_dim(
        jnp.zeros(mixer_input_taps.shape, jnp.float32), grad_kernel_local, channel_offset_begin, 1
    )
    grad_conv_x_bias = lax.dynamic_update_slice_in_dim(
        jnp.zeros(mixer_input_tap_bias.shape, jnp.float32),
        grad_conv_bias_local,
        channel_offset_begin,
        0,
    )
    mlp_big, mlp_down = collect_again(gate_up_weight, down_weight)
    d_mlp_low = d_after_mlp.astype(jnp.bfloat16)
    d_hid = matrix_product_transposed(d_mlp_low, mlp_down)
    grad_w_down = outer_product_sum(hid_low, d_mlp_low)
    d_gate, d_up = act_back(d_hid)
    d_gate_low = d_gate.astype(jnp.bfloat16)
    d_up_low = d_up.astype(jnp.bfloat16)
    d_xm = tensor_sum(
        matrix_product_transposed(d_gate_low, mlp_big[0])
        + matrix_product_transposed(d_up_low, mlp_big[1])
    )
    grad_w_gu = jnp.stack(
        [outer_product_sum(xm_low, d_gate_low), outer_product_sum(xm_low, d_up_low)]
    )
    d_norm_m, grad_g_mlp = norm_m_back(d_xm)
    d_after_attn = d_after_mlp + d_norm_m
    attention_block_full, attn_out = collect_again(query_key_value_weight, attention_output_weight)
    d_attn_low = d_after_attn.astype(jnp.bfloat16)
    d_tokens = matrix_product_transposed(d_attn_low, attn_out).astype(jnp.bfloat16)
    grad_w_o = outer_product_sum(attn_tokens, d_attn_low)
    d_core = heads_one(d_tokens)
    d_pairs, d_values = attn_pull(d_core.astype(jnp.float32))
    d_pair_tok, d_value_tok = tokens_pair(
        d_pairs.astype(jnp.bfloat16), d_values.astype(jnp.bfloat16)
    )
    d_paired = d_pair_tok.reshape(tok_rows, tp_heads, 2, AHD)
    projection_gradient = [
        d_paired[:, :, 0].reshape(tok_rows, tp_heads * AHD),
        d_paired[:, :, 1].reshape(tok_rows, tp_heads * AHD),
        d_value_tok,
    ]
    dxa_part = (
        matrix_product_transposed(projection_gradient[0], attention_block_full[0])
        + matrix_product_transposed(projection_gradient[1], attention_block_full[1])
        + matrix_product_transposed(projection_gradient[2], attention_block_full[2])
    )
    dmid_part = jnp.concatenate(
        [
            matrix_product_transposed(
                projection_gradient[group_member], adapter_up_maps[group_member]
            )
            for group_member in range(3)
        ],
        axis=1,
    )
    grad_w_qkv = jnp.stack(
        [
            outer_product_sum(attention_input_reduced, projection_gradient[group_member])
            for group_member in range(3)
        ]
    )
    adapter_up_gradient = jnp.stack(
        [
            outer_product_sum(
                middle_reduced_precision[group_member], projection_gradient[group_member]
            )
            for group_member in range(3)
        ]
    )
    dxa_sum, dmid_sum = tensor_pair(dxa_part, dmid_part)
    dmid_low = dmid_sum.astype(jnp.bfloat16)
    rank_column_block = adapter_down_maps.shape[2]
    middle_gradient_pieces = [
        dmid_low[:, group_member * rank_column_block : (group_member + 1) * rank_column_block]
        for group_member in range(3)
    ]
    dxa_total = (
        dxa_sum
        + matrix_product_transposed(middle_gradient_pieces[0], adapter_down_maps[0])
        + matrix_product_transposed(middle_gradient_pieces[1], adapter_down_maps[1])
        + matrix_product_transposed(middle_gradient_pieces[2], adapter_down_maps[2])
    )
    adapter_down_gradient = jnp.stack(
        [
            outer_product_sum(attention_input_reduced, middle_gradient_pieces[group_member])
            for group_member in range(3)
        ]
    )
    d_joined, grad_g_attn = norm_a_back(dxa_total)
    d_hidden = d_after_attn + d_joined[:, :MODEL_WIDTH]
    d_embeds = d_joined[:, MODEL_WIDTH:]
    grad_w_qkv, grad_w_o, grad_w_gu, grad_w_down, grad_w_zx, grad_w_out = (
        lax.psum_scatter(
            grad_w_qkv.astype(jnp.bfloat16), ("fsdp", "ctx"), scatter_dimension=1, tiled=True
        ).astype(jnp.float32),
        lax.psum_scatter(
            grad_w_o.astype(jnp.bfloat16), ("fsdp", "ctx"), scatter_dimension=1, tiled=True
        ).astype(jnp.float32),
        lax.psum_scatter(
            grad_w_gu.astype(jnp.bfloat16), ("fsdp", "ctx"), scatter_dimension=1, tiled=True
        ).astype(jnp.float32),
        lax.psum_scatter(
            grad_w_down.astype(jnp.bfloat16), ("fsdp", "ctx"), scatter_dimension=1, tiled=True
        ).astype(jnp.float32),
        lax.psum_scatter(
            grad_w_zx.astype(jnp.bfloat16), ("fsdp", "ctx"), scatter_dimension=1, tiled=True
        ).astype(jnp.float32),
        lax.psum_scatter(
            grad_w_out.astype(jnp.bfloat16), ("fsdp", "ctx"), scatter_dimension=1, tiled=True
        ).astype(jnp.float32),
    )
    (
        grad_g_attn,
        adapter_down_gradient,
        adapter_up_gradient,
        grad_g_mlp,
        grad_g_mamba,
        grad_w_bc,
        grad_w_dt,
        grad_conv_x,
        grad_conv_x_bias,
        grad_conv_bc,
        grad_conv_bc_bias,
        grad_dt_bias,
        grad_a_log,
        grad_d_skip,
        grad_g_gate,
    ) = (
        lax.psum(grad_g_attn.astype(jnp.bfloat16), ("fsdp", "ctx")).astype(jnp.float32),
        lax.psum(adapter_down_gradient.astype(jnp.bfloat16), ("fsdp", "ctx")).astype(jnp.float32),
        lax.psum(adapter_up_gradient.astype(jnp.bfloat16), ("fsdp", "ctx")).astype(jnp.float32),
        lax.psum(grad_g_mlp.astype(jnp.bfloat16), ("fsdp", "ctx")).astype(jnp.float32),
        lax.psum(grad_g_mamba.astype(jnp.bfloat16), ("fsdp", "ctx")).astype(jnp.float32),
        lax.psum(grad_w_bc.astype(jnp.bfloat16), ("fsdp", "ctx")).astype(jnp.float32),
        lax.psum(grad_w_dt.astype(jnp.bfloat16), ("fsdp", "ctx")).astype(jnp.float32),
        lax.psum(grad_conv_x.astype(jnp.bfloat16), ("fsdp", "ctx")).astype(jnp.float32),
        lax.psum(grad_conv_x_bias.astype(jnp.bfloat16), ("fsdp", "ctx")).astype(jnp.float32),
        lax.psum(grad_conv_bc.astype(jnp.bfloat16), ("fsdp", "ctx")).astype(jnp.float32),
        lax.psum(grad_conv_bc_bias.astype(jnp.bfloat16), ("fsdp", "ctx")).astype(jnp.float32),
        lax.psum(grad_dt_bias.astype(jnp.bfloat16), ("fsdp", "ctx")).astype(jnp.float32),
        lax.psum(grad_a_log.astype(jnp.bfloat16), ("fsdp", "ctx")).astype(jnp.float32),
        lax.psum(grad_d_skip.astype(jnp.bfloat16), ("fsdp", "ctx")).astype(jnp.float32),
        lax.psum(grad_g_gate.astype(jnp.bfloat16), ("fsdp", "ctx")).astype(jnp.float32),
    )
    return (
        result,
        d_hidden,
        d_embeds,
        grad_g_attn,
        adapter_down_gradient,
        grad_w_qkv,
        adapter_up_gradient,
        grad_w_o,
        grad_g_mlp,
        grad_w_gu,
        grad_w_down,
        grad_g_mamba,
        grad_w_zx,
        grad_w_bc,
        grad_w_dt,
        grad_conv_x,
        grad_conv_x_bias,
        grad_conv_bc,
        grad_conv_bc_bias,
        grad_dt_bias,
        grad_a_log,
        grad_d_skip,
        grad_g_gate,
        grad_w_out,
    )


PLANE = ("fsdp", "ctx")
EVERY = ("fsdp", "ctx", "tp")


def gather_rows(values):
    return lax.all_gather(values, EVERY, axis=0, tiled=True)


def scatter_rows(partial_sum):
    return lax.psum_scatter(partial_sum, EVERY, scatter_dimension=0, tiled=True).astype(jnp.float32)


def spread(weight, split, join):
    return lax.all_to_all(weight, PLANE, split_axis=split, concat_axis=join, tiled=True)


def shift_conv(values, kernel, bias, position):
    total = values * kernel[0][None, :] + bias[None, :]
    for lag in range(1, kernel.shape[0]):
        shifted = jnp.pad(values, ((lag, 0), (0, 0)))[: values.shape[0]]
        keep = (position >= lag).astype(values.dtype)[:, None]
        total = total + shifted * keep * kernel[lag][None, :]
    return jax.nn.silu(total)


def attend_groups(queries, keys_all, vals_all, segment, position):
    def rot(values):
        half_dim = values.shape[-1] // 2
        inverse = 10000.0 ** (-jnp.arange(half_dim, dtype=jnp.float32) / half_dim)
        angle = position.astype(jnp.float32)[..., None] * inverse
        cosine, sine = jnp.cos(angle), jnp.sin(angle)
        a, b = values[..., :half_dim], values[..., half_dim:]
        return jnp.concatenate([a * cosine - b * sine, b * cosine + a * sine], axis=-1).astype(
            jnp.bfloat16
        )

    rows = queries.shape[1]
    order = jnp.arange(rows)
    scores = jnp.einsum(
        "gqd,gkd->gqk", rot(queries), rot(keys_all), preferred_element_type=jnp.float32
    ) * AHD ** (-0.5)
    allowed = (segment[:, :, None] == segment[:, None, :]) & (order[:, None] >= order[None, :])
    weights = jnp.exp(jnp.where(allowed, scores, -1e30))
    low = (weights / jnp.sum(weights, axis=-1, keepdims=True)).astype(jnp.bfloat16)
    return jnp.einsum(
        "gqk,gkd->gqd", low, vals_all.astype(jnp.bfloat16), preferred_element_type=jnp.float32
    )


def mixer_groups(
    inner_in, step_in, bc_post, bias_in, decay_in, skip_in, kernel_in, conv_bias_in, position, segment
):
    groups, rows = segment.shape
    heads = step_in.shape[1]
    xc = shift_conv(inner_in, kernel_in, conv_bias_in, position.reshape(-1))
    xc = xc.reshape(groups, rows, heads, MIXER_HEAD_SIZE)
    step = jax.nn.softplus(step_in + bias_in[None, :]).reshape(groups, rows, heads)
    log_decay = step * -jnp.exp(decay_in)
    order = jnp.arange(rows)
    same = (segment[:, :, None] == segment[:, None, :]) & (order[:, None] >= order[None, :])
    running = jnp.einsum("gts,gsh->gth", same.astype(jnp.float32), log_decay, precision=highest)
    gap = running.transpose(0, 2, 1)
    gap = gap[:, :, :, None] - gap[:, :, None, :]
    decay = jnp.where(same[:, None], jnp.exp(jnp.where(same[:, None], gap, 0.0)), 0.0)
    b_mat = bc_post[:, :STATE].reshape(groups, rows, STATE)
    c_mat = bc_post[:, STATE:].reshape(groups, rows, STATE)
    meet = jnp.einsum("gtn,gsn->gts", c_mat, b_mat, precision=lax.Precision.HIGH)
    out = jnp.einsum(
        "ghts,gshp->gthp",
        decay * meet[:, None],
        xc * step[..., None],
        precision=lax.Precision.HIGH,
    )
    out = out + skip_in[:, None] * xc
    return out.reshape(groups * rows, heads * MIXER_HEAD_SIZE)


def per_device_split(
    hidden,
    embeds,
    cotangent,
    lengths,
    attention_norm_gain,
    adapter_down_maps,
    query_key_value_weight,
    adapter_up_maps,
    attention_output_weight,
    feedforward_norm_gain,
    gate_up_weight,
    down_weight,
    mixer_norm_gain,
    mixer_gate_input_weight,
    state_map_weight,
    step_size_weight,
    mixer_input_taps,
    mixer_input_tap_bias,
    state_map_taps,
    state_map_tap_bias,
    step_size_bias,
    log_decay_rate,
    head_skip_weight,
    gated_norm_gain,
    mixer_output_weight,
):
    bf16, f32 = jnp.bfloat16, jnp.float32
    tp_size, ctx_size, groups = (lax.axis_size(name) for name in ("tp", "ctx", "fsdp"))
    tp_index, ctx_index = lax.axis_index("tp"), lax.axis_index("ctx")
    plane_index = lax.axis_index("fsdp") * ctx_size + ctx_index
    plane_size = groups * ctx_size
    tok_rows = hidden.shape[0]
    mine = tok_rows // tp_size
    group_rows = tok_rows * ctx_size
    start = tp_index * mine

    def own_rows(values):
        return lax.dynamic_slice_in_dim(values, start, mine, 0)

    def own_part(values, axis=0):
        width = values.shape[axis] // plane_size
        return lax.dynamic_slice_in_dim(values, plane_index * width, width, axis)

    hidden_f = own_rows(hidden).astype(f32)
    embeds_f = own_rows(embeds).astype(f32)
    cot_low = own_rows(cotangent)

    w_qkv = spread(query_key_value_weight, 2, 1)
    w_o = spread(attention_output_weight, 0, 1)
    w_gu = spread(gate_up_weight, 2, 1)
    w_down = spread(down_weight, 0, 1)
    w_zx = spread(mixer_gate_input_weight, 2, 1)
    w_out = spread(mixer_output_weight, 0, 1)
    up_maps = own_part(adapter_up_maps, 2)
    w_step = own_part(step_size_weight, 1)
    taps, tap_bias = own_part(mixer_input_taps, 1), own_part(mixer_input_tap_bias)
    step_bias, decay_rate = own_part(step_size_bias), own_part(log_decay_rate)
    skip, gate_gain = own_part(head_skip_weight), own_part(gated_norm_gain)

    rank = adapter_down_maps.shape[2]
    width_a = adapter_down_maps.shape[1]
    down_all = jnp.concatenate([adapter_down_maps[j] for j in range(3)], axis=1)
    joined = jnp.concatenate([hidden_f, embeds_f], axis=1)
    normed_a, norm_a_back = jax.vjp(rms_scale, joined, attention_norm_gain)
    xa_mine = normed_a.astype(bf16)
    mid_mine = matrix_product(xa_mine, down_all).astype(bf16)
    segment_g, position_g, slot_g = layout(lengths[0], group_rows)
    first = ctx_index * tok_rows + start
    marks = jnp.stack(
        [
            lax.dynamic_slice_in_dim(segment_g, first, mine),
            lax.dynamic_slice_in_dim(position_g, first, mine),
        ],
        axis=1,
    ).astype(bf16)
    marks = jnp.pad(marks, ((0, 0), (0, 126)))
    gathered = gather_rows(jnp.concatenate([xa_mine, mid_mine, marks], axis=1))
    xa = gathered[:, :width_a]
    mid = gathered[:, width_a : width_a + 3 * rank]
    segment = gathered[:, width_a + 3 * rank].astype(jnp.int32).reshape(groups, group_rows)
    position = gathered[:, width_a + 3 * rank + 1].astype(jnp.int32).reshape(groups, group_rows)
    position_flat = position.reshape(-1)
    cot = gather_rows(cot_low)
    proj = [
        (
            matrix_product(xa, w_qkv[j])
            + matrix_product(mid[:, j * rank : (j + 1) * rank], up_maps[j])
        ).astype(bf16)
        for j in range(3)
    ]
    ao, attend_back = jax.vjp(
        lambda q, k, v: attend_groups(q, k, v, segment, position),
        *[piece.astype(f32).reshape(groups, group_rows, AHD) for piece in proj],
    )
    ao_low = ao.astype(bf16).reshape(groups * group_rows, AHD)
    after_attn = hidden_f + scatter_rows(matrix_product(ao_low, w_o).astype(bf16))

    normed_m, norm_m_back = jax.vjp(rms_scale, after_attn, feedforward_norm_gain)
    xm = gather_rows(normed_m.astype(bf16))
    gate_pre, up_pre = matrix_product(xm, w_gu[0]), matrix_product(xm, w_gu[1])
    activated, act_back = jax.vjp(gated_gelu, gate_pre, up_pre)
    hid_low = activated.astype(bf16)
    after_mlp = after_attn + scatter_rows(matrix_product(hid_low, w_down).astype(bf16))

    normed_n, norm_n_back = jax.vjp(rms_scale, after_mlp, mixer_norm_gain)
    xn = gather_rows(normed_n.astype(bf16))
    gate_z = matrix_product(xn, w_zx[0])
    inner_x = matrix_product(xn, w_zx[1]).astype(bf16)
    step_raw = matrix_product(xn, w_step).astype(bf16)
    bc_low = matrix_product(xn, state_map_weight).astype(bf16)
    bc_post, bc_conv_back = jax.vjp(
        lambda v, k, b: shift_conv(v, k, b, position_flat),
        bc_low.astype(f32),
        state_map_taps,
        state_map_tap_bias,
    )
    scan_out, scan_back = jax.vjp(
        lambda *parts: mixer_groups(*parts, position, segment),
        inner_x.astype(f32),
        step_raw.astype(f32),
        bc_post,
        step_bias,
        decay_rate,
        skip,
        taps,
        tap_bias,
    )
    y = scan_out.astype(bf16).astype(f32)
    silu_z = jax.nn.silu(gate_z)
    gated = y * silu_z
    d_yn = matrix_product_transposed(cot, w_out)
    gain_part = d_yn * gate_gain
    sums = lax.psum(
        jnp.stack([jnp.sum(gated * gated, axis=1), jnp.sum(gain_part * gated, axis=1)]), EVERY
    )
    inverse = lax.rsqrt(sums[0] / INNER + epsilon)[:, None]
    cross = (sums[1] / INNER)[:, None]
    yn_low = (gated * inverse * gate_gain).astype(bf16)
    out_mine = after_mlp + scatter_rows(matrix_product(yn_low, w_out).astype(bf16))
    result = lax.all_gather(out_mine.astype(bf16), "tp", axis=0, tiled=True)

    grad_w_out = outer_product_sum(yn_low, cot)
    grad_g_gate = jnp.sum(d_yn * gated * inverse, axis=0)
    d_gated = gain_part * inverse - gated * inverse**3 * cross
    d_y = (d_gated * silu_z).astype(bf16)
    sigmoid_z = jax.nn.sigmoid(gate_z)
    d_z = (d_gated * y * sigmoid_z * (1.0 + gate_z * (1.0 - sigmoid_z))).astype(bf16)
    (
        d_xs,
        d_step,
        d_bc_post,
        grad_dt_bias,
        grad_a_log,
        grad_d_skip,
        grad_conv_x,
        grad_conv_x_bias,
    ) = scan_back(d_y.astype(f32))
    d_xs, d_step = d_xs.astype(bf16), d_step.astype(bf16)
    d_bc_part, grad_conv_bc, grad_conv_bc_bias = bc_conv_back(d_bc_post)
    dxn_part = (
        matrix_product_transposed(d_z, w_zx[0])
        + matrix_product_transposed(d_xs, w_zx[1])
        + matrix_product_transposed(d_step, w_step)
    )
    sent = scatter_rows(jnp.concatenate([dxn_part, d_bc_part], axis=1).astype(bf16))
    width = hidden.shape[1]
    d_bc_mine = sent[:, width:].astype(bf16)
    dxn_mine = sent[:, :width] + matrix_product_transposed(d_bc_mine, state_map_weight)
    grad_w_zx = jnp.stack([outer_product_sum(xn, d_z), outer_product_sum(xn, d_xs)])
    grad_w_dt = outer_product_sum(xn, d_step)
    d_norm_n, grad_g_mamba = norm_n_back(dxn_mine)
    d_after_mlp = cot_low.astype(f32) + d_norm_n

    gathered = gather_rows(jnp.concatenate([d_after_mlp.astype(bf16), d_bc_mine], axis=1))
    d_mlp, d_bc = gathered[:, :width], gathered[:, width:]
    grad_w_bc = outer_product_sum(xn, d_bc)
    grad_w_down = outer_product_sum(hid_low, d_mlp)
    d_gate, d_up = act_back(matrix_product_transposed(d_mlp, w_down))
    d_gate, d_up = d_gate.astype(bf16), d_up.astype(bf16)
    d_xm = scatter_rows(
        (
            matrix_product_transposed(d_gate, w_gu[0]) + matrix_product_transposed(d_up, w_gu[1])
        ).astype(bf16)
    )
    grad_w_gu = jnp.stack([outer_product_sum(xm, d_gate), outer_product_sum(xm, d_up)])
    d_norm_m, grad_g_mlp = norm_m_back(d_xm)
    d_after_attn = d_after_mlp + d_norm_m

    d_attn = gather_rows(d_after_attn.astype(bf16))
    grad_w_o = outer_product_sum(ao_low, d_attn)
    d_ao = matrix_product_transposed(d_attn, w_o).astype(bf16)
    d_proj = [
        piece.reshape(groups * group_rows, AHD).astype(bf16)
        for piece in attend_back(d_ao.astype(f32).reshape(groups, group_rows, AHD))
    ]
    dxa_part = sum(matrix_product_transposed(d_proj[j], w_qkv[j]) for j in range(3))
    dmid_part = jnp.concatenate(
        [matrix_product_transposed(d_proj[j], up_maps[j]) for j in range(3)], axis=1
    )
    sent = scatter_rows(jnp.concatenate([dxa_part, dmid_part], axis=1).astype(bf16))
    dmid_mine = sent[:, width_a:].astype(bf16)
    dxa_mine = sent[:, :width_a] + matrix_product_transposed(dmid_mine, down_all)
    dmid = gather_rows(dmid_mine)
    adapter_down_gradient = jnp.stack(
        [outer_product_sum(xa, dmid[:, j * rank : (j + 1) * rank]) for j in range(3)]
    )
    grad_w_qkv = jnp.stack([outer_product_sum(xa, d_proj[j]) for j in range(3)])
    adapter_up_gradient = jnp.stack(
        [outer_product_sum(mid[:, j * rank : (j + 1) * rank], d_proj[j]) for j in range(3)]
    )
    d_joined, grad_g_attn = norm_a_back(dxa_mine)
    back = jnp.concatenate(
        [d_after_attn + d_joined[:, :width], d_joined[:, width:]], axis=1
    ).astype(bf16)
    back = lax.all_gather(back, "tp", axis=0, tiled=True).astype(f32)
    d_hidden, d_embeds = back[:, :width], back[:, width:]

    def home(grad, split, join):
        return spread(grad.astype(bf16), split, join).astype(f32)

    grad_w_qkv = home(grad_w_qkv, 1, 2)
    grad_w_o = home(grad_w_o, 1, 0)
    grad_w_gu = home(grad_w_gu, 1, 2)
    grad_w_down = home(grad_w_down, 1, 0)
    grad_w_zx = home(grad_w_zx, 1, 2)
    grad_w_out = home(grad_w_out, 1, 0)

    def whole(part, axis):
        return lax.all_gather(part.astype(bf16), PLANE, axis=axis, tiled=True).astype(f32)

    def total(part):
        return lax.psum(part, EVERY)

    return (
        result,
        d_hidden,
        d_embeds,
        total(grad_g_attn),
        adapter_down_gradient,
        grad_w_qkv,
        whole(adapter_up_gradient, 2),
        grad_w_o,
        total(grad_g_mlp),
        grad_w_gu,
        grad_w_down,
        total(grad_g_mamba),
        grad_w_zx,
        grad_w_bc,
        whole(grad_w_dt, 1),
        whole(grad_conv_x, 1),
        whole(grad_conv_x_bias, 0),
        total(grad_conv_bc),
        total(grad_conv_bc_bias),
        whole(grad_dt_bias, 0),
        whole(grad_a_log, 0),
        whole(grad_d_skip, 0),
        whole(grad_g_gate, 0),
        grad_w_out,
    )


def solution(mesh):
    placed = (
        P(("fsdp", "ctx"), None),
        P(("fsdp", "ctx"), None),
        P(("fsdp", "ctx"), None),
        P("fsdp", None),
        P(),
        P(),
        P(None, ("fsdp", "ctx"), "tp"),
        P(None, None, "tp"),
        P("tp", ("fsdp", "ctx")),
        P(),
        P(None, ("fsdp", "ctx"), "tp"),
        P("tp", ("fsdp", "ctx")),
        P(),
        P(None, ("fsdp", "ctx"), "tp"),
        P(),
        P(None, "tp"),
        P(None, "tp"),
        P("tp"),
        P(),
        P(),
        P("tp"),
        P("tp"),
        P("tp"),
        P("tp"),
        P("tp", ("fsdp", "ctx")),
    )
    devices = mesh.shape["fsdp"] * mesh.shape["ctx"] * mesh.shape["tp"]
    one_head_each = devices == AHEADS and MHEADS % devices == 0
    return jax.shard_map(
        per_device_split if one_head_each else per_device,
        mesh=mesh,
        in_specs=placed,
        out_specs=(
            P(("fsdp", "ctx"), None),
            P(("fsdp", "ctx"), None),
            P(("fsdp", "ctx"), None),
            P(),
            P(),
            P(None, ("fsdp", "ctx"), "tp"),
            P(None, None, "tp"),
            P("tp", ("fsdp", "ctx")),
            P(),
            P(None, ("fsdp", "ctx"), "tp"),
            P("tp", ("fsdp", "ctx")),
            P(),
            P(None, ("fsdp", "ctx"), "tp"),
            P(),
            P(None, "tp"),
            P(None, "tp"),
            P("tp"),
            P(),
            P(),
            P("tp"),
            P("tp"),
            P("tp"),
            P("tp"),
            P("tp", ("fsdp", "ctx")),
        ),
        check_vma=False,
    )
```

```python
import jax
import jax.numpy as jnp
from jax import lax
from jax.experimental import pallas as pl
from jax.experimental.pallas import tpu as pltpu
from jax.sharding import PartitionSpec as P

MODEL_WIDTH = 2048
AHEADS = 32
AHD = 128
INNER = 4096
MIXER_HEAD_SIZE = 64
STATE = 128
SPAN = 128


highest = lax.Precision.HIGHEST
epsilon = 1e-05


def matrix_product(left, right):
    return jnp.dot(left, right, preferred_element_type=jnp.float32)


def matrix_product_transposed(left, right):
    return lax.dot_general(
        left, right, (((1,), (1,)), ((), ())), preferred_element_type=jnp.float32
    )


def outer_product_sum(left, right):
    return lax.dot_general(
        left, right, (((0,), (0,)), ((), ())), preferred_element_type=jnp.float32
    )


def rms_scale(values, gain):
    return values * lax.rsqrt(jnp.mean(values * values, axis=-1, keepdims=True) + epsilon) * gain


def gated_gelu(gate_in, up_in):
    return jax.nn.gelu(gate_in, approximate=True) * up_in


def layout(lengths_row, total_rows):
    ends = jnp.cumsum(lengths_row)
    slot_index = jnp.arange(total_rows, dtype=jnp.int32)
    passed = (slot_index[:, None] >= ends[None, :]).astype(jnp.int32)
    segment = jnp.sum(passed, axis=1)
    position = slot_index - jnp.sum(passed * lengths_row[None, :], axis=1)
    return (segment, position, slot_index)


def causal_conv(values, kernel, bias, position):
    total_rows = values.shape[0]
    total = values * kernel[0][None, :] + bias[None, :]
    for lag in range(1, kernel.shape[0]):
        shifted = jnp.concatenate(
            [jnp.zeros((lag, values.shape[1]), values.dtype), values[: total_rows - lag]], axis=0
        )
        keep = (position >= lag).astype(values.dtype)[:, None]
        total = total + shifted * keep * kernel[lag][None, :]
    return jax.nn.silu(total)


def rotate(values, position):
    half_dim = values.shape[-1] // 2
    inverse = 10000.0 ** (-jnp.arange(half_dim, dtype=jnp.float32) / half_dim)
    angle = position.astype(jnp.float32)[:, None] * inverse[None, :]
    cosine = jnp.cos(angle)[:, None, :]
    sine_part = jnp.sin(angle)[:, None, :]
    first_half = values[..., :half_dim]
    second_half = values[..., half_dim:]
    return jnp.concatenate(
        [
            first_half * cosine - second_half * sine_part,
            second_half * cosine + first_half * sine_part,
        ],
        axis=-1,
    )


def attend_core(pair_data, values, segment, slot_index, position, block_rows):
    group_row_block = values.shape[0]
    count_of_heads = values.shape[1] // AHD
    paired = pair_data.reshape(group_row_block, count_of_heads, 2, AHD)
    queries = rotate(paired[:, :, 0], position).astype(jnp.bfloat16)
    keys_all = rotate(paired[:, :, 1], position).astype(jnp.bfloat16)
    vals_all = values.reshape(group_row_block, count_of_heads, AHD).astype(jnp.bfloat16)
    scaling = AHD ** (-0.5)
    block_count = group_row_block // block_rows

    def one_block(inputs):
        query_part, query_seg, query_slot = inputs
        scores = (
            jnp.einsum("qhd,khd->hqk", query_part, keys_all, preferred_element_type=jnp.float32)
            * scaling
        )
        allowed = (query_seg[:, None] == segment[None, :]) & (
            query_slot[:, None] >= slot_index[None, :]
        )
        scores = jnp.where(allowed[None], scores, -1e30)
        weights = jnp.exp(scores)
        weights_low = (weights / jnp.sum(weights, axis=-1, keepdims=True)).astype(jnp.bfloat16)
        return jnp.einsum("hqk,khd->qhd", weights_low, vals_all, preferred_element_type=jnp.float32)

    mapped = lax.map(
        jax.checkpoint(one_block),
        (
            queries.reshape(block_count, block_rows, count_of_heads, AHD),
            segment.reshape(block_count, block_rows),
            slot_index.reshape(block_count, block_rows),
        ),
    )
    return mapped.reshape(group_row_block, count_of_heads * AHD)


def state_scan(inputs_x, step_size, b_mat, c_mat, decay_rate, segment):
    total_rows, count_of_heads, head_dim = inputs_x.shape
    spans = total_rows // SPAN
    log_decay = step_size * decay_rate[None, :]
    weighted = inputs_x * step_size[:, :, None]
    causal = jnp.arange(SPAN)[:, None] >= jnp.arange(SPAN)[None, :]

    def advance(carried_in, inputs):
        memory, last_segment = carried_in
        decay_part, weighted_part, b_part, c_part, seg_part = inputs
        running = jnp.cumsum(decay_part, axis=0)
        same_seq = (seg_part[:, None] == seg_part[None, :]) & causal
        intersection = jnp.dot(c_part, b_part.T, precision=highest)
        log_gap = jnp.where(same_seq[:, :, None], running[:, None, :] - running[None, :, :], 0.0)
        mixing = jnp.where(same_seq[:, :, None], jnp.exp(log_gap), 0.0) * intersection[:, :, None]
        output = jnp.einsum("tsh,shp->thp", mixing, weighted_part, precision=highest)
        carried = (seg_part == last_segment).astype(jnp.float32)
        reach_back = jnp.exp(running) * carried[:, None]
        output = (
            output
            + jnp.einsum("tn,hpn->thp", c_part, memory, precision=highest) * reach_back[:, :, None]
        )
        tail_seg = seg_part[-1]
        toward = (
            jnp.exp(running[-1][None, :] - running)
            * (seg_part == tail_seg).astype(jnp.float32)[:, None]
        )
        next_state = jnp.einsum("sh,shp,sn->hpn", toward, weighted_part, b_part, precision=highest)
        keep_all = jnp.exp(running[-1]) * (tail_seg == last_segment).astype(jnp.float32)
        next_state = next_state + memory * keep_all[:, None, None]
        return ((next_state, tail_seg), output)

    initial = (jnp.zeros((count_of_heads, head_dim, b_mat.shape[1]), jnp.float32), jnp.int32(-1))
    pieces = (
        log_decay.reshape(spans, SPAN, count_of_heads),
        weighted.reshape(spans, SPAN, count_of_heads, head_dim),
        b_mat.reshape(spans, SPAN, -1),
        c_mat.reshape(spans, SPAN, -1),
        segment.reshape(spans, SPAN),
    )
    last_state, outputs = lax.scan(jax.checkpoint(advance), initial, pieces)
    return outputs.reshape(total_rows, count_of_heads, head_dim)


def mamba_core(
    inner_in,
    step_in,
    bc_post,
    bias_in,
    decay_in,
    skip_weight_input,
    kernel_in,
    conv_bias_in,
    position,
    segment,
):
    group_row_block = inner_in.shape[0]
    count_of_heads = step_in.shape[1]
    mixer_result = causal_conv(inner_in, kernel_in, conv_bias_in, position)
    reshaped_tensor = mixer_result.reshape(group_row_block, count_of_heads, MIXER_HEAD_SIZE)
    step_size = jax.nn.softplus(step_in + bias_in[None, :])
    scan_result = state_scan(
        reshaped_tensor,
        step_size,
        bc_post[:, :STATE],
        bc_post[:, STATE:],
        -jnp.exp(decay_in),
        segment,
    )
    return (scan_result + skip_weight_input[None, :, None] * reshaped_tensor).reshape(
        group_row_block, count_of_heads * MIXER_HEAD_SIZE
    )


def collect(first_part, second_part):
    return (
        lax.all_gather(first_part, ("fsdp", "ctx"), axis=1, tiled=True),
        lax.all_gather(second_part, ("fsdp", "ctx"), axis=1, tiled=True),
    )


def collect_again(first_part, second_part):
    return (
        lax.all_gather(first_part, ("fsdp", "ctx"), axis=1, tiled=True),
        lax.all_gather(second_part, ("fsdp", "ctx"), axis=1, tiled=True),
    )


def tensor_sum(partial_sum):
    return lax.psum(partial_sum, "tp")


def tensor_pair(first_part, second_part):
    return (
        lax.psum(first_part.astype(jnp.bfloat16), "tp").astype(jnp.float32),
        lax.psum(second_part.astype(jnp.bfloat16), "tp").astype(jnp.float32),
    )


def heads_pair(first_part, second_part):
    return (
        lax.all_to_all(first_part, "ctx", split_axis=1, concat_axis=0, tiled=True),
        lax.all_to_all(second_part, "ctx", split_axis=1, concat_axis=0, tiled=True),
    )


def heads_one(values):
    return lax.all_to_all(values, "ctx", split_axis=1, concat_axis=0, tiled=True)


def tokens_pair(first_part, second_part):
    return (
        lax.all_to_all(first_part, "ctx", split_axis=0, concat_axis=1, tiled=True),
        lax.all_to_all(second_part, "ctx", split_axis=0, concat_axis=1, tiled=True),
    )


def tokens_one(values):
    return lax.all_to_all(values, "ctx", split_axis=0, concat_axis=1, tiled=True)


def per_device(
    hidden,
    embeds,
    cotangent,
    lengths,
    attention_norm_gain,
    adapter_down_maps,
    query_key_value_weight,
    adapter_up_maps,
    attention_output_weight,
    feedforward_norm_gain,
    gate_up_weight,
    down_weight,
    mixer_norm_gain,
    mixer_gate_input_weight,
    state_map_weight,
    step_size_weight,
    mixer_input_taps,
    mixer_input_tap_bias,
    state_map_taps,
    state_map_tap_bias,
    step_size_bias,
    log_decay_rate,
    head_skip_weight,
    gated_norm_gain,
    mixer_output_weight,
):
    tok_rows = hidden.shape[0]
    ctx_size = lax.axis_size("ctx")
    ctx_index = lax.axis_index("ctx")
    group_row_block = tok_rows * ctx_size
    block_rows = group_row_block // max(1, group_row_block // 1024)
    segment, position, slot_index = layout(lengths[0], group_row_block)
    hidden_f = hidden.astype(jnp.float32)
    embeds_f = embeds.astype(jnp.float32)
    attention_block_full, attn_out = collect(query_key_value_weight, attention_output_weight)
    joined = jnp.concatenate([hidden_f, embeds_f], axis=1)
    normed_a, norm_a_back = jax.vjp(rms_scale, joined, attention_norm_gain)
    attention_input_reduced = normed_a.astype(jnp.bfloat16)
    middle_reduced_precision = [
        matrix_product(attention_input_reduced, adapter_down_maps[group_member]).astype(
            jnp.bfloat16
        )
        for group_member in range(3)
    ]
    projected_input = [
        (
            matrix_product(attention_input_reduced, attention_block_full[group_member])
            + matrix_product(middle_reduced_precision[group_member], adapter_up_maps[group_member])
        ).astype(jnp.bfloat16)
        for group_member in range(3)
    ]
    tp_heads = projected_input[0].shape[1] // AHD
    pair_data = jnp.stack(
        [
            projected_input[0].reshape(tok_rows, tp_heads, AHD),
            projected_input[1].reshape(tok_rows, tp_heads, AHD),
        ],
        axis=2,
    ).reshape(tok_rows, tp_heads * 2 * AHD)
    pair_heads, value_heads = heads_pair(pair_data, projected_input[2])
    attn_core, attn_pull = jax.vjp(
        lambda pairs_in, values_in: attend_core(
            pairs_in, values_in, segment, slot_index, position, block_rows
        ),
        pair_heads.astype(jnp.float32),
        value_heads.astype(jnp.float32),
    )
    attn_tokens = tokens_one(attn_core.astype(jnp.bfloat16))
    after_attn = hidden_f + tensor_sum(matrix_product(attn_tokens, attn_out))
    mlp_big, mlp_down = collect(gate_up_weight, down_weight)
    normed_m, norm_m_back = jax.vjp(rms_scale, after_attn, feedforward_norm_gain)
    xm_low = normed_m.astype(jnp.bfloat16)
    gate_pre = matrix_product(xm_low, mlp_big[0])
    up_pre = matrix_product(xm_low, mlp_big[1])
    activated, act_back = jax.vjp(gated_gelu, gate_pre, up_pre)
    hid_low = activated.astype(jnp.bfloat16)
    after_mlp = after_attn + tensor_sum(matrix_product(hid_low, mlp_down))
    mamba_big, mamba_out = collect(mixer_gate_input_weight, mixer_output_weight)
    normed_n, norm_n_back = jax.vjp(rms_scale, after_mlp, mixer_norm_gain)
    xn_low = normed_n.astype(jnp.bfloat16)
    gate_z = matrix_product(xn_low, mamba_big[0])
    inner_x = matrix_product(xn_low, mamba_big[1]).astype(jnp.bfloat16)
    step_raw = matrix_product(xn_low, step_size_weight).astype(jnp.bfloat16)
    bc_low = matrix_product(xn_low, state_map_weight).astype(jnp.bfloat16)
    x_heads, step_heads = heads_pair(inner_x, step_raw)
    bc_group = lax.all_gather(bc_low, "ctx", axis=0, tiled=True)
    bc_post, bc_conv_pull = jax.vjp(
        lambda values_in, kernel_in, conv_bias_in: causal_conv(
            values_in, kernel_in, conv_bias_in, position
        ),
        bc_group.astype(jnp.float32),
        state_map_taps,
        state_map_tap_bias,
    )
    heads_on_device_share = step_heads.shape[1]
    start_offset = ctx_index * heads_on_device_share
    channel_count_here = heads_on_device_share * MIXER_HEAD_SIZE
    channel_offset_begin = start_offset * MIXER_HEAD_SIZE
    bias_local = lax.dynamic_slice_in_dim(step_size_bias, start_offset, heads_on_device_share)
    decay_local = lax.dynamic_slice_in_dim(log_decay_rate, start_offset, heads_on_device_share)
    skip_local = lax.dynamic_slice_in_dim(head_skip_weight, start_offset, heads_on_device_share)
    kernel_local = lax.dynamic_slice_in_dim(
        mixer_input_taps, channel_offset_begin, channel_count_here, 1
    )
    conv_bias_local = lax.dynamic_slice_in_dim(
        mixer_input_tap_bias, channel_offset_begin, channel_count_here, 0
    )
    scan_out, scan_pull = jax.vjp(
        lambda xs_in, step_in, bcp_in, bias_in, decay_in, skip_weight_input, kernel_in, conv_bias_in: mamba_core(
            xs_in,
            step_in,
            bcp_in,
            bias_in,
            decay_in,
            skip_weight_input,
            kernel_in,
            conv_bias_in,
            position,
            segment,
        ),
        x_heads.astype(jnp.float32),
        step_heads.astype(jnp.float32),
        bc_post,
        bias_local,
        decay_local,
        skip_local,
        kernel_local,
        conv_bias_local,
    )
    y_tokens = tokens_one(scan_out.astype(jnp.bfloat16)).astype(jnp.float32)
    silu_z = jax.nn.silu(gate_z)
    gated = y_tokens * silu_z
    total_sq = tensor_sum(jnp.sum(gated * gated, axis=1))
    inverse = lax.rsqrt(total_sq / INNER + epsilon)[:, None]
    yn_low = (gated * inverse * gated_norm_gain).astype(jnp.bfloat16)
    after_mamba = after_mlp + tensor_sum(matrix_product(yn_low, mamba_out))
    result = after_mamba.astype(jnp.bfloat16)
    grad_out = cotangent.astype(jnp.float32)
    mamba_big, mamba_out = collect_again(mixer_gate_input_weight, mixer_output_weight)
    d_yn = matrix_product_transposed(cotangent, mamba_out)
    grad_w_out = outer_product_sum(yn_low, cotangent)
    gain_part = d_yn * gated_norm_gain
    cross = tensor_sum(jnp.sum(gain_part * gated, axis=1))
    grad_g_gate = jnp.sum(d_yn * gated * inverse, axis=0)
    d_gated = gain_part * inverse - gated * inverse**3 * (cross / INNER)[:, None]
    d_y = (d_gated * silu_z).astype(jnp.bfloat16)
    sigmoid_z = jax.nn.sigmoid(gate_z)
    d_z = (d_gated * y_tokens * sigmoid_z * (1.0 + gate_z * (1.0 - sigmoid_z))).astype(jnp.bfloat16)
    dy_heads = heads_one(d_y)
    (
        d_xs,
        d_step,
        d_bc_post,
        grad_bias_local,
        grad_decay_local,
        grad_skip_local,
        grad_kernel_local,
        grad_conv_bias_local,
    ) = scan_pull(dy_heads.astype(jnp.float32))
    d_xs_tok, d_step_tok = tokens_pair(d_xs.astype(jnp.bfloat16), d_step.astype(jnp.bfloat16))
    d_bc_ctx = lax.psum(d_bc_post.astype(jnp.bfloat16), "ctx").astype(jnp.float32)
    dxn_part = (
        matrix_product_transposed(d_z, mamba_big[0])
        + matrix_product_transposed(d_xs_tok, mamba_big[1])
        + matrix_product_transposed(d_step_tok, step_size_weight)
    )
    grad_w_zx = jnp.stack([outer_product_sum(xn_low, d_z), outer_product_sum(xn_low, d_xs_tok)])
    grad_w_dt = outer_product_sum(xn_low, d_step_tok)
    dxn_sum, d_bc_full = tensor_pair(dxn_part, d_bc_ctx)
    d_bc_pre = bc_conv_pull(d_bc_full)[0]
    d_bc_mine = lax.dynamic_slice_in_dim(d_bc_pre, ctx_index * tok_rows, tok_rows, 0)
    own_rows = (slot_index // tok_rows == ctx_index).astype(jnp.float32)[:, None]
    ignored_part, grad_conv_bc, grad_conv_bc_bias = bc_conv_pull(d_bc_full * own_rows)
    d_bc_low = d_bc_mine.astype(jnp.bfloat16)
    dxn_total = dxn_sum + matrix_product_transposed(d_bc_low, state_map_weight)
    grad_w_bc = outer_product_sum(xn_low, d_bc_low)
    d_norm_n, grad_g_mamba = norm_n_back(dxn_total)
    d_after_mlp = grad_out + d_norm_n
    shard_heads = step_size_bias.shape[0]
    zero_heads = jnp.zeros((shard_heads,), jnp.float32)
    grad_dt_bias = lax.dynamic_update_slice_in_dim(zero_heads, grad_bias_local, start_offset, 0)
    grad_a_log = lax.dynamic_update_slice_in_dim(zero_heads, grad_decay_local, start_offset, 0)
    grad_d_skip = lax.dynamic_update_slice_in_dim(zero_heads, grad_skip_local, start_offset, 0)
    grad_conv_x = lax.dynamic_update_slice_in_dim(
        jnp.zeros(mixer_input_taps.shape, jnp.float32), grad_kernel_local, channel_offset_begin, 1
    )
    grad_conv_x_bias = lax.dynamic_update_slice_in_dim(
        jnp.zeros(mixer_input_tap_bias.shape, jnp.float32),
        grad_conv_bias_local,
        channel_offset_begin,
        0,
    )
    mlp_big, mlp_down = collect_again(gate_up_weight, down_weight)
    d_mlp_low = d_after_mlp.astype(jnp.bfloat16)
    d_hid = matrix_product_transposed(d_mlp_low, mlp_down)
    grad_w_down = outer_product_sum(hid_low, d_mlp_low)
    d_gate, d_up = act_back(d_hid)
    d_gate_low = d_gate.astype(jnp.bfloat16)
    d_up_low = d_up.astype(jnp.bfloat16)
    d_xm = tensor_sum(
        matrix_product_transposed(d_gate_low, mlp_big[0])
        + matrix_product_transposed(d_up_low, mlp_big[1])
    )
    grad_w_gu = jnp.stack(
        [outer_product_sum(xm_low, d_gate_low), outer_product_sum(xm_low, d_up_low)]
    )
    d_norm_m, grad_g_mlp = norm_m_back(d_xm)
    d_after_attn = d_after_mlp + d_norm_m
    attention_block_full, attn_out = collect_again(query_key_value_weight, attention_output_weight)
    d_attn_low = d_after_attn.astype(jnp.bfloat16)
    d_tokens = matrix_product_transposed(d_attn_low, attn_out).astype(jnp.bfloat16)
    grad_w_o = outer_product_sum(attn_tokens, d_attn_low)
    d_core = heads_one(d_tokens)
    d_pairs, d_values = attn_pull(d_core.astype(jnp.float32))
    d_pair_tok, d_value_tok = tokens_pair(
        d_pairs.astype(jnp.bfloat16), d_values.astype(jnp.bfloat16)
    )
    d_paired = d_pair_tok.reshape(tok_rows, tp_heads, 2, AHD)
    projection_gradient = [
        d_paired[:, :, 0].reshape(tok_rows, tp_heads * AHD),
        d_paired[:, :, 1].reshape(tok_rows, tp_heads * AHD),
        d_value_tok,
    ]
    dxa_part = (
        matrix_product_transposed(projection_gradient[0], attention_block_full[0])
        + matrix_product_transposed(projection_gradient[1], attention_block_full[1])
        + matrix_product_transposed(projection_gradient[2], attention_block_full[2])
    )
    dmid_part = jnp.concatenate(
        [
            matrix_product_transposed(
                projection_gradient[group_member], adapter_up_maps[group_member]
            )
            for group_member in range(3)
        ],
        axis=1,
    )
    grad_w_qkv = jnp.stack(
        [
            outer_product_sum(attention_input_reduced, projection_gradient[group_member])
            for group_member in range(3)
        ]
    )
    adapter_up_gradient = jnp.stack(
        [
            outer_product_sum(
                middle_reduced_precision[group_member], projection_gradient[group_member]
            )
            for group_member in range(3)
        ]
    )
    dxa_sum, dmid_sum = tensor_pair(dxa_part, dmid_part)
    dmid_low = dmid_sum.astype(jnp.bfloat16)
    rank_column_block = adapter_down_maps.shape[2]
    middle_gradient_pieces = [
        dmid_low[:, group_member * rank_column_block : (group_member + 1) * rank_column_block]
        for group_member in range(3)
    ]
    dxa_total = (
        dxa_sum
        + matrix_product_transposed(middle_gradient_pieces[0], adapter_down_maps[0])
        + matrix_product_transposed(middle_gradient_pieces[1], adapter_down_maps[1])
        + matrix_product_transposed(middle_gradient_pieces[2], adapter_down_maps[2])
    )
    adapter_down_gradient = jnp.stack(
        [
            outer_product_sum(attention_input_reduced, middle_gradient_pieces[group_member])
            for group_member in range(3)
        ]
    )
    d_joined, grad_g_attn = norm_a_back(dxa_total)
    d_hidden = d_after_attn + d_joined[:, :MODEL_WIDTH]
    d_embeds = d_joined[:, MODEL_WIDTH:]
    grad_w_qkv, grad_w_o, grad_w_gu, grad_w_down, grad_w_zx, grad_w_out = (
        lax.psum_scatter(
            grad_w_qkv.astype(jnp.bfloat16), ("fsdp", "ctx"), scatter_dimension=1, tiled=True
        ).astype(jnp.float32),
        lax.psum_scatter(
            grad_w_o.astype(jnp.bfloat16), ("fsdp", "ctx"), scatter_dimension=1, tiled=True
        ).astype(jnp.float32),
        lax.psum_scatter(
            grad_w_gu.astype(jnp.bfloat16), ("fsdp", "ctx"), scatter_dimension=1, tiled=True
        ).astype(jnp.float32),
        lax.psum_scatter(
            grad_w_down.astype(jnp.bfloat16), ("fsdp", "ctx"), scatter_dimension=1, tiled=True
        ).astype(jnp.float32),
        lax.psum_scatter(
            grad_w_zx.astype(jnp.bfloat16), ("fsdp", "ctx"), scatter_dimension=1, tiled=True
        ).astype(jnp.float32),
        lax.psum_scatter(
            grad_w_out.astype(jnp.bfloat16), ("fsdp", "ctx"), scatter_dimension=1, tiled=True
        ).astype(jnp.float32),
    )
    (
        grad_g_attn,
        adapter_down_gradient,
        adapter_up_gradient,
        grad_g_mlp,
        grad_g_mamba,
        grad_w_bc,
        grad_w_dt,
        grad_conv_x,
        grad_conv_x_bias,
        grad_conv_bc,
        grad_conv_bc_bias,
        grad_dt_bias,
        grad_a_log,
        grad_d_skip,
        grad_g_gate,
    ) = (
        lax.psum(grad_g_attn.astype(jnp.bfloat16), ("fsdp", "ctx")).astype(jnp.float32),
        lax.psum(adapter_down_gradient.astype(jnp.bfloat16), ("fsdp", "ctx")).astype(jnp.float32),
        lax.psum(adapter_up_gradient.astype(jnp.bfloat16), ("fsdp", "ctx")).astype(jnp.float32),
        lax.psum(grad_g_mlp.astype(jnp.bfloat16), ("fsdp", "ctx")).astype(jnp.float32),
        lax.psum(grad_g_mamba.astype(jnp.bfloat16), ("fsdp", "ctx")).astype(jnp.float32),
        lax.psum(grad_w_bc.astype(jnp.bfloat16), ("fsdp", "ctx")).astype(jnp.float32),
        lax.psum(grad_w_dt.astype(jnp.bfloat16), ("fsdp", "ctx")).astype(jnp.float32),
        lax.psum(grad_conv_x.astype(jnp.bfloat16), ("fsdp", "ctx")).astype(jnp.float32),
        lax.psum(grad_conv_x_bias.astype(jnp.bfloat16), ("fsdp", "ctx")).astype(jnp.float32),
        lax.psum(grad_conv_bc.astype(jnp.bfloat16), ("fsdp", "ctx")).astype(jnp.float32),
        lax.psum(grad_conv_bc_bias.astype(jnp.bfloat16), ("fsdp", "ctx")).astype(jnp.float32),
        lax.psum(grad_dt_bias.astype(jnp.bfloat16), ("fsdp", "ctx")).astype(jnp.float32),
        lax.psum(grad_a_log.astype(jnp.bfloat16), ("fsdp", "ctx")).astype(jnp.float32),
        lax.psum(grad_d_skip.astype(jnp.bfloat16), ("fsdp", "ctx")).astype(jnp.float32),
        lax.psum(grad_g_gate.astype(jnp.bfloat16), ("fsdp", "ctx")).astype(jnp.float32),
    )
    return (
        result,
        d_hidden,
        d_embeds,
        grad_g_attn,
        adapter_down_gradient,
        grad_w_qkv,
        adapter_up_gradient,
        grad_w_o,
        grad_g_mlp,
        grad_w_gu,
        grad_w_down,
        grad_g_mamba,
        grad_w_zx,
        grad_w_bc,
        grad_w_dt,
        grad_conv_x,
        grad_conv_x_bias,
        grad_conv_bc,
        grad_conv_bc_bias,
        grad_dt_bias,
        grad_a_log,
        grad_d_skip,
        grad_g_gate,
        grad_w_out,
    )


PLANE = ("fsdp", "ctx")
EVERY = ("fsdp", "ctx", "tp")


MESH = pl.DeviceIdType.MESH
IN_VMEM = pl.BlockSpec(memory_space=pltpu.VMEM)
IN_HBM = pl.BlockSpec(memory_space=pltpu.HBM)
IN_SMEM = pl.BlockSpec(memory_space=pltpu.SMEM)
DMA = pltpu.SemaphoreType.DMA


class Place:
    def __init__(self, sizes):
        self.groups, self.ctx, self.tp = sizes
        g, c, t = (lax.axis_index(name) for name in EVERY)
        y, k = t // 2, lax.rem(t, 2)
        self.g, self.c, self.t, self.y, self.k = g, c, t, y, k
        self.core = (g, c, y * 2 + 1 - k)
        self.side_y = (g, c, (1 - y) * 2 + k)
        self.side_x = (g, 1 - c, t)
        self.line = [(lax.rem(g + d, self.groups), c, t) for d in range(1, self.groups)]
        self.plane = self.groups * self.ctx
        self.index = g * self.ctx + c

    def plane_peer(self, d):
        other = lax.rem(self.index + d, self.plane)
        return other, (other // self.ctx, lax.rem(other, self.ctx), self.t)

    def plane_source(self, d):
        return lax.rem(self.index + self.plane - d, self.plane)


def greet(devices):
    barrier = pltpu.get_barrier_semaphore()
    for device in devices:
        pl.semaphore_signal(barrier, inc=1, device_id=device, device_id_type=MESH)
    pl.semaphore_wait(barrier, len(devices))


def remote(src, dst, send_sem, recv_sem, device):
    return pltpu.make_async_remote_copy(
        src_ref=src,
        dst_ref=dst,
        send_sem=send_sem,
        recv_sem=recv_sem,
        device_id=device,
        device_id_type=MESH,
    )


def cut(ref, axis, index, width):
    if axis is None:
        return ref
    at = [slice(None)] * len(ref.shape)
    start = index * width
    if width % 128 == 0:
        start = pl.multiple_of(start, 128)
    at[axis] = pl.ds(start, width)
    return ref.at[tuple(at)]


class Moves:
    def __init__(self, place, specs, sources, targets, stages, send, recv, local):
        self.sent = []
        self.place, self.specs = place, specs
        self.sources, self.targets = sources, targets
        self.stages, self.send, self.recv, self.local = stages, send, recv, local

    def part(self, i, to, origin):
        split, join = self.specs[i]
        src, dst = self.sources[i], self.targets[i]
        n = self.place.plane
        if split is None:
            return src, dst.at[origin]
        return (
            cut(src, split, to, src.shape[split] // n),
            cut(dst, join, origin, dst.shape[join] // n),
        )

    def start(self):
        place = self.place
        self.loads, self.queue = [], []
        for i in range(len(self.specs)):
            self.queue += [(i, d) for d in range(1, place.plane)]
            src, _ = self.part(i, place.index, place.index)
            load = pltpu.make_async_copy(src, self.stages[i], self.local.at[i, 0])
            load.start()
            self.loads.append(load)

    def issue(self, count):
        for i, d in self.queue[:count]:
            other, device = self.place.plane_peer(d)
            src, dst = self.part(i, other, self.place.index)
            copy = remote(src, dst, self.send.at[i, d], self.recv.at[i, d], device)
            copy.start()
            self.sent.append(copy)
        self.queue = self.queue[count:]

    def settle(self):
        self.stores = []
        for i, load in enumerate(self.loads):
            load.wait()
            _, dst = self.part(i, self.place.index, self.place.index)
            store = pltpu.make_async_copy(self.stages[i], dst, self.local.at[i, 1])
            store.start()
            self.stores.append(store)

    def finish(self):
        place = self.place
        for i in range(len(self.specs)):
            for d in range(1, place.plane):
                _, device = place.plane_peer(d)
                src, dst = self.part(i, place.index, place.plane_source(d))
                remote(src, dst, self.send.at[i, d], self.recv.at[i, d], device).wait_recv()
        for copy in self.sent:
            copy.wait_send()
        for store in self.stores:
            store.wait()


def moves_setup(moves, plane):
    outs, scratch = [], []
    for array, split, join in moves:
        shape = list(array.shape)
        part = list(array.shape)
        if split is None:
            shape = [plane] + shape
        else:
            part[split] //= plane
            shape[split] //= plane
            shape[join] *= plane
        outs.append(jax.ShapeDtypeStruct(tuple(shape), array.dtype))
        scratch.append(pltpu.VMEM(tuple(part), array.dtype))
    n = len(moves)
    if n:
        scratch += [DMA((n, plane)), DMA((n, plane)), DMA((n, 2))]
    return outs, scratch


def spans(width, extra, count):
    step = width // count
    found = [(i * step, step) for i in range(count)]
    if extra:
        found.append((width, extra))
    return found


def gather_stage(place, x, o, pieces, sems, between):
    zs, zr, s2, r2, s3, r3, s4, r4, own_sem = sems
    g, c, y, k = place.g, place.c, place.y, place.k
    n = len(pieces)
    lines = place.groups - 1
    own = pltpu.make_async_copy(x, o.at[g, c, y, k], own_sem)
    own.start()
    first = []
    for q, (at, width) in enumerate(pieces):
        cols = pl.ds(at, width)
        for d in range(lines):
            copy = remote(
                x.at[:, cols], o.at[g, c, y, k, :, cols], zs.at[q, d], zr.at[q, d], place.line[d]
            )
            copy.start()
            first.append(copy)
    own.wait()
    second, third, fourth = [None] * n, [None] * n, [None] * n

    def to_side(q):
        cols = pl.ds(*pieces[q])
        for d in range(lines):
            src = lax.rem(g + place.groups - d - 1, place.groups)
            remote(
                x.at[:, cols], o.at[src, c, y, k, :, cols], zs.at[q, d], zr.at[q, d], place.line[d]
            ).wait_recv()
        part = o.at[:, c, y, k, :, cols]
        device = place.side_y if q % 2 == 0 else place.side_x
        second[q] = remote(part, part, s2.at[q], r2.at[q], device)
        second[q].start()

    def to_other_side(q):
        cols = pl.ds(*pieces[q])
        second[q].wait_recv()
        if q % 2 == 0:
            part, device = o.at[:, c, :, k, :, cols], place.side_x
        else:
            part, device = o.at[:, :, y, k, :, cols], place.side_y
        third[q] = remote(part, part, s3.at[q], r3.at[q], device)
        third[q].start()

    def to_core(q):
        cols = pl.ds(*pieces[q])
        third[q].wait_recv()
        part = o.at[:, :, :, k, :, cols]
        fourth[q] = remote(part, part, s4.at[q], r4.at[q], place.core)
        fourth[q].start()

    for step in range(n + 2):
        between()
        if step < n:
            to_side(step)
        if 0 <= step - 1 < n:
            to_other_side(step - 1)
        if 0 <= step - 2 < n:
            to_core(step - 2)
    for q in range(n):
        fourth[q].wait_recv()
    for copy in first + second + third + fourth:
        copy.wait_send()


def gather_sems(n, groups):
    return [DMA((n, groups - 1)), DMA((n, groups - 1))] + [DMA((n,))] * 6 + [DMA]


def scatter_stage(place, make, pieces, bufs, acc, sems, between):
    theirs, mine, b1, b2, b3, b4 = bufs
    sa, ra, sb, rb, sc, rc, sd, rd = sems
    g, c, y, k = place.g, place.c, place.y, place.k
    n = len(pieces)
    lines = place.groups - 1
    f32, bf16 = jnp.float32, jnp.bfloat16
    c1, c2, c3, c4 = [None] * n, [None] * n, [None] * n, [None] * n

    def to_core(q):
        cols = pl.ds(*pieces[q])
        make(q, theirs, 1 - k)
        c1[q] = remote(theirs.at[..., cols], b1.at[..., cols], sa.at[q], ra.at[q], place.core)
        c1[q].start()
        make(q, mine, k)

    def to_side(q):
        cols = pl.ds(*pieces[q])
        c1[q].wait_recv()
        b1[..., cols] = (b1[..., cols].astype(f32) + mine[..., cols].astype(f32)).astype(bf16)
        if q % 2 == 0:
            part, device = b1.at[:, :, 1 - y, :, cols], place.side_y
        else:
            part, device = b1.at[:, 1 - c, :, :, cols], place.side_x
        c2[q] = remote(part, b2.at[:, :, :, cols], sb.at[q], rb.at[q], device)
        c2[q].start()

    def to_other_side(q):
        cols = pl.ds(*pieces[q])
        c2[q].wait_recv()
        own = b1[:, :, y, :, cols] if q % 2 == 0 else b1[:, c, :, :, cols]
        b2[:, :, :, cols] = (b2[:, :, :, cols].astype(f32) + own.astype(f32)).astype(bf16)
        if q % 2 == 0:
            part, device = b2.at[:, 1 - c, :, cols], place.side_x
        else:
            part, device = b2.at[:, 1 - y, :, cols], place.side_y
        c3[q] = remote(part, b3.at[:, :, cols], sc.at[q], rc.at[q], device)
        c3[q].start()

    def along_line(q):
        cols = pl.ds(*pieces[q])
        c3[q].wait_recv()
        own = b2[:, c, :, cols] if q % 2 == 0 else b2[:, y, :, cols]
        b3[:, :, cols] = (b3[:, :, cols].astype(f32) + own.astype(f32)).astype(bf16)
        c4[q] = []
        for d in range(lines):
            to = lax.rem(g + d + 1, place.groups)
            copy = remote(
                b3.at[to, :, cols], b4.at[d, :, cols], sd.at[q, d], rd.at[q, d], place.line[d]
            )
            copy.start()
            c4[q].append(copy)

    def land(q):
        cols = pl.ds(*pieces[q])
        total = b3[g, :, cols].astype(f32)
        for d in range(lines):
            c4[q][d].wait_recv()
            total = total + b4[d, :, cols].astype(f32)
        acc[:, cols] = total

    for step in range(n + 4):
        for lag, stage in enumerate((to_core, to_side, to_other_side, along_line, land)):
            if 0 <= step - lag < n:
                stage(step - lag)
        between()
    for q in range(n):
        for copy in [c1[q], c2[q], c3[q]] + c4[q]:
            copy.wait_send()


def scatter_scratch(n, groups, rows, width):
    bf16 = jnp.bfloat16
    bufs = [
        pltpu.VMEM((groups, 2, 2, rows, width), bf16),
        pltpu.VMEM((groups, 2, 2, rows, width), bf16),
        pltpu.VMEM((groups, 2, 2, rows, width), bf16),
        pltpu.VMEM((groups, 2, rows, width), bf16),
        pltpu.VMEM((groups, rows, width), bf16),
        pltpu.VMEM((groups - 1, rows, width), bf16),
        pltpu.VMEM((rows, width), jnp.float32),
    ]
    sems = [DMA((n,))] * 6 + [DMA((n, groups - 1))] * 2
    return bufs, sems


def rms_rows(x, gain):
    return x * lax.rsqrt(jnp.mean(x * x, axis=-1, keepdims=True) + epsilon) * gain


def rms_back(x, gain, grad):
    inverse = lax.rsqrt(jnp.mean(x * x, axis=-1, keepdims=True) + epsilon)
    scaled = grad * gain
    along = jnp.mean(scaled * x, axis=-1, keepdims=True)
    d_gain = jnp.sum(grad * x * inverse, axis=0, keepdims=True)
    return scaled * inverse - x * inverse**3 * along, d_gain


NT = (((1,), (1,)), ((), ()))
NN = (((1,), (0,)), ((), ()))


def exchange(
    sizes,
    number,
    products,
    extra,
    finish,
    finish_args,
    finish_outs,
    gathered,
    moves,
    early_share=60,
    tail=0,
):
    groups, ctx, tp = sizes
    f32, bf16 = jnp.float32, jnp.bfloat16
    total_rows = products[0][0].shape[0]
    rows = total_rows // (groups * ctx * tp)
    width = products[0][1].shape[-2 if products[0][3] else -1]
    rights_all, places = [], []
    for _, right, _, _ in products:
        found = [i for i, other in enumerate(rights_all) if other is right]
        places.append(found[0] if found else len(rights_all))
        if not found:
            rights_all.append(right)
    more = 0 if extra is None else extra.shape[1]
    pieces = spans(width, more, 4)
    out_pieces = spans(gathered, 0, 1) if gathered < 1024 else spans(2048, gathered - 2048, 4)
    move_outs, move_scratch = moves_setup(moves, groups * ctx)
    bufs, sems = scatter_scratch(len(pieces), groups, rows, width + more)
    n_prod, n_args, n_outs, n_moves = len(products), len(finish_args), len(finish_outs), len(moves)
    move_specs = [(split, join) for _, split, join in moves]

    def kernel(*refs):
        refs = list(refs)

        def take(count):
            head = refs[:count]
            del refs[:count]
            return head

        lefts, rights = take(n_prod), take(len(rights_all))
        extra_ref = take(1)[0] if more else None
        args, sources = take(n_args), take(n_moves)
        o = take(1)[0]
        o_tail = take(1)[0] if tail else None
        outs, targets = take(n_outs), take(n_moves)
        b = take(len(bufs))
        acc = b.pop()
        s = take(len(sems))
        low = take(1)[0]
        gs = take(9)
        if tail:
            low_tail, ts = take(1)[0], take(5)
        place = Place(sizes)
        devices = [place.core, place.side_y]
        if n_moves:
            devices += [place.plane_peer(d)[1] for d in range(1, place.plane)]
        else:
            devices += [place.side_x] + place.line
        greet(devices)
        carried = None
        if n_moves:
            stages = take(n_moves)
            send, recv, local = take(3)
            carried = Moves(place, move_specs, sources, targets, stages, send, recv, local)

        def make(q, into, core):
            at, size = pieces[q]
            if at >= width:
                into[..., pl.ds(at, size)] = extra_ref[:, :, :, core]
                return

            def block(i, _):
                total = None
                for left, where, (_, _, lead, transposed) in zip(lefts, places, products):
                    right = rights[where] if lead is None else rights[where].at[lead]
                    a = left[i, :, :, core]
                    a = a.reshape(-1, a.shape[-1])
                    if transposed:
                        part = lax.dot_general(
                            a, right[pl.ds(at, size), :], NT, preferred_element_type=f32
                        )
                    else:
                        part = lax.dot_general(
                            a, right[:, pl.ds(at, size)], NN, preferred_element_type=f32
                        )
                    total = part if total is None else total + part
                into[i, :, :, :, pl.ds(at, size)] = total.astype(bf16).reshape(
                    ctx, tp // 2, rows, size
                )
                return 0

            lax.fori_loop(0, groups, block, 0)

        def between(count):
            return lambda: carried.issue(count) if carried is not None else None

        if carried is not None:
            carried.start()
        steps = len(pieces) + 4
        early = -(-(n_moves * (groups * ctx - 1) * early_share) // (100 * steps))
        scatter_stage(place, make, pieces, b, acc, s, between(early))
        if carried is not None:
            carried.settle()
        finish(place, acc, args, outs, low, low_tail if tail else None)
        if tail:
            ys, yr, ks, kr, own_sem = ts
            y, k = place.y, place.k
            own = pltpu.make_async_copy(low_tail, o_tail.at[y, k], own_sem)
            own.start()
            to_y = remote(low_tail, o_tail.at[y, k], ys, yr, place.side_y)
            to_y.start()
            own.wait()
        late = -(-n_moves * (groups * ctx - 1) // max(1, len(out_pieces)))
        gather_stage(place, low, o, out_pieces, gs, between(late))
        if tail:
            to_y.wait_recv()
            part = o_tail.at[:, k]
            to_k = remote(part, part, ks, kr, place.core)
            to_k.start()
            to_k.wait_recv()
            to_y.wait_send()
            to_k.wait_send()
        if carried is not None:
            carried.issue(10**6)
            carried.finish()

    S = jax.ShapeDtypeStruct
    out_shape = [S((groups, ctx, tp // 2, 2, rows, gathered), bf16)]
    out_specs = [IN_VMEM]
    if tail:
        out_shape.append(S((tp // 2, 2, rows, tail), bf16))
        out_specs.append(IN_VMEM)
    out_shape += [S(shape, f32) for shape in finish_outs] + move_outs
    out_specs += [IN_VMEM] * n_outs + [IN_HBM] * n_moves
    scratch = bufs + sems + [pltpu.VMEM((rows, gathered), bf16)]
    scratch += gather_sems(len(out_pieces), groups)
    if tail:
        scratch += [pltpu.VMEM((rows, tail), bf16)] + [DMA] * 5
    scratch += move_scratch
    split = (groups, ctx, tp // 2, 2, rows)
    operands = [product[0].reshape(*split, product[0].shape[1]) for product in products]
    operands += rights_all
    if more:
        operands.append(extra.reshape(*split, more))
    operands += list(finish_args)
    in_specs = [IN_VMEM] * len(operands) + [IN_HBM] * n_moves
    operands += [array for array, _, _ in moves]
    results = pl.pallas_call(
        kernel,
        out_shape=out_shape,
        in_specs=in_specs,
        out_specs=out_specs,
        scratch_shapes=scratch,
        name=f"exchange_{number}",
        compiler_params=pltpu.CompilerParams(
            collective_id=number, has_side_effects=True, vmem_limit_bytes=62 * 2**20
        ),
    )(*operands)
    results = list(results)
    spread_out = results.pop(0).reshape(total_rows, gathered)
    tail_out = [results.pop(0).reshape(tp * rows, tail)] if tail else []
    return [spread_out] + tail_out + results


def opening(sizes, number, hidden, embeds, lengths, gain, down_all, moves):
    groups, ctx, tp = sizes
    f32, bf16 = jnp.float32, jnp.bfloat16
    rows = hidden.shape[0] // tp
    half = hidden.shape[1]
    mids = down_all.shape[1]
    width = 2 * half + mids + 128
    out_pieces = spans(4096, width - 4096, 4)
    move_outs, move_scratch = moves_setup(moves, groups * ctx)
    move_specs = [(split, join) for _, split, join in moves]
    n_moves = len(moves)

    def kernel(*refs):
        hid, emb, lens, gain_ref, down_ref = refs[:5]
        refs = list(refs[5:])
        sources = refs[:n_moves]
        o = refs[n_moves]
        targets = refs[n_moves + 1 : 2 * n_moves + 1]
        rest = refs[2 * n_moves + 1 :]
        low, gs = rest[0], rest[1:10]
        stages = rest[10 : 10 + n_moves]
        send, recv, local = rest[10 + n_moves :]
        place = Place(sizes)
        greet(
            [place.core, place.side_y]
            + [place.plane_peer(d)[1] for d in range(1, place.plane)]
        )
        carried = Moves(place, move_specs, sources, targets, stages, send, recv, local)
        carried.start()
        carried.issue(2)
        mine = pl.ds(pl.multiple_of(place.t * rows, 16), rows)
        a, b = hid[mine, :].astype(f32), emb[mine, :].astype(f32)
        squares = jnp.sum(a * a, axis=1, keepdims=True) + jnp.sum(b * b, axis=1, keepdims=True)
        inverse = lax.rsqrt(squares / (2 * half) + epsilon)
        low[:, :half] = (a * inverse * gain_ref[:, :half]).astype(bf16)
        low[:, half : 2 * half] = (b * inverse * gain_ref[:, half:]).astype(bf16)
        low[:, 2 * half : 2 * half + mids] = lax.dot_general(
            low[:, : 2 * half], down_ref[...], NN, preferred_element_type=f32
        ).astype(bf16)
        slot = lax.broadcasted_iota(jnp.int32, (rows, 128), 0)
        slot = slot + (place.c * tp + place.t) * rows
        lane = lax.broadcasted_iota(jnp.int32, (rows, 128), 1)
        segment, position, end = jnp.zeros_like(slot), slot, 0
        for i in range(lengths.shape[1]):
            length = lens[0, i]
            end = end + length
            passed = (slot >= end).astype(jnp.int32)
            segment = segment + passed
            position = position - passed * length
        marks = jnp.where(lane == 0, segment, position)
        low[:, 2 * half + mids :] = marks.astype(f32).astype(bf16)
        gather_stage(place, low, o, out_pieces, gs, lambda: carried.issue(4))
        carried.issue(10**6)
        carried.settle()
        carried.finish()

    S = jax.ShapeDtypeStruct
    results = pl.pallas_call(
        kernel,
        out_shape=[S((groups, ctx, tp // 2, 2, rows, width), bf16)] + move_outs,
        in_specs=[IN_VMEM, IN_VMEM, IN_SMEM, IN_VMEM, IN_VMEM] + [IN_HBM] * n_moves,
        out_specs=[IN_VMEM] + [IN_HBM] * n_moves,
        scratch_shapes=[pltpu.VMEM((rows, width), bf16)]
        + gather_sems(len(out_pieces), groups)
        + move_scratch,
        name=f"opening_{number}",
        compiler_params=pltpu.CompilerParams(
            collective_id=number, has_side_effects=True, vmem_limit_bytes=62 * 2**20
        ),
    )(hidden, embeds, lengths, gain.reshape(1, -1), down_all, *[array for array, _, _ in moves])
    return [results[0].reshape(-1, width)] + list(results[1:])


def sum_small(sizes, number, values):
    groups, ctx, tp = sizes
    f32 = jnp.float32

    def kernel(x, o, zbuf, buf, zs, zr, ss, rs):
        place = Place(sizes)
        greet([place.core, place.side_y, place.side_x] + place.line)
        copies = []
        for d, device in enumerate(place.line):
            copy = remote(x, zbuf.at[d], zs.at[d], zr.at[d], device)
            copy.start()
            copies.append(copy)
        total = x[...]
        for d in range(groups - 1):
            copies[d].wait_recv()
        order = [zbuf[d] for d in range(groups - 1)]
        parts = []
        for g in range(groups):
            part = total
            for d in range(groups - 1):
                src = lax.rem(place.g + groups - d - 1, groups)
                part = jnp.where(src == g, order[d], part)
            parts.append(part)
        total = parts[0]
        for part in parts[1:]:
            total = total + part
        for i, device in enumerate((place.side_x, place.side_y, place.core)):
            o[...] = total
            copy = remote(o, buf.at[i], ss.at[i], rs.at[i], device)
            copy.start()
            copy.wait_recv()
            copy.wait_send()
            total = total + buf[i]
        o[...] = total
        for copy in copies:
            copy.wait_send()

    shape = values.shape
    return pl.pallas_call(
        kernel,
        out_shape=jax.ShapeDtypeStruct(shape, f32),
        in_specs=[IN_VMEM],
        out_specs=IN_VMEM,
        scratch_shapes=[
            pltpu.VMEM((groups - 1, *shape), f32),
            pltpu.VMEM((3, *shape), f32),
            DMA((groups - 1,)),
            DMA((groups - 1,)),
            DMA((3,)),
            DMA((3,)),
        ],
        name=f"sum_small_{number}",
        compiler_params=pltpu.CompilerParams(collective_id=number, has_side_effects=True),
    )(values)


def finish_forward(place, acc, args, outs, low, low_tail):
    rest, gain = args
    outs[0][...] = rest[...] + acc[...]
    low[...] = rms_rows(outs[0][...], gain[...]).astype(jnp.bfloat16)


def finish_mixer_back(place, acc, args, outs, low, low_tail):
    after_mlp, gain, cot, state_map = args
    width = after_mlp.shape[1]
    low[:, width:] = acc[:, width:].astype(jnp.bfloat16)
    d_normed = acc[:, :width] + lax.dot_general(
        low[:, width:], state_map[...], NT, preferred_element_type=jnp.float32
    )
    d_rows, d_gain = rms_back(after_mlp[...], gain[...], d_normed)
    outs[1][...] = d_gain
    d_rows = cot[...].astype(jnp.float32) + d_rows
    outs[0][...] = d_rows
    low[:, :width] = d_rows.astype(jnp.bfloat16)


def finish_mlp_back(place, acc, args, outs, low, low_tail):
    after_attn, gain, d_after_mlp = args
    d_rows, d_gain = rms_back(after_attn[...], gain[...], acc[...])
    outs[1][...] = d_gain
    d_rows = d_after_mlp[...] + d_rows
    outs[0][...] = d_rows
    low[...] = d_rows.astype(jnp.bfloat16)


def finish_attention_back(place, acc, args, outs, low, low_tail):
    hidden, embeds, gain, d_after_attn, down_all, out_mine = args
    half = hidden.shape[1]
    bf16, f32 = jnp.bfloat16, jnp.float32
    low[...] = acc[:, 2 * half :].astype(bf16)
    inputs = (hidden, embeds)
    squares = sum(jnp.sum(part[...] * part[...], axis=1, keepdims=True) for part in inputs)
    inverse = lax.rsqrt(squares / (2 * half) + epsilon)
    along = jnp.zeros_like(squares)
    for i, part in enumerate(inputs):
        cols = slice(i * half, (i + 1) * half)
        grad = acc[:, cols] + lax.dot_general(
            low[...], down_all[cols, :], NT, preferred_element_type=f32
        )
        acc[:, cols] = grad
        along = along + jnp.sum(grad * gain[:, cols] * part[...], axis=1, keepdims=True)
    along = along / (2 * half)
    low_tail[:, :half] = out_mine[...]
    for i, part in enumerate(inputs):
        cols = slice(i * half, (i + 1) * half)
        grad = acc[:, cols]
        outs[0][:, cols] = jnp.sum(grad * part[...] * inverse, axis=0, keepdims=True)
        d_rows = grad * gain[:, cols] * inverse - part[...] * inverse**3 * along
        if i == 0:
            d_rows = d_rows + d_after_attn[...]
        low_tail[:, (i + 1) * half : (i + 2) * half] = d_rows.astype(bf16)


def pack(parts, dtype):
    flat = jnp.concatenate([part.reshape(-1).astype(dtype) for part in parts])
    count = -(-flat.shape[0] // 2048) * 2048
    return jnp.pad(flat, (0, count - flat.shape[0])).reshape(-1, 128)


def unpack(packed, parts):
    flat, at, found = packed.reshape(-1), 0, []
    for part in parts:
        found.append(flat[at : at + part.size].reshape(part.shape))
        at += part.size
    return found


def shift_conv(values, kernel, bias, position):
    total = values * kernel[0][None, :] + bias[None, :]
    for lag in range(1, kernel.shape[0]):
        shifted = jnp.pad(values, ((lag, 0), (0, 0)))[: values.shape[0]]
        keep = (position >= lag).astype(values.dtype)[:, None]
        total = total + shifted * keep * kernel[lag][None, :]
    return jax.nn.silu(total)


def attend_groups(queries, keys_all, vals_all, segment, position):
    def rot(values):
        half_dim = values.shape[-1] // 2
        inverse = 10000.0 ** (-jnp.arange(half_dim, dtype=jnp.float32) / half_dim)
        angle = position.astype(jnp.float32)[..., None] * inverse
        cosine, sine = jnp.cos(angle), jnp.sin(angle)
        a, b = values[..., :half_dim], values[..., half_dim:]
        return jnp.concatenate([a * cosine - b * sine, b * cosine + a * sine], axis=-1).astype(
            jnp.bfloat16
        )

    rows = queries.shape[1]
    order = jnp.arange(rows)
    scores = jnp.einsum(
        "gqd,gkd->gqk", rot(queries), rot(keys_all), preferred_element_type=jnp.float32
    ) * AHD ** (-0.5)
    allowed = (segment[:, :, None] == segment[:, None, :]) & (order[:, None] >= order[None, :])
    weights = jnp.exp(jnp.where(allowed, scores, -1e30))
    low = (weights / jnp.sum(weights, axis=-1, keepdims=True)).astype(jnp.bfloat16)
    return jnp.einsum(
        "gqk,gkd->gqd", low, vals_all.astype(jnp.bfloat16), preferred_element_type=jnp.float32
    )


def mixer_groups(
    inner_in, step_in, bc_post, bias_in, decay_in, skip_in, kernel_in, conv_bias_in, position, segment
):
    groups, rows = segment.shape
    heads = step_in.shape[1]
    xc = shift_conv(inner_in, kernel_in, conv_bias_in, position.reshape(-1))
    xc = xc.reshape(groups, rows, heads, MIXER_HEAD_SIZE)
    step = jax.nn.softplus(step_in + bias_in[None, :]).reshape(groups, rows, heads)
    log_decay = step * -jnp.exp(decay_in)
    order = jnp.arange(rows)
    same = (segment[:, :, None] == segment[:, None, :]) & (order[:, None] >= order[None, :])
    running = jnp.einsum("gts,gsh->gth", same.astype(jnp.float32), log_decay, precision=highest)
    gap = running.transpose(0, 2, 1)
    gap = gap[:, :, :, None] - gap[:, :, None, :]
    decay = jnp.where(same[:, None], jnp.exp(jnp.where(same[:, None], gap, 0.0)), 0.0)
    b_mat = bc_post[:, :STATE].reshape(groups, rows, STATE)
    c_mat = bc_post[:, STATE:].reshape(groups, rows, STATE)
    meet = jnp.einsum("gtn,gsn->gts", c_mat, b_mat, precision=lax.Precision.HIGH)
    out = jnp.einsum(
        "ghts,gshp->gthp",
        decay * meet[:, None],
        xc * step[..., None],
        precision=lax.Precision.HIGH,
    )
    out = out + skip_in[:, None] * xc
    return out.reshape(groups * rows, heads * MIXER_HEAD_SIZE)


def per_device_split(
    hidden,
    embeds,
    cotangent,
    lengths,
    attention_norm_gain,
    adapter_down_maps,
    query_key_value_weight,
    adapter_up_maps,
    attention_output_weight,
    feedforward_norm_gain,
    gate_up_weight,
    down_weight,
    mixer_norm_gain,
    mixer_gate_input_weight,
    state_map_weight,
    step_size_weight,
    mixer_input_taps,
    mixer_input_tap_bias,
    state_map_taps,
    state_map_tap_bias,
    step_size_bias,
    log_decay_rate,
    head_skip_weight,
    gated_norm_gain,
    mixer_output_weight,
):
    bf16, f32 = jnp.bfloat16, jnp.float32
    tp_size, ctx_size, groups = (lax.axis_size(name) for name in ("tp", "ctx", "fsdp"))
    tp_index, ctx_index = lax.axis_index("tp"), lax.axis_index("ctx")
    plane_index = lax.axis_index("fsdp") * ctx_size + ctx_index
    plane_size = groups * ctx_size
    tok_rows = hidden.shape[0]
    mine = tok_rows // tp_size
    group_rows = tok_rows * ctx_size
    start = tp_index * mine

    sizes = (groups, ctx_size, tp_size)

    def own_rows(values):
        return lax.dynamic_slice_in_dim(values, start, mine, 0)

    def own_part(values, axis=0):
        width = values.shape[axis] // plane_size
        return lax.dynamic_slice_in_dim(values, plane_index * width, width, axis)

    width = hidden.shape[1]
    hidden_f = own_rows(hidden).astype(f32)
    embeds_f = own_rows(embeds).astype(f32)
    cot_low = own_rows(cotangent)

    up_maps = own_part(adapter_up_maps, 2)
    w_step = own_part(step_size_weight, 1)
    taps, tap_bias = own_part(mixer_input_taps, 1), own_part(mixer_input_tap_bias)
    step_bias, decay_rate = own_part(step_size_bias), own_part(log_decay_rate)
    skip, gate_gain = own_part(head_skip_weight), own_part(gated_norm_gain)

    rank = adapter_down_maps.shape[2]
    width_a = adapter_down_maps.shape[1]
    down_all = jnp.concatenate([adapter_down_maps[j] for j in range(3)], axis=1)
    gathered, w_qkv, w_o = opening(
        sizes,
        1,
        hidden,
        embeds,
        lengths,
        attention_norm_gain,
        down_all,
        [(query_key_value_weight, 2, 1), (attention_output_weight, 0, 1)],
    )
    xa = gathered[:, :width_a]
    mid = gathered[:, width_a : width_a + 3 * rank]
    segment = gathered[:, width_a + 3 * rank].astype(jnp.int32).reshape(groups, group_rows)
    position = gathered[:, width_a + 3 * rank + 1].astype(jnp.int32).reshape(groups, group_rows)
    position_flat = position.reshape(-1)
    late_cot, _ = lax.optimization_barrier((cot_low, w_o))
    cot = lax.all_gather(late_cot, EVERY, axis=0, tiled=True)
    proj = [
        (
            matrix_product(xa, w_qkv[j])
            + matrix_product(mid[:, j * rank : (j + 1) * rank], up_maps[j])
        ).astype(bf16)
        for j in range(3)
    ]
    ao, attend_back = jax.vjp(
        lambda q, k, v: attend_groups(q, k, v, segment, position),
        *[piece.astype(f32).reshape(groups, group_rows, AHD) for piece in proj],
    )
    ao_low = ao.astype(bf16).reshape(groups * group_rows, AHD)

    gain_m = feedforward_norm_gain.reshape(1, -1)
    xm, after_attn, w_gu, w_down = exchange(
        sizes,
        2,
        [(ao_low, w_o, None, False)],
        None,
        finish_forward,
        [hidden_f, gain_m],
        [hidden_f.shape],
        width,
        [(gate_up_weight, 2, 1), (down_weight, 0, 1)],
    )
    gate_pre, up_pre = matrix_product(xm, w_gu[0]), matrix_product(xm, w_gu[1])
    activated, act_back = jax.vjp(gated_gelu, gate_pre, up_pre)
    hid_low = activated.astype(bf16)

    gain_n = mixer_norm_gain.reshape(1, -1)
    xn, after_mlp, w_zx, w_out = exchange(
        sizes,
        3,
        [(hid_low, w_down, None, False)],
        None,
        finish_forward,
        [after_attn, gain_n],
        [hidden_f.shape],
        width,
        [(mixer_gate_input_weight, 2, 1), (mixer_output_weight, 0, 1)],
    )
    gate_z = matrix_product(xn, w_zx[0])
    inner_x = matrix_product(xn, w_zx[1]).astype(bf16)
    step_raw = matrix_product(xn, w_step).astype(bf16)
    bc_low = matrix_product(xn, state_map_weight).astype(bf16)
    bc_post, bc_conv_back = jax.vjp(
        lambda v, k, b: shift_conv(v, k, b, position_flat),
        bc_low.astype(f32),
        state_map_taps,
        state_map_tap_bias,
    )
    scan_out, scan_back = jax.vjp(
        lambda *parts: mixer_groups(*parts, position, segment),
        inner_x.astype(f32),
        step_raw.astype(f32),
        bc_post,
        step_bias,
        decay_rate,
        skip,
        taps,
        tap_bias,
    )
    y = scan_out.astype(bf16).astype(f32)
    silu_z = jax.nn.silu(gate_z)
    gated = y * silu_z
    d_yn = matrix_product_transposed(cot, w_out)
    gain_part = d_yn * gate_gain
    sums = jnp.stack([jnp.sum(gated * gated, axis=1), jnp.sum(gain_part * gated, axis=1)])
    sums = sum_small(sizes, 4, sums.reshape(-1, 128)).reshape(2, -1)
    inverse = lax.rsqrt(sums[0] / INNER + epsilon)[:, None]
    cross = (sums[1] / INNER)[:, None]
    yn_low = (gated * inverse * gate_gain).astype(bf16)
    out_part = matrix_product(yn_low, w_out).astype(bf16)
    out_mine = lax.psum_scatter(out_part, EVERY, scatter_dimension=0, tiled=True)
    out_mine = (after_mlp + out_mine.astype(f32)).astype(bf16)

    grad_w_out = outer_product_sum(yn_low, cot)
    grad_g_gate = jnp.sum(d_yn * gated * inverse, axis=0)
    d_gated = gain_part * inverse - gated * inverse**3 * cross
    d_y = (d_gated * silu_z).astype(bf16)
    sigmoid_z = jax.nn.sigmoid(gate_z)
    d_z = (d_gated * y * sigmoid_z * (1.0 + gate_z * (1.0 - sigmoid_z))).astype(bf16)
    (
        d_xs,
        d_step,
        d_bc_post,
        grad_dt_bias,
        grad_a_log,
        grad_d_skip,
        grad_conv_x,
        grad_conv_x_bias,
    ) = scan_back(d_y.astype(f32))
    d_xs, d_step = d_xs.astype(bf16), d_step.astype(bf16)
    d_bc_part, grad_conv_bc, grad_conv_bc_bias = bc_conv_back(d_bc_post)
    grad_w_zx = jnp.stack(
        [outer_product_sum(xn, d_z).astype(bf16), outer_product_sum(xn, d_xs).astype(bf16)]
    )
    grad_w_dt = outer_product_sum(xn, d_step)
    lanes = ((0, 0), (0, 128 - d_step.shape[1]))
    gathered, d_after_mlp, grad_g_mamba, grad_w_zx, grad_w_out = exchange(
        sizes,
        5,
        [
            (d_z, w_zx, 0, True),
            (d_xs, w_zx, 1, True),
            (jnp.pad(d_step, lanes), jnp.pad(w_step, lanes), None, True),
        ],
        d_bc_part.astype(bf16),
        finish_mixer_back,
        [after_mlp, gain_n, cot_low, state_map_weight],
        [hidden_f.shape, gain_n.shape],
        width + d_bc_part.shape[1],
        [(grad_w_zx, 1, 2), (grad_w_out.astype(bf16), 1, 0)],
    )

    d_mlp, d_bc = gathered[:, :width], gathered[:, width:]
    grad_w_bc = outer_product_sum(xn, d_bc)
    grad_w_down = outer_product_sum(hid_low, d_mlp)
    d_gate, d_up = act_back(matrix_product_transposed(d_mlp, w_down))
    d_gate, d_up = d_gate.astype(bf16), d_up.astype(bf16)
    grad_w_gu = jnp.stack(
        [outer_product_sum(xm, d_gate).astype(bf16), outer_product_sum(xm, d_up).astype(bf16)]
    )

    d_attn, d_after_attn, grad_g_mlp, grad_w_gu, grad_w_down = exchange(
        sizes,
        6,
        [(d_gate, w_gu, 0, True), (d_up, w_gu, 1, True)],
        None,
        finish_mlp_back,
        [after_attn, gain_m, d_after_mlp],
        [hidden_f.shape, gain_m.shape],
        width,
        [(grad_w_gu, 1, 2), (grad_w_down.astype(bf16), 1, 0)],
    )
    grad_w_o = outer_product_sum(ao_low, d_attn)
    d_ao = matrix_product_transposed(d_attn, w_o).astype(bf16)
    d_proj = [
        piece.reshape(groups * group_rows, AHD).astype(bf16)
        for piece in attend_back(d_ao.astype(f32).reshape(groups, group_rows, AHD))
    ]
    dmid_part = jnp.concatenate(
        [matrix_product_transposed(d_proj[j], up_maps[j]).astype(bf16) for j in range(3)], axis=1
    )
    grad_w_qkv = jnp.stack([outer_product_sum(xa, d_proj[j]).astype(bf16) for j in range(3)])
    adapter_up_gradient = jnp.stack(
        [outer_product_sum(mid[:, j * rank : (j + 1) * rank], d_proj[j]) for j in range(3)]
    )
    shares = [
        adapter_up_gradient,
        grad_w_dt,
        grad_conv_x,
        grad_conv_x_bias,
        grad_g_gate,
        grad_dt_bias,
        grad_a_log,
        grad_d_skip,
    ]
    joins = (2, 1, 1, 0, 0, 0, 0, 0)
    dmid, back, grad_g_attn, grad_w_qkv, grad_w_o, shared = exchange(
        sizes,
        7,
        [(d_proj[j], w_qkv, j, True) for j in range(3)],
        dmid_part,
        finish_attention_back,
        [
            hidden_f,
            embeds_f,
            attention_norm_gain.reshape(1, -1),
            d_after_attn,
            down_all,
            out_mine,
        ],
        [(1, width_a)],
        3 * rank,
        [(grad_w_qkv, 1, 2), (grad_w_o.astype(bf16), 1, 0), (pack(shares, bf16), None, 0)],
        early_share=100,
        tail=3 * width,
    )
    adapter_down_gradient = jnp.stack(
        [outer_product_sum(xa, dmid[:, j * rank : (j + 1) * rank]) for j in range(3)]
    )
    result = back[:, :width]
    d_hidden = back[:, width : 2 * width].astype(f32)
    d_embeds = back[:, 2 * width :].astype(f32)
    (
        adapter_up_gradient,
        grad_w_dt,
        grad_conv_x,
        grad_conv_x_bias,
        grad_g_gate,
        grad_dt_bias,
        grad_a_log,
        grad_d_skip,
    ) = [
        jnp.concatenate(parts, axis=join).astype(f32)
        for parts, join in zip(
            zip(*[unpack(shared[i], shares) for i in range(plane_size)]), joins
        )
    ]
    sums = [grad_g_attn, grad_g_mlp, grad_g_mamba, grad_conv_bc, grad_conv_bc_bias]
    grad_g_attn, grad_g_mlp, grad_g_mamba, grad_conv_bc, grad_conv_bc_bias = unpack(
        sum_small(sizes, 8, pack(sums, f32)), sums
    )

    return (
        result,
        d_hidden,
        d_embeds,
        grad_g_attn[0],
        adapter_down_gradient,
        grad_w_qkv.astype(f32),
        adapter_up_gradient,
        grad_w_o.astype(f32),
        grad_g_mlp[0],
        grad_w_gu.astype(f32),
        grad_w_down.astype(f32),
        grad_g_mamba[0],
        grad_w_zx.astype(f32),
        grad_w_bc,
        grad_w_dt,
        grad_conv_x,
        grad_conv_x_bias,
        grad_conv_bc,
        grad_conv_bc_bias,
        grad_dt_bias,
        grad_a_log,
        grad_d_skip,
        grad_g_gate,
        grad_w_out.astype(f32),
    )


def solution(mesh):
    placed = (
        P(("fsdp", "ctx"), None),
        P(("fsdp", "ctx"), None),
        P(("fsdp", "ctx"), None),
        P("fsdp", None),
        P(),
        P(),
        P(None, ("fsdp", "ctx"), "tp"),
        P(None, None, "tp"),
        P("tp", ("fsdp", "ctx")),
        P(),
        P(None, ("fsdp", "ctx"), "tp"),
        P("tp", ("fsdp", "ctx")),
        P(),
        P(None, ("fsdp", "ctx"), "tp"),
        P(),
        P(None, "tp"),
        P(None, "tp"),
        P("tp"),
        P(),
        P(),
        P("tp"),
        P("tp"),
        P("tp"),
        P("tp"),
        P("tp", ("fsdp", "ctx")),
    )
    devices = mesh.shape["fsdp"] * mesh.shape["ctx"] * mesh.shape["tp"]
    one_head_each = devices == AHEADS and mesh.shape["ctx"] == 2 and mesh.shape["tp"] == 4
    return jax.shard_map(
        per_device_split if one_head_each else per_device,
        mesh=mesh,
        in_specs=placed,
        out_specs=(
            P(("fsdp", "ctx"), None),
            P(("fsdp", "ctx"), None),
            P(("fsdp", "ctx"), None),
            P(),
            P(),
            P(None, ("fsdp", "ctx"), "tp"),
            P(None, None, "tp"),
            P("tp", ("fsdp", "ctx")),
            P(),
            P(None, ("fsdp", "ctx"), "tp"),
            P("tp", ("fsdp", "ctx")),
            P(),
            P(None, ("fsdp", "ctx"), "tp"),
            P(),
            P(None, "tp"),
            P(None, "tp"),
            P("tp"),
            P(),
            P(),
            P("tp"),
            P("tp"),
            P("tp"),
            P("tp"),
            P("tp", ("fsdp", "ctx")),
        ),
        check_vma=False,
    )
```

```python
import functools

import jax
import jax.numpy as jnp
from jax import lax
from jax.experimental import pallas as pl
from jax.experimental.pallas import tpu as pltpu
from jax.sharding import PartitionSpec as P

MODEL_WIDTH = 2048
AHEADS = 32
AHD = 128
INNER = 4096
MIXER_HEAD_SIZE = 64
STATE = 128
SPAN = 128


highest = lax.Precision.HIGHEST
epsilon = 1e-05


def matrix_product(left, right):
    return jnp.dot(left, right, preferred_element_type=jnp.float32)


def matrix_product_transposed(left, right):
    return lax.dot_general(
        left, right, (((1,), (1,)), ((), ())), preferred_element_type=jnp.float32
    )


def outer_product_sum(left, right):
    return lax.dot_general(
        left, right, (((0,), (0,)), ((), ())), preferred_element_type=jnp.float32
    )


def rms_scale(values, gain):
    return values * lax.rsqrt(jnp.mean(values * values, axis=-1, keepdims=True) + epsilon) * gain


def gated_gelu(gate_in, up_in):
    return jax.nn.gelu(gate_in, approximate=True) * up_in


def layout(lengths_row, total_rows):
    ends = jnp.cumsum(lengths_row)
    slot_index = jnp.arange(total_rows, dtype=jnp.int32)
    passed = (slot_index[:, None] >= ends[None, :]).astype(jnp.int32)
    segment = jnp.sum(passed, axis=1)
    position = slot_index - jnp.sum(passed * lengths_row[None, :], axis=1)
    return (segment, position, slot_index)


def causal_conv(values, kernel, bias, position):
    total_rows = values.shape[0]
    total = values * kernel[0][None, :] + bias[None, :]
    for lag in range(1, kernel.shape[0]):
        shifted = jnp.concatenate(
            [jnp.zeros((lag, values.shape[1]), values.dtype), values[: total_rows - lag]], axis=0
        )
        keep = (position >= lag).astype(values.dtype)[:, None]
        total = total + shifted * keep * kernel[lag][None, :]
    return jax.nn.silu(total)


def rotate(values, position):
    half_dim = values.shape[-1] // 2
    inverse = 10000.0 ** (-jnp.arange(half_dim, dtype=jnp.float32) / half_dim)
    angle = position.astype(jnp.float32)[:, None] * inverse[None, :]
    cosine = jnp.cos(angle)[:, None, :]
    sine_part = jnp.sin(angle)[:, None, :]
    first_half = values[..., :half_dim]
    second_half = values[..., half_dim:]
    return jnp.concatenate(
        [
            first_half * cosine - second_half * sine_part,
            second_half * cosine + first_half * sine_part,
        ],
        axis=-1,
    )


def attend_core(pair_data, values, segment, slot_index, position, block_rows):
    group_row_block = values.shape[0]
    count_of_heads = values.shape[1] // AHD
    paired = pair_data.reshape(group_row_block, count_of_heads, 2, AHD)
    queries = rotate(paired[:, :, 0], position).astype(jnp.bfloat16)
    keys_all = rotate(paired[:, :, 1], position).astype(jnp.bfloat16)
    vals_all = values.reshape(group_row_block, count_of_heads, AHD).astype(jnp.bfloat16)
    scaling = AHD ** (-0.5)
    block_count = group_row_block // block_rows

    def one_block(inputs):
        query_part, query_seg, query_slot = inputs
        scores = (
            jnp.einsum("qhd,khd->hqk", query_part, keys_all, preferred_element_type=jnp.float32)
            * scaling
        )
        allowed = (query_seg[:, None] == segment[None, :]) & (
            query_slot[:, None] >= slot_index[None, :]
        )
        scores = jnp.where(allowed[None], scores, -1e30)
        weights = jnp.exp(scores)
        weights_low = (weights / jnp.sum(weights, axis=-1, keepdims=True)).astype(jnp.bfloat16)
        return jnp.einsum("hqk,khd->qhd", weights_low, vals_all, preferred_element_type=jnp.float32)

    mapped = lax.map(
        jax.checkpoint(one_block),
        (
            queries.reshape(block_count, block_rows, count_of_heads, AHD),
            segment.reshape(block_count, block_rows),
            slot_index.reshape(block_count, block_rows),
        ),
    )
    return mapped.reshape(group_row_block, count_of_heads * AHD)


def state_scan(inputs_x, step_size, b_mat, c_mat, decay_rate, segment):
    total_rows, count_of_heads, head_dim = inputs_x.shape
    spans = total_rows // SPAN
    log_decay = step_size * decay_rate[None, :]
    weighted = inputs_x * step_size[:, :, None]
    causal = jnp.arange(SPAN)[:, None] >= jnp.arange(SPAN)[None, :]

    def advance(carried_in, inputs):
        memory, last_segment = carried_in
        decay_part, weighted_part, b_part, c_part, seg_part = inputs
        running = jnp.cumsum(decay_part, axis=0)
        same_seq = (seg_part[:, None] == seg_part[None, :]) & causal
        intersection = jnp.dot(c_part, b_part.T, precision=highest)
        log_gap = jnp.where(same_seq[:, :, None], running[:, None, :] - running[None, :, :], 0.0)
        mixing = jnp.where(same_seq[:, :, None], jnp.exp(log_gap), 0.0) * intersection[:, :, None]
        output = jnp.einsum("tsh,shp->thp", mixing, weighted_part, precision=highest)
        carried = (seg_part == last_segment).astype(jnp.float32)
        reach_back = jnp.exp(running) * carried[:, None]
        output = (
            output
            + jnp.einsum("tn,hpn->thp", c_part, memory, precision=highest) * reach_back[:, :, None]
        )
        tail_seg = seg_part[-1]
        toward = (
            jnp.exp(running[-1][None, :] - running)
            * (seg_part == tail_seg).astype(jnp.float32)[:, None]
        )
        next_state = jnp.einsum("sh,shp,sn->hpn", toward, weighted_part, b_part, precision=highest)
        keep_all = jnp.exp(running[-1]) * (tail_seg == last_segment).astype(jnp.float32)
        next_state = next_state + memory * keep_all[:, None, None]
        return ((next_state, tail_seg), output)

    initial = (jnp.zeros((count_of_heads, head_dim, b_mat.shape[1]), jnp.float32), jnp.int32(-1))
    pieces = (
        log_decay.reshape(spans, SPAN, count_of_heads),
        weighted.reshape(spans, SPAN, count_of_heads, head_dim),
        b_mat.reshape(spans, SPAN, -1),
        c_mat.reshape(spans, SPAN, -1),
        segment.reshape(spans, SPAN),
    )
    last_state, outputs = lax.scan(jax.checkpoint(advance), initial, pieces)
    return outputs.reshape(total_rows, count_of_heads, head_dim)


def mamba_core(
    inner_in,
    step_in,
    bc_post,
    bias_in,
    decay_in,
    skip_weight_input,
    kernel_in,
    conv_bias_in,
    position,
    segment,
):
    group_row_block = inner_in.shape[0]
    count_of_heads = step_in.shape[1]
    mixer_result = causal_conv(inner_in, kernel_in, conv_bias_in, position)
    reshaped_tensor = mixer_result.reshape(group_row_block, count_of_heads, MIXER_HEAD_SIZE)
    step_size = jax.nn.softplus(step_in + bias_in[None, :])
    scan_result = state_scan(
        reshaped_tensor,
        step_size,
        bc_post[:, :STATE],
        bc_post[:, STATE:],
        -jnp.exp(decay_in),
        segment,
    )
    return (scan_result + skip_weight_input[None, :, None] * reshaped_tensor).reshape(
        group_row_block, count_of_heads * MIXER_HEAD_SIZE
    )


def collect(first_part, second_part):
    return (
        lax.all_gather(first_part, ("fsdp", "ctx"), axis=1, tiled=True),
        lax.all_gather(second_part, ("fsdp", "ctx"), axis=1, tiled=True),
    )


def collect_again(first_part, second_part):
    return (
        lax.all_gather(first_part, ("fsdp", "ctx"), axis=1, tiled=True),
        lax.all_gather(second_part, ("fsdp", "ctx"), axis=1, tiled=True),
    )


def tensor_sum(partial_sum):
    return lax.psum(partial_sum, "tp")


def tensor_pair(first_part, second_part):
    return (
        lax.psum(first_part.astype(jnp.bfloat16), "tp").astype(jnp.float32),
        lax.psum(second_part.astype(jnp.bfloat16), "tp").astype(jnp.float32),
    )


def heads_pair(first_part, second_part):
    return (
        lax.all_to_all(first_part, "ctx", split_axis=1, concat_axis=0, tiled=True),
        lax.all_to_all(second_part, "ctx", split_axis=1, concat_axis=0, tiled=True),
    )


def heads_one(values):
    return lax.all_to_all(values, "ctx", split_axis=1, concat_axis=0, tiled=True)


def tokens_pair(first_part, second_part):
    return (
        lax.all_to_all(first_part, "ctx", split_axis=0, concat_axis=1, tiled=True),
        lax.all_to_all(second_part, "ctx", split_axis=0, concat_axis=1, tiled=True),
    )


def tokens_one(values):
    return lax.all_to_all(values, "ctx", split_axis=0, concat_axis=1, tiled=True)


def per_device(
    hidden,
    embeds,
    cotangent,
    lengths,
    attention_norm_gain,
    adapter_down_maps,
    query_key_value_weight,
    adapter_up_maps,
    attention_output_weight,
    feedforward_norm_gain,
    gate_up_weight,
    down_weight,
    mixer_norm_gain,
    mixer_gate_input_weight,
    state_map_weight,
    step_size_weight,
    mixer_input_taps,
    mixer_input_tap_bias,
    state_map_taps,
    state_map_tap_bias,
    step_size_bias,
    log_decay_rate,
    head_skip_weight,
    gated_norm_gain,
    mixer_output_weight,
):
    tok_rows = hidden.shape[0]
    ctx_size = lax.axis_size("ctx")
    ctx_index = lax.axis_index("ctx")
    group_row_block = tok_rows * ctx_size
    block_rows = group_row_block // max(1, group_row_block // 1024)
    segment, position, slot_index = layout(lengths[0], group_row_block)
    hidden_f = hidden.astype(jnp.float32)
    embeds_f = embeds.astype(jnp.float32)
    attention_block_full, attn_out = collect(query_key_value_weight, attention_output_weight)
    joined = jnp.concatenate([hidden_f, embeds_f], axis=1)
    normed_a, norm_a_back = jax.vjp(rms_scale, joined, attention_norm_gain)
    attention_input_reduced = normed_a.astype(jnp.bfloat16)
    middle_reduced_precision = [
        matrix_product(attention_input_reduced, adapter_down_maps[group_member]).astype(
            jnp.bfloat16
        )
        for group_member in range(3)
    ]
    projected_input = [
        (
            matrix_product(attention_input_reduced, attention_block_full[group_member])
            + matrix_product(middle_reduced_precision[group_member], adapter_up_maps[group_member])
        ).astype(jnp.bfloat16)
        for group_member in range(3)
    ]
    tp_heads = projected_input[0].shape[1] // AHD
    pair_data = jnp.stack(
        [
            projected_input[0].reshape(tok_rows, tp_heads, AHD),
            projected_input[1].reshape(tok_rows, tp_heads, AHD),
        ],
        axis=2,
    ).reshape(tok_rows, tp_heads * 2 * AHD)
    pair_heads, value_heads = heads_pair(pair_data, projected_input[2])
    attn_core, attn_pull = jax.vjp(
        lambda pairs_in, values_in: attend_core(
            pairs_in, values_in, segment, slot_index, position, block_rows
        ),
        pair_heads.astype(jnp.float32),
        value_heads.astype(jnp.float32),
    )
    attn_tokens = tokens_one(attn_core.astype(jnp.bfloat16))
    after_attn = hidden_f + tensor_sum(matrix_product(attn_tokens, attn_out))
    mlp_big, mlp_down = collect(gate_up_weight, down_weight)
    normed_m, norm_m_back = jax.vjp(rms_scale, after_attn, feedforward_norm_gain)
    xm_low = normed_m.astype(jnp.bfloat16)
    gate_pre = matrix_product(xm_low, mlp_big[0])
    up_pre = matrix_product(xm_low, mlp_big[1])
    activated, act_back = jax.vjp(gated_gelu, gate_pre, up_pre)
    hid_low = activated.astype(jnp.bfloat16)
    after_mlp = after_attn + tensor_sum(matrix_product(hid_low, mlp_down))
    mamba_big, mamba_out = collect(mixer_gate_input_weight, mixer_output_weight)
    normed_n, norm_n_back = jax.vjp(rms_scale, after_mlp, mixer_norm_gain)
    xn_low = normed_n.astype(jnp.bfloat16)
    gate_z = matrix_product(xn_low, mamba_big[0])
    inner_x = matrix_product(xn_low, mamba_big[1]).astype(jnp.bfloat16)
    step_raw = matrix_product(xn_low, step_size_weight).astype(jnp.bfloat16)
    bc_low = matrix_product(xn_low, state_map_weight).astype(jnp.bfloat16)
    x_heads, step_heads = heads_pair(inner_x, step_raw)
    bc_group = lax.all_gather(bc_low, "ctx", axis=0, tiled=True)
    bc_post, bc_conv_pull = jax.vjp(
        lambda values_in, kernel_in, conv_bias_in: causal_conv(
            values_in, kernel_in, conv_bias_in, position
        ),
        bc_group.astype(jnp.float32),
        state_map_taps,
        state_map_tap_bias,
    )
    heads_on_device_share = step_heads.shape[1]
    start_offset = ctx_index * heads_on_device_share
    channel_count_here = heads_on_device_share * MIXER_HEAD_SIZE
    channel_offset_begin = start_offset * MIXER_HEAD_SIZE
    bias_local = lax.dynamic_slice_in_dim(step_size_bias, start_offset, heads_on_device_share)
    decay_local = lax.dynamic_slice_in_dim(log_decay_rate, start_offset, heads_on_device_share)
    skip_local = lax.dynamic_slice_in_dim(head_skip_weight, start_offset, heads_on_device_share)
    kernel_local = lax.dynamic_slice_in_dim(
        mixer_input_taps, channel_offset_begin, channel_count_here, 1
    )
    conv_bias_local = lax.dynamic_slice_in_dim(
        mixer_input_tap_bias, channel_offset_begin, channel_count_here, 0
    )
    scan_out, scan_pull = jax.vjp(
        lambda xs_in, step_in, bcp_in, bias_in, decay_in, skip_weight_input, kernel_in, conv_bias_in: mamba_core(
            xs_in,
            step_in,
            bcp_in,
            bias_in,
            decay_in,
            skip_weight_input,
            kernel_in,
            conv_bias_in,
            position,
            segment,
        ),
        x_heads.astype(jnp.float32),
        step_heads.astype(jnp.float32),
        bc_post,
        bias_local,
        decay_local,
        skip_local,
        kernel_local,
        conv_bias_local,
    )
    y_tokens = tokens_one(scan_out.astype(jnp.bfloat16)).astype(jnp.float32)
    silu_z = jax.nn.silu(gate_z)
    gated = y_tokens * silu_z
    total_sq = tensor_sum(jnp.sum(gated * gated, axis=1))
    inverse = lax.rsqrt(total_sq / INNER + epsilon)[:, None]
    yn_low = (gated * inverse * gated_norm_gain).astype(jnp.bfloat16)
    after_mamba = after_mlp + tensor_sum(matrix_product(yn_low, mamba_out))
    result = after_mamba.astype(jnp.bfloat16)
    grad_out = cotangent.astype(jnp.float32)
    mamba_big, mamba_out = collect_again(mixer_gate_input_weight, mixer_output_weight)
    d_yn = matrix_product_transposed(cotangent, mamba_out)
    grad_w_out = outer_product_sum(yn_low, cotangent)
    gain_part = d_yn * gated_norm_gain
    cross = tensor_sum(jnp.sum(gain_part * gated, axis=1))
    grad_g_gate = jnp.sum(d_yn * gated * inverse, axis=0)
    d_gated = gain_part * inverse - gated * inverse**3 * (cross / INNER)[:, None]
    d_y = (d_gated * silu_z).astype(jnp.bfloat16)
    sigmoid_z = jax.nn.sigmoid(gate_z)
    d_z = (d_gated * y_tokens * sigmoid_z * (1.0 + gate_z * (1.0 - sigmoid_z))).astype(jnp.bfloat16)
    dy_heads = heads_one(d_y)
    (
        d_xs,
        d_step,
        d_bc_post,
        grad_bias_local,
        grad_decay_local,
        grad_skip_local,
        grad_kernel_local,
        grad_conv_bias_local,
    ) = scan_pull(dy_heads.astype(jnp.float32))
    d_xs_tok, d_step_tok = tokens_pair(d_xs.astype(jnp.bfloat16), d_step.astype(jnp.bfloat16))
    d_bc_ctx = lax.psum(d_bc_post.astype(jnp.bfloat16), "ctx").astype(jnp.float32)
    dxn_part = (
        matrix_product_transposed(d_z, mamba_big[0])
        + matrix_product_transposed(d_xs_tok, mamba_big[1])
        + matrix_product_transposed(d_step_tok, step_size_weight)
    )
    grad_w_zx = jnp.stack([outer_product_sum(xn_low, d_z), outer_product_sum(xn_low, d_xs_tok)])
    grad_w_dt = outer_product_sum(xn_low, d_step_tok)
    dxn_sum, d_bc_full = tensor_pair(dxn_part, d_bc_ctx)
    d_bc_pre = bc_conv_pull(d_bc_full)[0]
    d_bc_mine = lax.dynamic_slice_in_dim(d_bc_pre, ctx_index * tok_rows, tok_rows, 0)
    own_rows = (slot_index // tok_rows == ctx_index).astype(jnp.float32)[:, None]
    ignored_part, grad_conv_bc, grad_conv_bc_bias = bc_conv_pull(d_bc_full * own_rows)
    d_bc_low = d_bc_mine.astype(jnp.bfloat16)
    dxn_total = dxn_sum + matrix_product_transposed(d_bc_low, state_map_weight)
    grad_w_bc = outer_product_sum(xn_low, d_bc_low)
    d_norm_n, grad_g_mamba = norm_n_back(dxn_total)
    d_after_mlp = grad_out + d_norm_n
    shard_heads = step_size_bias.shape[0]
    zero_heads = jnp.zeros((shard_heads,), jnp.float32)
    grad_dt_bias = lax.dynamic_update_slice_in_dim(zero_heads, grad_bias_local, start_offset, 0)
    grad_a_log = lax.dynamic_update_slice_in_dim(zero_heads, grad_decay_local, start_offset, 0)
    grad_d_skip = lax.dynamic_update_slice_in_dim(zero_heads, grad_skip_local, start_offset, 0)
    grad_conv_x = lax.dynamic_update_slice_in_dim(
        jnp.zeros(mixer_input_taps.shape, jnp.float32), grad_kernel_local, channel_offset_begin, 1
    )
    grad_conv_x_bias = lax.dynamic_update_slice_in_dim(
        jnp.zeros(mixer_input_tap_bias.shape, jnp.float32),
        grad_conv_bias_local,
        channel_offset_begin,
        0,
    )
    mlp_big, mlp_down = collect_again(gate_up_weight, down_weight)
    d_mlp_low = d_after_mlp.astype(jnp.bfloat16)
    d_hid = matrix_product_transposed(d_mlp_low, mlp_down)
    grad_w_down = outer_product_sum(hid_low, d_mlp_low)
    d_gate, d_up = act_back(d_hid)
    d_gate_low = d_gate.astype(jnp.bfloat16)
    d_up_low = d_up.astype(jnp.bfloat16)
    d_xm = tensor_sum(
        matrix_product_transposed(d_gate_low, mlp_big[0])
        + matrix_product_transposed(d_up_low, mlp_big[1])
    )
    grad_w_gu = jnp.stack(
        [outer_product_sum(xm_low, d_gate_low), outer_product_sum(xm_low, d_up_low)]
    )
    d_norm_m, grad_g_mlp = norm_m_back(d_xm)
    d_after_attn = d_after_mlp + d_norm_m
    attention_block_full, attn_out = collect_again(query_key_value_weight, attention_output_weight)
    d_attn_low = d_after_attn.astype(jnp.bfloat16)
    d_tokens = matrix_product_transposed(d_attn_low, attn_out).astype(jnp.bfloat16)
    grad_w_o = outer_product_sum(attn_tokens, d_attn_low)
    d_core = heads_one(d_tokens)
    d_pairs, d_values = attn_pull(d_core.astype(jnp.float32))
    d_pair_tok, d_value_tok = tokens_pair(
        d_pairs.astype(jnp.bfloat16), d_values.astype(jnp.bfloat16)
    )
    d_paired = d_pair_tok.reshape(tok_rows, tp_heads, 2, AHD)
    projection_gradient = [
        d_paired[:, :, 0].reshape(tok_rows, tp_heads * AHD),
        d_paired[:, :, 1].reshape(tok_rows, tp_heads * AHD),
        d_value_tok,
    ]
    dxa_part = (
        matrix_product_transposed(projection_gradient[0], attention_block_full[0])
        + matrix_product_transposed(projection_gradient[1], attention_block_full[1])
        + matrix_product_transposed(projection_gradient[2], attention_block_full[2])
    )
    dmid_part = jnp.concatenate(
        [
            matrix_product_transposed(
                projection_gradient[group_member], adapter_up_maps[group_member]
            )
            for group_member in range(3)
        ],
        axis=1,
    )
    grad_w_qkv = jnp.stack(
        [
            outer_product_sum(attention_input_reduced, projection_gradient[group_member])
            for group_member in range(3)
        ]
    )
    adapter_up_gradient = jnp.stack(
        [
            outer_product_sum(
                middle_reduced_precision[group_member], projection_gradient[group_member]
            )
            for group_member in range(3)
        ]
    )
    dxa_sum, dmid_sum = tensor_pair(dxa_part, dmid_part)
    dmid_low = dmid_sum.astype(jnp.bfloat16)
    rank_column_block = adapter_down_maps.shape[2]
    middle_gradient_pieces = [
        dmid_low[:, group_member * rank_column_block : (group_member + 1) * rank_column_block]
        for group_member in range(3)
    ]
    dxa_total = (
        dxa_sum
        + matrix_product_transposed(middle_gradient_pieces[0], adapter_down_maps[0])
        + matrix_product_transposed(middle_gradient_pieces[1], adapter_down_maps[1])
        + matrix_product_transposed(middle_gradient_pieces[2], adapter_down_maps[2])
    )
    adapter_down_gradient = jnp.stack(
        [
            outer_product_sum(attention_input_reduced, middle_gradient_pieces[group_member])
            for group_member in range(3)
        ]
    )
    d_joined, grad_g_attn = norm_a_back(dxa_total)
    d_hidden = d_after_attn + d_joined[:, :MODEL_WIDTH]
    d_embeds = d_joined[:, MODEL_WIDTH:]
    grad_w_qkv, grad_w_o, grad_w_gu, grad_w_down, grad_w_zx, grad_w_out = (
        lax.psum_scatter(
            grad_w_qkv.astype(jnp.bfloat16), ("fsdp", "ctx"), scatter_dimension=1, tiled=True
        ).astype(jnp.float32),
        lax.psum_scatter(
            grad_w_o.astype(jnp.bfloat16), ("fsdp", "ctx"), scatter_dimension=1, tiled=True
        ).astype(jnp.float32),
        lax.psum_scatter(
            grad_w_gu.astype(jnp.bfloat16), ("fsdp", "ctx"), scatter_dimension=1, tiled=True
        ).astype(jnp.float32),
        lax.psum_scatter(
            grad_w_down.astype(jnp.bfloat16), ("fsdp", "ctx"), scatter_dimension=1, tiled=True
        ).astype(jnp.float32),
        lax.psum_scatter(
            grad_w_zx.astype(jnp.bfloat16), ("fsdp", "ctx"), scatter_dimension=1, tiled=True
        ).astype(jnp.float32),
        lax.psum_scatter(
            grad_w_out.astype(jnp.bfloat16), ("fsdp", "ctx"), scatter_dimension=1, tiled=True
        ).astype(jnp.float32),
    )
    (
        grad_g_attn,
        adapter_down_gradient,
        adapter_up_gradient,
        grad_g_mlp,
        grad_g_mamba,
        grad_w_bc,
        grad_w_dt,
        grad_conv_x,
        grad_conv_x_bias,
        grad_conv_bc,
        grad_conv_bc_bias,
        grad_dt_bias,
        grad_a_log,
        grad_d_skip,
        grad_g_gate,
    ) = (
        lax.psum(grad_g_attn.astype(jnp.bfloat16), ("fsdp", "ctx")).astype(jnp.float32),
        lax.psum(adapter_down_gradient.astype(jnp.bfloat16), ("fsdp", "ctx")).astype(jnp.float32),
        lax.psum(adapter_up_gradient.astype(jnp.bfloat16), ("fsdp", "ctx")).astype(jnp.float32),
        lax.psum(grad_g_mlp.astype(jnp.bfloat16), ("fsdp", "ctx")).astype(jnp.float32),
        lax.psum(grad_g_mamba.astype(jnp.bfloat16), ("fsdp", "ctx")).astype(jnp.float32),
        lax.psum(grad_w_bc.astype(jnp.bfloat16), ("fsdp", "ctx")).astype(jnp.float32),
        lax.psum(grad_w_dt.astype(jnp.bfloat16), ("fsdp", "ctx")).astype(jnp.float32),
        lax.psum(grad_conv_x.astype(jnp.bfloat16), ("fsdp", "ctx")).astype(jnp.float32),
        lax.psum(grad_conv_x_bias.astype(jnp.bfloat16), ("fsdp", "ctx")).astype(jnp.float32),
        lax.psum(grad_conv_bc.astype(jnp.bfloat16), ("fsdp", "ctx")).astype(jnp.float32),
        lax.psum(grad_conv_bc_bias.astype(jnp.bfloat16), ("fsdp", "ctx")).astype(jnp.float32),
        lax.psum(grad_dt_bias.astype(jnp.bfloat16), ("fsdp", "ctx")).astype(jnp.float32),
        lax.psum(grad_a_log.astype(jnp.bfloat16), ("fsdp", "ctx")).astype(jnp.float32),
        lax.psum(grad_d_skip.astype(jnp.bfloat16), ("fsdp", "ctx")).astype(jnp.float32),
        lax.psum(grad_g_gate.astype(jnp.bfloat16), ("fsdp", "ctx")).astype(jnp.float32),
    )
    return (
        result,
        d_hidden,
        d_embeds,
        grad_g_attn,
        adapter_down_gradient,
        grad_w_qkv,
        adapter_up_gradient,
        grad_w_o,
        grad_g_mlp,
        grad_w_gu,
        grad_w_down,
        grad_g_mamba,
        grad_w_zx,
        grad_w_bc,
        grad_w_dt,
        grad_conv_x,
        grad_conv_x_bias,
        grad_conv_bc,
        grad_conv_bc_bias,
        grad_dt_bias,
        grad_a_log,
        grad_d_skip,
        grad_g_gate,
        grad_w_out,
    )


PLANE = ("fsdp", "ctx")
EVERY = ("fsdp", "ctx", "tp")


MESH = pl.DeviceIdType.MESH
IN_VMEM = pl.BlockSpec(memory_space=pltpu.VMEM)
IN_HBM = pl.BlockSpec(memory_space=pltpu.HBM)
IN_SMEM = pl.BlockSpec(memory_space=pltpu.SMEM)
DMA = pltpu.SemaphoreType.DMA
GATHER_SHARES = (4, 4, 4, 4)
SUM_SHARES = (4, 4, 4, 4)


class Place:
    def __init__(self, sizes):
        self.groups, self.ctx, self.tp = sizes
        g, c, t = (lax.axis_index(name) for name in EVERY)
        y, k = t // 2, lax.rem(t, 2)
        self.g, self.c, self.t, self.y, self.k = g, c, t, y, k
        self.core = (g, c, y * 2 + 1 - k)
        self.side_y = (g, c, (1 - y) * 2 + k)
        self.side_x = (g, 1 - c, t)
        self.line = [(lax.rem(g + d, self.groups), c, t) for d in range(1, self.groups)]
        self.plane = self.groups * self.ctx
        self.index = g * self.ctx + c

    def plane_peer(self, d):
        other = lax.rem(self.index + d, self.plane)
        return other, (other // self.ctx, lax.rem(other, self.ctx), self.t)

    def plane_source(self, d):
        return lax.rem(self.index + self.plane - d, self.plane)


def greet(devices):
    barrier = pltpu.get_barrier_semaphore()
    for device in devices:
        pl.semaphore_signal(barrier, inc=1, device_id=device, device_id_type=MESH)
    pl.semaphore_wait(barrier, len(devices))


def remote(src, dst, send_sem, recv_sem, device):
    return pltpu.make_async_remote_copy(
        src_ref=src,
        dst_ref=dst,
        send_sem=send_sem,
        recv_sem=recv_sem,
        device_id=device,
        device_id_type=MESH,
    )


def cut(ref, axis, index, width):
    if axis is None:
        return ref
    at = [slice(None)] * len(ref.shape)
    start = index * width
    if width % 128 == 0:
        start = pl.multiple_of(start, 128)
    at[axis] = pl.ds(start, width)
    return ref.at[tuple(at)]


class Moves:
    def __init__(self, place, specs, sources, targets, stages, send, recv, local):
        self.sent = []
        self.place, self.specs = place, specs
        self.sources, self.targets = sources, targets
        self.stages, self.send, self.recv, self.local = stages, send, recv, local

    def part(self, i, to, origin):
        split, join = self.specs[i]
        src, dst = self.sources[i], self.targets[i]
        n = self.place.plane
        if split is None:
            return src, cut(dst, join, origin, src.shape[join])
        return (
            cut(src, split, to, src.shape[split] // n),
            cut(dst, join, origin, dst.shape[join] // n),
        )

    def start(self):
        place = self.place
        self.loads, self.queue = [], []
        for i in range(len(self.specs)):
            self.queue += [(i, d) for d in range(1, place.plane)]
            src, _ = self.part(i, place.index, place.index)
            load = pltpu.make_async_copy(src, self.stages[i], self.local.at[i, 0])
            load.start()
            self.loads.append(load)

    def issue(self, count):
        for i, d in self.queue[:count]:
            other, device = self.place.plane_peer(d)
            src, dst = self.part(i, other, self.place.index)
            copy = remote(src, dst, self.send.at[i, d], self.recv.at[i, d], device)
            copy.start()
            self.sent.append(copy)
        self.queue = self.queue[count:]

    def settle(self):
        self.stores = []
        for i, load in enumerate(self.loads):
            load.wait()
            _, dst = self.part(i, self.place.index, self.place.index)
            store = pltpu.make_async_copy(self.stages[i], dst, self.local.at[i, 1])
            store.start()
            self.stores.append(store)

    def finish(self):
        place = self.place
        for i in range(len(self.specs)):
            for d in range(1, place.plane):
                _, device = place.plane_peer(d)
                src, dst = self.part(i, place.index, place.plane_source(d))
                remote(src, dst, self.send.at[i, d], self.recv.at[i, d], device).wait_recv()
        for copy in self.sent:
            copy.wait_send()
        for store in self.stores:
            store.wait()


def moves_setup(moves, plane):
    outs, scratch = [], []
    for array, split, join in moves:
        shape = list(array.shape)
        part = list(array.shape)
        if split is not None:
            part[split] //= plane
            shape[split] //= plane
        shape[join] *= plane
        outs.append(jax.ShapeDtypeStruct(tuple(shape), array.dtype))
        scratch.append(pltpu.VMEM(tuple(part), array.dtype))
    n = len(moves)
    if n:
        scratch += [DMA((n, plane)), DMA((n, plane)), DMA((n, 2))]
    return outs, scratch


class Gather:
    def __init__(self, place, x, o, pieces, sems):
        self.place, self.x, self.o, self.pieces, self.sems = place, x, o, pieces, sems
        self.n = len(pieces)
        self.first, self.second = [], [None] * self.n
        self.third, self.fourth = [None] * self.n, [None] * self.n

    def line_copy(self, q, d, owner):
        place, cols = self.place, pl.ds(*self.pieces[q])
        return remote(
            self.x.at[:, cols],
            self.o.at[owner, place.c, place.y, place.k, :, cols],
            self.sems[0].at[q, d],
            self.sems[1].at[q, d],
            place.line[d],
        )

    def begin(self):
        place = self.place
        own_at = self.o.at[place.g, place.c, place.y, place.k]
        own = pltpu.make_async_copy(self.x, own_at, self.sems[8])
        own.start()
        for q in range(self.n):
            for d in range(place.groups - 1):
                copy = self.line_copy(q, d, place.g)
                copy.start()
                self.first.append(copy)
        own.wait()

    def to_side(self, q):
        place = self.place
        for d in range(place.groups - 1):
            source = lax.rem(place.g + place.groups - d - 1, place.groups)
            self.line_copy(q, d, source).wait_recv()
        part = self.o.at[:, place.c, place.y, place.k, :, pl.ds(*self.pieces[q])]
        device = place.side_y if q % 2 == 0 else place.side_x
        self.second[q] = remote(part, part, self.sems[2].at[q], self.sems[3].at[q], device)
        self.second[q].start()

    def to_other_side(self, q):
        place, cols = self.place, pl.ds(*self.pieces[q])
        self.second[q].wait_recv()
        if q % 2 == 0:
            part, device = self.o.at[:, place.c, :, place.k, :, cols], place.side_x
        else:
            part, device = self.o.at[:, :, place.y, place.k, :, cols], place.side_y
        self.third[q] = remote(part, part, self.sems[4].at[q], self.sems[5].at[q], device)
        self.third[q].start()

    def to_core(self, q):
        place = self.place
        self.third[q].wait_recv()
        part = self.o.at[:, :, :, place.k, :, pl.ds(*self.pieces[q])]
        self.fourth[q] = remote(part, part, self.sems[6].at[q], self.sems[7].at[q], place.core)
        self.fourth[q].start()

    def steps(self):
        return pipelined(self.n, (self.to_side, self.to_other_side, self.to_core))

    def end(self):
        for copy in self.fourth:
            copy.wait_recv()
        for copy in self.first + self.second + self.third + self.fourth:
            copy.wait_send()


def pipelined(count, stages):
    def step(at):
        for lag, stage in enumerate(stages):
            if 0 <= at - lag < count:
                stage(at - lag)

    return [functools.partial(step, at) for at in range(count + len(stages) - 1)]


def gather_sems(n, groups):
    return [DMA((n, groups - 1)), DMA((n, groups - 1))] + [DMA((n,))] * 6 + [DMA]


class Scatter:
    def __init__(self, place, make, pieces, bufs, acc, sems):
        self.place, self.make, self.pieces, self.bufs, self.acc = place, make, pieces, bufs, acc
        self.sems = sems
        n = len(pieces)
        self.n = n
        self.c1, self.c2, self.c3, self.c4 = [None] * n, [None] * n, [None] * n, [None] * n

    def to_core(self, q):
        theirs, mine, b1 = self.bufs[:3]
        cols, k = pl.ds(*self.pieces[q]), self.place.k
        self.make(q, theirs, 1 - k)
        self.c1[q] = remote(
            theirs.at[..., cols],
            b1.at[..., cols],
            self.sems[0].at[q],
            self.sems[1].at[q],
            self.place.core,
        )
        self.c1[q].start()
        self.make(q, mine, k)

    def to_side(self, q):
        _, mine, b1, b2, _, _ = self.bufs
        place, cols = self.place, pl.ds(*self.pieces[q])
        f32 = jnp.float32
        self.c1[q].wait_recv()
        b1[..., cols] = (b1[..., cols].astype(f32) + mine[..., cols].astype(f32)).astype(b1.dtype)
        if q % 2 == 0:
            part, device = b1.at[:, :, 1 - place.y, :, cols], place.side_y
        else:
            part, device = b1.at[:, 1 - place.c, :, :, cols], place.side_x
        self.c2[q] = remote(
            part, b2.at[:, :, :, cols], self.sems[2].at[q], self.sems[3].at[q], device
        )
        self.c2[q].start()

    def to_other_side(self, q):
        _, _, b1, b2, b3, _ = self.bufs
        place, cols = self.place, pl.ds(*self.pieces[q])
        f32 = jnp.float32
        self.c2[q].wait_recv()
        own = b1[:, :, place.y, :, cols] if q % 2 == 0 else b1[:, place.c, :, :, cols]
        b2[:, :, :, cols] = (b2[:, :, :, cols].astype(f32) + own.astype(f32)).astype(b2.dtype)
        if q % 2 == 0:
            part, device = b2.at[:, 1 - place.c, :, cols], place.side_x
        else:
            part, device = b2.at[:, 1 - place.y, :, cols], place.side_y
        self.c3[q] = remote(part, b3.at[:, :, cols], self.sems[4].at[q], self.sems[5].at[q], device)
        self.c3[q].start()

    def along_line(self, q):
        _, _, _, b2, b3, b4 = self.bufs
        place, cols = self.place, pl.ds(*self.pieces[q])
        f32 = jnp.float32
        self.c3[q].wait_recv()
        own = b2[:, place.c, :, cols] if q % 2 == 0 else b2[:, place.y, :, cols]
        b3[:, :, cols] = (b3[:, :, cols].astype(f32) + own.astype(f32)).astype(b3.dtype)
        self.c4[q] = []
        for d in range(place.groups - 1):
            to = lax.rem(place.g + d + 1, place.groups)
            copy = remote(
                b3.at[to, :, cols],
                b4.at[d, :, cols],
                self.sems[6].at[q, d],
                self.sems[7].at[q, d],
                place.line[d],
            )
            copy.start()
            self.c4[q].append(copy)

    def land(self, q):
        b3, b4 = self.bufs[4:]
        cols = pl.ds(*self.pieces[q])
        total = b3[self.place.g, :, cols].astype(jnp.float32)
        for d in range(self.place.groups - 1):
            self.c4[q][d].wait_recv()
            total = total + b4[d, :, cols].astype(jnp.float32)
        self.acc[:, cols] = total

    def steps(self):
        stages = (self.to_core, self.to_side, self.to_other_side, self.along_line, self.land)
        return pipelined(self.n, stages)

    def end(self):
        for q in range(self.n):
            for copy in [self.c1[q], self.c2[q], self.c3[q]] + self.c4[q]:
                copy.wait_send()


class SmallSum:
    def __init__(self, place, x, o, zbuf, buf, zs, zr, ss, rs):
        self.place, self.x, self.o, self.zbuf, self.buf = place, x, o, zbuf, buf
        self.zs, self.zr, self.ss, self.rs = zs, zr, ss, rs

    def begin(self):
        self.copies = []
        for d, device in enumerate(self.place.line):
            copy = remote(self.x, self.zbuf.at[d], self.zs.at[d], self.zr.at[d], device)
            copy.start()
            self.copies.append(copy)

    def line(self):
        place, groups = self.place, self.place.groups
        for copy in self.copies:
            copy.wait_recv()
        total = None
        for owner in range(groups):
            part = self.x[...]
            for d in range(groups - 1):
                source = lax.rem(place.g + groups - d - 1, groups)
                part = jnp.where(source == owner, self.zbuf[d], part)
            total = part if total is None else total + part
        self.o[...] = total
        self.send(0)

    def send(self, i):
        device = (self.place.side_x, self.place.side_y, self.place.core)[i]
        self.copy = remote(self.o, self.buf.at[i], self.ss.at[i], self.rs.at[i], device)
        self.copy.start()

    def add(self, i):
        self.copy.wait_recv()
        self.copy.wait_send()
        self.o[...] = self.o[...] + self.buf[i]
        if i < 2:
            self.send(i + 1)

    def steps(self):
        return [self.line] + [functools.partial(self.add, i) for i in range(3)]

    def end(self):
        for copy in self.copies:
            copy.wait_send()


def small_scratch(shape, groups):
    f32 = jnp.float32
    return [
        pltpu.VMEM((groups - 1, *shape), f32),
        pltpu.VMEM((3, *shape), f32),
        DMA((groups - 1,)),
        DMA((groups - 1,)),
        DMA((3,)),
        DMA((3,)),
    ]


def weave(*streams):
    found = []
    rounds = max((start + len(steps) for start, steps in streams), default=0)
    for at in range(rounds):
        for start, steps in streams:
            if 0 <= at - start < len(steps):
                found.append(steps[at - start])
    return found


def scatter_scratch(n, groups, rows, width):
    bf16 = jnp.bfloat16
    bufs = [
        pltpu.VMEM((groups, 2, 2, rows, width), bf16),
        pltpu.VMEM((groups, 2, 2, rows, width), bf16),
        pltpu.VMEM((groups, 2, 2, rows, width), bf16),
        pltpu.VMEM((groups, 2, rows, width), bf16),
        pltpu.VMEM((groups, rows, width), bf16),
        pltpu.VMEM((groups - 1, rows, width), bf16),
        pltpu.VMEM((rows, width), jnp.float32),
    ]
    sems = [DMA((n,))] * 6 + [DMA((n, groups - 1))] * 2
    return bufs, sems


def rms_rows(x, gain):
    return x * lax.rsqrt(jnp.mean(x * x, axis=-1, keepdims=True) + epsilon) * gain


def rms_back(x, gain, grad):
    inverse = lax.rsqrt(jnp.mean(x * x, axis=-1, keepdims=True) + epsilon)
    scaled = grad * gain
    along = jnp.mean(scaled * x, axis=-1, keepdims=True)
    d_gain = jnp.sum(grad * x * inverse, axis=0, keepdims=True)
    return scaled * inverse - x * inverse**3 * along, d_gain


NT = (((1,), (1,)), ((), ()))
NN = (((1,), (0,)), ((), ()))


class Summed:
    def __init__(self, sizes, products, extra=None, pieces=SUM_SHARES):
        self.sizes, self.products, self.extra = sizes, products, extra
        self.rows = products[0][0].shape[0] // (sizes[0] * sizes[1] * sizes[2])
        self.width = products[0][1].shape[-2 if products[0][3] else -1]
        self.more = 0 if extra is None else extra.shape[1]
        self.rights, self.places = [], []
        for _, right, _, _ in products:
            found = [i for i, other in enumerate(self.rights) if other is right]
            self.places.append(found[0] if found else len(self.rights))
            if not found:
                self.rights.append(right)
        at, self.pieces = 0, []
        for share in pieces:
            self.pieces.append((at, self.width * share // 16))
            at += self.width * share // 16
        if self.more:
            self.pieces.append((self.width, self.more))
        self.bufs, self.sems = scatter_scratch(
            len(self.pieces), sizes[0], self.rows, self.width + self.more
        )

    def operands(self):
        groups, ctx, tp = self.sizes
        split = (groups, ctx, tp // 2, 2, self.rows)
        found = [product[0].reshape(*split, product[0].shape[1]) for product in self.products]
        found += self.rights
        if self.more:
            found.append(self.extra.reshape(*split, self.more))
        return found

    def stage(self, place, inputs, scratch):
        count = len(self.products)
        lefts, rights = inputs[:count], inputs[count : count + len(self.rights)]
        bufs, sems = scratch[: len(self.bufs)], scratch[len(self.bufs) :]
        groups, ctx, tp = self.sizes

        def make(q, into, core):
            at, size = self.pieces[q]
            if at >= self.width:
                into[..., pl.ds(at, size)] = inputs[-1][:, :, :, core]
                return

            def block(i, _):
                total = None
                for left, where, (_, _, lead, transposed) in zip(
                    lefts, self.places, self.products
                ):
                    right = rights[where] if lead is None else rights[where].at[lead]
                    a = left[i, :, :, core]
                    a = a.reshape(-1, a.shape[-1])
                    some = right[pl.ds(at, size), :] if transposed else right[:, pl.ds(at, size)]
                    part = lax.dot_general(
                        a, some, NT if transposed else NN, preferred_element_type=jnp.float32
                    )
                    total = part if total is None else total + part
                into[i, :, :, :, pl.ds(at, size)] = total.astype(into.dtype).reshape(
                    ctx, tp // 2, self.rows, size
                )
                return 0

            lax.fori_loop(0, groups, block, 0)

        return Scatter(place, make, self.pieces, bufs[:-1], bufs[-1], sems)


def exchange(
    sizes,
    number,
    summed,
    finish,
    finish_args,
    finish_outs,
    gathered,
    moves,
    early_share=60,
    also_gather=None,
    also_sum=None,
    tail=0,
    small=0,
):
    groups, ctx, tp = sizes
    f32, bf16 = jnp.float32, jnp.bfloat16
    rows = summed.rows
    out_pieces = gather_pieces(gathered)
    move_outs, move_scratch = moves_setup(moves, groups * ctx)
    n_moves = len(moves)
    move_specs = [(split, join) for _, split, join in moves]
    S = jax.ShapeDtypeStruct

    operands, in_specs, out_shape, out_specs, scratch = [], [], [], [], []

    def add_in(arrays, spec=IN_VMEM):
        at = len(operands)
        operands.extend(arrays)
        in_specs.extend([spec] * len(arrays))
        return slice(at, len(operands))

    def add_out(shapes, spec=IN_VMEM):
        at = len(out_shape)
        out_shape.extend(shapes)
        out_specs.extend([spec] * len(shapes))
        return slice(at, len(out_shape))

    def add_scratch(shapes):
        at = len(scratch)
        scratch.extend(shapes)
        return slice(at, len(scratch))

    in_sum = add_in(summed.operands())
    in_args = add_in(list(finish_args))
    o_main = add_out([S((groups, ctx, tp // 2, 2, rows, gathered), bf16)])
    o_finish = add_out([S(shape, f32) for shape in finish_outs])
    s_sum = add_scratch(summed.bufs + summed.sems)
    s_main = add_scratch(
        [pltpu.VMEM((rows, gathered), bf16)] + gather_sems(len(out_pieces), groups)
    )
    if also_gather is not None:
        also_pieces = gather_pieces(also_gather.shape[1])
        in_also = add_in([also_gather])
        o_also = add_out([S((groups, ctx, tp // 2, 2, rows, also_gather.shape[1]), bf16)])
        s_also = add_scratch(gather_sems(len(also_pieces), groups))
    if also_sum is not None:
        second, second_finish, second_args, second_out = also_sum
        in_second, in_second_args = add_in(second.operands()), add_in(second_args)
        o_second = add_out([second_out])
        s_second = add_scratch(second.bufs + second.sems)
    if tail:
        o_tail = add_out([S((tp // 2, 2, rows, tail), bf16)])
        s_tail = add_scratch([pltpu.VMEM((rows, tail), bf16)] + [DMA] * 5)
    if small:
        o_small = add_out([S((1, small), f32)])
        s_small = add_scratch([pltpu.VMEM((1, small), f32)] + small_scratch((1, small), groups))
    in_moves = add_in([array for array, _, _ in moves], IN_HBM)
    o_moves = add_out(move_outs, IN_HBM)
    s_moves = add_scratch(move_scratch)

    def kernel(*refs):
        ins = refs[: len(operands)]
        outs = refs[len(operands) : len(operands) + len(out_shape)]
        scr = refs[len(operands) + len(out_shape) :]
        place = Place(sizes)
        devices = [place.core, place.side_y]
        if n_moves:
            devices += [place.plane_peer(d)[1] for d in range(1, place.plane)]
        else:
            devices += [place.side_x] + place.line
        greet(devices)
        carried = None
        if n_moves:
            parts = scr[s_moves]
            carried = Moves(
                place, move_specs, ins[in_moves], outs[o_moves], parts[:n_moves], *parts[n_moves:]
            )
            carried.start()
        main_sum = summed.stage(place, ins[in_sum], scr[s_sum])
        low, *main_sems = scr[s_main]
        main_gather = Gather(place, low, outs[o_main][0], out_pieces, main_sems)
        streams = [(0, main_sum.steps())]
        ends = [main_sum, main_gather]
        if also_gather is not None:
            side_gather = Gather(place, ins[in_also][0], outs[o_also][0], also_pieces, scr[s_also])
            side_gather.begin()
            streams.append((2, side_gather.steps()))
            ends.append(side_gather)
        later = []
        if also_sum is not None:
            side_sum = second.stage(place, ins[in_second], scr[s_second])
            side_steps = side_sum.steps()
            streams.append((6, side_steps[:3]))
            later.append((0, side_steps[3:]))
            ends.append(side_sum)
        total = n_moves * (groups * ctx - 1)
        steps = weave(*streams)
        per_step = -(-total * early_share // (100 * len(steps)))
        for step in steps:
            step()
            if carried is not None:
                carried.issue(per_step)
        if carried is not None:
            carried.settle()
        low_tail = scr[s_tail][0] if tail else None
        low_small = scr[s_small][0] if small else None
        finish(place, main_sum.acc, ins[in_args], outs[o_finish], low, low_tail, low_small)
        main_gather.begin()
        if small:
            small_sum = SmallSum(place, low_small, outs[o_small][0], *scr[s_small][1:])
            small_sum.begin()
            later.append((1, small_sum.steps()))
            ends.append(small_sum)
        if tail:
            ys, yr, ks, kr, own_sem = scr[s_tail][1:]
            y, k, spot = place.y, place.k, outs[o_tail][0]
            own = pltpu.make_async_copy(low_tail, spot.at[y, k], own_sem)
            own.start()
            to_y = remote(low_tail, spot.at[y, k], ys, yr, place.side_y)
            to_y.start()
            own.wait()
        steps = weave((0, main_gather.steps()), *later)
        left = 0 if carried is None else len(carried.queue)
        per_step = -(-left // max(1, len(steps) - 2))
        for step in steps:
            if carried is not None:
                carried.issue(per_step)
            step()
        if tail:
            to_y.wait_recv()
            part = spot.at[:, k]
            to_k = remote(part, part, ks, kr, place.core)
            to_k.start()
            to_k.wait_recv()
            to_y.wait_send()
            to_k.wait_send()
        if also_sum is not None:
            second_finish(side_sum.acc, ins[in_second_args], outs[o_second][0])
        for stage in ends:
            stage.end()
        if carried is not None:
            carried.issue(total)
            carried.finish()

    results = pl.pallas_call(
        kernel,
        out_shape=out_shape,
        in_specs=in_specs,
        out_specs=out_specs,
        scratch_shapes=scratch,
        name=f"exchange_{number}",
        compiler_params=pltpu.CompilerParams(
            collective_id=number, has_side_effects=True, vmem_limit_bytes=62 * 2**20
        ),
    )(*operands)
    found = {"gathered": results[0].reshape(-1, gathered), "finish": results[o_finish]}
    if also_gather is not None:
        found["also"] = results[o_also][0].reshape(-1, also_gather.shape[1])
    if also_sum is not None:
        found["second"] = results[o_second][0]
    if tail:
        found["tail"] = results[o_tail][0].reshape(-1, tail)
    if small:
        found["small"] = results[o_small][0]
    found["moves"] = results[o_moves]
    return found


def gather_pieces(width):
    if width < 1024:
        return [(0, width)]
    whole = width // 2048 * 2048
    at, found = 0, []
    for share in GATHER_SHARES:
        found.append((at, whole * share // 16))
        at += whole * share // 16
    if width > whole:
        found.append((whole, width - whole))
    return found


def opening(sizes, number, hidden, embeds, lengths, gain, down_all, moves):
    groups, ctx, tp = sizes
    f32, bf16 = jnp.float32, jnp.bfloat16
    rows = hidden.shape[0] // tp
    half = hidden.shape[1]
    mids = down_all.shape[1]
    width = 2 * half + mids + 128
    out_pieces = gather_pieces(width)
    move_outs, move_scratch = moves_setup(moves, groups * ctx)
    move_specs = [(split, join) for _, split, join in moves]
    n_moves = len(moves)

    def kernel(*refs):
        hid, emb, lens, gain_ref, down_ref = refs[:5]
        refs = list(refs[5:])
        sources = refs[:n_moves]
        o = refs[n_moves]
        targets = refs[n_moves + 1 : 2 * n_moves + 1]
        rest = refs[2 * n_moves + 1 :]
        low, gs = rest[0], rest[1:10]
        stages = rest[10 : 10 + n_moves]
        send, recv, local = rest[10 + n_moves :]
        place = Place(sizes)
        greet(
            [place.core, place.side_y]
            + [place.plane_peer(d)[1] for d in range(1, place.plane)]
        )
        carried = Moves(place, move_specs, sources, targets, stages, send, recv, local)
        carried.start()
        carried.issue(2)
        mine = pl.ds(pl.multiple_of(place.t * rows, 16), rows)
        a, b = hid[mine, :].astype(f32), emb[mine, :].astype(f32)
        squares = jnp.sum(a * a, axis=1, keepdims=True) + jnp.sum(b * b, axis=1, keepdims=True)
        inverse = lax.rsqrt(squares / (2 * half) + epsilon)
        low[:, :half] = (a * inverse * gain_ref[:, :half]).astype(bf16)
        low[:, half : 2 * half] = (b * inverse * gain_ref[:, half:]).astype(bf16)
        low[:, 2 * half : 2 * half + mids] = lax.dot_general(
            low[:, : 2 * half], down_ref[...], NN, preferred_element_type=f32
        ).astype(bf16)
        slot = lax.broadcasted_iota(jnp.int32, (rows, 128), 0)
        slot = slot + (place.c * tp + place.t) * rows
        lane = lax.broadcasted_iota(jnp.int32, (rows, 128), 1)
        segment, position, end = jnp.zeros_like(slot), slot, 0
        for i in range(lengths.shape[1]):
            length = lens[0, i]
            end = end + length
            passed = (slot >= end).astype(jnp.int32)
            segment = segment + passed
            position = position - passed * length
        marks = jnp.where(lane == 0, segment, position)
        low[:, 2 * half + mids :] = marks.astype(f32).astype(bf16)
        gather = Gather(place, low, o, out_pieces, gs)
        gather.begin()
        for step in gather.steps():
            carried.issue(4)
            step()
        carried.issue(len(carried.queue))
        carried.settle()
        gather.end()
        carried.finish()

    S = jax.ShapeDtypeStruct
    results = pl.pallas_call(
        kernel,
        out_shape=[S((groups, ctx, tp // 2, 2, rows, width), bf16)] + move_outs,
        in_specs=[IN_VMEM, IN_VMEM, IN_SMEM, IN_VMEM, IN_VMEM] + [IN_HBM] * n_moves,
        out_specs=[IN_VMEM] + [IN_HBM] * n_moves,
        scratch_shapes=[pltpu.VMEM((rows, width), bf16)]
        + gather_sems(len(out_pieces), groups)
        + move_scratch,
        name=f"opening_{number}",
        compiler_params=pltpu.CompilerParams(
            collective_id=number, has_side_effects=True, vmem_limit_bytes=62 * 2**20
        ),
    )(hidden, embeds, lengths, gain.reshape(1, -1), down_all, *[array for array, _, _ in moves])
    return [results[0].reshape(-1, width)] + list(results[1:])


def sum_small(sizes, number, values):
    def kernel(x, o, *scratch):
        place = Place(sizes)
        greet([place.core, place.side_y, place.side_x] + place.line)
        summing = SmallSum(place, x, o, *scratch)
        summing.begin()
        for step in summing.steps():
            step()
        summing.end()

    return pl.pallas_call(
        kernel,
        out_shape=jax.ShapeDtypeStruct(values.shape, jnp.float32),
        in_specs=[IN_VMEM],
        out_specs=IN_VMEM,
        scratch_shapes=small_scratch(values.shape, sizes[0]),
        name=f"sum_small_{number}",
        compiler_params=pltpu.CompilerParams(collective_id=number, has_side_effects=True),
    )(values)


def finish_forward(place, acc, args, outs, low, low_tail, low_small):
    rest, gain = args
    outs[0][...] = rest[...] + acc[...]
    low[...] = rms_rows(outs[0][...], gain[...]).astype(jnp.bfloat16)


def finish_mixer_back(place, acc, args, outs, low, low_tail, low_small):
    after_mlp, gain, cot, state_map = args
    width = after_mlp.shape[1]
    low[:, width:] = acc[:, width:].astype(jnp.bfloat16)
    d_normed = acc[:, :width] + lax.dot_general(
        low[:, width:], state_map[...], NT, preferred_element_type=jnp.float32
    )
    d_rows, d_gain = rms_back(after_mlp[...], gain[...], d_normed)
    outs[1][...] = d_gain
    d_rows = cot[...].astype(jnp.float32) + d_rows
    outs[0][...] = d_rows
    low[:, :width] = d_rows.astype(jnp.bfloat16)


def finish_mlp_back(place, acc, args, outs, low, low_tail, low_small):
    after_attn, gain, d_after_mlp = args
    d_rows, d_gain = rms_back(after_attn[...], gain[...], acc[...])
    outs[1][...] = d_gain
    d_rows = d_after_mlp[...] + d_rows
    outs[0][...] = d_rows
    low[...] = d_rows.astype(jnp.bfloat16)


def finish_attention_back(place, acc, args, outs, low, low_tail, low_small):
    hidden, embeds, gain, d_after_attn, down_all, out_mine, row = args
    half = hidden.shape[1]
    bf16, f32 = jnp.bfloat16, jnp.float32
    low[...] = acc[:, 2 * half :].astype(bf16)
    inputs = (hidden, embeds)
    squares = sum(jnp.sum(part[...] * part[...], axis=1, keepdims=True) for part in inputs)
    inverse = lax.rsqrt(squares / (2 * half) + epsilon)
    along = jnp.zeros_like(squares)
    for i, part in enumerate(inputs):
        cols = slice(i * half, (i + 1) * half)
        grad = acc[:, cols] + lax.dot_general(
            low[...], down_all[cols, :], NT, preferred_element_type=f32
        )
        acc[:, cols] = grad
        along = along + jnp.sum(grad * gain[:, cols] * part[...], axis=1, keepdims=True)
    along = along / (2 * half)
    low_tail[:, :half] = out_mine[...]
    low_small[:, 2 * half :] = row[...]
    for i, part in enumerate(inputs):
        cols = slice(i * half, (i + 1) * half)
        grad = acc[:, cols]
        low_small[:, cols] = jnp.sum(grad * part[...] * inverse, axis=0, keepdims=True)
        d_rows = grad * gain[:, cols] * inverse - part[...] * inverse**3 * along
        if i == 0:
            d_rows = d_rows + d_after_attn[...]
        low_tail[:, (i + 1) * half : (i + 2) * half] = d_rows.astype(bf16)


def finish_out(acc, args, out):
    out[...] = (args[0][...] + acc[...]).astype(out.dtype)


def adapter_products(xa, dmid, width):
    block, rank = 512, dmid.shape[1] // 3

    def kernel(a, b, o):
        both = lax.dot_general(
            a[...], b[...], (((0,), (0,)), ((), ())), preferred_element_type=jnp.float32
        )
        for j in range(3):
            o[j] = both[:, j * rank : (j + 1) * rank]

    return pl.pallas_call(
        kernel,
        out_shape=jax.ShapeDtypeStruct((3, width, rank), jnp.float32),
        grid=(width // block,),
        in_specs=[
            pl.BlockSpec((xa.shape[0], block), lambda i: (0, i)),
            pl.BlockSpec(dmid.shape, lambda i: (0, 0)),
        ],
        out_specs=pl.BlockSpec((3, block, rank), lambda i: (0, i, 0)),
        name="adapter_products",
    )(xa, dmid)


def unpack(packed, parts):
    flat, at, found = packed.reshape(-1), 0, []
    for part in parts:
        found.append(flat[at : at + part.size].reshape(part.shape))
        at += part.size
    return found


def shift_conv(values, kernel, bias, position):
    total = values * kernel[0][None, :] + bias[None, :]
    for lag in range(1, kernel.shape[0]):
        shifted = jnp.pad(values, ((lag, 0), (0, 0)))[: values.shape[0]]
        keep = (position >= lag).astype(values.dtype)[:, None]
        total = total + shifted * keep * kernel[lag][None, :]
    return jax.nn.silu(total)


def attend_groups(queries, keys_all, vals_all, segment, position):
    def rot(values):
        half_dim = values.shape[-1] // 2
        inverse = 10000.0 ** (-jnp.arange(half_dim, dtype=jnp.float32) / half_dim)
        angle = position.astype(jnp.float32)[..., None] * inverse
        cosine, sine = jnp.cos(angle), jnp.sin(angle)
        a, b = values[..., :half_dim], values[..., half_dim:]
        return jnp.concatenate([a * cosine - b * sine, b * cosine + a * sine], axis=-1).astype(
            jnp.bfloat16
        )

    rows = queries.shape[1]
    order = jnp.arange(rows)
    scores = jnp.einsum(
        "gqd,gkd->gqk", rot(queries), rot(keys_all), preferred_element_type=jnp.float32
    ) * AHD ** (-0.5)
    allowed = (segment[:, :, None] == segment[:, None, :]) & (order[:, None] >= order[None, :])
    weights = jnp.exp(jnp.where(allowed, scores, -1e30))
    low = (weights / jnp.sum(weights, axis=-1, keepdims=True)).astype(jnp.bfloat16)
    return jnp.einsum(
        "gqk,gkd->gqd", low, vals_all.astype(jnp.bfloat16), preferred_element_type=jnp.float32
    )


def mixer_groups(
    inner_in, step_in, bc_post, bias_in, decay_in, skip_in, kernel_in, conv_bias_in, position, segment
):
    groups, rows = segment.shape
    heads = step_in.shape[1]
    xc = shift_conv(inner_in, kernel_in, conv_bias_in, position.reshape(-1))
    xc = xc.reshape(groups, rows, heads, MIXER_HEAD_SIZE)
    step = jax.nn.softplus(step_in + bias_in[None, :]).reshape(groups, rows, heads)
    log_decay = step * -jnp.exp(decay_in)
    order = jnp.arange(rows)
    same = (segment[:, :, None] == segment[:, None, :]) & (order[:, None] >= order[None, :])
    running = jnp.einsum("gts,gsh->gth", same.astype(jnp.float32), log_decay, precision=highest)
    gap = running.transpose(0, 2, 1)
    gap = gap[:, :, :, None] - gap[:, :, None, :]
    decay = jnp.where(same[:, None], jnp.exp(jnp.where(same[:, None], gap, 0.0)), 0.0)
    b_mat = bc_post[:, :STATE].reshape(groups, rows, STATE)
    c_mat = bc_post[:, STATE:].reshape(groups, rows, STATE)
    meet = jnp.einsum("gtn,gsn->gts", c_mat, b_mat, precision=lax.Precision.HIGH)
    out = jnp.einsum(
        "ghts,gshp->gthp",
        decay * meet[:, None],
        xc * step[..., None],
        precision=lax.Precision.HIGH,
    )
    out = out + skip_in[:, None] * xc
    return out.reshape(groups * rows, heads * MIXER_HEAD_SIZE)


def per_device_split(
    hidden,
    embeds,
    cotangent,
    lengths,
    attention_norm_gain,
    adapter_down_maps,
    query_key_value_weight,
    adapter_up_maps,
    attention_output_weight,
    feedforward_norm_gain,
    gate_up_weight,
    down_weight,
    mixer_norm_gain,
    mixer_gate_input_weight,
    state_map_weight,
    step_size_weight,
    mixer_input_taps,
    mixer_input_tap_bias,
    state_map_taps,
    state_map_tap_bias,
    step_size_bias,
    log_decay_rate,
    head_skip_weight,
    gated_norm_gain,
    mixer_output_weight,
):
    bf16, f32 = jnp.bfloat16, jnp.float32
    tp_size, ctx_size, groups = (lax.axis_size(name) for name in ("tp", "ctx", "fsdp"))
    tp_index, ctx_index = lax.axis_index("tp"), lax.axis_index("ctx")
    plane_index = lax.axis_index("fsdp") * ctx_size + ctx_index
    plane_size = groups * ctx_size
    tok_rows = hidden.shape[0]
    mine = tok_rows // tp_size
    group_rows = tok_rows * ctx_size
    start = tp_index * mine

    sizes = (groups, ctx_size, tp_size)

    def own_rows(values):
        return lax.dynamic_slice_in_dim(values, start, mine, 0)

    def own_part(values, axis=0):
        width = values.shape[axis] // plane_size
        return lax.dynamic_slice_in_dim(values, plane_index * width, width, axis)

    width = hidden.shape[1]
    hidden_f = own_rows(hidden).astype(f32)
    embeds_f = own_rows(embeds).astype(f32)
    cot_low = own_rows(cotangent)

    up_maps = own_part(adapter_up_maps, 2)
    w_step = own_part(step_size_weight, 1)
    taps, tap_bias = own_part(mixer_input_taps, 1), own_part(mixer_input_tap_bias)
    step_bias, decay_rate = own_part(step_size_bias), own_part(log_decay_rate)
    skip, gate_gain = own_part(head_skip_weight), own_part(gated_norm_gain)

    rank = adapter_down_maps.shape[2]
    width_a = adapter_down_maps.shape[1]
    down_all = jnp.concatenate([adapter_down_maps[j] for j in range(3)], axis=1)
    xa_wide, w_qkv, w_o = opening(
        sizes,
        1,
        hidden,
        embeds,
        lengths,
        attention_norm_gain,
        down_all,
        [(query_key_value_weight, 2, 1), (attention_output_weight, 0, 1)],
    )
    xa = xa_wide[:, :width_a]
    mid = xa_wide[:, width_a : width_a + 3 * rank]
    segment = xa_wide[:, width_a + 3 * rank].astype(jnp.int32).reshape(groups, group_rows)
    position = xa_wide[:, width_a + 3 * rank + 1].astype(jnp.int32).reshape(groups, group_rows)
    position_flat = position.reshape(-1)
    proj = [
        (
            matrix_product(xa, w_qkv[j])
            + matrix_product(mid[:, j * rank : (j + 1) * rank], up_maps[j])
        ).astype(bf16)
        for j in range(3)
    ]
    ao, attend_back = jax.vjp(
        lambda q, k, v: attend_groups(q, k, v, segment, position),
        *[piece.astype(f32).reshape(groups, group_rows, AHD) for piece in proj],
    )
    ao_low = ao.astype(bf16).reshape(groups * group_rows, AHD)

    gain_m = feedforward_norm_gain.reshape(1, -1)
    found = exchange(
        sizes,
        2,
        Summed(sizes, [(ao_low, w_o, None, False)]),
        finish_forward,
        [hidden_f, gain_m],
        [hidden_f.shape],
        width,
        [(gate_up_weight, 2, 1), (down_weight, 0, 1)],
    )
    xm, (after_attn,), (w_gu, w_down) = found["gathered"], found["finish"], found["moves"]
    gate_pre, up_pre = matrix_product(xm, w_gu[0]), matrix_product(xm, w_gu[1])
    activated, act_back = jax.vjp(gated_gelu, gate_pre, up_pre)
    hid_low = activated.astype(bf16)

    gain_n = mixer_norm_gain.reshape(1, -1)
    found = exchange(
        sizes,
        3,
        Summed(sizes, [(hid_low, w_down, None, False)]),
        finish_forward,
        [after_attn, gain_n],
        [hidden_f.shape],
        width,
        [(mixer_gate_input_weight, 2, 1), (mixer_output_weight, 0, 1)],
        also_gather=cot_low,
    )
    xn, cot, (after_mlp,) = found["gathered"], found["also"], found["finish"]
    w_zx, w_out = found["moves"]
    gate_z = matrix_product(xn, w_zx[0])
    inner_x = matrix_product(xn, w_zx[1]).astype(bf16)
    step_raw = matrix_product(xn, w_step).astype(bf16)
    bc_low = matrix_product(xn, state_map_weight).astype(bf16)
    bc_post, bc_conv_back = jax.vjp(
        lambda v, k, b: shift_conv(v, k, b, position_flat),
        bc_low.astype(f32),
        state_map_taps,
        state_map_tap_bias,
    )
    scan_out, scan_back = jax.vjp(
        lambda *parts: mixer_groups(*parts, position, segment),
        inner_x.astype(f32),
        step_raw.astype(f32),
        bc_post,
        step_bias,
        decay_rate,
        skip,
        taps,
        tap_bias,
    )
    y = scan_out.astype(bf16).astype(f32)
    silu_z = jax.nn.silu(gate_z)
    gated = y * silu_z
    d_yn = matrix_product_transposed(cot, w_out)
    gain_part = d_yn * gate_gain
    sums = jnp.stack([jnp.sum(gated * gated, axis=1), jnp.sum(gain_part * gated, axis=1)])
    sums = sum_small(sizes, 4, sums.reshape(-1, 128)).reshape(2, -1)
    inverse = lax.rsqrt(sums[0] / INNER + epsilon)[:, None]
    cross = (sums[1] / INNER)[:, None]
    yn_low = (gated * inverse * gate_gain).astype(bf16)

    grad_w_out = outer_product_sum(yn_low, cot)
    grad_g_gate = jnp.sum(d_yn * gated * inverse, axis=0)
    d_gated = gain_part * inverse - gated * inverse**3 * cross
    d_y = (d_gated * silu_z).astype(bf16)
    sigmoid_z = jax.nn.sigmoid(gate_z)
    d_z = (d_gated * y * sigmoid_z * (1.0 + gate_z * (1.0 - sigmoid_z))).astype(bf16)
    (
        d_xs,
        d_step,
        d_bc_post,
        grad_dt_bias,
        grad_a_log,
        grad_d_skip,
        grad_conv_x,
        grad_conv_x_bias,
    ) = scan_back(d_y.astype(f32))
    d_xs, d_step = d_xs.astype(bf16), d_step.astype(bf16)
    d_bc_part, grad_conv_bc, grad_conv_bc_bias = bc_conv_back(d_bc_post)
    grad_w_zx = jnp.stack(
        [outer_product_sum(xn, d_z).astype(bf16), outer_product_sum(xn, d_xs).astype(bf16)]
    )
    grad_w_dt = outer_product_sum(xn, d_step)
    lanes = ((0, 0), (0, 128 - d_step.shape[1]))
    found = exchange(
        sizes,
        5,
        Summed(
            sizes,
            [
                (d_z, w_zx, 0, True),
                (d_xs, w_zx, 1, True),
                (jnp.pad(d_step, lanes), jnp.pad(w_step, lanes), None, True),
            ],
            d_bc_part.astype(bf16),
        ),
        finish_mixer_back,
        [after_mlp, gain_n, cot_low, state_map_weight],
        [hidden_f.shape, gain_n.shape],
        width + d_bc_part.shape[1],
        [(grad_w_zx, 1, 2), (grad_w_out.astype(bf16), 1, 0)],
        also_sum=(
            Summed(sizes, [(yn_low, w_out, None, False)]),
            finish_out,
            [after_mlp],
            jax.ShapeDtypeStruct(hidden_f.shape, bf16),
        ),
    )
    gathered, (d_after_mlp, grad_g_mamba) = found["gathered"], found["finish"]
    out_mine, (grad_w_zx, grad_w_out) = found["second"], found["moves"]

    d_mlp, d_bc = gathered[:, :width], gathered[:, width:]
    grad_w_bc = outer_product_sum(xn, d_bc)
    grad_w_down = outer_product_sum(hid_low, d_mlp)
    d_gate, d_up = act_back(matrix_product_transposed(d_mlp, w_down))
    d_gate, d_up = d_gate.astype(bf16), d_up.astype(bf16)
    grad_w_gu = jnp.stack(
        [outer_product_sum(xm, d_gate).astype(bf16), outer_product_sum(xm, d_up).astype(bf16)]
    )

    found = exchange(
        sizes,
        6,
        Summed(sizes, [(d_gate, w_gu, 0, True), (d_up, w_gu, 1, True)]),
        finish_mlp_back,
        [after_attn, gain_m, d_after_mlp],
        [hidden_f.shape, gain_m.shape],
        width,
        [(grad_w_gu, 1, 2), (grad_w_down.astype(bf16), 1, 0)],
    )
    d_attn, (d_after_attn, grad_g_mlp) = found["gathered"], found["finish"]
    grad_w_gu, grad_w_down = found["moves"]
    grad_w_o = outer_product_sum(ao_low, d_attn)
    d_ao = matrix_product_transposed(d_attn, w_o).astype(bf16)
    d_proj = [
        piece.reshape(groups * group_rows, AHD).astype(bf16)
        for piece in attend_back(d_ao.astype(f32).reshape(groups, group_rows, AHD))
    ]
    dmid_part = jnp.concatenate(
        [matrix_product_transposed(d_proj[j], up_maps[j]).astype(bf16) for j in range(3)], axis=1
    )
    grad_w_qkv = jnp.stack([outer_product_sum(xa, d_proj[j]).astype(bf16) for j in range(3)])
    adapter_up_gradient = jnp.stack(
        [outer_product_sum(mid[:, j * rank : (j + 1) * rank], d_proj[j]) for j in range(3)]
    )
    shares = [
        jnp.pad(part, (0, 128 - part.shape[0]))[None]
        for part in (grad_dt_bias, grad_a_log, grad_d_skip)
    ]
    shares = jnp.concatenate(
        [grad_conv_x, grad_conv_x_bias[None], grad_g_gate[None]] + shares
        + [jnp.zeros((7, 128), f32), jnp.pad(grad_w_dt.T.reshape(-1, 128), ((0, 0), (0, 0)))]
    ).astype(bf16)
    sums = [grad_g_mlp[0], grad_g_mamba[0], grad_conv_bc, grad_conv_bc_bias]
    row = jnp.concatenate([part.reshape(-1) for part in sums])[None]
    found = exchange(
        sizes,
        7,
        Summed(sizes, [(d_proj[j], w_qkv, j, True) for j in range(3)], dmid_part),
        finish_attention_back,
        [
            hidden_f,
            embeds_f,
            attention_norm_gain.reshape(1, -1),
            d_after_attn,
            down_all,
            out_mine,
            row,
        ],
        [],
        3 * rank,
        [
            (grad_w_qkv, 1, 2),
            (grad_w_o.astype(bf16), 1, 0),
            (adapter_up_gradient.astype(bf16), None, 2),
            (shares, None, 1),
        ],
        early_share=100,
        tail=3 * width,
        small=width_a + row.shape[1],
    )
    dmid, back, row = found["gathered"], found["tail"], found["small"][0]
    grad_w_qkv, grad_w_o, adapter_up_gradient, shared = found["moves"]
    adapter_down_gradient = adapter_products(xa_wide, dmid, width_a)
    result = back[:, :width]
    d_hidden = back[:, width : 2 * width].astype(f32)
    d_embeds = back[:, 2 * width :].astype(f32)
    adapter_up_gradient = adapter_up_gradient.astype(f32)
    shared = shared.astype(f32)
    grad_conv_x, grad_conv_x_bias, grad_g_gate = shared[:4], shared[4], shared[5]
    few = step_bias.shape[0]
    grad_dt_bias, grad_a_log, grad_d_skip = [
        shared[i].reshape(plane_size, 128)[:, :few].reshape(-1) for i in (6, 7, 8)
    ]
    grad_w_dt = shared[16:].reshape(few, -1, plane_size, 128).transpose(1, 3, 2, 0)
    grad_w_dt = grad_w_dt.reshape(-1, plane_size * few)
    grad_g_attn = row[:width_a]
    grad_g_mlp, grad_g_mamba, grad_conv_bc, grad_conv_bc_bias = unpack(row[width_a:], sums)

    return (
        result,
        d_hidden,
        d_embeds,
        grad_g_attn,
        adapter_down_gradient,
        grad_w_qkv.astype(f32),
        adapter_up_gradient,
        grad_w_o.astype(f32),
        grad_g_mlp,
        grad_w_gu.astype(f32),
        grad_w_down.astype(f32),
        grad_g_mamba,
        grad_w_zx.astype(f32),
        grad_w_bc,
        grad_w_dt,
        grad_conv_x,
        grad_conv_x_bias,
        grad_conv_bc,
        grad_conv_bc_bias,
        grad_dt_bias,
        grad_a_log,
        grad_d_skip,
        grad_g_gate,
        grad_w_out.astype(f32),
    )


def solution(mesh):
    placed = (
        P(("fsdp", "ctx"), None),
        P(("fsdp", "ctx"), None),
        P(("fsdp", "ctx"), None),
        P("fsdp", None),
        P(),
        P(),
        P(None, ("fsdp", "ctx"), "tp"),
        P(None, None, "tp"),
        P("tp", ("fsdp", "ctx")),
        P(),
        P(None, ("fsdp", "ctx"), "tp"),
        P("tp", ("fsdp", "ctx")),
        P(),
        P(None, ("fsdp", "ctx"), "tp"),
        P(),
        P(None, "tp"),
        P(None, "tp"),
        P("tp"),
        P(),
        P(),
        P("tp"),
        P("tp"),
        P("tp"),
        P("tp"),
        P("tp", ("fsdp", "ctx")),
    )
    devices = mesh.shape["fsdp"] * mesh.shape["ctx"] * mesh.shape["tp"]
    one_head_each = devices == AHEADS and mesh.shape["ctx"] == 2 and mesh.shape["tp"] == 4
    return jax.shard_map(
        per_device_split if one_head_each else per_device,
        mesh=mesh,
        in_specs=placed,
        out_specs=(
            P(("fsdp", "ctx"), None),
            P(("fsdp", "ctx"), None),
            P(("fsdp", "ctx"), None),
            P(),
            P(),
            P(None, ("fsdp", "ctx"), "tp"),
            P(None, None, "tp"),
            P("tp", ("fsdp", "ctx")),
            P(),
            P(None, ("fsdp", "ctx"), "tp"),
            P("tp", ("fsdp", "ctx")),
            P(),
            P(None, ("fsdp", "ctx"), "tp"),
            P(),
            P(None, "tp"),
            P(None, "tp"),
            P("tp"),
            P(),
            P(),
            P("tp"),
            P("tp"),
            P("tp"),
            P("tp"),
            P("tp", ("fsdp", "ctx")),
        ),
        check_vma=False,
    )
```

```python
import functools

import jax
import jax.numpy as jnp
from jax import lax
from jax.experimental import pallas as pl
from jax.experimental.pallas import tpu as pltpu
from jax.sharding import PartitionSpec as P

MODEL_WIDTH = 2048
AHEADS = 32
AHD = 128
INNER = 4096
MIXER_HEAD_SIZE = 64
STATE = 128
SPAN = 128


highest = lax.Precision.HIGHEST
epsilon = 1e-05


def matrix_product(left, right):
    return jnp.dot(left, right, preferred_element_type=jnp.float32)


def matrix_product_transposed(left, right):
    return lax.dot_general(
        left, right, (((1,), (1,)), ((), ())), preferred_element_type=jnp.float32
    )


def outer_product_sum(left, right):
    return lax.dot_general(
        left, right, (((0,), (0,)), ((), ())), preferred_element_type=jnp.float32
    )


def rms_scale(values, gain):
    return values * lax.rsqrt(jnp.mean(values * values, axis=-1, keepdims=True) + epsilon) * gain


def gated_gelu(gate_in, up_in):
    return jax.nn.gelu(gate_in, approximate=True) * up_in


def layout(lengths_row, total_rows):
    ends = jnp.cumsum(lengths_row)
    slot_index = jnp.arange(total_rows, dtype=jnp.int32)
    passed = (slot_index[:, None] >= ends[None, :]).astype(jnp.int32)
    segment = jnp.sum(passed, axis=1)
    position = slot_index - jnp.sum(passed * lengths_row[None, :], axis=1)
    return (segment, position, slot_index)


def causal_conv(values, kernel, bias, position):
    total_rows = values.shape[0]
    total = values * kernel[0][None, :] + bias[None, :]
    for lag in range(1, kernel.shape[0]):
        shifted = jnp.concatenate(
            [jnp.zeros((lag, values.shape[1]), values.dtype), values[: total_rows - lag]], axis=0
        )
        keep = (position >= lag).astype(values.dtype)[:, None]
        total = total + shifted * keep * kernel[lag][None, :]
    return jax.nn.silu(total)


def rotate(values, position):
    half_dim = values.shape[-1] // 2
    inverse = 10000.0 ** (-jnp.arange(half_dim, dtype=jnp.float32) / half_dim)
    angle = position.astype(jnp.float32)[:, None] * inverse[None, :]
    cosine = jnp.cos(angle)[:, None, :]
    sine_part = jnp.sin(angle)[:, None, :]
    first_half = values[..., :half_dim]
    second_half = values[..., half_dim:]
    return jnp.concatenate(
        [
            first_half * cosine - second_half * sine_part,
            second_half * cosine + first_half * sine_part,
        ],
        axis=-1,
    )


def attend_core(pair_data, values, segment, slot_index, position, block_rows):
    group_row_block = values.shape[0]
    count_of_heads = values.shape[1] // AHD
    paired = pair_data.reshape(group_row_block, count_of_heads, 2, AHD)
    queries = rotate(paired[:, :, 0], position).astype(jnp.bfloat16)
    keys_all = rotate(paired[:, :, 1], position).astype(jnp.bfloat16)
    vals_all = values.reshape(group_row_block, count_of_heads, AHD).astype(jnp.bfloat16)
    scaling = AHD ** (-0.5)
    block_count = group_row_block // block_rows

    def one_block(inputs):
        query_part, query_seg, query_slot = inputs
        scores = (
            jnp.einsum("qhd,khd->hqk", query_part, keys_all, preferred_element_type=jnp.float32)
            * scaling
        )
        allowed = (query_seg[:, None] == segment[None, :]) & (
            query_slot[:, None] >= slot_index[None, :]
        )
        scores = jnp.where(allowed[None], scores, -1e30)
        weights = jnp.exp(scores)
        weights_low = (weights / jnp.sum(weights, axis=-1, keepdims=True)).astype(jnp.bfloat16)
        return jnp.einsum("hqk,khd->qhd", weights_low, vals_all, preferred_element_type=jnp.float32)

    mapped = lax.map(
        jax.checkpoint(one_block),
        (
            queries.reshape(block_count, block_rows, count_of_heads, AHD),
            segment.reshape(block_count, block_rows),
            slot_index.reshape(block_count, block_rows),
        ),
    )
    return mapped.reshape(group_row_block, count_of_heads * AHD)


def state_scan(inputs_x, step_size, b_mat, c_mat, decay_rate, segment):
    total_rows, count_of_heads, head_dim = inputs_x.shape
    spans = total_rows // SPAN
    log_decay = step_size * decay_rate[None, :]
    weighted = inputs_x * step_size[:, :, None]
    causal = jnp.arange(SPAN)[:, None] >= jnp.arange(SPAN)[None, :]

    def advance(carried_in, inputs):
        memory, last_segment = carried_in
        decay_part, weighted_part, b_part, c_part, seg_part = inputs
        running = jnp.cumsum(decay_part, axis=0)
        same_seq = (seg_part[:, None] == seg_part[None, :]) & causal
        intersection = jnp.dot(c_part, b_part.T, precision=highest)
        log_gap = jnp.where(same_seq[:, :, None], running[:, None, :] - running[None, :, :], 0.0)
        mixing = jnp.where(same_seq[:, :, None], jnp.exp(log_gap), 0.0) * intersection[:, :, None]
        output = jnp.einsum("tsh,shp->thp", mixing, weighted_part, precision=highest)
        carried = (seg_part == last_segment).astype(jnp.float32)
        reach_back = jnp.exp(running) * carried[:, None]
        output = (
            output
            + jnp.einsum("tn,hpn->thp", c_part, memory, precision=highest) * reach_back[:, :, None]
        )
        tail_seg = seg_part[-1]
        toward = (
            jnp.exp(running[-1][None, :] - running)
            * (seg_part == tail_seg).astype(jnp.float32)[:, None]
        )
        next_state = jnp.einsum("sh,shp,sn->hpn", toward, weighted_part, b_part, precision=highest)
        keep_all = jnp.exp(running[-1]) * (tail_seg == last_segment).astype(jnp.float32)
        next_state = next_state + memory * keep_all[:, None, None]
        return ((next_state, tail_seg), output)

    initial = (jnp.zeros((count_of_heads, head_dim, b_mat.shape[1]), jnp.float32), jnp.int32(-1))
    pieces = (
        log_decay.reshape(spans, SPAN, count_of_heads),
        weighted.reshape(spans, SPAN, count_of_heads, head_dim),
        b_mat.reshape(spans, SPAN, -1),
        c_mat.reshape(spans, SPAN, -1),
        segment.reshape(spans, SPAN),
    )
    last_state, outputs = lax.scan(jax.checkpoint(advance), initial, pieces)
    return outputs.reshape(total_rows, count_of_heads, head_dim)


def mamba_core(
    inner_in,
    step_in,
    bc_post,
    bias_in,
    decay_in,
    skip_weight_input,
    kernel_in,
    conv_bias_in,
    position,
    segment,
):
    group_row_block = inner_in.shape[0]
    count_of_heads = step_in.shape[1]
    mixer_result = causal_conv(inner_in, kernel_in, conv_bias_in, position)
    reshaped_tensor = mixer_result.reshape(group_row_block, count_of_heads, MIXER_HEAD_SIZE)
    step_size = jax.nn.softplus(step_in + bias_in[None, :])
    scan_result = state_scan(
        reshaped_tensor,
        step_size,
        bc_post[:, :STATE],
        bc_post[:, STATE:],
        -jnp.exp(decay_in),
        segment,
    )
    return (scan_result + skip_weight_input[None, :, None] * reshaped_tensor).reshape(
        group_row_block, count_of_heads * MIXER_HEAD_SIZE
    )


def collect(first_part, second_part):
    return (
        lax.all_gather(first_part, ("fsdp", "ctx"), axis=1, tiled=True),
        lax.all_gather(second_part, ("fsdp", "ctx"), axis=1, tiled=True),
    )


def collect_again(first_part, second_part):
    return (
        lax.all_gather(first_part, ("fsdp", "ctx"), axis=1, tiled=True),
        lax.all_gather(second_part, ("fsdp", "ctx"), axis=1, tiled=True),
    )


def tensor_sum(partial_sum):
    return lax.psum(partial_sum, "tp")


def tensor_pair(first_part, second_part):
    return (
        lax.psum(first_part.astype(jnp.bfloat16), "tp").astype(jnp.float32),
        lax.psum(second_part.astype(jnp.bfloat16), "tp").astype(jnp.float32),
    )


def heads_pair(first_part, second_part):
    return (
        lax.all_to_all(first_part, "ctx", split_axis=1, concat_axis=0, tiled=True),
        lax.all_to_all(second_part, "ctx", split_axis=1, concat_axis=0, tiled=True),
    )


def heads_one(values):
    return lax.all_to_all(values, "ctx", split_axis=1, concat_axis=0, tiled=True)


def tokens_pair(first_part, second_part):
    return (
        lax.all_to_all(first_part, "ctx", split_axis=0, concat_axis=1, tiled=True),
        lax.all_to_all(second_part, "ctx", split_axis=0, concat_axis=1, tiled=True),
    )


def tokens_one(values):
    return lax.all_to_all(values, "ctx", split_axis=0, concat_axis=1, tiled=True)


def per_device(
    hidden,
    embeds,
    cotangent,
    lengths,
    attention_norm_gain,
    adapter_down_maps,
    query_key_value_weight,
    adapter_up_maps,
    attention_output_weight,
    feedforward_norm_gain,
    gate_up_weight,
    down_weight,
    mixer_norm_gain,
    mixer_gate_input_weight,
    state_map_weight,
    step_size_weight,
    mixer_input_taps,
    mixer_input_tap_bias,
    state_map_taps,
    state_map_tap_bias,
    step_size_bias,
    log_decay_rate,
    head_skip_weight,
    gated_norm_gain,
    mixer_output_weight,
):
    tok_rows = hidden.shape[0]
    ctx_size = lax.axis_size("ctx")
    ctx_index = lax.axis_index("ctx")
    group_row_block = tok_rows * ctx_size
    block_rows = group_row_block // max(1, group_row_block // 1024)
    segment, position, slot_index = layout(lengths[0], group_row_block)
    hidden_f = hidden.astype(jnp.float32)
    embeds_f = embeds.astype(jnp.float32)
    attention_block_full, attn_out = collect(query_key_value_weight, attention_output_weight)
    joined = jnp.concatenate([hidden_f, embeds_f], axis=1)
    normed_a, norm_a_back = jax.vjp(rms_scale, joined, attention_norm_gain)
    attention_input_reduced = normed_a.astype(jnp.bfloat16)
    middle_reduced_precision = [
        matrix_product(attention_input_reduced, adapter_down_maps[group_member]).astype(
            jnp.bfloat16
        )
        for group_member in range(3)
    ]
    projected_input = [
        (
            matrix_product(attention_input_reduced, attention_block_full[group_member])
            + matrix_product(middle_reduced_precision[group_member], adapter_up_maps[group_member])
        ).astype(jnp.bfloat16)
        for group_member in range(3)
    ]
    tp_heads = projected_input[0].shape[1] // AHD
    pair_data = jnp.stack(
        [
            projected_input[0].reshape(tok_rows, tp_heads, AHD),
            projected_input[1].reshape(tok_rows, tp_heads, AHD),
        ],
        axis=2,
    ).reshape(tok_rows, tp_heads * 2 * AHD)
    pair_heads, value_heads = heads_pair(pair_data, projected_input[2])
    attn_core, attn_pull = jax.vjp(
        lambda pairs_in, values_in: attend_core(
            pairs_in, values_in, segment, slot_index, position, block_rows
        ),
        pair_heads.astype(jnp.float32),
        value_heads.astype(jnp.float32),
    )
    attn_tokens = tokens_one(attn_core.astype(jnp.bfloat16))
    after_attn = hidden_f + tensor_sum(matrix_product(attn_tokens, attn_out))
    mlp_big, mlp_down = collect(gate_up_weight, down_weight)
    normed_m, norm_m_back = jax.vjp(rms_scale, after_attn, feedforward_norm_gain)
    xm_low = normed_m.astype(jnp.bfloat16)
    gate_pre = matrix_product(xm_low, mlp_big[0])
    up_pre = matrix_product(xm_low, mlp_big[1])
    activated, act_back = jax.vjp(gated_gelu, gate_pre, up_pre)
    hid_low = activated.astype(jnp.bfloat16)
    after_mlp = after_attn + tensor_sum(matrix_product(hid_low, mlp_down))
    mamba_big, mamba_out = collect(mixer_gate_input_weight, mixer_output_weight)
    normed_n, norm_n_back = jax.vjp(rms_scale, after_mlp, mixer_norm_gain)
    xn_low = normed_n.astype(jnp.bfloat16)
    gate_z = matrix_product(xn_low, mamba_big[0])
    inner_x = matrix_product(xn_low, mamba_big[1]).astype(jnp.bfloat16)
    step_raw = matrix_product(xn_low, step_size_weight).astype(jnp.bfloat16)
    bc_low = matrix_product(xn_low, state_map_weight).astype(jnp.bfloat16)
    x_heads, step_heads = heads_pair(inner_x, step_raw)
    bc_group = lax.all_gather(bc_low, "ctx", axis=0, tiled=True)
    bc_post, bc_conv_pull = jax.vjp(
        lambda values_in, kernel_in, conv_bias_in: causal_conv(
            values_in, kernel_in, conv_bias_in, position
        ),
        bc_group.astype(jnp.float32),
        state_map_taps,
        state_map_tap_bias,
    )
    heads_on_device_share = step_heads.shape[1]
    start_offset = ctx_index * heads_on_device_share
    channel_count_here = heads_on_device_share * MIXER_HEAD_SIZE
    channel_offset_begin = start_offset * MIXER_HEAD_SIZE
    bias_local = lax.dynamic_slice_in_dim(step_size_bias, start_offset, heads_on_device_share)
    decay_local = lax.dynamic_slice_in_dim(log_decay_rate, start_offset, heads_on_device_share)
    skip_local = lax.dynamic_slice_in_dim(head_skip_weight, start_offset, heads_on_device_share)
    kernel_local = lax.dynamic_slice_in_dim(
        mixer_input_taps, channel_offset_begin, channel_count_here, 1
    )
    conv_bias_local = lax.dynamic_slice_in_dim(
        mixer_input_tap_bias, channel_offset_begin, channel_count_here, 0
    )
    scan_out, scan_pull = jax.vjp(
        lambda xs_in, step_in, bcp_in, bias_in, decay_in, skip_weight_input, kernel_in, conv_bias_in: mamba_core(
            xs_in,
            step_in,
            bcp_in,
            bias_in,
            decay_in,
            skip_weight_input,
            kernel_in,
            conv_bias_in,
            position,
            segment,
        ),
        x_heads.astype(jnp.float32),
        step_heads.astype(jnp.float32),
        bc_post,
        bias_local,
        decay_local,
        skip_local,
        kernel_local,
        conv_bias_local,
    )
    y_tokens = tokens_one(scan_out.astype(jnp.bfloat16)).astype(jnp.float32)
    silu_z = jax.nn.silu(gate_z)
    gated = y_tokens * silu_z
    total_sq = tensor_sum(jnp.sum(gated * gated, axis=1))
    inverse = lax.rsqrt(total_sq / INNER + epsilon)[:, None]
    yn_low = (gated * inverse * gated_norm_gain).astype(jnp.bfloat16)
    after_mamba = after_mlp + tensor_sum(matrix_product(yn_low, mamba_out))
    result = after_mamba.astype(jnp.bfloat16)
    grad_out = cotangent.astype(jnp.float32)
    mamba_big, mamba_out = collect_again(mixer_gate_input_weight, mixer_output_weight)
    d_yn = matrix_product_transposed(cotangent, mamba_out)
    grad_w_out = outer_product_sum(yn_low, cotangent)
    gain_part = d_yn * gated_norm_gain
    cross = tensor_sum(jnp.sum(gain_part * gated, axis=1))
    grad_g_gate = jnp.sum(d_yn * gated * inverse, axis=0)
    d_gated = gain_part * inverse - gated * inverse**3 * (cross / INNER)[:, None]
    d_y = (d_gated * silu_z).astype(jnp.bfloat16)
    sigmoid_z = jax.nn.sigmoid(gate_z)
    d_z = (d_gated * y_tokens * sigmoid_z * (1.0 + gate_z * (1.0 - sigmoid_z))).astype(jnp.bfloat16)
    dy_heads = heads_one(d_y)
    (
        d_xs,
        d_step,
        d_bc_post,
        grad_bias_local,
        grad_decay_local,
        grad_skip_local,
        grad_kernel_local,
        grad_conv_bias_local,
    ) = scan_pull(dy_heads.astype(jnp.float32))
    d_xs_tok, d_step_tok = tokens_pair(d_xs.astype(jnp.bfloat16), d_step.astype(jnp.bfloat16))
    d_bc_ctx = lax.psum(d_bc_post.astype(jnp.bfloat16), "ctx").astype(jnp.float32)
    dxn_part = (
        matrix_product_transposed(d_z, mamba_big[0])
        + matrix_product_transposed(d_xs_tok, mamba_big[1])
        + matrix_product_transposed(d_step_tok, step_size_weight)
    )
    grad_w_zx = jnp.stack([outer_product_sum(xn_low, d_z), outer_product_sum(xn_low, d_xs_tok)])
    grad_w_dt = outer_product_sum(xn_low, d_step_tok)
    dxn_sum, d_bc_full = tensor_pair(dxn_part, d_bc_ctx)
    d_bc_pre = bc_conv_pull(d_bc_full)[0]
    d_bc_mine = lax.dynamic_slice_in_dim(d_bc_pre, ctx_index * tok_rows, tok_rows, 0)
    own_rows = (slot_index // tok_rows == ctx_index).astype(jnp.float32)[:, None]
    ignored_part, grad_conv_bc, grad_conv_bc_bias = bc_conv_pull(d_bc_full * own_rows)
    d_bc_low = d_bc_mine.astype(jnp.bfloat16)
    dxn_total = dxn_sum + matrix_product_transposed(d_bc_low, state_map_weight)
    grad_w_bc = outer_product_sum(xn_low, d_bc_low)
    d_norm_n, grad_g_mamba = norm_n_back(dxn_total)
    d_after_mlp = grad_out + d_norm_n
    shard_heads = step_size_bias.shape[0]
    zero_heads = jnp.zeros((shard_heads,), jnp.float32)
    grad_dt_bias = lax.dynamic_update_slice_in_dim(zero_heads, grad_bias_local, start_offset, 0)
    grad_a_log = lax.dynamic_update_slice_in_dim(zero_heads, grad_decay_local, start_offset, 0)
    grad_d_skip = lax.dynamic_update_slice_in_dim(zero_heads, grad_skip_local, start_offset, 0)
    grad_conv_x = lax.dynamic_update_slice_in_dim(
        jnp.zeros(mixer_input_taps.shape, jnp.float32), grad_kernel_local, channel_offset_begin, 1
    )
    grad_conv_x_bias = lax.dynamic_update_slice_in_dim(
        jnp.zeros(mixer_input_tap_bias.shape, jnp.float32),
        grad_conv_bias_local,
        channel_offset_begin,
        0,
    )
    mlp_big, mlp_down = collect_again(gate_up_weight, down_weight)
    d_mlp_low = d_after_mlp.astype(jnp.bfloat16)
    d_hid = matrix_product_transposed(d_mlp_low, mlp_down)
    grad_w_down = outer_product_sum(hid_low, d_mlp_low)
    d_gate, d_up = act_back(d_hid)
    d_gate_low = d_gate.astype(jnp.bfloat16)
    d_up_low = d_up.astype(jnp.bfloat16)
    d_xm = tensor_sum(
        matrix_product_transposed(d_gate_low, mlp_big[0])
        + matrix_product_transposed(d_up_low, mlp_big[1])
    )
    grad_w_gu = jnp.stack(
        [outer_product_sum(xm_low, d_gate_low), outer_product_sum(xm_low, d_up_low)]
    )
    d_norm_m, grad_g_mlp = norm_m_back(d_xm)
    d_after_attn = d_after_mlp + d_norm_m
    attention_block_full, attn_out = collect_again(query_key_value_weight, attention_output_weight)
    d_attn_low = d_after_attn.astype(jnp.bfloat16)
    d_tokens = matrix_product_transposed(d_attn_low, attn_out).astype(jnp.bfloat16)
    grad_w_o = outer_product_sum(attn_tokens, d_attn_low)
    d_core = heads_one(d_tokens)
    d_pairs, d_values = attn_pull(d_core.astype(jnp.float32))
    d_pair_tok, d_value_tok = tokens_pair(
        d_pairs.astype(jnp.bfloat16), d_values.astype(jnp.bfloat16)
    )
    d_paired = d_pair_tok.reshape(tok_rows, tp_heads, 2, AHD)
    projection_gradient = [
        d_paired[:, :, 0].reshape(tok_rows, tp_heads * AHD),
        d_paired[:, :, 1].reshape(tok_rows, tp_heads * AHD),
        d_value_tok,
    ]
    dxa_part = (
        matrix_product_transposed(projection_gradient[0], attention_block_full[0])
        + matrix_product_transposed(projection_gradient[1], attention_block_full[1])
        + matrix_product_transposed(projection_gradient[2], attention_block_full[2])
    )
    dmid_part = jnp.concatenate(
        [
            matrix_product_transposed(
                projection_gradient[group_member], adapter_up_maps[group_member]
            )
            for group_member in range(3)
        ],
        axis=1,
    )
    grad_w_qkv = jnp.stack(
        [
            outer_product_sum(attention_input_reduced, projection_gradient[group_member])
            for group_member in range(3)
        ]
    )
    adapter_up_gradient = jnp.stack(
        [
            outer_product_sum(
                middle_reduced_precision[group_member], projection_gradient[group_member]
            )
            for group_member in range(3)
        ]
    )
    dxa_sum, dmid_sum = tensor_pair(dxa_part, dmid_part)
    dmid_low = dmid_sum.astype(jnp.bfloat16)
    rank_column_block = adapter_down_maps.shape[2]
    middle_gradient_pieces = [
        dmid_low[:, group_member * rank_column_block : (group_member + 1) * rank_column_block]
        for group_member in range(3)
    ]
    dxa_total = (
        dxa_sum
        + matrix_product_transposed(middle_gradient_pieces[0], adapter_down_maps[0])
        + matrix_product_transposed(middle_gradient_pieces[1], adapter_down_maps[1])
        + matrix_product_transposed(middle_gradient_pieces[2], adapter_down_maps[2])
    )
    adapter_down_gradient = jnp.stack(
        [
            outer_product_sum(attention_input_reduced, middle_gradient_pieces[group_member])
            for group_member in range(3)
        ]
    )
    d_joined, grad_g_attn = norm_a_back(dxa_total)
    d_hidden = d_after_attn + d_joined[:, :MODEL_WIDTH]
    d_embeds = d_joined[:, MODEL_WIDTH:]
    grad_w_qkv, grad_w_o, grad_w_gu, grad_w_down, grad_w_zx, grad_w_out = (
        lax.psum_scatter(
            grad_w_qkv.astype(jnp.bfloat16), ("fsdp", "ctx"), scatter_dimension=1, tiled=True
        ).astype(jnp.float32),
        lax.psum_scatter(
            grad_w_o.astype(jnp.bfloat16), ("fsdp", "ctx"), scatter_dimension=1, tiled=True
        ).astype(jnp.float32),
        lax.psum_scatter(
            grad_w_gu.astype(jnp.bfloat16), ("fsdp", "ctx"), scatter_dimension=1, tiled=True
        ).astype(jnp.float32),
        lax.psum_scatter(
            grad_w_down.astype(jnp.bfloat16), ("fsdp", "ctx"), scatter_dimension=1, tiled=True
        ).astype(jnp.float32),
        lax.psum_scatter(
            grad_w_zx.astype(jnp.bfloat16), ("fsdp", "ctx"), scatter_dimension=1, tiled=True
        ).astype(jnp.float32),
        lax.psum_scatter(
            grad_w_out.astype(jnp.bfloat16), ("fsdp", "ctx"), scatter_dimension=1, tiled=True
        ).astype(jnp.float32),
    )
    (
        grad_g_attn,
        adapter_down_gradient,
        adapter_up_gradient,
        grad_g_mlp,
        grad_g_mamba,
        grad_w_bc,
        grad_w_dt,
        grad_conv_x,
        grad_conv_x_bias,
        grad_conv_bc,
        grad_conv_bc_bias,
        grad_dt_bias,
        grad_a_log,
        grad_d_skip,
        grad_g_gate,
    ) = (
        lax.psum(grad_g_attn.astype(jnp.bfloat16), ("fsdp", "ctx")).astype(jnp.float32),
        lax.psum(adapter_down_gradient.astype(jnp.bfloat16), ("fsdp", "ctx")).astype(jnp.float32),
        lax.psum(adapter_up_gradient.astype(jnp.bfloat16), ("fsdp", "ctx")).astype(jnp.float32),
        lax.psum(grad_g_mlp.astype(jnp.bfloat16), ("fsdp", "ctx")).astype(jnp.float32),
        lax.psum(grad_g_mamba.astype(jnp.bfloat16), ("fsdp", "ctx")).astype(jnp.float32),
        lax.psum(grad_w_bc.astype(jnp.bfloat16), ("fsdp", "ctx")).astype(jnp.float32),
        lax.psum(grad_w_dt.astype(jnp.bfloat16), ("fsdp", "ctx")).astype(jnp.float32),
        lax.psum(grad_conv_x.astype(jnp.bfloat16), ("fsdp", "ctx")).astype(jnp.float32),
        lax.psum(grad_conv_x_bias.astype(jnp.bfloat16), ("fsdp", "ctx")).astype(jnp.float32),
        lax.psum(grad_conv_bc.astype(jnp.bfloat16), ("fsdp", "ctx")).astype(jnp.float32),
        lax.psum(grad_conv_bc_bias.astype(jnp.bfloat16), ("fsdp", "ctx")).astype(jnp.float32),
        lax.psum(grad_dt_bias.astype(jnp.bfloat16), ("fsdp", "ctx")).astype(jnp.float32),
        lax.psum(grad_a_log.astype(jnp.bfloat16), ("fsdp", "ctx")).astype(jnp.float32),
        lax.psum(grad_d_skip.astype(jnp.bfloat16), ("fsdp", "ctx")).astype(jnp.float32),
        lax.psum(grad_g_gate.astype(jnp.bfloat16), ("fsdp", "ctx")).astype(jnp.float32),
    )
    return (
        result,
        d_hidden,
        d_embeds,
        grad_g_attn,
        adapter_down_gradient,
        grad_w_qkv,
        adapter_up_gradient,
        grad_w_o,
        grad_g_mlp,
        grad_w_gu,
        grad_w_down,
        grad_g_mamba,
        grad_w_zx,
        grad_w_bc,
        grad_w_dt,
        grad_conv_x,
        grad_conv_x_bias,
        grad_conv_bc,
        grad_conv_bc_bias,
        grad_dt_bias,
        grad_a_log,
        grad_d_skip,
        grad_g_gate,
        grad_w_out,
    )


PLANE = ("fsdp", "ctx")
EVERY = ("fsdp", "ctx", "tp")


MESH = pl.DeviceIdType.MESH
IN_VMEM = pl.BlockSpec(memory_space=pltpu.VMEM)
IN_HBM = pl.BlockSpec(memory_space=pltpu.HBM)
IN_SMEM = pl.BlockSpec(memory_space=pltpu.SMEM)
DMA = pltpu.SemaphoreType.DMA
GATHER_SHARES = (4, 4, 4, 4)
SUM_SHARES = (4, 4, 4, 4)


class Place:
    def __init__(self, sizes):
        self.groups, self.ctx, self.tp = sizes
        g, c, t = (lax.axis_index(name) for name in EVERY)
        y, k = t // 2, lax.rem(t, 2)
        self.g, self.c, self.t, self.y, self.k = g, c, t, y, k
        self.core = (g, c, y * 2 + 1 - k)
        self.side_y = (g, c, (1 - y) * 2 + k)
        self.side_x = (g, 1 - c, t)
        self.line = [(lax.rem(g + d, self.groups), c, t) for d in range(1, self.groups)]
        self.plane = self.groups * self.ctx
        self.index = g * self.ctx + c

    def plane_peer(self, d):
        other = lax.rem(self.index + d, self.plane)
        return other, (other // self.ctx, lax.rem(other, self.ctx), self.t)

    def plane_source(self, d):
        return lax.rem(self.index + self.plane - d, self.plane)


def greet(devices):
    barrier = pltpu.get_barrier_semaphore()
    for device in devices:
        pl.semaphore_signal(barrier, inc=1, device_id=device, device_id_type=MESH)
    pl.semaphore_wait(barrier, len(devices))


def remote(src, dst, send_sem, recv_sem, device):
    return pltpu.make_async_remote_copy(
        src_ref=src,
        dst_ref=dst,
        send_sem=send_sem,
        recv_sem=recv_sem,
        device_id=device,
        device_id_type=MESH,
    )


def cut(ref, axis, index, width):
    if axis is None:
        return ref
    at = [slice(None)] * len(ref.shape)
    start = index * width
    if width % 128 == 0:
        start = pl.multiple_of(start, 128)
    at[axis] = pl.ds(start, width)
    return ref.at[tuple(at)]


class Moves:
    def __init__(self, place, specs, sources, targets, stages, send, recv, local):
        self.sent = []
        self.place, self.specs = place, specs
        self.sources, self.targets = sources, targets
        self.stages, self.send, self.recv, self.local = stages, send, recv, local

    def part(self, i, to, origin):
        split, join = self.specs[i]
        src, dst = self.sources[i], self.targets[i]
        n = self.place.plane
        if split is None:
            return src, cut(dst, join, origin, src.shape[join])
        return (
            cut(src, split, to, src.shape[split] // n),
            cut(dst, join, origin, dst.shape[join] // n),
        )

    def start(self, first=0):
        place = self.place
        self.loads, self.queue = [], []
        for i in range(len(self.specs)):
            self.queue += [(i, d) for d in range(1, place.plane)]
            src, _ = self.part(i, place.index, place.index)
            load = pltpu.make_async_copy(src, self.stages[i], self.local.at[i, 0])
            load.start()
            self.loads.append(load)
        self.queue.sort(key=lambda one: one[1] % place.ctx != first)

    def issue(self, count):
        for i, d in self.queue[:count]:
            other, device = self.place.plane_peer(d)
            src, dst = self.part(i, other, self.place.index)
            copy = remote(src, dst, self.send.at[i, d], self.recv.at[i, d], device)
            copy.start()
            self.sent.append(copy)
        self.queue = self.queue[count:]

    def settle(self):
        self.stores = []
        for i, load in enumerate(self.loads):
            load.wait()
            _, dst = self.part(i, self.place.index, self.place.index)
            store = pltpu.make_async_copy(self.stages[i], dst, self.local.at[i, 1])
            store.start()
            self.stores.append(store)

    def finish(self):
        place = self.place
        for i in range(len(self.specs)):
            for d in range(1, place.plane):
                _, device = place.plane_peer(d)
                src, dst = self.part(i, place.index, place.plane_source(d))
                remote(src, dst, self.send.at[i, d], self.recv.at[i, d], device).wait_recv()
        for copy in self.sent:
            copy.wait_send()
        for store in self.stores:
            store.wait()


def moves_setup(moves, plane):
    outs, scratch = [], []
    for array, split, join in moves:
        shape = list(array.shape)
        part = list(array.shape)
        if split is not None:
            part[split] //= plane
            shape[split] //= plane
        shape[join] *= plane
        outs.append(jax.ShapeDtypeStruct(tuple(shape), array.dtype))
        scratch.append(pltpu.VMEM(tuple(part), array.dtype))
    n = len(moves)
    if n:
        scratch += [DMA((n, plane)), DMA((n, plane)), DMA((n, 2))]
    return outs, scratch


class Gather:
    def __init__(self, place, x, o, pieces, sems):
        self.place, self.x, self.o, self.pieces, self.sems = place, x, o, pieces, sems
        self.n = len(pieces)
        self.first, self.second = [], [None] * self.n
        self.third, self.fourth = [None] * self.n, [None] * self.n

    def line_copy(self, q, d, owner):
        place, cols = self.place, pl.ds(*self.pieces[q])
        return remote(
            self.x.at[:, cols],
            self.o.at[owner, place.c, place.y, place.k, :, cols],
            self.sems[0].at[q, d],
            self.sems[1].at[q, d],
            place.line[d],
        )

    def begin(self):
        place = self.place
        own_at = self.o.at[place.g, place.c, place.y, place.k]
        own = pltpu.make_async_copy(self.x, own_at, self.sems[8])
        own.start()
        for q in range(self.n):
            for d in range(place.groups - 1):
                copy = self.line_copy(q, d, place.g)
                copy.start()
                self.first.append(copy)
        own.wait()

    def to_side(self, q):
        place = self.place
        for d in range(place.groups - 1):
            source = lax.rem(place.g + place.groups - d - 1, place.groups)
            self.line_copy(q, d, source).wait_recv()
        part = self.o.at[:, place.c, place.y, place.k, :, pl.ds(*self.pieces[q])]
        device = place.side_y if q % 2 == 0 else place.side_x
        self.second[q] = remote(part, part, self.sems[2].at[q], self.sems[3].at[q], device)
        self.second[q].start()

    def to_other_side(self, q):
        place, cols = self.place, pl.ds(*self.pieces[q])
        self.second[q].wait_recv()
        if q % 2 == 0:
            part, device = self.o.at[:, place.c, :, place.k, :, cols], place.side_x
        else:
            part, device = self.o.at[:, :, place.y, place.k, :, cols], place.side_y
        self.third[q] = remote(part, part, self.sems[4].at[q], self.sems[5].at[q], device)
        self.third[q].start()

    def to_core(self, q):
        place = self.place
        self.third[q].wait_recv()
        part = self.o.at[:, :, :, place.k, :, pl.ds(*self.pieces[q])]
        self.fourth[q] = remote(part, part, self.sems[6].at[q], self.sems[7].at[q], place.core)
        self.fourth[q].start()

    def steps(self):
        return pipelined(self.n, (self.to_side, self.to_other_side, self.to_core))

    def end(self):
        for copy in self.fourth:
            copy.wait_recv()
        for copy in self.first + self.second + self.third + self.fourth:
            copy.wait_send()


def pipelined(count, stages):
    def step(at):
        for lag, stage in enumerate(stages):
            if 0 <= at - lag < count:
                stage(at - lag)

    return [functools.partial(step, at) for at in range(count + len(stages) - 1)]


def gather_sems(n, groups):
    return [DMA((n, groups - 1)), DMA((n, groups - 1))] + [DMA((n,))] * 6 + [DMA]


class Scatter:
    def __init__(self, place, make, pieces, bufs, acc, sems):
        self.place, self.make, self.pieces, self.bufs, self.acc = place, make, pieces, bufs, acc
        self.sems = sems
        n = len(pieces)
        self.n = n
        self.c1, self.c2, self.c3, self.c4 = [None] * n, [None] * n, [None] * n, [None] * n

    def to_core(self, q):
        theirs, mine, b1 = self.bufs[:3]
        cols, k = pl.ds(*self.pieces[q]), self.place.k
        self.make(q, theirs, 1 - k)
        self.c1[q] = remote(
            theirs.at[..., cols],
            b1.at[..., cols],
            self.sems[0].at[q],
            self.sems[1].at[q],
            self.place.core,
        )
        self.c1[q].start()
        self.make(q, mine, k)

    def to_side(self, q):
        _, mine, b1, b2, _, _ = self.bufs
        place, cols = self.place, pl.ds(*self.pieces[q])
        f32 = jnp.float32
        self.c1[q].wait_recv()
        b1[..., cols] = (b1[..., cols].astype(f32) + mine[..., cols].astype(f32)).astype(b1.dtype)
        if q % 2 == 0:
            part, device = b1.at[:, :, 1 - place.y, :, cols], place.side_y
        else:
            part, device = b1.at[:, 1 - place.c, :, :, cols], place.side_x
        self.c2[q] = remote(
            part, b2.at[:, :, :, cols], self.sems[2].at[q], self.sems[3].at[q], device
        )
        self.c2[q].start()

    def to_other_side(self, q):
        _, _, b1, b2, b3, _ = self.bufs
        place, cols = self.place, pl.ds(*self.pieces[q])
        f32 = jnp.float32
        self.c2[q].wait_recv()
        own = b1[:, :, place.y, :, cols] if q % 2 == 0 else b1[:, place.c, :, :, cols]
        b2[:, :, :, cols] = (b2[:, :, :, cols].astype(f32) + own.astype(f32)).astype(b2.dtype)
        if q % 2 == 0:
            part, device = b2.at[:, 1 - place.c, :, cols], place.side_x
        else:
            part, device = b2.at[:, 1 - place.y, :, cols], place.side_y
        self.c3[q] = remote(part, b3.at[:, :, cols], self.sems[4].at[q], self.sems[5].at[q], device)
        self.c3[q].start()

    def along_line(self, q):
        _, _, _, b2, b3, b4 = self.bufs
        place, cols = self.place, pl.ds(*self.pieces[q])
        f32 = jnp.float32
        self.c3[q].wait_recv()
        own = b2[:, place.c, :, cols] if q % 2 == 0 else b2[:, place.y, :, cols]
        b3[:, :, cols] = (b3[:, :, cols].astype(f32) + own.astype(f32)).astype(b3.dtype)
        self.c4[q] = []
        for d in range(place.groups - 1):
            to = lax.rem(place.g + d + 1, place.groups)
            copy = remote(
                b3.at[to, :, cols],
                b4.at[d, :, cols],
                self.sems[6].at[q, d],
                self.sems[7].at[q, d],
                place.line[d],
            )
            copy.start()
            self.c4[q].append(copy)

    def land(self, q):
        b3, b4 = self.bufs[4:]
        cols = pl.ds(*self.pieces[q])
        total = b3[self.place.g, :, cols].astype(jnp.float32)
        for d in range(self.place.groups - 1):
            self.c4[q][d].wait_recv()
            total = total + b4[d, :, cols].astype(jnp.float32)
        self.acc[:, cols] = total

    def steps(self):
        stages = (self.to_core, self.to_side, self.to_other_side, self.along_line, self.land)
        return pipelined(self.n, stages)

    def end(self):
        for q in range(self.n):
            for copy in [self.c1[q], self.c2[q], self.c3[q]] + self.c4[q]:
                copy.wait_send()


class SmallSum:
    def __init__(self, place, x, o, zbuf, buf, zs, zr, ss, rs):
        self.place, self.x, self.o, self.zbuf, self.buf = place, x, o, zbuf, buf
        self.zs, self.zr, self.ss, self.rs = zs, zr, ss, rs

    def begin(self):
        self.copies = []
        for d, device in enumerate(self.place.line):
            copy = remote(self.x, self.zbuf.at[d], self.zs.at[d], self.zr.at[d], device)
            copy.start()
            self.copies.append(copy)

    def line(self):
        place, groups = self.place, self.place.groups
        for copy in self.copies:
            copy.wait_recv()
        total = None
        for owner in range(groups):
            part = self.x[...]
            for d in range(groups - 1):
                source = lax.rem(place.g + groups - d - 1, groups)
                part = jnp.where(source == owner, self.zbuf[d], part)
            total = part if total is None else total + part
        self.o[...] = total
        self.send(0)

    def send(self, i):
        device = (self.place.side_x, self.place.side_y, self.place.core)[i]
        self.copy = remote(self.o, self.buf.at[i], self.ss.at[i], self.rs.at[i], device)
        self.copy.start()

    def add(self, i):
        self.copy.wait_recv()
        self.copy.wait_send()
        self.o[...] = self.o[...] + self.buf[i]
        if i < 2:
            self.send(i + 1)

    def steps(self):
        return [self.line] + [functools.partial(self.add, i) for i in range(3)]

    def end(self):
        for copy in self.copies:
            copy.wait_send()


def small_scratch(shape, groups):
    f32 = jnp.float32
    return [
        pltpu.VMEM((groups - 1, *shape), f32),
        pltpu.VMEM((3, *shape), f32),
        DMA((groups - 1,)),
        DMA((groups - 1,)),
        DMA((3,)),
        DMA((3,)),
    ]


def weave(*streams):
    found = []
    rounds = max((start + len(steps) for start, steps in streams), default=0)
    for at in range(rounds):
        for start, steps in streams:
            if 0 <= at - start < len(steps):
                found.append(steps[at - start])
    return found


def scatter_scratch(n, groups, rows, width):
    bf16 = jnp.bfloat16
    bufs = [
        pltpu.VMEM((groups, 2, 2, rows, width), bf16),
        pltpu.VMEM((groups, 2, 2, rows, width), bf16),
        pltpu.VMEM((groups, 2, 2, rows, width), bf16),
        pltpu.VMEM((groups, 2, rows, width), bf16),
        pltpu.VMEM((groups, rows, width), bf16),
        pltpu.VMEM((groups - 1, rows, width), bf16),
        pltpu.VMEM((rows, width), jnp.float32),
    ]
    sems = [DMA((n,))] * 6 + [DMA((n, groups - 1))] * 2
    return bufs, sems


def rms_rows(x, gain):
    return x * lax.rsqrt(jnp.mean(x * x, axis=-1, keepdims=True) + epsilon) * gain


def rms_back(x, gain, grad):
    inverse = lax.rsqrt(jnp.mean(x * x, axis=-1, keepdims=True) + epsilon)
    scaled = grad * gain
    along = jnp.mean(scaled * x, axis=-1, keepdims=True)
    d_gain = jnp.sum(grad * x * inverse, axis=0, keepdims=True)
    return scaled * inverse - x * inverse**3 * along, d_gain


NT = (((1,), (1,)), ((), ()))
NN = (((1,), (0,)), ((), ()))


class Summed:
    def __init__(self, sizes, products, extra=None, pieces=SUM_SHARES):
        self.sizes, self.products, self.extra = sizes, products, extra
        self.rows = products[0][0].shape[0] // (sizes[0] * sizes[1] * sizes[2])
        self.width = products[0][1].shape[-2 if products[0][3] else -1]
        self.more = 0 if extra is None else extra.shape[1]
        self.rights, self.places = [], []
        for _, right, _, _ in products:
            found = [i for i, other in enumerate(self.rights) if other is right]
            self.places.append(found[0] if found else len(self.rights))
            if not found:
                self.rights.append(right)
        at, self.pieces = 0, []
        for share in pieces:
            self.pieces.append((at, self.width * share // 16))
            at += self.width * share // 16
        if self.more:
            self.pieces.append((self.width, self.more))
        self.bufs, self.sems = scatter_scratch(
            len(self.pieces), sizes[0], self.rows, self.width + self.more
        )

    def operands(self):
        groups, ctx, tp = self.sizes
        split = (groups, ctx, tp // 2, 2, self.rows)
        found = [product[0].reshape(*split, product[0].shape[1]) for product in self.products]
        found += self.rights
        if self.more:
            found.append(self.extra.reshape(*split, self.more))
        return found

    def stage(self, place, inputs, scratch):
        count = len(self.products)
        lefts, rights = inputs[:count], inputs[count : count + len(self.rights)]
        bufs, sems = scratch[: len(self.bufs)], scratch[len(self.bufs) :]
        groups, ctx, tp = self.sizes

        def make(q, into, core):
            at, size = self.pieces[q]
            if at >= self.width:
                into[..., pl.ds(at, size)] = inputs[-1][:, :, :, core]
                return

            def block(i, _):
                total = None
                for left, where, (_, _, lead, transposed) in zip(
                    lefts, self.places, self.products
                ):
                    right = rights[where] if lead is None else rights[where].at[lead]
                    a = left[i, :, :, core]
                    a = a.reshape(-1, a.shape[-1])
                    some = right[pl.ds(at, size), :] if transposed else right[:, pl.ds(at, size)]
                    part = lax.dot_general(
                        a, some, NT if transposed else NN, preferred_element_type=jnp.float32
                    )
                    total = part if total is None else total + part
                into[i, :, :, :, pl.ds(at, size)] = total.astype(into.dtype).reshape(
                    ctx, tp // 2, self.rows, size
                )
                return 0

            lax.fori_loop(0, groups, block, 0)

        return Scatter(place, make, self.pieces, bufs[:-1], bufs[-1], sems)


def exchange(
    sizes,
    number,
    summed,
    finish,
    finish_args,
    finish_outs,
    gathered,
    moves,
    early_share=22,
    also_gather=None,
    also_sum=None,
    tail=0,
    small=0,
):
    groups, ctx, tp = sizes
    f32, bf16 = jnp.float32, jnp.bfloat16
    rows = summed.rows
    out_pieces = gather_pieces(gathered)
    move_outs, move_scratch = moves_setup(moves, groups * ctx)
    n_moves = len(moves)
    move_specs = [(split, join) for _, split, join in moves]
    S = jax.ShapeDtypeStruct

    operands, in_specs, out_shape, out_specs, scratch = [], [], [], [], []

    def add_in(arrays, spec=IN_VMEM):
        at = len(operands)
        operands.extend(arrays)
        in_specs.extend([spec] * len(arrays))
        return slice(at, len(operands))

    def add_out(shapes, spec=IN_VMEM):
        at = len(out_shape)
        out_shape.extend(shapes)
        out_specs.extend([spec] * len(shapes))
        return slice(at, len(out_shape))

    def add_scratch(shapes):
        at = len(scratch)
        scratch.extend(shapes)
        return slice(at, len(scratch))

    in_sum = add_in(summed.operands())
    in_args = add_in(list(finish_args))
    o_main = add_out([S((groups, ctx, tp // 2, 2, rows, gathered), bf16)])
    o_finish = add_out([S(shape, f32) for shape in finish_outs])
    s_sum = add_scratch(summed.bufs + summed.sems)
    s_main = add_scratch(
        [pltpu.VMEM((rows, gathered), bf16)] + gather_sems(len(out_pieces), groups)
    )
    if also_gather is not None:
        also_pieces = gather_pieces(also_gather.shape[1])
        in_also = add_in([also_gather])
        o_also = add_out([S((groups, ctx, tp // 2, 2, rows, also_gather.shape[1]), bf16)])
        s_also = add_scratch(gather_sems(len(also_pieces), groups))
    if also_sum is not None:
        second, second_finish, second_args, second_out = also_sum
        in_second, in_second_args = add_in(second.operands()), add_in(second_args)
        o_second = add_out([second_out])
        s_second = add_scratch(second.bufs + second.sems)
    if tail:
        o_tail = add_out([S((tp // 2, 2, rows, tail), bf16)])
        s_tail = add_scratch([pltpu.VMEM((rows, tail), bf16)] + [DMA] * 5)
    if small:
        o_small = add_out([S((1, small), f32)])
        s_small = add_scratch([pltpu.VMEM((1, small), f32)] + small_scratch((1, small), groups))
    in_moves = add_in([array for array, _, _ in moves], IN_HBM)
    o_moves = add_out(move_outs, IN_HBM)
    s_moves = add_scratch(move_scratch)

    def kernel(*refs):
        ins = refs[: len(operands)]
        outs = refs[len(operands) : len(operands) + len(out_shape)]
        scr = refs[len(operands) + len(out_shape) :]
        place = Place(sizes)
        devices = [place.core, place.side_y]
        if n_moves:
            devices += [place.plane_peer(d)[1] for d in range(1, place.plane)]
        else:
            devices += [place.side_x] + place.line
        greet(devices)
        carried = None
        if n_moves:
            parts = scr[s_moves]
            carried = Moves(
                place, move_specs, ins[in_moves], outs[o_moves], parts[:n_moves], *parts[n_moves:]
            )
            carried.start()
        main_sum = summed.stage(place, ins[in_sum], scr[s_sum])
        low, *main_sems = scr[s_main]
        main_gather = Gather(place, low, outs[o_main][0], out_pieces, main_sems)
        streams = [(0, main_sum.steps())]
        ends = [main_sum, main_gather]
        if also_gather is not None:
            side_gather = Gather(place, ins[in_also][0], outs[o_also][0], also_pieces, scr[s_also])
            side_gather.begin()
            streams.append((2, side_gather.steps()))
            ends.append(side_gather)
        later = []
        if also_sum is not None:
            side_sum = second.stage(place, ins[in_second], scr[s_second])
            side_steps = side_sum.steps()
            streams.append((6, side_steps[:3]))
            later.append((0, side_steps[3:]))
            ends.append(side_sum)
        total = n_moves * (groups * ctx - 1)
        steps = weave(*streams)
        if carried is not None:
            carried.issue(total * early_share // 100)
        for step in steps:
            step()
        if carried is not None:
            carried.settle()
        low_tail = scr[s_tail][0] if tail else None
        low_small = scr[s_small][0] if small else None
        finish(place, main_sum.acc, ins[in_args], outs[o_finish], low, low_tail, low_small)
        main_gather.begin()
        if small:
            small_sum = SmallSum(place, low_small, outs[o_small][0], *scr[s_small][1:])
            small_sum.begin()
            later.append((1, small_sum.steps()))
            ends.append(small_sum)
        if tail:
            ys, yr, ks, kr, own_sem = scr[s_tail][1:]
            y, k, spot = place.y, place.k, outs[o_tail][0]
            own = pltpu.make_async_copy(low_tail, spot.at[y, k], own_sem)
            own.start()
            to_y = remote(low_tail, spot.at[y, k], ys, yr, place.side_y)
            to_y.start()
            own.wait()
        steps = weave((0, main_gather.steps()), *later)
        if carried is not None:
            carried.issue(total)
        for step in steps:
            step()
        if tail:
            to_y.wait_recv()
            part = spot.at[:, k]
            to_k = remote(part, part, ks, kr, place.core)
            to_k.start()
            to_k.wait_recv()
            to_y.wait_send()
            to_k.wait_send()
        if also_sum is not None:
            second_finish(side_sum.acc, ins[in_second_args], outs[o_second][0])
        for stage in ends:
            stage.end()
        if carried is not None:
            carried.finish()

    results = pl.pallas_call(
        kernel,
        out_shape=out_shape,
        in_specs=in_specs,
        out_specs=out_specs,
        scratch_shapes=scratch,
        name=f"exchange_{number}",
        compiler_params=pltpu.CompilerParams(
            collective_id=number, has_side_effects=True, vmem_limit_bytes=62 * 2**20
        ),
    )(*operands)
    found = {"gathered": results[0].reshape(-1, gathered), "finish": results[o_finish]}
    if also_gather is not None:
        found["also"] = results[o_also][0].reshape(-1, also_gather.shape[1])
    if also_sum is not None:
        found["second"] = results[o_second][0]
    if tail:
        found["tail"] = results[o_tail][0].reshape(-1, tail)
    if small:
        found["small"] = results[o_small][0]
    found["moves"] = results[o_moves]
    return found


def gather_pieces(width):
    if width < 1024:
        return [(0, width)]
    whole = width // 2048 * 2048
    at, found = 0, []
    for share in GATHER_SHARES:
        found.append((at, whole * share // 16))
        at += whole * share // 16
    if width > whole:
        found.append((whole, width - whole))
    return found


def opening(sizes, number, hidden, embeds, lengths, gain, down_all, moves):
    groups, ctx, tp = sizes
    f32, bf16 = jnp.float32, jnp.bfloat16
    rows = hidden.shape[0] // tp
    half = hidden.shape[1]
    mids = down_all.shape[1]
    width = 2 * half + mids + 128
    out_pieces = gather_pieces(width)
    move_outs, move_scratch = moves_setup(moves, groups * ctx)
    move_specs = [(split, join) for _, split, join in moves]
    n_moves = len(moves)

    def kernel(*refs):
        hid, emb, lens, gain_ref, down_ref = refs[:5]
        refs = list(refs[5:])
        sources = refs[:n_moves]
        o = refs[n_moves]
        targets = refs[n_moves + 1 : 2 * n_moves + 1]
        rest = refs[2 * n_moves + 1 :]
        low, gs = rest[0], rest[1:10]
        stages = rest[10 : 10 + n_moves]
        send, recv, local = rest[10 + n_moves :]
        place = Place(sizes)
        greet(
            [place.core, place.side_y]
            + [place.plane_peer(d)[1] for d in range(1, place.plane)]
        )
        carried = Moves(place, move_specs, sources, targets, stages, send, recv, local)
        carried.start(1)
        mine = pl.ds(pl.multiple_of(place.t * rows, 16), rows)
        a, b = hid[mine, :].astype(f32), emb[mine, :].astype(f32)
        squares = jnp.sum(a * a, axis=1, keepdims=True) + jnp.sum(b * b, axis=1, keepdims=True)
        inverse = lax.rsqrt(squares / (2 * half) + epsilon)
        low[:, :half] = (a * inverse * gain_ref[:, :half]).astype(bf16)
        low[:, half : 2 * half] = (b * inverse * gain_ref[:, half:]).astype(bf16)
        low[:, 2 * half : 2 * half + mids] = lax.dot_general(
            low[:, : 2 * half], down_ref[...], NN, preferred_element_type=f32
        ).astype(bf16)
        slot = lax.broadcasted_iota(jnp.int32, (rows, 128), 0)
        slot = slot + (place.c * tp + place.t) * rows
        lane = lax.broadcasted_iota(jnp.int32, (rows, 128), 1)
        segment, position, end = jnp.zeros_like(slot), slot, 0
        for i in range(lengths.shape[1]):
            length = lens[0, i]
            end = end + length
            passed = (slot >= end).astype(jnp.int32)
            segment = segment + passed
            position = position - passed * length
        marks = jnp.where(lane == 0, segment, position)
        low[:, 2 * half + mids :] = marks.astype(f32).astype(bf16)
        gather = Gather(place, low, o, out_pieces, gs)
        gather.begin()
        carried.issue(len(carried.queue))
        for step in gather.steps():
            step()
        carried.settle()
        gather.end()
        carried.finish()

    S = jax.ShapeDtypeStruct
    results = pl.pallas_call(
        kernel,
        out_shape=[S((groups, ctx, tp // 2, 2, rows, width), bf16)] + move_outs,
        in_specs=[IN_VMEM, IN_VMEM, IN_SMEM, IN_VMEM, IN_VMEM] + [IN_HBM] * n_moves,
        out_specs=[IN_VMEM] + [IN_HBM] * n_moves,
        scratch_shapes=[pltpu.VMEM((rows, width), bf16)]
        + gather_sems(len(out_pieces), groups)
        + move_scratch,
        name=f"opening_{number}",
        compiler_params=pltpu.CompilerParams(
            collective_id=number, has_side_effects=True, vmem_limit_bytes=62 * 2**20
        ),
    )(hidden, embeds, lengths, gain.reshape(1, -1), down_all, *[array for array, _, _ in moves])
    return [results[0].reshape(-1, width)] + list(results[1:])


def sum_small(sizes, number, values):
    def kernel(x, o, *scratch):
        place = Place(sizes)
        greet([place.core, place.side_y, place.side_x] + place.line)
        summing = SmallSum(place, x, o, *scratch)
        summing.begin()
        for step in summing.steps():
            step()
        summing.end()

    return pl.pallas_call(
        kernel,
        out_shape=jax.ShapeDtypeStruct(values.shape, jnp.float32),
        in_specs=[IN_VMEM],
        out_specs=IN_VMEM,
        scratch_shapes=small_scratch(values.shape, sizes[0]),
        name=f"sum_small_{number}",
        compiler_params=pltpu.CompilerParams(collective_id=number, has_side_effects=True),
    )(values)


def finish_forward(place, acc, args, outs, low, low_tail, low_small):
    rest, gain = args
    outs[0][...] = rest[...] + acc[...]
    low[...] = rms_rows(outs[0][...], gain[...]).astype(jnp.bfloat16)


def finish_mixer_back(place, acc, args, outs, low, low_tail, low_small):
    after_mlp, gain, cot, state_map = args
    width = after_mlp.shape[1]
    low[:, width:] = acc[:, width:].astype(jnp.bfloat16)
    d_normed = acc[:, :width] + lax.dot_general(
        low[:, width:], state_map[...], NT, preferred_element_type=jnp.float32
    )
    d_rows, d_gain = rms_back(after_mlp[...], gain[...], d_normed)
    outs[1][...] = d_gain
    d_rows = cot[...].astype(jnp.float32) + d_rows
    outs[0][...] = d_rows
    low[:, :width] = d_rows.astype(jnp.bfloat16)


def finish_mlp_back(place, acc, args, outs, low, low_tail, low_small):
    after_attn, gain, d_after_mlp = args
    d_rows, d_gain = rms_back(after_attn[...], gain[...], acc[...])
    outs[1][...] = d_gain
    d_rows = d_after_mlp[...] + d_rows
    outs[0][...] = d_rows
    low[...] = d_rows.astype(jnp.bfloat16)


def finish_attention_back(place, acc, args, outs, low, low_tail, low_small):
    hidden, embeds, gain, d_after_attn, down_all, out_mine, row = args
    half = hidden.shape[1]
    bf16, f32 = jnp.bfloat16, jnp.float32
    low[...] = acc[:, 2 * half :].astype(bf16)
    inputs = (hidden, embeds)
    squares = sum(jnp.sum(part[...] * part[...], axis=1, keepdims=True) for part in inputs)
    inverse = lax.rsqrt(squares / (2 * half) + epsilon)
    along = jnp.zeros_like(squares)
    for i, part in enumerate(inputs):
        cols = slice(i * half, (i + 1) * half)
        grad = acc[:, cols] + lax.dot_general(
            low[...], down_all[cols, :], NT, preferred_element_type=f32
        )
        acc[:, cols] = grad
        along = along + jnp.sum(grad * gain[:, cols] * part[...], axis=1, keepdims=True)
    along = along / (2 * half)
    low_tail[:, :half] = out_mine[...]
    low_small[:, 2 * half :] = row[...]
    for i, part in enumerate(inputs):
        cols = slice(i * half, (i + 1) * half)
        grad = acc[:, cols]
        low_small[:, cols] = jnp.sum(grad * part[...] * inverse, axis=0, keepdims=True)
        d_rows = grad * gain[:, cols] * inverse - part[...] * inverse**3 * along
        if i == 0:
            d_rows = d_rows + d_after_attn[...]
        low_tail[:, (i + 1) * half : (i + 2) * half] = d_rows.astype(bf16)


def finish_out(acc, args, out):
    out[...] = (args[0][...] + acc[...]).astype(out.dtype)


def adapter_products(xa, dmid, width):
    block, rank = 512, dmid.shape[1] // 3

    def kernel(a, b, o):
        both = lax.dot_general(
            a[...], b[...], (((0,), (0,)), ((), ())), preferred_element_type=jnp.float32
        )
        for j in range(3):
            o[j] = both[:, j * rank : (j + 1) * rank]

    return pl.pallas_call(
        kernel,
        out_shape=jax.ShapeDtypeStruct((3, width, rank), jnp.float32),
        grid=(width // block,),
        in_specs=[
            pl.BlockSpec((xa.shape[0], block), lambda i: (0, i)),
            pl.BlockSpec(dmid.shape, lambda i: (0, 0)),
        ],
        out_specs=pl.BlockSpec((3, block, rank), lambda i: (0, i, 0)),
        name="adapter_products",
    )(xa, dmid)


def unpack(packed, parts):
    flat, at, found = packed.reshape(-1), 0, []
    for part in parts:
        found.append(flat[at : at + part.size].reshape(part.shape))
        at += part.size
    return found


def attend_groups(queries, keys_all, vals_all, segment, position):
    def rot(values):
        half_dim = values.shape[-1] // 2
        inverse = 10000.0 ** (-jnp.arange(half_dim, dtype=jnp.float32) / half_dim)
        angle = position.astype(jnp.float32)[..., None] * inverse
        cosine, sine = jnp.cos(angle), jnp.sin(angle)
        a, b = values[..., :half_dim], values[..., half_dim:]
        return jnp.concatenate([a * cosine - b * sine, b * cosine + a * sine], axis=-1).astype(
            jnp.bfloat16
        )

    rows = queries.shape[1]
    order = jnp.arange(rows)
    scores = jnp.einsum(
        "gqd,gkd->gqk", rot(queries), rot(keys_all), preferred_element_type=jnp.float32
    ) * AHD ** (-0.5)
    allowed = (segment[:, :, None] == segment[:, None, :]) & (order[:, None] >= order[None, :])
    weights = jnp.exp(jnp.where(allowed, scores, -1e30))
    low = (weights / jnp.sum(weights, axis=-1, keepdims=True)).astype(jnp.bfloat16)
    return jnp.einsum(
        "gqk,gkd->gqd", low, vals_all.astype(jnp.bfloat16), preferred_element_type=jnp.float32
    )


TN = (((0,), (0,)), ((), ()))


def exact(left, right, dims):
    return lax.dot_general(left, right, dims, precision=highest, preferred_element_type=jnp.float32)


def quick(left, right, dims):
    return lax.dot_general(left, right, dims, preferred_element_type=jnp.float32)


def down_rows(values, by):
    return pltpu.roll(values, by, 0)


def up_rows(values, by):
    return pltpu.roll(values, values.shape[0] - by, 0)


def taps_forward(values, taps, bias, position):
    total = values * taps[0:1, :] + bias
    for lag in range(1, taps.shape[0]):
        kept = jnp.where(position >= lag, down_rows(values, lag), 0.0)
        total = total + kept * taps[lag : lag + 1, :]
    return total


def taps_backward(d_total, values, taps, position):
    d_values = d_total * taps[0:1, :]
    rows = [jnp.sum(d_total * values, axis=0, keepdims=True)]
    for lag in range(1, taps.shape[0]):
        kept = jnp.where(position >= lag, d_total, 0.0)
        rows.append(jnp.sum(kept * down_rows(values, lag), axis=0, keepdims=True))
        d_values = d_values + up_rows(kept, lag) * taps[lag : lag + 1, :]
    return d_values, rows + [jnp.sum(d_total, axis=0, keepdims=True)]


def silu_slope(values):
    sigmoid = jax.nn.sigmoid(values)
    return sigmoid * (1.0 + values * (1.0 - sigmoid))


class Scan:
    def __init__(self, xs, raw, bc, marks, taps, bias, bc_taps, bc_bias, heads):
        f32 = jnp.float32
        rows, lanes = xs.shape
        self.rows, self.half = rows, lanes // 2
        self.position = marks[:, 1:2].astype(f32)
        self.lane = lax.broadcasted_iota(jnp.int32, (rows, lanes), 1)
        self.xs, self.bc = xs.astype(f32), bc.astype(f32)
        self.pre_x = taps_forward(self.xs, taps, bias, self.position)
        self.pre_bc = taps_forward(self.bc, bc_taps, bc_bias, self.position)
        self.xc, bcc = jax.nn.silu(self.pre_x), jax.nn.silu(self.pre_bc)
        self.b_mat, self.c_mat = bcc[:, :STATE], bcc[:, STATE:]
        self.step_in = raw.astype(f32) + heads[0:1, :]
        self.dt = jax.nn.softplus(self.step_in)
        self.rate = -jnp.exp(heads[1:2, :])
        self.log_decay = self.dt * self.rate
        running, by = self.log_decay, 1
        while by < rows:
            running = running + jnp.where(self.position >= by, down_rows(running, by), 0.0)
            by *= 2
        self.running = running
        self.across = running.T
        row = lax.broadcasted_iota(jnp.int32, (rows, rows), 0)
        col = lax.broadcasted_iota(jnp.int32, (rows, rows), 1)
        first = row.astype(f32) - self.position
        self.same = (col <= row) & (col.astype(f32) >= first)
        self.meet = exact(self.c_mat, self.b_mat, NT)
        self.dt_wide = self.by_head([self.dt[:, h : h + 1] for h in range(2)])
        self.weighted = self.xc * self.dt_wide

    def by_head(self, values):
        return jnp.where(self.lane < self.half, values[0], values[1])

    def in_lane(self, values):
        return jnp.where(self.lane == 0, values[0], jnp.where(self.lane == 1, values[1], 0.0))

    def decay(self, h):
        gap = self.running[:, h : h + 1] - self.across[h : h + 1, :]
        return jnp.where(self.same, jnp.exp(jnp.where(self.same, gap, 0.0)), 0.0)

    def forward(self, skip):
        outs = [exact(self.decay(h) * self.meet, self.weighted, NN) for h in range(2)]
        return self.by_head(outs) + skip * self.xc

    def to_ends(self, values):
        rows = values.shape[0]
        row = lax.broadcasted_iota(jnp.int32, values.shape, 0)
        wide = jnp.broadcast_to(self.position, values.shape)
        by = 1
        while by < rows:
            inside = (up_rows(wide, by) >= by) & (row < rows - by)
            values = values + jnp.where(inside, up_rows(values, by), 0.0)
            by *= 2
        return values


def mixer_forward(xn, cot, marked, mark_block, w_zx, w_step, state_map, w_out, small, bc_small, groups):
    f32, bf16 = jnp.float32, jnp.bfloat16
    total, width = xn.shape
    rows, lanes = total // groups, w_zx.shape[2]
    state2 = state_map.shape[1]

    def kernel(xn_r, cot_r, marks_r, zx_r, st_r, sm_r, wo_r, sml, bsml, z_o, xs_o, raw_o, bc_o, y_o, dyn_o, sums_o):
        x = xn_r[...]
        z = quick(x, zx_r[0], NN)
        xs = quick(x, zx_r[1], NN).astype(bf16)
        raw = quick(x, st_r[...], NN).astype(bf16)
        bc = quick(x, sm_r[...], NN).astype(bf16)
        z_o[...], xs_o[...], raw_o[...], bc_o[...] = z, xs, raw, bc
        scan = Scan(
            xs, raw, bc, marks_r[...].astype(f32), sml[0:4, :], sml[4:5, :], bsml[0:4, :], bsml[4:5, :], sml[8:10, :]
        )
        y = scan.forward(sml[5:6, :]).astype(bf16)
        y_o[...] = y
        gated = y.astype(f32) * jax.nn.silu(z)
        d_yn = quick(cot_r[...], wo_r[...], NT)
        dyn_o[...] = d_yn
        ones = jnp.ones((8, lanes), f32)
        sums_o[0, 0:1] = exact(ones, gated * gated, NT)[0:1]
        sums_o[0, 1:2] = exact(ones, d_yn * sml[6:7, :] * gated, NT)[0:1]

    def by_group(columns):
        return pl.BlockSpec((rows, columns), lambda g: (g, 0))

    def whole(array):
        return pl.BlockSpec(array.shape, lambda g: (0,) * array.ndim)

    S = jax.ShapeDtypeStruct
    return pl.pallas_call(
        kernel,
        grid=(groups,),
        in_specs=[by_group(width), by_group(width), pl.BlockSpec((rows, 128), lambda g: (g, mark_block))]
        + [whole(array) for array in (w_zx, w_step, state_map, w_out, small, bc_small)],
        out_specs=[by_group(lanes)] * 3
        + [by_group(state2), by_group(lanes), by_group(lanes), pl.BlockSpec((1, 2, rows), lambda g: (g, 0, 0))],
        out_shape=[
            S((total, lanes), f32),
            S((total, lanes), bf16),
            S((total, lanes), bf16),
            S((total, state2), bf16),
            S((total, lanes), bf16),
            S((total, lanes), f32),
            S((groups, 2, rows), f32),
        ],
        compiler_params=pltpu.CompilerParams(vmem_limit_bytes=60 * 2**20),
        name="mixer_forward",
    )(xn, cot, marked, w_zx, w_step, state_map, w_out, small, bc_small)


def mixer_backward(xn, cot, marked, mark_block, kept, sums, small, bc_small, groups):
    f32, bf16 = jnp.float32, jnp.bfloat16
    z, xs, raw, bc, y, d_yn = kept
    total, width = xn.shape
    rows, lanes, state2 = total // groups, z.shape[1], bc.shape[1]

    def kernel(
        xn_r, cot_r, marks_r, z_r, xs_r, raw_r, bc_r, y_r, dyn_r, sums_r, sml, bsml,
        dz_o, dxs_o, draw_o, dbc_o, yn_o, gzx_o, gst_o, gout_o, gsm_o, gbc_o, acc_in, acc_out,
    ):
        group = pl.program_id(0)
        scan = Scan(
            xs_r[...], raw_r[...], bc_r[...], marks_r[...].astype(f32),
            sml[0:4, :], sml[4:5, :], bsml[0:4, :], bsml[4:5, :], sml[8:10, :],
        )
        skip, gain = sml[5:6, :], sml[6:7, :]
        sums_wide = [jnp.broadcast_to(sums_r[0, i : i + 1], (128, rows)).T for i in range(2)]
        inverse = lax.rsqrt(sums_wide[0] / INNER + epsilon)
        cross = sums_wide[1] / INNER
        gate, out, d_normed = z_r[...], y_r[...].astype(f32), dyn_r[...]
        silu_z = jax.nn.silu(gate)
        gated = out * silu_z
        yn = (gated * inverse * gain).astype(bf16)
        yn_o[...] = yn
        g_gate = jnp.sum(d_normed * gated * inverse, axis=0, keepdims=True)
        d_gated = d_normed * gain * inverse - gated * inverse**3 * cross
        d_y = (d_gated * silu_z).astype(bf16).astype(f32)
        d_z = (d_gated * out * silu_slope(gate)).astype(bf16)
        dz_o[...] = d_z
        g_skip = jnp.sum(d_y * scan.xc, axis=0, keepdims=True)
        d_weighted, d_meet = jnp.zeros_like(d_y), jnp.zeros_like(scan.meet)
        by_row, by_col = [], []
        for h in range(2):
            mine = (scan.lane < scan.half) if h == 0 else (scan.lane >= scan.half)
            d_head = jnp.where(mine, d_y, 0.0)
            decay = scan.decay(h)
            mixing = decay * scan.meet
            d_mixing = exact(d_head, scan.weighted, NT)
            d_weighted = d_weighted + exact(mixing, d_head, TN)
            d_meet = d_meet + d_mixing * decay
            moved = d_mixing * mixing
            by_row.append(jnp.sum(moved, axis=1, keepdims=True))
            by_col.append(jnp.sum(moved, axis=0, keepdims=True))
        columns = [jnp.broadcast_to(by_col[h], (128, rows)).T for h in range(2)]
        d_running = scan.in_lane([by_row[h] - columns[h] for h in range(2)])
        d_log = scan.to_ends(d_running)
        shared = d_weighted * scan.xc
        d_dt = scan.in_lane(
            [
                jnp.sum(jnp.where(scan.lane < scan.half, shared, 0.0), axis=1, keepdims=True),
                jnp.sum(jnp.where(scan.lane >= scan.half, shared, 0.0), axis=1, keepdims=True),
            ]
        )
        d_step = (d_dt + d_log * scan.rate) * jax.nn.sigmoid(scan.step_in)
        g_bias = jnp.sum(d_step, axis=0, keepdims=True)
        g_decay = jnp.sum(d_log * scan.log_decay, axis=0, keepdims=True)
        d_raw = d_step.astype(bf16)
        draw_o[...] = d_raw
        d_xc = skip * d_y + d_weighted * scan.dt_wide
        d_xs, g_taps = taps_backward(
            d_xc * silu_slope(scan.pre_x), scan.xs, sml[0:4, :], scan.position
        )
        d_xs = d_xs.astype(bf16)
        dxs_o[...] = d_xs
        d_bcc = jnp.concatenate(
            [exact(d_meet, scan.c_mat, TN), exact(d_meet, scan.b_mat, NN)], axis=1
        )
        d_bc, g_bc_taps = taps_backward(
            d_bcc * silu_slope(scan.pre_bc), scan.bc, bsml[0:4, :], scan.position
        )
        dbc_o[...] = d_bc.astype(bf16)
        in_part = quick(jnp.concatenate([d_z, d_xs, d_raw], axis=1), xn_r[...], TN)
        out_part = quick(yn, cot_r[...], TN)
        blank = jnp.zeros((1, lanes), f32)
        few = jnp.concatenate(
            g_taps + [g_gate, g_bias, g_decay, g_skip] + [blank] * 7, axis=0
        )
        few_bc = jnp.concatenate(g_bc_taps + [jnp.zeros((3, state2), f32)], axis=0)

        @pl.when(group == 0)
        def _():
            acc_in[...], acc_out[...] = in_part, out_part
            gsm_o[...], gbc_o[...] = few, few_bc

        @pl.when(group > 0)
        def _():
            acc_in[...] += in_part
            acc_out[...] += out_part
            gsm_o[...] += few
            gbc_o[...] += few_bc

        @pl.when(group == groups - 1)
        def _():
            for i in range(2):
                gzx_o[i] = acc_in[i * lanes : (i + 1) * lanes, :].T.astype(bf16)
            gst_o[...] = acc_in[2 * lanes : 2 * lanes + 8, :]
            gout_o[...] = acc_out[...].astype(bf16)

    def by_group(columns):
        return pl.BlockSpec((rows, columns), lambda g: (g, 0))

    def whole(shape):
        return pl.BlockSpec(shape, lambda g: (0,) * len(shape))

    S = jax.ShapeDtypeStruct
    return pl.pallas_call(
        kernel,
        grid=(groups,),
        in_specs=[by_group(width), by_group(width), pl.BlockSpec((rows, 128), lambda g: (g, mark_block))]
        + [by_group(array.shape[1]) for array in kept]
        + [pl.BlockSpec((1, 2, rows), lambda g: (g, 0, 0)), whole(small.shape), whole(bc_small.shape)],
        out_specs=[by_group(lanes)] * 3
        + [by_group(state2), by_group(lanes)]
        + [
            whole((2, width, lanes)),
            whole((8, width)),
            whole((lanes, width)),
            whole((16, lanes)),
            whole((8, state2)),
        ],
        out_shape=[
            S((total, lanes), bf16),
            S((total, lanes), bf16),
            S((total, lanes), bf16),
            S((total, state2), bf16),
            S((total, lanes), bf16),
            S((2, width, lanes), bf16),
            S((8, width), f32),
            S((lanes, width), bf16),
            S((16, lanes), f32),
            S((8, state2), f32),
        ],
        scratch_shapes=[pltpu.VMEM((3 * lanes, width), f32), pltpu.VMEM((lanes, width), f32)],
        compiler_params=pltpu.CompilerParams(vmem_limit_bytes=60 * 2**20),
        name="mixer_backward",
    )(xn, cot, marked, z, xs, raw, bc, y, d_yn, sums, small, bc_small)


def per_device_split(
    hidden,
    embeds,
    cotangent,
    lengths,
    attention_norm_gain,
    adapter_down_maps,
    query_key_value_weight,
    adapter_up_maps,
    attention_output_weight,
    feedforward_norm_gain,
    gate_up_weight,
    down_weight,
    mixer_norm_gain,
    mixer_gate_input_weight,
    state_map_weight,
    step_size_weight,
    mixer_input_taps,
    mixer_input_tap_bias,
    state_map_taps,
    state_map_tap_bias,
    step_size_bias,
    log_decay_rate,
    head_skip_weight,
    gated_norm_gain,
    mixer_output_weight,
):
    bf16, f32 = jnp.bfloat16, jnp.float32
    tp_size, ctx_size, groups = (lax.axis_size(name) for name in ("tp", "ctx", "fsdp"))
    tp_index, ctx_index = lax.axis_index("tp"), lax.axis_index("ctx")
    plane_index = lax.axis_index("fsdp") * ctx_size + ctx_index
    plane_size = groups * ctx_size
    tok_rows = hidden.shape[0]
    mine = tok_rows // tp_size
    group_rows = tok_rows * ctx_size
    start = tp_index * mine

    sizes = (groups, ctx_size, tp_size)

    def own_rows(values):
        return lax.dynamic_slice_in_dim(values, start, mine, 0)

    def own_part(values, axis=0):
        width = values.shape[axis] // plane_size
        return lax.dynamic_slice_in_dim(values, plane_index * width, width, axis)

    width = hidden.shape[1]
    hidden_f = own_rows(hidden).astype(f32)
    embeds_f = own_rows(embeds).astype(f32)
    cot_low = own_rows(cotangent)

    up_maps = own_part(adapter_up_maps, 2)
    w_step = own_part(step_size_weight, 1)
    taps, tap_bias = own_part(mixer_input_taps, 1), own_part(mixer_input_tap_bias)
    step_bias, decay_rate = own_part(step_size_bias), own_part(log_decay_rate)
    skip, gate_gain = own_part(head_skip_weight), own_part(gated_norm_gain)

    rank = adapter_down_maps.shape[2]
    width_a = adapter_down_maps.shape[1]
    down_all = jnp.concatenate([adapter_down_maps[j] for j in range(3)], axis=1)
    xa_wide, w_o, w_qkv = opening(
        sizes,
        1,
        hidden,
        embeds,
        lengths,
        attention_norm_gain,
        down_all,
        [(attention_output_weight, 0, 1), (query_key_value_weight, 2, 1)],
    )
    xa = xa_wide[:, :width_a]
    mid = xa_wide[:, width_a : width_a + 3 * rank]
    segment = xa_wide[:, width_a + 3 * rank].astype(jnp.int32).reshape(groups, group_rows)
    position = xa_wide[:, width_a + 3 * rank + 1].astype(jnp.int32).reshape(groups, group_rows)
    proj = [
        (
            matrix_product(xa, w_qkv[j])
            + matrix_product(mid[:, j * rank : (j + 1) * rank], up_maps[j])
        ).astype(bf16)
        for j in range(3)
    ]
    ao, attend_back = jax.vjp(
        lambda q, k, v: attend_groups(q, k, v, segment, position),
        *[piece.astype(f32).reshape(groups, group_rows, AHD) for piece in proj],
    )
    ao_low = ao.astype(bf16).reshape(groups * group_rows, AHD)

    gain_m = feedforward_norm_gain.reshape(1, -1)
    found = exchange(
        sizes,
        2,
        Summed(sizes, [(ao_low, w_o, None, False)]),
        finish_forward,
        [hidden_f, gain_m],
        [hidden_f.shape],
        width,
        [(gate_up_weight, 2, 1), (down_weight, 0, 1)],
    )
    xm, (after_attn,), (w_gu, w_down) = found["gathered"], found["finish"], found["moves"]
    gate_pre, up_pre = matrix_product(xm, w_gu[0]), matrix_product(xm, w_gu[1])
    activated, act_back = jax.vjp(gated_gelu, gate_pre, up_pre)
    hid_low = activated.astype(bf16)

    gain_n = mixer_norm_gain.reshape(1, -1)
    found = exchange(
        sizes,
        3,
        Summed(sizes, [(hid_low, w_down, None, False)]),
        finish_forward,
        [after_attn, gain_n],
        [hidden_f.shape],
        width,
        [(mixer_gate_input_weight, 2, 1), (mixer_output_weight, 0, 1)],
        early_share=0,
        also_gather=cot_low,
    )
    xn, cot, (after_mlp,) = found["gathered"], found["also"], found["finish"]
    w_zx, w_out = found["moves"]
    few = step_bias.shape[0]
    lanes = ((0, 0), (0, 128 - few))
    row_of = lambda part: jnp.pad(part[None], lanes)
    small = jnp.concatenate(
        [
            taps,
            tap_bias[None],
            jnp.repeat(skip, MIXER_HEAD_SIZE)[None],
            gate_gain[None],
            jnp.zeros((1, 128), f32),
            row_of(step_bias),
            row_of(decay_rate),
        ]
    )
    bc_small = jnp.concatenate([state_map_taps, state_map_tap_bias[None]])
    mark_block = (width_a + 3 * rank) // 128
    w_step = jnp.pad(w_step, lanes)
    *kept, sums = mixer_forward(
        xn, cot, xa_wide, mark_block, w_zx, w_step, state_map_weight, w_out, small, bc_small, groups
    )
    sums = sum_small(sizes, 4, sums)
    d_z, d_xs, d_step, d_bc_part, yn_low, grad_w_zx, grad_w_dt, grad_w_out, few_x, few_bc = (
        mixer_backward(xn, cot, xa_wide, mark_block, kept, sums, small, bc_small, groups)
    )
    grad_conv_bc, grad_conv_bc_bias = few_bc[:4], few_bc[4]
    found = exchange(
        sizes,
        5,
        Summed(
            sizes,
            [
                (d_z, w_zx, 0, True),
                (d_xs, w_zx, 1, True),
                (d_step, w_step, None, True),
            ],
            d_bc_part,
        ),
        finish_mixer_back,
        [after_mlp, gain_n, cot_low, state_map_weight],
        [hidden_f.shape, gain_n.shape],
        width + d_bc_part.shape[1],
        [(grad_w_zx, 1, 2), (grad_w_out, 1, 0)],
        early_share=43,
        also_sum=(
            Summed(sizes, [(yn_low, w_out, None, False)]),
            finish_out,
            [after_mlp],
            jax.ShapeDtypeStruct(hidden_f.shape, bf16),
        ),
    )
    gathered, (d_after_mlp, grad_g_mamba) = found["gathered"], found["finish"]
    out_mine, (grad_w_zx, grad_w_out) = found["second"], found["moves"]

    d_mlp, d_bc = gathered[:, :width], gathered[:, width:]
    grad_w_bc = outer_product_sum(xn, d_bc)
    grad_w_down = outer_product_sum(hid_low, d_mlp)
    d_gate, d_up = act_back(matrix_product_transposed(d_mlp, w_down))
    d_gate, d_up = d_gate.astype(bf16), d_up.astype(bf16)
    grad_w_gu = jnp.stack(
        [outer_product_sum(xm, d_gate).astype(bf16), outer_product_sum(xm, d_up).astype(bf16)]
    )

    found = exchange(
        sizes,
        6,
        Summed(sizes, [(d_gate, w_gu, 0, True), (d_up, w_gu, 1, True)]),
        finish_mlp_back,
        [after_attn, gain_m, d_after_mlp],
        [hidden_f.shape, gain_m.shape],
        width,
        [(grad_w_gu, 1, 2), (grad_w_down.astype(bf16), 1, 0)],
    )
    d_attn, (d_after_attn, grad_g_mlp) = found["gathered"], found["finish"]
    grad_w_gu, grad_w_down = found["moves"]
    grad_w_o = outer_product_sum(ao_low, d_attn)
    d_ao = matrix_product_transposed(d_attn, w_o).astype(bf16)
    d_proj = [
        piece.reshape(groups * group_rows, AHD).astype(bf16)
        for piece in attend_back(d_ao.astype(f32).reshape(groups, group_rows, AHD))
    ]
    dmid_part = jnp.concatenate(
        [matrix_product_transposed(d_proj[j], up_maps[j]).astype(bf16) for j in range(3)], axis=1
    )
    grad_w_qkv = jnp.stack([outer_product_sum(xa, d_proj[j]).astype(bf16) for j in range(3)])
    adapter_up_gradient = jnp.stack(
        [outer_product_sum(mid[:, j * rank : (j + 1) * rank], d_proj[j]) for j in range(3)]
    )
    shares = jnp.concatenate([few_x, grad_w_dt[:few].reshape(-1, 128)]).astype(bf16)
    sums = [grad_g_mlp[0], grad_g_mamba[0], grad_conv_bc, grad_conv_bc_bias]
    row = jnp.concatenate([part.reshape(-1) for part in sums])[None]
    found = exchange(
        sizes,
        7,
        Summed(sizes, [(d_proj[j], w_qkv, j, True) for j in range(3)], dmid_part),
        finish_attention_back,
        [
            hidden_f,
            embeds_f,
            attention_norm_gain.reshape(1, -1),
            d_after_attn,
            down_all,
            out_mine,
            row,
        ],
        [],
        3 * rank,
        [
            (grad_w_qkv, 1, 2),
            (grad_w_o.astype(bf16), 1, 0),
            (adapter_up_gradient.astype(bf16), None, 2),
            (shares, None, 1),
        ],
        early_share=30,
        tail=3 * width,
        small=width_a + row.shape[1],
    )
    dmid, back, row = found["gathered"], found["tail"], found["small"][0]
    grad_w_qkv, grad_w_o, adapter_up_gradient, shared = found["moves"]
    adapter_down_gradient = adapter_products(xa_wide, dmid, width_a)
    result = back[:, :width]
    d_hidden = back[:, width : 2 * width].astype(f32)
    d_embeds = back[:, 2 * width :].astype(f32)
    adapter_up_gradient = adapter_up_gradient.astype(f32)
    shared = shared.astype(f32)
    grad_conv_x, grad_conv_x_bias, grad_g_gate = shared[:4], shared[4], shared[5]
    heads = shared.reshape(-1, plane_size, 128)
    grad_dt_bias = heads[6, :, :few].reshape(-1)
    grad_a_log = heads[7, :, :few].reshape(-1)
    grad_d_skip = heads[8].reshape(plane_size, few, MIXER_HEAD_SIZE).sum(axis=2).reshape(-1)
    grad_w_dt = shared[16:].reshape(few, -1, plane_size, 128).transpose(1, 3, 2, 0)
    grad_w_dt = grad_w_dt.reshape(-1, plane_size * few)
    grad_g_attn = row[:width_a]
    grad_g_mlp, grad_g_mamba, grad_conv_bc, grad_conv_bc_bias = unpack(row[width_a:], sums)

    return (
        result,
        d_hidden,
        d_embeds,
        grad_g_attn,
        adapter_down_gradient,
        grad_w_qkv.astype(f32),
        adapter_up_gradient,
        grad_w_o.astype(f32),
        grad_g_mlp,
        grad_w_gu.astype(f32),
        grad_w_down.astype(f32),
        grad_g_mamba,
        grad_w_zx.astype(f32),
        grad_w_bc,
        grad_w_dt,
        grad_conv_x,
        grad_conv_x_bias,
        grad_conv_bc,
        grad_conv_bc_bias,
        grad_dt_bias,
        grad_a_log,
        grad_d_skip,
        grad_g_gate,
        grad_w_out.astype(f32),
    )


def solution(mesh):
    placed = (
        P(("fsdp", "ctx"), None),
        P(("fsdp", "ctx"), None),
        P(("fsdp", "ctx"), None),
        P("fsdp", None),
        P(),
        P(),
        P(None, ("fsdp", "ctx"), "tp"),
        P(None, None, "tp"),
        P("tp", ("fsdp", "ctx")),
        P(),
        P(None, ("fsdp", "ctx"), "tp"),
        P("tp", ("fsdp", "ctx")),
        P(),
        P(None, ("fsdp", "ctx"), "tp"),
        P(),
        P(None, "tp"),
        P(None, "tp"),
        P("tp"),
        P(),
        P(),
        P("tp"),
        P("tp"),
        P("tp"),
        P("tp"),
        P("tp", ("fsdp", "ctx")),
    )
    devices = mesh.shape["fsdp"] * mesh.shape["ctx"] * mesh.shape["tp"]
    one_head_each = devices == AHEADS and mesh.shape["ctx"] == 2 and mesh.shape["tp"] == 4
    return jax.shard_map(
        per_device_split if one_head_each else per_device,
        mesh=mesh,
        in_specs=placed,
        out_specs=(
            P(("fsdp", "ctx"), None),
            P(("fsdp", "ctx"), None),
            P(("fsdp", "ctx"), None),
            P(),
            P(),
            P(None, ("fsdp", "ctx"), "tp"),
            P(None, None, "tp"),
            P("tp", ("fsdp", "ctx")),
            P(),
            P(None, ("fsdp", "ctx"), "tp"),
            P("tp", ("fsdp", "ctx")),
            P(),
            P(None, ("fsdp", "ctx"), "tp"),
            P(),
            P(None, "tp"),
            P(None, "tp"),
            P("tp"),
            P(),
            P(),
            P("tp"),
            P("tp"),
            P("tp"),
            P("tp"),
            P("tp", ("fsdp", "ctx")),
        ),
        check_vma=False,
    )
```

```python
import functools

import jax
import jax.numpy as jnp
from jax import lax
from jax.experimental import pallas as pl
from jax.experimental.pallas import tpu as pltpu
from jax.sharding import PartitionSpec as P

MODEL_WIDTH = 2048
AHEADS = 32
AHD = 128
INNER = 4096
MIXER_HEAD_SIZE = 64
STATE = 128
SPAN = 128


highest = lax.Precision.HIGHEST
epsilon = 1e-05


def matrix_product(left, right):
    return jnp.dot(left, right, preferred_element_type=jnp.float32)


def matrix_product_transposed(left, right):
    return lax.dot_general(
        left, right, (((1,), (1,)), ((), ())), preferred_element_type=jnp.float32
    )


def outer_product_sum(left, right):
    return lax.dot_general(
        left, right, (((0,), (0,)), ((), ())), preferred_element_type=jnp.float32
    )


def rms_scale(values, gain):
    return values * lax.rsqrt(jnp.mean(values * values, axis=-1, keepdims=True) + epsilon) * gain


def gated_gelu(gate_in, up_in):
    return jax.nn.gelu(gate_in, approximate=True) * up_in


def layout(lengths_row, total_rows):
    ends = jnp.cumsum(lengths_row)
    slot_index = jnp.arange(total_rows, dtype=jnp.int32)
    passed = (slot_index[:, None] >= ends[None, :]).astype(jnp.int32)
    segment = jnp.sum(passed, axis=1)
    position = slot_index - jnp.sum(passed * lengths_row[None, :], axis=1)
    return (segment, position, slot_index)


def causal_conv(values, kernel, bias, position):
    total_rows = values.shape[0]
    total = values * kernel[0][None, :] + bias[None, :]
    for lag in range(1, kernel.shape[0]):
        shifted = jnp.concatenate(
            [jnp.zeros((lag, values.shape[1]), values.dtype), values[: total_rows - lag]], axis=0
        )
        keep = (position >= lag).astype(values.dtype)[:, None]
        total = total + shifted * keep * kernel[lag][None, :]
    return jax.nn.silu(total)


def rotate(values, position):
    half_dim = values.shape[-1] // 2
    inverse = 10000.0 ** (-jnp.arange(half_dim, dtype=jnp.float32) / half_dim)
    angle = position.astype(jnp.float32)[:, None] * inverse[None, :]
    cosine = jnp.cos(angle)[:, None, :]
    sine_part = jnp.sin(angle)[:, None, :]
    first_half = values[..., :half_dim]
    second_half = values[..., half_dim:]
    return jnp.concatenate(
        [
            first_half * cosine - second_half * sine_part,
            second_half * cosine + first_half * sine_part,
        ],
        axis=-1,
    )


def attend_core(pair_data, values, segment, slot_index, position, block_rows):
    group_row_block = values.shape[0]
    count_of_heads = values.shape[1] // AHD
    paired = pair_data.reshape(group_row_block, count_of_heads, 2, AHD)
    queries = rotate(paired[:, :, 0], position).astype(jnp.bfloat16)
    keys_all = rotate(paired[:, :, 1], position).astype(jnp.bfloat16)
    vals_all = values.reshape(group_row_block, count_of_heads, AHD).astype(jnp.bfloat16)
    scaling = AHD ** (-0.5)
    block_count = group_row_block // block_rows

    def one_block(inputs):
        query_part, query_seg, query_slot = inputs
        scores = (
            jnp.einsum("qhd,khd->hqk", query_part, keys_all, preferred_element_type=jnp.float32)
            * scaling
        )
        allowed = (query_seg[:, None] == segment[None, :]) & (
            query_slot[:, None] >= slot_index[None, :]
        )
        scores = jnp.where(allowed[None], scores, -1e30)
        weights = jnp.exp(scores)
        weights_low = (weights / jnp.sum(weights, axis=-1, keepdims=True)).astype(jnp.bfloat16)
        return jnp.einsum("hqk,khd->qhd", weights_low, vals_all, preferred_element_type=jnp.float32)

    mapped = lax.map(
        jax.checkpoint(one_block),
        (
            queries.reshape(block_count, block_rows, count_of_heads, AHD),
            segment.reshape(block_count, block_rows),
            slot_index.reshape(block_count, block_rows),
        ),
    )
    return mapped.reshape(group_row_block, count_of_heads * AHD)


def state_scan(inputs_x, step_size, b_mat, c_mat, decay_rate, segment):
    total_rows, count_of_heads, head_dim = inputs_x.shape
    spans = total_rows // SPAN
    log_decay = step_size * decay_rate[None, :]
    weighted = inputs_x * step_size[:, :, None]
    causal = jnp.arange(SPAN)[:, None] >= jnp.arange(SPAN)[None, :]

    def advance(carried_in, inputs):
        memory, last_segment = carried_in
        decay_part, weighted_part, b_part, c_part, seg_part = inputs
        running = jnp.cumsum(decay_part, axis=0)
        same_seq = (seg_part[:, None] == seg_part[None, :]) & causal
        intersection = jnp.dot(c_part, b_part.T, precision=highest)
        log_gap = jnp.where(same_seq[:, :, None], running[:, None, :] - running[None, :, :], 0.0)
        mixing = jnp.where(same_seq[:, :, None], jnp.exp(log_gap), 0.0) * intersection[:, :, None]
        output = jnp.einsum("tsh,shp->thp", mixing, weighted_part, precision=highest)
        carried = (seg_part == last_segment).astype(jnp.float32)
        reach_back = jnp.exp(running) * carried[:, None]
        output = (
            output
            + jnp.einsum("tn,hpn->thp", c_part, memory, precision=highest) * reach_back[:, :, None]
        )
        tail_seg = seg_part[-1]
        toward = (
            jnp.exp(running[-1][None, :] - running)
            * (seg_part == tail_seg).astype(jnp.float32)[:, None]
        )
        next_state = jnp.einsum("sh,shp,sn->hpn", toward, weighted_part, b_part, precision=highest)
        keep_all = jnp.exp(running[-1]) * (tail_seg == last_segment).astype(jnp.float32)
        next_state = next_state + memory * keep_all[:, None, None]
        return ((next_state, tail_seg), output)

    initial = (jnp.zeros((count_of_heads, head_dim, b_mat.shape[1]), jnp.float32), jnp.int32(-1))
    pieces = (
        log_decay.reshape(spans, SPAN, count_of_heads),
        weighted.reshape(spans, SPAN, count_of_heads, head_dim),
        b_mat.reshape(spans, SPAN, -1),
        c_mat.reshape(spans, SPAN, -1),
        segment.reshape(spans, SPAN),
    )
    last_state, outputs = lax.scan(jax.checkpoint(advance), initial, pieces)
    return outputs.reshape(total_rows, count_of_heads, head_dim)


def mamba_core(
    inner_in,
    step_in,
    bc_post,
    bias_in,
    decay_in,
    skip_weight_input,
    kernel_in,
    conv_bias_in,
    position,
    segment,
):
    group_row_block = inner_in.shape[0]
    count_of_heads = step_in.shape[1]
    mixer_result = causal_conv(inner_in, kernel_in, conv_bias_in, position)
    reshaped_tensor = mixer_result.reshape(group_row_block, count_of_heads, MIXER_HEAD_SIZE)
    step_size = jax.nn.softplus(step_in + bias_in[None, :])
    scan_result = state_scan(
        reshaped_tensor,
        step_size,
        bc_post[:, :STATE],
        bc_post[:, STATE:],
        -jnp.exp(decay_in),
        segment,
    )
    return (scan_result + skip_weight_input[None, :, None] * reshaped_tensor).reshape(
        group_row_block, count_of_heads * MIXER_HEAD_SIZE
    )


def collect(first_part, second_part):
    return (
        lax.all_gather(first_part, ("fsdp", "ctx"), axis=1, tiled=True),
        lax.all_gather(second_part, ("fsdp", "ctx"), axis=1, tiled=True),
    )


def collect_again(first_part, second_part):
    return (
        lax.all_gather(first_part, ("fsdp", "ctx"), axis=1, tiled=True),
        lax.all_gather(second_part, ("fsdp", "ctx"), axis=1, tiled=True),
    )


def tensor_sum(partial_sum):
    return lax.psum(partial_sum, "tp")


def tensor_pair(first_part, second_part):
    return (
        lax.psum(first_part.astype(jnp.bfloat16), "tp").astype(jnp.float32),
        lax.psum(second_part.astype(jnp.bfloat16), "tp").astype(jnp.float32),
    )


def heads_pair(first_part, second_part):
    return (
        lax.all_to_all(first_part, "ctx", split_axis=1, concat_axis=0, tiled=True),
        lax.all_to_all(second_part, "ctx", split_axis=1, concat_axis=0, tiled=True),
    )


def heads_one(values):
    return lax.all_to_all(values, "ctx", split_axis=1, concat_axis=0, tiled=True)


def tokens_pair(first_part, second_part):
    return (
        lax.all_to_all(first_part, "ctx", split_axis=0, concat_axis=1, tiled=True),
        lax.all_to_all(second_part, "ctx", split_axis=0, concat_axis=1, tiled=True),
    )


def tokens_one(values):
    return lax.all_to_all(values, "ctx", split_axis=0, concat_axis=1, tiled=True)


def per_device(
    hidden,
    embeds,
    cotangent,
    lengths,
    attention_norm_gain,
    adapter_down_maps,
    query_key_value_weight,
    adapter_up_maps,
    attention_output_weight,
    feedforward_norm_gain,
    gate_up_weight,
    down_weight,
    mixer_norm_gain,
    mixer_gate_input_weight,
    state_map_weight,
    step_size_weight,
    mixer_input_taps,
    mixer_input_tap_bias,
    state_map_taps,
    state_map_tap_bias,
    step_size_bias,
    log_decay_rate,
    head_skip_weight,
    gated_norm_gain,
    mixer_output_weight,
):
    tok_rows = hidden.shape[0]
    ctx_size = lax.axis_size("ctx")
    ctx_index = lax.axis_index("ctx")
    group_row_block = tok_rows * ctx_size
    block_rows = group_row_block // max(1, group_row_block // 1024)
    segment, position, slot_index = layout(lengths[0], group_row_block)
    hidden_f = hidden.astype(jnp.float32)
    embeds_f = embeds.astype(jnp.float32)
    attention_block_full, attn_out = collect(query_key_value_weight, attention_output_weight)
    joined = jnp.concatenate([hidden_f, embeds_f], axis=1)
    normed_a, norm_a_back = jax.vjp(rms_scale, joined, attention_norm_gain)
    attention_input_reduced = normed_a.astype(jnp.bfloat16)
    middle_reduced_precision = [
        matrix_product(attention_input_reduced, adapter_down_maps[group_member]).astype(
            jnp.bfloat16
        )
        for group_member in range(3)
    ]
    projected_input = [
        (
            matrix_product(attention_input_reduced, attention_block_full[group_member])
            + matrix_product(middle_reduced_precision[group_member], adapter_up_maps[group_member])
        ).astype(jnp.bfloat16)
        for group_member in range(3)
    ]
    tp_heads = projected_input[0].shape[1] // AHD
    pair_data = jnp.stack(
        [
            projected_input[0].reshape(tok_rows, tp_heads, AHD),
            projected_input[1].reshape(tok_rows, tp_heads, AHD),
        ],
        axis=2,
    ).reshape(tok_rows, tp_heads * 2 * AHD)
    pair_heads, value_heads = heads_pair(pair_data, projected_input[2])
    attn_core, attn_pull = jax.vjp(
        lambda pairs_in, values_in: attend_core(
            pairs_in, values_in, segment, slot_index, position, block_rows
        ),
        pair_heads.astype(jnp.float32),
        value_heads.astype(jnp.float32),
    )
    attn_tokens = tokens_one(attn_core.astype(jnp.bfloat16))
    after_attn = hidden_f + tensor_sum(matrix_product(attn_tokens, attn_out))
    mlp_big, mlp_down = collect(gate_up_weight, down_weight)
    normed_m, norm_m_back = jax.vjp(rms_scale, after_attn, feedforward_norm_gain)
    xm_low = normed_m.astype(jnp.bfloat16)
    gate_pre = matrix_product(xm_low, mlp_big[0])
    up_pre = matrix_product(xm_low, mlp_big[1])
    activated, act_back = jax.vjp(gated_gelu, gate_pre, up_pre)
    hid_low = activated.astype(jnp.bfloat16)
    after_mlp = after_attn + tensor_sum(matrix_product(hid_low, mlp_down))
    mamba_big, mamba_out = collect(mixer_gate_input_weight, mixer_output_weight)
    normed_n, norm_n_back = jax.vjp(rms_scale, after_mlp, mixer_norm_gain)
    xn_low = normed_n.astype(jnp.bfloat16)
    gate_z = matrix_product(xn_low, mamba_big[0])
    inner_x = matrix_product(xn_low, mamba_big[1]).astype(jnp.bfloat16)
    step_raw = matrix_product(xn_low, step_size_weight).astype(jnp.bfloat16)
    bc_low = matrix_product(xn_low, state_map_weight).astype(jnp.bfloat16)
    x_heads, step_heads = heads_pair(inner_x, step_raw)
    bc_group = lax.all_gather(bc_low, "ctx", axis=0, tiled=True)
    bc_post, bc_conv_pull = jax.vjp(
        lambda values_in, kernel_in, conv_bias_in: causal_conv(
            values_in, kernel_in, conv_bias_in, position
        ),
        bc_group.astype(jnp.float32),
        state_map_taps,
        state_map_tap_bias,
    )
    heads_on_device_share = step_heads.shape[1]
    start_offset = ctx_index * heads_on_device_share
    channel_count_here = heads_on_device_share * MIXER_HEAD_SIZE
    channel_offset_begin = start_offset * MIXER_HEAD_SIZE
    bias_local = lax.dynamic_slice_in_dim(step_size_bias, start_offset, heads_on_device_share)
    decay_local = lax.dynamic_slice_in_dim(log_decay_rate, start_offset, heads_on_device_share)
    skip_local = lax.dynamic_slice_in_dim(head_skip_weight, start_offset, heads_on_device_share)
    kernel_local = lax.dynamic_slice_in_dim(
        mixer_input_taps, channel_offset_begin, channel_count_here, 1
    )
    conv_bias_local = lax.dynamic_slice_in_dim(
        mixer_input_tap_bias, channel_offset_begin, channel_count_here, 0
    )
    scan_out, scan_pull = jax.vjp(
        lambda xs_in, step_in, bcp_in, bias_in, decay_in, skip_weight_input, kernel_in, conv_bias_in: mamba_core(
            xs_in,
            step_in,
            bcp_in,
            bias_in,
            decay_in,
            skip_weight_input,
            kernel_in,
            conv_bias_in,
            position,
            segment,
        ),
        x_heads.astype(jnp.float32),
        step_heads.astype(jnp.float32),
        bc_post,
        bias_local,
        decay_local,
        skip_local,
        kernel_local,
        conv_bias_local,
    )
    y_tokens = tokens_one(scan_out.astype(jnp.bfloat16)).astype(jnp.float32)
    silu_z = jax.nn.silu(gate_z)
    gated = y_tokens * silu_z
    total_sq = tensor_sum(jnp.sum(gated * gated, axis=1))
    inverse = lax.rsqrt(total_sq / INNER + epsilon)[:, None]
    yn_low = (gated * inverse * gated_norm_gain).astype(jnp.bfloat16)
    after_mamba = after_mlp + tensor_sum(matrix_product(yn_low, mamba_out))
    result = after_mamba.astype(jnp.bfloat16)
    grad_out = cotangent.astype(jnp.float32)
    mamba_big, mamba_out = collect_again(mixer_gate_input_weight, mixer_output_weight)
    d_yn = matrix_product_transposed(cotangent, mamba_out)
    grad_w_out = outer_product_sum(yn_low, cotangent)
    gain_part = d_yn * gated_norm_gain
    cross = tensor_sum(jnp.sum(gain_part * gated, axis=1))
    grad_g_gate = jnp.sum(d_yn * gated * inverse, axis=0)
    d_gated = gain_part * inverse - gated * inverse**3 * (cross / INNER)[:, None]
    d_y = (d_gated * silu_z).astype(jnp.bfloat16)
    sigmoid_z = jax.nn.sigmoid(gate_z)
    d_z = (d_gated * y_tokens * sigmoid_z * (1.0 + gate_z * (1.0 - sigmoid_z))).astype(jnp.bfloat16)
    dy_heads = heads_one(d_y)
    (
        d_xs,
        d_step,
        d_bc_post,
        grad_bias_local,
        grad_decay_local,
        grad_skip_local,
        grad_kernel_local,
        grad_conv_bias_local,
    ) = scan_pull(dy_heads.astype(jnp.float32))
    d_xs_tok, d_step_tok = tokens_pair(d_xs.astype(jnp.bfloat16), d_step.astype(jnp.bfloat16))
    d_bc_ctx = lax.psum(d_bc_post.astype(jnp.bfloat16), "ctx").astype(jnp.float32)
    dxn_part = (
        matrix_product_transposed(d_z, mamba_big[0])
        + matrix_product_transposed(d_xs_tok, mamba_big[1])
        + matrix_product_transposed(d_step_tok, step_size_weight)
    )
    grad_w_zx = jnp.stack([outer_product_sum(xn_low, d_z), outer_product_sum(xn_low, d_xs_tok)])
    grad_w_dt = outer_product_sum(xn_low, d_step_tok)
    dxn_sum, d_bc_full = tensor_pair(dxn_part, d_bc_ctx)
    d_bc_pre = bc_conv_pull(d_bc_full)[0]
    d_bc_mine = lax.dynamic_slice_in_dim(d_bc_pre, ctx_index * tok_rows, tok_rows, 0)
    own_rows = (slot_index // tok_rows == ctx_index).astype(jnp.float32)[:, None]
    ignored_part, grad_conv_bc, grad_conv_bc_bias = bc_conv_pull(d_bc_full * own_rows)
    d_bc_low = d_bc_mine.astype(jnp.bfloat16)
    dxn_total = dxn_sum + matrix_product_transposed(d_bc_low, state_map_weight)
    grad_w_bc = outer_product_sum(xn_low, d_bc_low)
    d_norm_n, grad_g_mamba = norm_n_back(dxn_total)
    d_after_mlp = grad_out + d_norm_n
    shard_heads = step_size_bias.shape[0]
    zero_heads = jnp.zeros((shard_heads,), jnp.float32)
    grad_dt_bias = lax.dynamic_update_slice_in_dim(zero_heads, grad_bias_local, start_offset, 0)
    grad_a_log = lax.dynamic_update_slice_in_dim(zero_heads, grad_decay_local, start_offset, 0)
    grad_d_skip = lax.dynamic_update_slice_in_dim(zero_heads, grad_skip_local, start_offset, 0)
    grad_conv_x = lax.dynamic_update_slice_in_dim(
        jnp.zeros(mixer_input_taps.shape, jnp.float32), grad_kernel_local, channel_offset_begin, 1
    )
    grad_conv_x_bias = lax.dynamic_update_slice_in_dim(
        jnp.zeros(mixer_input_tap_bias.shape, jnp.float32),
        grad_conv_bias_local,
        channel_offset_begin,
        0,
    )
    mlp_big, mlp_down = collect_again(gate_up_weight, down_weight)
    d_mlp_low = d_after_mlp.astype(jnp.bfloat16)
    d_hid = matrix_product_transposed(d_mlp_low, mlp_down)
    grad_w_down = outer_product_sum(hid_low, d_mlp_low)
    d_gate, d_up = act_back(d_hid)
    d_gate_low = d_gate.astype(jnp.bfloat16)
    d_up_low = d_up.astype(jnp.bfloat16)
    d_xm = tensor_sum(
        matrix_product_transposed(d_gate_low, mlp_big[0])
        + matrix_product_transposed(d_up_low, mlp_big[1])
    )
    grad_w_gu = jnp.stack(
        [outer_product_sum(xm_low, d_gate_low), outer_product_sum(xm_low, d_up_low)]
    )
    d_norm_m, grad_g_mlp = norm_m_back(d_xm)
    d_after_attn = d_after_mlp + d_norm_m
    attention_block_full, attn_out = collect_again(query_key_value_weight, attention_output_weight)
    d_attn_low = d_after_attn.astype(jnp.bfloat16)
    d_tokens = matrix_product_transposed(d_attn_low, attn_out).astype(jnp.bfloat16)
    grad_w_o = outer_product_sum(attn_tokens, d_attn_low)
    d_core = heads_one(d_tokens)
    d_pairs, d_values = attn_pull(d_core.astype(jnp.float32))
    d_pair_tok, d_value_tok = tokens_pair(
        d_pairs.astype(jnp.bfloat16), d_values.astype(jnp.bfloat16)
    )
    d_paired = d_pair_tok.reshape(tok_rows, tp_heads, 2, AHD)
    projection_gradient = [
        d_paired[:, :, 0].reshape(tok_rows, tp_heads * AHD),
        d_paired[:, :, 1].reshape(tok_rows, tp_heads * AHD),
        d_value_tok,
    ]
    dxa_part = (
        matrix_product_transposed(projection_gradient[0], attention_block_full[0])
        + matrix_product_transposed(projection_gradient[1], attention_block_full[1])
        + matrix_product_transposed(projection_gradient[2], attention_block_full[2])
    )
    dmid_part = jnp.concatenate(
        [
            matrix_product_transposed(
                projection_gradient[group_member], adapter_up_maps[group_member]
            )
            for group_member in range(3)
        ],
        axis=1,
    )
    grad_w_qkv = jnp.stack(
        [
            outer_product_sum(attention_input_reduced, projection_gradient[group_member])
            for group_member in range(3)
        ]
    )
    adapter_up_gradient = jnp.stack(
        [
            outer_product_sum(
                middle_reduced_precision[group_member], projection_gradient[group_member]
            )
            for group_member in range(3)
        ]
    )
    dxa_sum, dmid_sum = tensor_pair(dxa_part, dmid_part)
    dmid_low = dmid_sum.astype(jnp.bfloat16)
    rank_column_block = adapter_down_maps.shape[2]
    middle_gradient_pieces = [
        dmid_low[:, group_member * rank_column_block : (group_member + 1) * rank_column_block]
        for group_member in range(3)
    ]
    dxa_total = (
        dxa_sum
        + matrix_product_transposed(middle_gradient_pieces[0], adapter_down_maps[0])
        + matrix_product_transposed(middle_gradient_pieces[1], adapter_down_maps[1])
        + matrix_product_transposed(middle_gradient_pieces[2], adapter_down_maps[2])
    )
    adapter_down_gradient = jnp.stack(
        [
            outer_product_sum(attention_input_reduced, middle_gradient_pieces[group_member])
            for group_member in range(3)
        ]
    )
    d_joined, grad_g_attn = norm_a_back(dxa_total)
    d_hidden = d_after_attn + d_joined[:, :MODEL_WIDTH]
    d_embeds = d_joined[:, MODEL_WIDTH:]
    grad_w_qkv, grad_w_o, grad_w_gu, grad_w_down, grad_w_zx, grad_w_out = (
        lax.psum_scatter(
            grad_w_qkv.astype(jnp.bfloat16), ("fsdp", "ctx"), scatter_dimension=1, tiled=True
        ).astype(jnp.float32),
        lax.psum_scatter(
            grad_w_o.astype(jnp.bfloat16), ("fsdp", "ctx"), scatter_dimension=1, tiled=True
        ).astype(jnp.float32),
        lax.psum_scatter(
            grad_w_gu.astype(jnp.bfloat16), ("fsdp", "ctx"), scatter_dimension=1, tiled=True
        ).astype(jnp.float32),
        lax.psum_scatter(
            grad_w_down.astype(jnp.bfloat16), ("fsdp", "ctx"), scatter_dimension=1, tiled=True
        ).astype(jnp.float32),
        lax.psum_scatter(
            grad_w_zx.astype(jnp.bfloat16), ("fsdp", "ctx"), scatter_dimension=1, tiled=True
        ).astype(jnp.float32),
        lax.psum_scatter(
            grad_w_out.astype(jnp.bfloat16), ("fsdp", "ctx"), scatter_dimension=1, tiled=True
        ).astype(jnp.float32),
    )
    (
        grad_g_attn,
        adapter_down_gradient,
        adapter_up_gradient,
        grad_g_mlp,
        grad_g_mamba,
        grad_w_bc,
        grad_w_dt,
        grad_conv_x,
        grad_conv_x_bias,
        grad_conv_bc,
        grad_conv_bc_bias,
        grad_dt_bias,
        grad_a_log,
        grad_d_skip,
        grad_g_gate,
    ) = (
        lax.psum(grad_g_attn.astype(jnp.bfloat16), ("fsdp", "ctx")).astype(jnp.float32),
        lax.psum(adapter_down_gradient.astype(jnp.bfloat16), ("fsdp", "ctx")).astype(jnp.float32),
        lax.psum(adapter_up_gradient.astype(jnp.bfloat16), ("fsdp", "ctx")).astype(jnp.float32),
        lax.psum(grad_g_mlp.astype(jnp.bfloat16), ("fsdp", "ctx")).astype(jnp.float32),
        lax.psum(grad_g_mamba.astype(jnp.bfloat16), ("fsdp", "ctx")).astype(jnp.float32),
        lax.psum(grad_w_bc.astype(jnp.bfloat16), ("fsdp", "ctx")).astype(jnp.float32),
        lax.psum(grad_w_dt.astype(jnp.bfloat16), ("fsdp", "ctx")).astype(jnp.float32),
        lax.psum(grad_conv_x.astype(jnp.bfloat16), ("fsdp", "ctx")).astype(jnp.float32),
        lax.psum(grad_conv_x_bias.astype(jnp.bfloat16), ("fsdp", "ctx")).astype(jnp.float32),
        lax.psum(grad_conv_bc.astype(jnp.bfloat16), ("fsdp", "ctx")).astype(jnp.float32),
        lax.psum(grad_conv_bc_bias.astype(jnp.bfloat16), ("fsdp", "ctx")).astype(jnp.float32),
        lax.psum(grad_dt_bias.astype(jnp.bfloat16), ("fsdp", "ctx")).astype(jnp.float32),
        lax.psum(grad_a_log.astype(jnp.bfloat16), ("fsdp", "ctx")).astype(jnp.float32),
        lax.psum(grad_d_skip.astype(jnp.bfloat16), ("fsdp", "ctx")).astype(jnp.float32),
        lax.psum(grad_g_gate.astype(jnp.bfloat16), ("fsdp", "ctx")).astype(jnp.float32),
    )
    return (
        result,
        d_hidden,
        d_embeds,
        grad_g_attn,
        adapter_down_gradient,
        grad_w_qkv,
        adapter_up_gradient,
        grad_w_o,
        grad_g_mlp,
        grad_w_gu,
        grad_w_down,
        grad_g_mamba,
        grad_w_zx,
        grad_w_bc,
        grad_w_dt,
        grad_conv_x,
        grad_conv_x_bias,
        grad_conv_bc,
        grad_conv_bc_bias,
        grad_dt_bias,
        grad_a_log,
        grad_d_skip,
        grad_g_gate,
        grad_w_out,
    )


PLANE = ("fsdp", "ctx")
EVERY = ("fsdp", "ctx", "tp")


MESH = pl.DeviceIdType.MESH
IN_VMEM = pl.BlockSpec(memory_space=pltpu.VMEM)
IN_HBM = pl.BlockSpec(memory_space=pltpu.HBM)
IN_SMEM = pl.BlockSpec(memory_space=pltpu.SMEM)
DMA = pltpu.SemaphoreType.DMA
GATHER_SHARES = (2,) * 8
SUM_SHARES = (2,) * 8
GATHER_LAGS = (0, 2, 4)
SUM_LAGS = (0, 1, 3, 5, 7)


class Place:
    def __init__(self, sizes):
        self.groups, self.ctx, self.tp = sizes
        g, c, t = (lax.axis_index(name) for name in EVERY)
        y, k = t // 2, lax.rem(t, 2)
        self.g, self.c, self.t, self.y, self.k = g, c, t, y, k
        self.core = (g, c, y * 2 + 1 - k)
        self.side_y = (g, c, (1 - y) * 2 + k)
        self.side_x = (g, 1 - c, t)
        self.line = [(lax.rem(g + d, self.groups), c, t) for d in range(1, self.groups)]
        self.plane = self.groups * self.ctx
        self.index = g * self.ctx + c

    def plane_peer(self, d):
        other = lax.rem(self.index + d, self.plane)
        return other, (other // self.ctx, lax.rem(other, self.ctx), self.t)

    def plane_source(self, d):
        return lax.rem(self.index + self.plane - d, self.plane)


def greet(devices):
    barrier = pltpu.get_barrier_semaphore()
    for device in devices:
        pl.semaphore_signal(barrier, inc=1, device_id=device, device_id_type=MESH)
    pl.semaphore_wait(barrier, len(devices))


def remote(src, dst, send_sem, recv_sem, device):
    return pltpu.make_async_remote_copy(
        src_ref=src,
        dst_ref=dst,
        send_sem=send_sem,
        recv_sem=recv_sem,
        device_id=device,
        device_id_type=MESH,
    )


def cut(ref, axis, index, width):
    if axis is None:
        return ref
    at = [slice(None)] * len(ref.shape)
    start = index * width
    if width % 128 == 0:
        start = pl.multiple_of(start, 128)
    at[axis] = pl.ds(start, width)
    return ref.at[tuple(at)]


class Moves:
    def __init__(self, place, specs, sources, targets, stages, send, recv, local):
        self.sent = []
        self.place, self.specs = place, specs
        self.sources, self.targets = sources, targets
        self.stages, self.send, self.recv, self.local = stages, send, recv, local

    def part(self, i, to, origin):
        split, join = self.specs[i]
        src, dst = self.sources[i], self.targets[i]
        n = self.place.plane
        if split is None:
            return src, cut(dst, join, origin, src.shape[join])
        return (
            cut(src, split, to, src.shape[split] // n),
            cut(dst, join, origin, dst.shape[join] // n),
        )

    def start(self, first=0):
        place = self.place
        self.loads, self.queue = [], []
        for i in range(len(self.specs)):
            self.queue += [(i, d) for d in range(1, place.plane)]
            src, _ = self.part(i, place.index, place.index)
            load = pltpu.make_async_copy(src, self.stages[i], self.local.at[i, 0])
            load.start()
            self.loads.append(load)
        self.queue.sort(key=lambda one: one[1] % place.ctx != first)

    def issue(self, count):
        for i, d in self.queue[:count]:
            other, device = self.place.plane_peer(d)
            src, dst = self.part(i, other, self.place.index)
            copy = remote(src, dst, self.send.at[i, d], self.recv.at[i, d], device)
            copy.start()
            self.sent.append(copy)
        self.queue = self.queue[count:]

    def settle(self):
        self.stores = []
        for i, load in enumerate(self.loads):
            load.wait()
            _, dst = self.part(i, self.place.index, self.place.index)
            store = pltpu.make_async_copy(self.stages[i], dst, self.local.at[i, 1])
            store.start()
            self.stores.append(store)

    def finish(self):
        place = self.place
        for i in range(len(self.specs)):
            for d in range(1, place.plane):
                _, device = place.plane_peer(d)
                src, dst = self.part(i, place.index, place.plane_source(d))
                remote(src, dst, self.send.at[i, d], self.recv.at[i, d], device).wait_recv()
        for copy in self.sent:
            copy.wait_send()
        for store in self.stores:
            store.wait()


def moves_setup(moves, plane):
    outs, scratch = [], []
    for array, split, join in moves:
        shape = list(array.shape)
        part = list(array.shape)
        if split is not None:
            part[split] //= plane
            shape[split] //= plane
        shape[join] *= plane
        outs.append(jax.ShapeDtypeStruct(tuple(shape), array.dtype))
        scratch.append(pltpu.VMEM(tuple(part), array.dtype))
    n = len(moves)
    if n:
        scratch += [DMA((n, plane)), DMA((n, plane)), DMA((n, 2))]
    return outs, scratch


class Gather:
    def __init__(self, place, x, o, pieces, sems):
        self.place, self.x, self.o, self.pieces, self.sems = place, x, o, pieces, sems
        self.n = len(pieces)
        self.first, self.second = [], [None] * self.n
        self.third, self.fourth = [None] * self.n, [None] * self.n

    def line_copy(self, q, d, owner):
        place, cols = self.place, pl.ds(*self.pieces[q])
        return remote(
            self.x.at[:, cols],
            self.o.at[owner, place.c, place.y, place.k, :, cols],
            self.sems[0].at[q, d],
            self.sems[1].at[q, d],
            place.line[d],
        )

    def begin(self):
        place = self.place
        own_at = self.o.at[place.g, place.c, place.y, place.k]
        own = pltpu.make_async_copy(self.x, own_at, self.sems[8])
        own.start()
        for q in range(self.n):
            for d in range(place.groups - 1):
                copy = self.line_copy(q, d, place.g)
                copy.start()
                self.first.append(copy)
        own.wait()

    def to_side(self, q):
        place = self.place
        for d in range(place.groups - 1):
            source = lax.rem(place.g + place.groups - d - 1, place.groups)
            self.line_copy(q, d, source).wait_recv()
        part = self.o.at[:, place.c, place.y, place.k, :, pl.ds(*self.pieces[q])]
        device = place.side_y if q % 2 == 0 else place.side_x
        self.second[q] = remote(part, part, self.sems[2].at[q], self.sems[3].at[q], device)
        self.second[q].start()

    def to_other_side(self, q):
        place, cols = self.place, pl.ds(*self.pieces[q])
        self.second[q].wait_recv()
        if q % 2 == 0:
            part, device = self.o.at[:, place.c, :, place.k, :, cols], place.side_x
        else:
            part, device = self.o.at[:, :, place.y, place.k, :, cols], place.side_y
        self.third[q] = remote(part, part, self.sems[4].at[q], self.sems[5].at[q], device)
        self.third[q].start()

    def to_core(self, q):
        place = self.place
        self.third[q].wait_recv()
        part = self.o.at[:, :, :, place.k, :, pl.ds(*self.pieces[q])]
        self.fourth[q] = remote(part, part, self.sems[6].at[q], self.sems[7].at[q], place.core)
        self.fourth[q].start()

    def steps(self):
        return pipelined(self.n, (self.to_side, self.to_other_side, self.to_core), GATHER_LAGS)

    def end(self):
        for copy in self.fourth:
            copy.wait_recv()
        for copy in self.first + self.second + self.third + self.fourth:
            copy.wait_send()


def pipelined(count, stages, lags):
    def step(at):
        for stage, lag in zip(stages, lags):
            if 0 <= at - lag < count:
                stage(at - lag)

    return [functools.partial(step, at) for at in range(count + max(lags))]


def gather_sems(n, groups):
    return [DMA((n, groups - 1)), DMA((n, groups - 1))] + [DMA((n,))] * 6 + [DMA]


class Scatter:
    def __init__(self, place, make, pieces, bufs, acc, sems):
        self.place, self.make, self.pieces, self.bufs, self.acc = place, make, pieces, bufs, acc
        self.sems = sems
        n = len(pieces)
        self.n = n
        self.c1, self.c2, self.c3, self.c4 = [None] * n, [None] * n, [None] * n, [None] * n

    def to_core(self, q):
        theirs, mine, b1 = self.bufs[:3]
        cols, k = pl.ds(*self.pieces[q]), self.place.k
        self.make(q, theirs, 1 - k)
        self.c1[q] = remote(
            theirs.at[..., cols],
            b1.at[..., cols],
            self.sems[0].at[q],
            self.sems[1].at[q],
            self.place.core,
        )
        self.c1[q].start()
        self.make(q, mine, k)

    def to_side(self, q):
        _, mine, b1, b2, _, _ = self.bufs
        place, cols = self.place, pl.ds(*self.pieces[q])
        f32 = jnp.float32
        self.c1[q].wait_recv()
        b1[..., cols] = (b1[..., cols].astype(f32) + mine[..., cols].astype(f32)).astype(b1.dtype)
        if q % 2 == 0:
            part, device = b1.at[:, :, 1 - place.y, :, cols], place.side_y
        else:
            part, device = b1.at[:, 1 - place.c, :, :, cols], place.side_x
        self.c2[q] = remote(
            part, b2.at[:, :, :, cols], self.sems[2].at[q], self.sems[3].at[q], device
        )
        self.c2[q].start()

    def to_other_side(self, q):
        _, _, b1, b2, b3, _ = self.bufs
        place, cols = self.place, pl.ds(*self.pieces[q])
        f32 = jnp.float32
        self.c2[q].wait_recv()
        own = b1[:, :, place.y, :, cols] if q % 2 == 0 else b1[:, place.c, :, :, cols]
        b2[:, :, :, cols] = (b2[:, :, :, cols].astype(f32) + own.astype(f32)).astype(b2.dtype)
        if q % 2 == 0:
            part, device = b2.at[:, 1 - place.c, :, cols], place.side_x
        else:
            part, device = b2.at[:, 1 - place.y, :, cols], place.side_y
        self.c3[q] = remote(part, b3.at[:, :, cols], self.sems[4].at[q], self.sems[5].at[q], device)
        self.c3[q].start()

    def along_line(self, q):
        _, _, _, b2, b3, b4 = self.bufs
        place, cols = self.place, pl.ds(*self.pieces[q])
        f32 = jnp.float32
        self.c3[q].wait_recv()
        own = b2[:, place.c, :, cols] if q % 2 == 0 else b2[:, place.y, :, cols]
        b3[:, :, cols] = (b3[:, :, cols].astype(f32) + own.astype(f32)).astype(b3.dtype)
        self.c4[q] = []
        for d in range(place.groups - 1):
            to = lax.rem(place.g + d + 1, place.groups)
            copy = remote(
                b3.at[to, :, cols],
                b4.at[d, :, cols],
                self.sems[6].at[q, d],
                self.sems[7].at[q, d],
                place.line[d],
            )
            copy.start()
            self.c4[q].append(copy)

    def land(self, q):
        b3, b4 = self.bufs[4:]
        cols = pl.ds(*self.pieces[q])
        total = b3[self.place.g, :, cols].astype(jnp.float32)
        for d in range(self.place.groups - 1):
            self.c4[q][d].wait_recv()
            total = total + b4[d, :, cols].astype(jnp.float32)
        self.acc[:, cols] = total

    def steps(self):
        stages = (self.to_core, self.to_side, self.to_other_side, self.along_line, self.land)
        return pipelined(self.n, stages, SUM_LAGS)

    def end(self):
        for q in range(self.n):
            for copy in [self.c1[q], self.c2[q], self.c3[q]] + self.c4[q]:
                copy.wait_send()


class SmallSum:
    def __init__(self, place, x, o, zbuf, buf, zs, zr, ss, rs):
        self.place, self.x, self.o, self.zbuf, self.buf = place, x, o, zbuf, buf
        self.zs, self.zr, self.ss, self.rs = zs, zr, ss, rs

    def begin(self):
        self.copies = []
        for d, device in enumerate(self.place.line):
            copy = remote(self.x, self.zbuf.at[d], self.zs.at[d], self.zr.at[d], device)
            copy.start()
            self.copies.append(copy)

    def line(self):
        place, groups = self.place, self.place.groups
        for copy in self.copies:
            copy.wait_recv()
        total = None
        for owner in range(groups):
            part = self.x[...]
            for d in range(groups - 1):
                source = lax.rem(place.g + groups - d - 1, groups)
                part = jnp.where(source == owner, self.zbuf[d], part)
            total = part if total is None else total + part
        self.o[...] = total
        self.send(0)

    def send(self, i):
        device = (self.place.side_x, self.place.side_y, self.place.core)[i]
        self.copy = remote(self.o, self.buf.at[i], self.ss.at[i], self.rs.at[i], device)
        self.copy.start()

    def add(self, i):
        self.copy.wait_recv()
        self.copy.wait_send()
        self.o[...] = self.o[...] + self.buf[i]
        if i < 2:
            self.send(i + 1)

    def steps(self):
        return [self.line] + [functools.partial(self.add, i) for i in range(3)]

    def end(self):
        for copy in self.copies:
            copy.wait_send()


def small_scratch(shape, groups):
    f32 = jnp.float32
    return [
        pltpu.VMEM((groups - 1, *shape), f32),
        pltpu.VMEM((3, *shape), f32),
        DMA((groups - 1,)),
        DMA((groups - 1,)),
        DMA((3,)),
        DMA((3,)),
    ]


def weave(*streams):
    found = []
    rounds = max((start + len(steps) for start, steps in streams), default=0)
    for at in range(rounds):
        for start, steps in streams:
            if 0 <= at - start < len(steps):
                found.append(steps[at - start])
    return found


def scatter_scratch(n, groups, rows, width):
    bf16 = jnp.bfloat16
    bufs = [
        pltpu.VMEM((groups, 2, 2, rows, width), bf16),
        pltpu.VMEM((groups, 2, 2, rows, width), bf16),
        pltpu.VMEM((groups, 2, 2, rows, width), bf16),
        pltpu.VMEM((groups, 2, rows, width), bf16),
        pltpu.VMEM((groups, rows, width), bf16),
        pltpu.VMEM((groups - 1, rows, width), bf16),
        pltpu.VMEM((rows, width), jnp.float32),
    ]
    sems = [DMA((n,))] * 6 + [DMA((n, groups - 1))] * 2
    return bufs, sems


def rms_rows(x, gain):
    return x * lax.rsqrt(jnp.mean(x * x, axis=-1, keepdims=True) + epsilon) * gain


def rms_back(x, gain, grad):
    inverse = lax.rsqrt(jnp.mean(x * x, axis=-1, keepdims=True) + epsilon)
    scaled = grad * gain
    along = jnp.mean(scaled * x, axis=-1, keepdims=True)
    d_gain = jnp.sum(grad * x * inverse, axis=0, keepdims=True)
    return scaled * inverse - x * inverse**3 * along, d_gain


NT = (((1,), (1,)), ((), ()))
NN = (((1,), (0,)), ((), ()))


class Summed:
    def __init__(self, sizes, products, extra=None, pieces=SUM_SHARES):
        self.sizes, self.products, self.extra = sizes, products, extra
        self.rows = products[0][0].shape[0] // (sizes[0] * sizes[1] * sizes[2])
        self.width = products[0][1].shape[-2 if products[0][3] else -1]
        self.more = 0 if extra is None else extra.shape[1]
        self.rights, self.places = [], []
        for _, right, _, _ in products:
            found = [i for i, other in enumerate(self.rights) if other is right]
            self.places.append(found[0] if found else len(self.rights))
            if not found:
                self.rights.append(right)
        at, self.pieces = 0, []
        for share in pieces:
            self.pieces.append((at, self.width * share // 16))
            at += self.width * share // 16
        if self.more:
            self.pieces.append((self.width, self.more))
        self.bufs, self.sems = scatter_scratch(
            len(self.pieces), sizes[0], self.rows, self.width + self.more
        )

    def operands(self):
        groups, ctx, tp = self.sizes
        split = (groups, ctx, tp // 2, 2, self.rows)
        found = [product[0].reshape(*split, product[0].shape[1]) for product in self.products]
        found += self.rights
        if self.more:
            found.append(self.extra.reshape(*split, self.more))
        return found

    def stage(self, place, inputs, scratch):
        count = len(self.products)
        lefts, rights = inputs[:count], inputs[count : count + len(self.rights)]
        bufs, sems = scratch[: len(self.bufs)], scratch[len(self.bufs) :]
        groups, ctx, tp = self.sizes

        def make(q, into, core):
            at, size = self.pieces[q]
            if at >= self.width:
                into[..., pl.ds(at, size)] = inputs[-1][:, :, :, core]
                return

            def block(i, _):
                total = None
                for left, where, (_, _, lead, transposed) in zip(
                    lefts, self.places, self.products
                ):
                    right = rights[where] if lead is None else rights[where].at[lead]
                    a = left[i, :, :, core]
                    a = a.reshape(-1, a.shape[-1])
                    some = right[pl.ds(at, size), :] if transposed else right[:, pl.ds(at, size)]
                    part = lax.dot_general(
                        a, some, NT if transposed else NN, preferred_element_type=jnp.float32
                    )
                    total = part if total is None else total + part
                into[i, :, :, :, pl.ds(at, size)] = total.astype(into.dtype).reshape(
                    ctx, tp // 2, self.rows, size
                )
                return 0

            lax.fori_loop(0, groups, block, 0)

        return Scatter(place, make, self.pieces, bufs[:-1], bufs[-1], sems)


def exchange(
    sizes,
    number,
    summed,
    finish,
    finish_args,
    finish_outs,
    gathered,
    moves,
    plan=(3,),
    start_also=5,
    start_second=10,
    also_gather=None,
    also_sum=None,
    tail=0,
    small=0,
):
    groups, ctx, tp = sizes
    f32, bf16 = jnp.float32, jnp.bfloat16
    rows = summed.rows
    out_pieces = gather_pieces(gathered)
    move_outs, move_scratch = moves_setup(moves, groups * ctx)
    n_moves = len(moves)
    move_specs = [(split, join) for _, split, join in moves]
    S = jax.ShapeDtypeStruct

    operands, in_specs, out_shape, out_specs, scratch = [], [], [], [], []

    def add_in(arrays, spec=IN_VMEM):
        at = len(operands)
        operands.extend(arrays)
        in_specs.extend([spec] * len(arrays))
        return slice(at, len(operands))

    def add_out(shapes, spec=IN_VMEM):
        at = len(out_shape)
        out_shape.extend(shapes)
        out_specs.extend([spec] * len(shapes))
        return slice(at, len(out_shape))

    def add_scratch(shapes):
        at = len(scratch)
        scratch.extend(shapes)
        return slice(at, len(scratch))

    in_sum = add_in(summed.operands())
    in_args = add_in(list(finish_args))
    o_main = add_out([S((groups, ctx, tp // 2, 2, rows, gathered), bf16)])
    o_finish = add_out([S(shape, f32) for shape in finish_outs])
    s_sum = add_scratch(summed.bufs + summed.sems)
    s_main = add_scratch(
        [pltpu.VMEM((rows, gathered), bf16)] + gather_sems(len(out_pieces), groups)
    )
    if also_gather is not None:
        also_pieces = gather_pieces(also_gather.shape[1])
        in_also = add_in([also_gather])
        o_also = add_out([S((groups, ctx, tp // 2, 2, rows, also_gather.shape[1]), bf16)])
        s_also = add_scratch(gather_sems(len(also_pieces), groups))
    if also_sum is not None:
        second, second_finish, second_args, second_out = also_sum
        in_second, in_second_args = add_in(second.operands()), add_in(second_args)
        o_second = add_out([second_out])
        s_second = add_scratch(second.bufs + second.sems)
    if tail:
        o_tail = add_out([S((tp // 2, 2, rows, tail), bf16)])
        s_tail = add_scratch([pltpu.VMEM((rows, tail), bf16)] + [DMA] * 5)
    if small:
        o_small = add_out([S((1, small), f32)])
        s_small = add_scratch([pltpu.VMEM((1, small), f32)] + small_scratch((1, small), groups))
    in_moves = add_in([array for array, _, _ in moves], IN_HBM)
    o_moves = add_out(move_outs, IN_HBM)
    s_moves = add_scratch(move_scratch)

    def kernel(*refs):
        ins = refs[: len(operands)]
        outs = refs[len(operands) : len(operands) + len(out_shape)]
        scr = refs[len(operands) + len(out_shape) :]
        place = Place(sizes)
        devices = [place.core, place.side_y]
        if n_moves:
            devices += [place.plane_peer(d)[1] for d in range(1, place.plane)]
        else:
            devices += [place.side_x] + place.line
        greet(devices)
        carried = None
        if n_moves:
            parts = scr[s_moves]
            carried = Moves(
                place, move_specs, ins[in_moves], outs[o_moves], parts[:n_moves], *parts[n_moves:]
            )
            carried.start()
        main_sum = summed.stage(place, ins[in_sum], scr[s_sum])
        low, *main_sems = scr[s_main]
        main_gather = Gather(place, low, outs[o_main][0], out_pieces, main_sems)
        streams = [(0, main_sum.steps())]
        ends = [main_sum, main_gather]
        if also_gather is not None:
            side_gather = Gather(place, ins[in_also][0], outs[o_also][0], also_pieces, scr[s_also])
            side_gather.begin()
            streams.append((start_also, side_gather.steps()))
            ends.append(side_gather)
        later = []
        if also_sum is not None:
            side_sum = second.stage(place, ins[in_second], scr[s_second])
            side_steps = side_sum.steps()
            ready = max(0, min(len(side_steps), len(summed.pieces) + SUM_LAGS[-1] - start_second))
            streams.append((start_second, side_steps[:ready]))
            later.append((0, side_steps[ready:]))
            ends.append(side_sum)
        total = n_moves * (groups * ctx - 1)
        steps = weave(*streams)
        for i, step in enumerate(steps):
            if carried is not None and i < len(plan):
                carried.issue(plan[i])
            step()
        if carried is not None:
            carried.settle()
        low_tail = scr[s_tail][0] if tail else None
        low_small = scr[s_small][0] if small else None
        finish(place, main_sum.acc, ins[in_args], outs[o_finish], low, low_tail, low_small)
        main_gather.begin()
        if small:
            small_sum = SmallSum(place, low_small, outs[o_small][0], *scr[s_small][1:])
            small_sum.begin()
            later.append((1, small_sum.steps()))
            ends.append(small_sum)
        if tail:
            ys, yr, ks, kr, own_sem = scr[s_tail][1:]
            y, k, spot = place.y, place.k, outs[o_tail][0]
            own = pltpu.make_async_copy(low_tail, spot.at[y, k], own_sem)
            own.start()
            to_y = remote(low_tail, spot.at[y, k], ys, yr, place.side_y)
            to_y.start()
            own.wait()
        steps = weave((0, main_gather.steps()), *later)
        if carried is not None:
            carried.issue(total)
        for step in steps:
            step()
        if tail:
            to_y.wait_recv()
            part = spot.at[:, k]
            to_k = remote(part, part, ks, kr, place.core)
            to_k.start()
            to_k.wait_recv()
            to_y.wait_send()
            to_k.wait_send()
        if also_sum is not None:
            second_finish(side_sum.acc, ins[in_second_args], outs[o_second][0])
        for stage in ends:
            stage.end()
        if carried is not None:
            carried.finish()

    results = pl.pallas_call(
        kernel,
        out_shape=out_shape,
        in_specs=in_specs,
        out_specs=out_specs,
        scratch_shapes=scratch,
        name=f"exchange_{number}",
        compiler_params=pltpu.CompilerParams(
            collective_id=number, has_side_effects=True, vmem_limit_bytes=62 * 2**20
        ),
    )(*operands)
    found = {"gathered": results[0].reshape(-1, gathered), "finish": results[o_finish]}
    if also_gather is not None:
        found["also"] = results[o_also][0].reshape(-1, also_gather.shape[1])
    if also_sum is not None:
        found["second"] = results[o_second][0]
    if tail:
        found["tail"] = results[o_tail][0].reshape(-1, tail)
    if small:
        found["small"] = results[o_small][0]
    found["moves"] = results[o_moves]
    return found


def gather_pieces(width):
    if width < 1024:
        return [(0, width)]
    whole = width // 2048 * 2048
    at, found = 0, []
    for share in GATHER_SHARES:
        found.append((at, whole * share // 16))
        at += whole * share // 16
    if width > whole:
        found.append((whole, width - whole))
    return found


def opening(sizes, number, hidden, embeds, lengths, gain, down_maps, moves):
    groups, ctx, tp = sizes
    f32, bf16 = jnp.float32, jnp.bfloat16
    rows = hidden.shape[0] // tp
    half = hidden.shape[1]
    rank = down_maps.shape[2]
    mids = down_maps.shape[0] * rank
    width = 2 * half + mids + 128
    out_pieces = gather_pieces(width)
    move_outs, move_scratch = moves_setup(moves, groups * ctx)
    move_specs = [(split, join) for _, split, join in moves]
    n_moves = len(moves)

    def kernel(*refs):
        hid, emb, lens, gain_ref, down_ref = refs[:5]
        refs = list(refs[5:])
        sources = refs[:n_moves]
        o = refs[n_moves]
        targets = refs[n_moves + 1 : 2 * n_moves + 1]
        rest = refs[2 * n_moves + 1 :]
        low, gs = rest[0], rest[1:10]
        stages = rest[10 : 10 + n_moves]
        send, recv, local = rest[10 + n_moves :]
        place = Place(sizes)
        greet(
            [place.core, place.side_y]
            + [place.plane_peer(d)[1] for d in range(1, place.plane)]
        )
        carried = Moves(place, move_specs, sources, targets, stages, send, recv, local)
        carried.start(1)
        mine = pl.ds(pl.multiple_of(place.t * rows, 16), rows)
        a, b = hid[mine, :].astype(f32), emb[mine, :].astype(f32)
        squares = jnp.sum(a * a, axis=1, keepdims=True) + jnp.sum(b * b, axis=1, keepdims=True)
        inverse = lax.rsqrt(squares / (2 * half) + epsilon)
        low[:, :half] = (a * inverse * gain_ref[:, :half]).astype(bf16)
        low[:, half : 2 * half] = (b * inverse * gain_ref[:, half:]).astype(bf16)
        for j in range(down_maps.shape[0]):
            at = 2 * half + j * rank
            low[:, at : at + rank] = lax.dot_general(
                low[:, : 2 * half], down_ref[j], NN, preferred_element_type=f32
            ).astype(bf16)
        slot = lax.broadcasted_iota(jnp.int32, (rows, 128), 0)
        slot = slot + (place.c * tp + place.t) * rows
        lane = lax.broadcasted_iota(jnp.int32, (rows, 128), 1)
        segment, position, end = jnp.zeros_like(slot), slot, 0
        for i in range(lengths.shape[1]):
            length = lens[0, i]
            end = end + length
            passed = (slot >= end).astype(jnp.int32)
            segment = segment + passed
            position = position - passed * length
        marks = jnp.where(lane == 0, segment, position)
        low[:, 2 * half + mids :] = marks.astype(f32).astype(bf16)
        gather = Gather(place, low, o, out_pieces, gs)
        gather.begin()
        carried.issue(len(carried.queue))
        for step in gather.steps():
            step()
        carried.settle()
        gather.end()
        carried.finish()

    S = jax.ShapeDtypeStruct
    results = pl.pallas_call(
        kernel,
        out_shape=[S((groups, ctx, tp // 2, 2, rows, width), bf16)] + move_outs,
        in_specs=[IN_VMEM, IN_VMEM, IN_SMEM, IN_VMEM, IN_VMEM] + [IN_HBM] * n_moves,
        out_specs=[IN_VMEM] + [IN_HBM] * n_moves,
        scratch_shapes=[pltpu.VMEM((rows, width), bf16)]
        + gather_sems(len(out_pieces), groups)
        + move_scratch,
        name=f"opening_{number}",
        compiler_params=pltpu.CompilerParams(
            collective_id=number, has_side_effects=True, vmem_limit_bytes=62 * 2**20
        ),
    )(hidden, embeds, lengths, gain.reshape(1, -1), down_maps, *[array for array, _, _ in moves])
    return [results[0].reshape(-1, width)] + list(results[1:])


def sum_small(sizes, number, values):
    def kernel(x, o, *scratch):
        place = Place(sizes)
        greet([place.core, place.side_y, place.side_x] + place.line)
        summing = SmallSum(place, x, o, *scratch)
        summing.begin()
        for step in summing.steps():
            step()
        summing.end()

    return pl.pallas_call(
        kernel,
        out_shape=jax.ShapeDtypeStruct(values.shape, jnp.float32),
        in_specs=[IN_VMEM],
        out_specs=IN_VMEM,
        scratch_shapes=small_scratch(values.shape, sizes[0]),
        name=f"sum_small_{number}",
        compiler_params=pltpu.CompilerParams(collective_id=number, has_side_effects=True),
    )(values)


def own_of(place, ref, rows):
    if ref.shape[0] == rows:
        return ref[...].astype(jnp.float32)
    return ref[pl.ds(pl.multiple_of(place.t * rows, 16), rows), :].astype(jnp.float32)


def finish_forward(place, acc, args, outs, low, low_tail, low_small):
    rest, gain = args
    outs[0][...] = own_of(place, rest, acc.shape[0]) + acc[...]
    low[...] = rms_rows(outs[0][...], gain[...]).astype(jnp.bfloat16)


def finish_mixer_back(place, acc, args, outs, low, low_tail, low_small):
    after_mlp, gain, cot, state_map = args
    width = after_mlp.shape[1]
    low[:, width:] = acc[:, width:].astype(jnp.bfloat16)
    d_normed = acc[:, :width] + lax.dot_general(
        low[:, width:], state_map[...], NT, preferred_element_type=jnp.float32
    )
    d_rows, d_gain = rms_back(after_mlp[...], gain[...], d_normed)
    outs[1][...] = d_gain
    d_rows = cot[...].astype(jnp.float32) + d_rows
    outs[0][...] = d_rows
    low[:, :width] = d_rows.astype(jnp.bfloat16)


def finish_mlp_back(place, acc, args, outs, low, low_tail, low_small):
    after_attn, gain, d_after_mlp = args
    d_rows, d_gain = rms_back(after_attn[...], gain[...], acc[...])
    outs[1][...] = d_gain
    d_rows = d_after_mlp[...] + d_rows
    outs[0][...] = d_rows
    low[...] = d_rows.astype(jnp.bfloat16)


def finish_attention_back(place, acc, args, outs, low, low_tail, low_small):
    hidden, embeds, gain, d_after_attn, down_maps, out_mine, row = args
    half = hidden.shape[1]
    bf16, f32 = jnp.bfloat16, jnp.float32
    low[...] = acc[:, 2 * half :].astype(bf16)
    inputs = [own_of(place, part, acc.shape[0]) for part in (hidden, embeds)]
    squares = sum(jnp.sum(part * part, axis=1, keepdims=True) for part in inputs)
    inverse = lax.rsqrt(squares / (2 * half) + epsilon)
    along = jnp.zeros_like(squares)
    for i, part in enumerate(inputs):
        cols = slice(i * half, (i + 1) * half)
        grad = acc[:, cols]
        for j in range(down_maps.shape[0]):
            rank = down_maps.shape[2]
            grad = grad + lax.dot_general(
                low[:, j * rank : (j + 1) * rank],
                down_maps[j, cols, :],
                NT,
                preferred_element_type=f32,
            )
        acc[:, cols] = grad
        along = along + jnp.sum(grad * gain[:, cols] * part, axis=1, keepdims=True)
    along = along / (2 * half)
    low_tail[:, :half] = out_mine[...]
    low_small[:, 2 * half :] = row[...]
    for i, part in enumerate(inputs):
        cols = slice(i * half, (i + 1) * half)
        grad = acc[:, cols]
        low_small[:, cols] = jnp.sum(grad * part * inverse, axis=0, keepdims=True)
        d_rows = grad * gain[:, cols] * inverse - part * inverse**3 * along
        if i == 0:
            d_rows = d_rows + d_after_attn[...]
        low_tail[:, (i + 1) * half : (i + 2) * half] = d_rows.astype(bf16)


def finish_out(acc, args, out):
    out[...] = (args[0][...] + acc[...]).astype(out.dtype)


def adapter_products(xa, dmid, width):
    block, rank = 512, dmid.shape[1] // 3

    def kernel(a, b, o):
        both = quick(b[...], a[...], TN)
        for j in range(3):
            o[j] = both[j * rank : (j + 1) * rank].T

    return pl.pallas_call(
        kernel,
        out_shape=jax.ShapeDtypeStruct((3, width, rank), jnp.float32),
        grid=(width // block,),
        in_specs=[
            pl.BlockSpec((xa.shape[0], block), lambda i: (0, i)),
            pl.BlockSpec(dmid.shape, lambda i: (0, 0)),
        ],
        out_specs=pl.BlockSpec((3, block, rank), lambda i: (0, i, 0)),
        name="adapter_products",
    )(xa, dmid)


def unpack(packed, parts):
    flat, at, found = packed.reshape(-1), 0, []
    for part in parts:
        found.append(flat[at : at + part.size].reshape(part.shape))
        at += part.size
    return found


TN = (((0,), (0,)), ((), ()))


def exact(left, right, dims):
    return lax.dot_general(left, right, dims, precision=highest, preferred_element_type=jnp.float32)


def quick(left, right, dims):
    return lax.dot_general(left, right, dims, preferred_element_type=jnp.float32)


def down_rows(values, by):
    return pltpu.roll(values, by, 0)


def up_rows(values, by):
    return pltpu.roll(values, values.shape[0] - by, 0)


def taps_forward(values, taps, bias, position):
    total = values * taps[0:1, :] + bias
    for lag in range(1, taps.shape[0]):
        kept = jnp.where(position >= lag, down_rows(values, lag), 0.0)
        total = total + kept * taps[lag : lag + 1, :]
    return total


def taps_backward(d_total, values, taps, position):
    d_values = d_total * taps[0:1, :]
    rows = [jnp.sum(d_total * values, axis=0, keepdims=True)]
    for lag in range(1, taps.shape[0]):
        kept = jnp.where(position >= lag, d_total, 0.0)
        rows.append(jnp.sum(kept * down_rows(values, lag), axis=0, keepdims=True))
        d_values = d_values + up_rows(kept, lag) * taps[lag : lag + 1, :]
    return d_values, rows + [jnp.sum(d_total, axis=0, keepdims=True)]


def silu_slope(values):
    sigmoid = jax.nn.sigmoid(values)
    return sigmoid * (1.0 + values * (1.0 - sigmoid))


class Scan:
    def __init__(self, xs, raw, bc, marks, taps, bias, bc_taps, bc_bias, heads):
        f32 = jnp.float32
        rows, lanes = xs.shape
        self.rows, self.half = rows, lanes // 2
        self.position = marks[:, 1:2].astype(f32)
        self.lane = lax.broadcasted_iota(jnp.int32, (rows, lanes), 1)
        self.xs, self.bc = xs.astype(f32), bc.astype(f32)
        self.pre_x = taps_forward(self.xs, taps, bias, self.position)
        self.pre_bc = taps_forward(self.bc, bc_taps, bc_bias, self.position)
        self.xc, bcc = jax.nn.silu(self.pre_x), jax.nn.silu(self.pre_bc)
        self.b_mat, self.c_mat = bcc[:, :STATE], bcc[:, STATE:]
        self.step_in = raw.astype(f32) + heads[0:1, :]
        self.dt = jax.nn.softplus(self.step_in)
        self.rate = -jnp.exp(heads[1:2, :])
        self.log_decay = self.dt * self.rate
        running, by = self.log_decay, 1
        while by < rows:
            running = running + jnp.where(self.position >= by, down_rows(running, by), 0.0)
            by *= 2
        self.running = running
        self.across = running.T
        row = lax.broadcasted_iota(jnp.int32, (rows, rows), 0)
        col = lax.broadcasted_iota(jnp.int32, (rows, rows), 1)
        first = row.astype(f32) - self.position
        self.same = (col <= row) & (col.astype(f32) >= first)
        self.meet = exact(self.c_mat, self.b_mat, NT)
        self.dt_wide = self.by_head([self.dt[:, h : h + 1] for h in range(2)])
        self.weighted = self.xc * self.dt_wide

    def by_head(self, values):
        return jnp.where(self.lane < self.half, values[0], values[1])

    def in_lane(self, values):
        return jnp.where(self.lane == 0, values[0], jnp.where(self.lane == 1, values[1], 0.0))

    def decay(self, h):
        gap = self.running[:, h : h + 1] - self.across[h : h + 1, :]
        return jnp.where(self.same, jnp.exp(jnp.where(self.same, gap, 0.0)), 0.0)

    def forward(self, skip):
        outs = [exact(self.decay(h) * self.meet, self.weighted, NN) for h in range(2)]
        return self.by_head(outs) + skip * self.xc

    def to_ends(self, values):
        rows = values.shape[0]
        row = lax.broadcasted_iota(jnp.int32, values.shape, 0)
        wide = jnp.broadcast_to(self.position, values.shape)
        by = 1
        while by < rows:
            inside = (up_rows(wide, by) >= by) & (row < rows - by)
            values = values + jnp.where(inside, up_rows(values, by), 0.0)
            by *= 2
        return values


def mixer_forward(xn, cot, marked, mark_block, w_zx, w_step, state_map, w_out, small, bc_small, groups):
    f32, bf16 = jnp.float32, jnp.bfloat16
    total, width = xn.shape
    rows, lanes = total // groups, w_zx.shape[2]
    state2 = state_map.shape[1]

    def kernel(xn_r, cot_r, marks_r, zx_r, st_r, sm_r, wo_r, sml, bsml, z_o, xs_o, raw_o, bc_o, y_o, dyn_o, sums_o):
        x = xn_r[...]
        z = quick(x, zx_r[0], NN)
        xs = quick(x, zx_r[1], NN).astype(bf16)
        raw = quick(x, st_r[...], NN).astype(bf16)
        bc = quick(x, sm_r[...], NN).astype(bf16)
        z_o[...], xs_o[...], raw_o[...], bc_o[...] = z, xs, raw, bc
        scan = Scan(
            xs, raw, bc, marks_r[...].astype(f32), sml[0:4, :], sml[4:5, :], bsml[0:4, :], bsml[4:5, :], sml[8:10, :]
        )
        y = scan.forward(sml[5:6, :]).astype(bf16)
        y_o[...] = y
        gated = y.astype(f32) * jax.nn.silu(z)
        d_yn = quick(cot_r[...], wo_r[...], NT)
        dyn_o[...] = d_yn
        ones = jnp.ones((8, lanes), f32)
        sums_o[0, 0:1] = exact(ones, gated * gated, NT)[0:1]
        sums_o[0, 1:2] = exact(ones, d_yn * sml[6:7, :] * gated, NT)[0:1]

    def by_group(columns):
        return pl.BlockSpec((rows, columns), lambda g: (g, 0))

    def whole(array):
        return pl.BlockSpec(array.shape, lambda g: (0,) * array.ndim)

    S = jax.ShapeDtypeStruct
    return pl.pallas_call(
        kernel,
        grid=(groups,),
        in_specs=[by_group(width), by_group(width), pl.BlockSpec((rows, 128), lambda g: (g, mark_block))]
        + [whole(array) for array in (w_zx, w_step, state_map, w_out, small, bc_small)],
        out_specs=[by_group(lanes)] * 3
        + [by_group(state2), by_group(lanes), by_group(lanes), pl.BlockSpec((1, 2, rows), lambda g: (g, 0, 0))],
        out_shape=[
            S((total, lanes), f32),
            S((total, lanes), bf16),
            S((total, lanes), bf16),
            S((total, state2), bf16),
            S((total, lanes), bf16),
            S((total, lanes), f32),
            S((groups, 2, rows), f32),
        ],
        compiler_params=pltpu.CompilerParams(vmem_limit_bytes=60 * 2**20),
        name="mixer_forward",
    )(xn, cot, marked, w_zx, w_step, state_map, w_out, small, bc_small)


def mixer_backward(xn, cot, marked, mark_block, kept, sums, small, bc_small, groups):
    f32, bf16 = jnp.float32, jnp.bfloat16
    z, xs, raw, bc, y, d_yn = kept
    total, width = xn.shape
    rows, lanes, state2 = total // groups, z.shape[1], bc.shape[1]

    def kernel(
        xn_r, cot_r, marks_r, z_r, xs_r, raw_r, bc_r, y_r, dyn_r, sums_r, sml, bsml,
        dz_o, dxs_o, draw_o, dbc_o, yn_o, gzx_o, gst_o, gout_o, gsm_o, gbc_o, acc_in, acc_out,
    ):
        group = pl.program_id(0)
        scan = Scan(
            xs_r[...], raw_r[...], bc_r[...], marks_r[...].astype(f32),
            sml[0:4, :], sml[4:5, :], bsml[0:4, :], bsml[4:5, :], sml[8:10, :],
        )
        skip, gain = sml[5:6, :], sml[6:7, :]
        sums_wide = [jnp.broadcast_to(sums_r[0, i : i + 1], (128, rows)).T for i in range(2)]
        inverse = lax.rsqrt(sums_wide[0] / INNER + epsilon)
        cross = sums_wide[1] / INNER
        gate, out, d_normed = z_r[...], y_r[...].astype(f32), dyn_r[...]
        silu_z = jax.nn.silu(gate)
        gated = out * silu_z
        yn = (gated * inverse * gain).astype(bf16)
        yn_o[...] = yn
        g_gate = jnp.sum(d_normed * gated * inverse, axis=0, keepdims=True)
        d_gated = d_normed * gain * inverse - gated * inverse**3 * cross
        d_y = (d_gated * silu_z).astype(bf16).astype(f32)
        d_z = (d_gated * out * silu_slope(gate)).astype(bf16)
        dz_o[...] = d_z
        g_skip = jnp.sum(d_y * scan.xc, axis=0, keepdims=True)
        d_weighted, d_meet = jnp.zeros_like(d_y), jnp.zeros_like(scan.meet)
        by_row, by_col = [], []
        for h in range(2):
            mine = (scan.lane < scan.half) if h == 0 else (scan.lane >= scan.half)
            d_head = jnp.where(mine, d_y, 0.0)
            decay = scan.decay(h)
            mixing = decay * scan.meet
            d_mixing = exact(d_head, scan.weighted, NT)
            d_weighted = d_weighted + exact(mixing, d_head, TN)
            d_meet = d_meet + d_mixing * decay
            moved = d_mixing * mixing
            by_row.append(jnp.sum(moved, axis=1, keepdims=True))
            by_col.append(jnp.sum(moved, axis=0, keepdims=True))
        columns = [jnp.broadcast_to(by_col[h], (128, rows)).T for h in range(2)]
        d_running = scan.in_lane([by_row[h] - columns[h] for h in range(2)])
        d_log = scan.to_ends(d_running)
        shared = d_weighted * scan.xc
        d_dt = scan.in_lane(
            [
                jnp.sum(jnp.where(scan.lane < scan.half, shared, 0.0), axis=1, keepdims=True),
                jnp.sum(jnp.where(scan.lane >= scan.half, shared, 0.0), axis=1, keepdims=True),
            ]
        )
        d_step = (d_dt + d_log * scan.rate) * jax.nn.sigmoid(scan.step_in)
        g_bias = jnp.sum(d_step, axis=0, keepdims=True)
        g_decay = jnp.sum(d_log * scan.log_decay, axis=0, keepdims=True)
        d_raw = d_step.astype(bf16)
        draw_o[...] = d_raw
        d_xc = skip * d_y + d_weighted * scan.dt_wide
        d_xs, g_taps = taps_backward(
            d_xc * silu_slope(scan.pre_x), scan.xs, sml[0:4, :], scan.position
        )
        d_xs = d_xs.astype(bf16)
        dxs_o[...] = d_xs
        d_bcc = jnp.concatenate(
            [exact(d_meet, scan.c_mat, TN), exact(d_meet, scan.b_mat, NN)], axis=1
        )
        d_bc, g_bc_taps = taps_backward(
            d_bcc * silu_slope(scan.pre_bc), scan.bc, bsml[0:4, :], scan.position
        )
        dbc_o[...] = d_bc.astype(bf16)
        in_part = quick(jnp.concatenate([d_z, d_xs, d_raw], axis=1), xn_r[...], TN)
        out_part = quick(yn, cot_r[...], TN)
        blank = jnp.zeros((1, lanes), f32)
        few = jnp.concatenate(
            g_taps + [g_gate, g_bias, g_decay, g_skip] + [blank] * 7, axis=0
        )
        few_bc = jnp.concatenate(g_bc_taps + [jnp.zeros((3, state2), f32)], axis=0)

        @pl.when(group == 0)
        def _():
            acc_in[...], acc_out[...] = in_part, out_part
            gsm_o[...], gbc_o[...] = few, few_bc

        @pl.when(group > 0)
        def _():
            acc_in[...] += in_part
            acc_out[...] += out_part
            gsm_o[...] += few
            gbc_o[...] += few_bc

        @pl.when(group == groups - 1)
        def _():
            for i in range(2):
                gzx_o[i] = acc_in[i * lanes : (i + 1) * lanes, :].T.astype(bf16)
            gst_o[...] = acc_in[2 * lanes : 2 * lanes + 8, :]
            gout_o[...] = acc_out[...].astype(bf16)

    def by_group(columns):
        return pl.BlockSpec((rows, columns), lambda g: (g, 0))

    def whole(shape):
        return pl.BlockSpec(shape, lambda g: (0,) * len(shape))

    S = jax.ShapeDtypeStruct
    return pl.pallas_call(
        kernel,
        grid=(groups,),
        in_specs=[by_group(width), by_group(width), pl.BlockSpec((rows, 128), lambda g: (g, mark_block))]
        + [by_group(array.shape[1]) for array in kept]
        + [pl.BlockSpec((1, 2, rows), lambda g: (g, 0, 0)), whole(small.shape), whole(bc_small.shape)],
        out_specs=[by_group(lanes)] * 3
        + [by_group(state2), by_group(lanes)]
        + [
            whole((2, width, lanes)),
            whole((8, width)),
            whole((lanes, width)),
            whole((16, lanes)),
            whole((8, state2)),
        ],
        out_shape=[
            S((total, lanes), bf16),
            S((total, lanes), bf16),
            S((total, lanes), bf16),
            S((total, state2), bf16),
            S((total, lanes), bf16),
            S((2, width, lanes), bf16),
            S((8, width), f32),
            S((lanes, width), bf16),
            S((16, lanes), f32),
            S((8, state2), f32),
        ],
        scratch_shapes=[pltpu.VMEM((3 * lanes, width), f32), pltpu.VMEM((lanes, width), f32)],
        compiler_params=pltpu.CompilerParams(vmem_limit_bytes=60 * 2**20),
        name="mixer_backward",
    )(xn, cot, marked, z, xs, raw, bc, y, d_yn, sums, small, bc_small)


def swap_halves(values):
    return pltpu.roll(values, values.shape[1] // 2, 1)


def attend_weights(qr, kr, marks, rows):
    f32 = jnp.float32
    row = lax.broadcasted_iota(jnp.int32, (rows, rows), 0)
    col = lax.broadcasted_iota(jnp.int32, (rows, rows), 1)
    first = row.astype(f32) - marks[:, 1:2]
    allowed = (col <= row) & (col.astype(f32) >= first)
    weights = jnp.exp(jnp.where(allowed, quick(qr, kr, NT) * AHD ** (-0.5), -1e30))
    return weights / jnp.sum(weights, axis=-1, keepdims=True)


def attention_forward(xa, width, w_qkv, up_maps, frequencies, groups):
    f32, bf16 = jnp.float32, jnp.bfloat16
    total, columns = xa.shape
    rows, rank = total // groups, up_maps.shape[1]

    def kernel(xa_r, w_r, up_r, freq_r, ao_o, q_o, k_o, v_o, cos_o, sin_o, w_all):
        @pl.when(pl.program_id(0) == 0)
        def _():
            for j in range(3):
                w_all[:, j * AHD : (j + 1) * AHD] = w_r[j]

        marks = xa_r[:, width + 3 * rank :].astype(f32)
        wide = quick(xa_r[:, :width], w_all[...], NN)
        proj = []
        for j in range(3):
            mid = xa_r[:, width + j * rank : width + (j + 1) * rank]
            proj.append((wide[:, j * AHD : (j + 1) * AHD] + quick(mid, up_r[j], NN)).astype(bf16))
        angle = marks[:, 1:2] * freq_r[...]
        lane = lax.broadcasted_iota(jnp.int32, angle.shape, 1)
        cosine, sine = jnp.cos(angle), jnp.sin(angle)
        sine = jnp.where(lane < AHD // 2, -sine, sine)
        cos_o[...], sin_o[...] = cosine, sine
        qr, kr = [
            (piece * cosine + swap_halves(piece) * sine).astype(bf16)
            for piece in (proj[0].astype(f32), proj[1].astype(f32))
        ]
        q_o[...], k_o[...], v_o[...] = qr, kr, proj[2]
        low = attend_weights(qr, kr, marks, rows).astype(bf16)
        ao_o[...] = quick(low, proj[2], NN).astype(bf16)

    def by_group(size):
        return pl.BlockSpec((rows, size), lambda g: (g, 0))

    def whole(array):
        return pl.BlockSpec(array.shape, lambda g: (0,) * array.ndim)

    S = jax.ShapeDtypeStruct
    return pl.pallas_call(
        kernel,
        grid=(groups,),
        in_specs=[by_group(columns), whole(w_qkv), whole(up_maps), whole(frequencies)],
        out_specs=[by_group(AHD)] * 6,
        out_shape=[S((total, AHD), bf16)] * 4 + [S((total, AHD), f32)] * 2,
        scratch_shapes=[pltpu.VMEM((width, 3 * AHD), bf16)],
        compiler_params=pltpu.CompilerParams(vmem_limit_bytes=60 * 2**20),
        name="attention_forward",
    )(xa, w_qkv, up_maps, frequencies)


def attention_backward(d_attn, xa, width, w_o, up_maps, kept, groups):
    f32, bf16 = jnp.float32, jnp.bfloat16
    total, columns = xa.shape
    rows, rank = total // groups, up_maps.shape[1]
    model = d_attn.shape[1]

    def kernel(
        da_r, xa_r, wo_r, up_r, ao_r, q_r, k_r, v_r, cos_r, sin_r,
        dq_o, dk_o, dv_o, dmid_o, gw_o, go_o, gup_o, acc_w, acc_o,
    ):
        group = pl.program_id(0)
        d_rows = da_r[...]
        marks = xa_r[:, width + 3 * rank :].astype(f32)
        d_ao = quick(d_rows, wo_r[...], NT).astype(bf16)
        qr, kr, vals = q_r[...], k_r[...], v_r[...]
        weights = attend_weights(qr, kr, marks, rows)
        d_vals = quick(weights.astype(bf16), d_ao, TN)
        d_weights = quick(d_ao, vals, NT).astype(bf16).astype(f32)
        along = jnp.sum(d_weights * weights, axis=-1, keepdims=True)
        d_scores = (weights * (d_weights - along) * AHD ** (-0.5)).astype(bf16)
        cosine, sine = cos_r[...], sin_r[...]
        pieces = []
        for d_turned in (quick(d_scores, kr, NN), quick(d_scores, qr, TN)):
            d_turned = d_turned.astype(bf16).astype(f32)
            pieces.append((d_turned * cosine + swap_halves(d_turned * sine)).astype(bf16))
        pieces.append(d_vals.astype(bf16))
        for j, out in enumerate((dq_o, dk_o, dv_o)):
            out[...] = pieces[j]
            dmid_o[:, j * rank : (j + 1) * rank] = quick(pieces[j], up_r[j], NT).astype(bf16)
        part = quick(jnp.concatenate(pieces, axis=1), xa_r[:, :width], TN)
        part_o = quick(ao_r[...], d_rows, TN)
        parts_up = [
            quick(xa_r[:, width + j * rank : width + (j + 1) * rank], pieces[j], TN)
            for j in range(3)
        ]

        @pl.when(group == 0)
        def _():
            acc_w[...], acc_o[...] = part, part_o
            for j in range(3):
                gup_o[j] = parts_up[j]

        @pl.when(group > 0)
        def _():
            acc_w[...] += part
            acc_o[...] += part_o
            for j in range(3):
                gup_o[j] += parts_up[j]

        @pl.when(group == groups - 1)
        def _():
            for j in range(3):
                gw_o[j] = acc_w[j * AHD : (j + 1) * AHD, :].T.astype(bf16)
            go_o[...] = acc_o[...].astype(bf16)

    def by_group(size):
        return pl.BlockSpec((rows, size), lambda g: (g, 0))

    def whole(shape):
        return pl.BlockSpec(shape, lambda g: (0,) * len(shape))

    S = jax.ShapeDtypeStruct
    return pl.pallas_call(
        kernel,
        grid=(groups,),
        in_specs=[by_group(model), by_group(columns), whole(w_o.shape), whole(up_maps.shape)]
        + [by_group(AHD)] * 6,
        out_specs=[by_group(AHD)] * 3
        + [by_group(3 * rank)]
        + [whole((3, width, AHD)), whole((AHD, model)), whole((3, rank, AHD))],
        out_shape=[S((total, AHD), bf16)] * 3
        + [
            S((total, 3 * rank), bf16),
            S((3, width, AHD), bf16),
            S((AHD, model), bf16),
            S((3, rank, AHD), f32),
        ],
        scratch_shapes=[pltpu.VMEM((3 * AHD, width), f32), pltpu.VMEM((AHD, model), f32)],
        compiler_params=pltpu.CompilerParams(vmem_limit_bytes=60 * 2**20),
        name="attention_backward",
    )(d_attn, xa, w_o, up_maps, *kept)


def per_device_split(
    hidden,
    embeds,
    cotangent,
    lengths,
    attention_norm_gain,
    adapter_down_maps,
    query_key_value_weight,
    adapter_up_maps,
    attention_output_weight,
    feedforward_norm_gain,
    gate_up_weight,
    down_weight,
    mixer_norm_gain,
    mixer_gate_input_weight,
    state_map_weight,
    step_size_weight,
    mixer_input_taps,
    mixer_input_tap_bias,
    state_map_taps,
    state_map_tap_bias,
    step_size_bias,
    log_decay_rate,
    head_skip_weight,
    gated_norm_gain,
    mixer_output_weight,
):
    bf16, f32 = jnp.bfloat16, jnp.float32
    tp_size, ctx_size, groups = (lax.axis_size(name) for name in ("tp", "ctx", "fsdp"))
    tp_index, ctx_index = lax.axis_index("tp"), lax.axis_index("ctx")
    plane_index = lax.axis_index("fsdp") * ctx_size + ctx_index
    plane_size = groups * ctx_size
    tok_rows = hidden.shape[0]
    mine = tok_rows // tp_size
    group_rows = tok_rows * ctx_size
    start = tp_index * mine

    sizes = (groups, ctx_size, tp_size)

    def own_rows(values):
        return lax.dynamic_slice_in_dim(values, start, mine, 0)

    def own_part(values, axis=0):
        width = values.shape[axis] // plane_size
        return lax.dynamic_slice_in_dim(values, plane_index * width, width, axis)

    width = hidden.shape[1]
    own_shape = (mine, width)
    cot_low = own_rows(cotangent)

    up_maps = own_part(adapter_up_maps, 2)
    w_step = own_part(step_size_weight, 1)
    taps, tap_bias = own_part(mixer_input_taps, 1), own_part(mixer_input_tap_bias)
    step_bias, decay_rate = own_part(step_size_bias), own_part(log_decay_rate)
    skip, gate_gain = own_part(head_skip_weight), own_part(gated_norm_gain)

    rank = adapter_down_maps.shape[2]
    width_a = adapter_down_maps.shape[1]
    xa_wide, w_o, w_qkv = opening(
        sizes,
        1,
        hidden,
        embeds,
        lengths,
        attention_norm_gain,
        adapter_down_maps,
        [(attention_output_weight, 0, 1), (query_key_value_weight, 2, 1)],
    )
    half = AHD // 2
    frequencies = 10000.0 ** (-jnp.arange(half, dtype=f32) / half)
    frequencies = jnp.concatenate([frequencies, frequencies])[None]
    kept_a = attention_forward(xa_wide, width_a, w_qkv, up_maps, frequencies, groups)
    ao_low = kept_a[0]

    gain_m = feedforward_norm_gain.reshape(1, -1)
    found = exchange(
        sizes,
        2,
        Summed(sizes, [(ao_low, w_o, None, False)]),
        finish_forward,
        [hidden, gain_m],
        [own_shape],
        width,
        [(gate_up_weight, 2, 1), (down_weight, 0, 1)],
    )
    xm, (after_attn,), (w_gu, w_down) = found["gathered"], found["finish"], found["moves"]
    gate_pre, up_pre = matrix_product(xm, w_gu[0]), matrix_product(xm, w_gu[1])
    activated, act_back = jax.vjp(gated_gelu, gate_pre, up_pre)
    hid_low = activated.astype(bf16)

    gain_n = mixer_norm_gain.reshape(1, -1)
    found = exchange(
        sizes,
        3,
        Summed(sizes, [(hid_low, w_down, None, False)]),
        finish_forward,
        [after_attn, gain_n],
        [own_shape],
        width,
        [(mixer_gate_input_weight, 2, 1), (mixer_output_weight, 0, 1)],
        plan=(),
        also_gather=cot_low,
    )
    xn, cot, (after_mlp,) = found["gathered"], found["also"], found["finish"]
    w_zx, w_out = found["moves"]
    few = step_bias.shape[0]
    lanes = ((0, 0), (0, 128 - few))
    row_of = lambda part: jnp.pad(part[None], lanes)
    small = jnp.concatenate(
        [
            taps,
            tap_bias[None],
            jnp.repeat(skip, MIXER_HEAD_SIZE)[None],
            gate_gain[None],
            jnp.zeros((1, 128), f32),
            row_of(step_bias),
            row_of(decay_rate),
        ]
    )
    bc_small = jnp.concatenate([state_map_taps, state_map_tap_bias[None]])
    mark_block = (width_a + 3 * rank) // 128
    w_step = jnp.pad(w_step, lanes)
    *kept, sums = mixer_forward(
        xn, cot, xa_wide, mark_block, w_zx, w_step, state_map_weight, w_out, small, bc_small, groups
    )
    sums = sum_small(sizes, 4, sums)
    d_z, d_xs, d_step, d_bc_part, yn_low, grad_w_zx, grad_w_dt, grad_w_out, few_x, few_bc = (
        mixer_backward(xn, cot, xa_wide, mark_block, kept, sums, small, bc_small, groups)
    )
    grad_conv_bc, grad_conv_bc_bias = few_bc[:4], few_bc[4]
    found = exchange(
        sizes,
        5,
        Summed(
            sizes,
            [
                (d_z, w_zx, 0, True),
                (d_xs, w_zx, 1, True),
                (d_step, w_step, None, True),
            ],
            d_bc_part,
        ),
        finish_mixer_back,
        [after_mlp, gain_n, cot_low, state_map_weight],
        [own_shape, gain_n.shape],
        width + d_bc_part.shape[1],
        [(grad_w_zx, 1, 2), (grad_w_out, 1, 0)],
        plan=(6,),
        also_sum=(
            Summed(sizes, [(yn_low, w_out, None, False)]),
            finish_out,
            [after_mlp],
            jax.ShapeDtypeStruct(own_shape, bf16),
        ),
    )
    gathered, (d_after_mlp, grad_g_mamba) = found["gathered"], found["finish"]
    out_mine, (grad_w_zx, grad_w_out) = found["second"], found["moves"]

    d_mlp, d_bc = gathered[:, :width], gathered[:, width:]
    grad_w_bc = outer_product_sum(xn, d_bc)
    grad_w_down = outer_product_sum(hid_low, d_mlp)
    d_gate, d_up = act_back(matrix_product_transposed(d_mlp, w_down))
    d_gate, d_up = d_gate.astype(bf16), d_up.astype(bf16)
    grad_w_gu = jnp.stack(
        [outer_product_sum(xm, d_gate).astype(bf16), outer_product_sum(xm, d_up).astype(bf16)]
    )

    found = exchange(
        sizes,
        6,
        Summed(sizes, [(d_gate, w_gu, 0, True), (d_up, w_gu, 1, True)]),
        finish_mlp_back,
        [after_attn, gain_m, d_after_mlp],
        [own_shape, gain_m.shape],
        width,
        [(grad_w_gu, 1, 2), (grad_w_down.astype(bf16), 1, 0)],
    )
    d_attn, (d_after_attn, grad_g_mlp) = found["gathered"], found["finish"]
    grad_w_gu, grad_w_down = found["moves"]
    *d_proj, dmid_part, grad_w_qkv, grad_w_o, adapter_up_gradient = attention_backward(
        d_attn, xa_wide, width_a, w_o, up_maps, kept_a, groups
    )
    shares = jnp.concatenate([few_x, grad_w_dt[:few].reshape(-1, 128)]).astype(bf16)
    sums = [grad_g_mlp[0], grad_g_mamba[0], grad_conv_bc, grad_conv_bc_bias]
    row = jnp.concatenate([part.reshape(-1) for part in sums])[None]
    found = exchange(
        sizes,
        7,
        Summed(sizes, [(d_proj[j], w_qkv, j, True) for j in range(3)], dmid_part),
        finish_attention_back,
        [
            hidden,
            embeds,
            attention_norm_gain.reshape(1, -1),
            d_after_attn,
            adapter_down_maps,
            out_mine,
            row,
        ],
        [],
        3 * rank,
        [
            (grad_w_qkv, 1, 2),
            (grad_w_o, 1, 0),
            (adapter_up_gradient.astype(bf16), None, 2),
            (shares, None, 1),
        ],
        plan=(5,),
        tail=3 * width,
        small=width_a + row.shape[1],
    )
    dmid, back, row = found["gathered"], found["tail"], found["small"][0]
    grad_w_qkv, grad_w_o, adapter_up_gradient, shared = found["moves"]
    adapter_down_gradient = adapter_products(xa_wide, dmid, width_a)
    result = back[:, :width]
    d_hidden = back[:, width : 2 * width].astype(f32)
    d_embeds = back[:, 2 * width :].astype(f32)
    adapter_up_gradient = adapter_up_gradient.astype(f32)
    shared = shared.astype(f32)
    grad_conv_x, grad_conv_x_bias, grad_g_gate = shared[:4], shared[4], shared[5]
    heads = shared.reshape(-1, plane_size, 128)
    grad_dt_bias = heads[6, :, :few].reshape(-1)
    grad_a_log = heads[7, :, :few].reshape(-1)
    grad_d_skip = heads[8].reshape(plane_size, few, MIXER_HEAD_SIZE).sum(axis=2).reshape(-1)
    grad_w_dt = shared[16:].reshape(few, -1, plane_size, 128).transpose(1, 3, 2, 0)
    grad_w_dt = grad_w_dt.reshape(-1, plane_size * few)
    grad_g_attn = row[:width_a]
    grad_g_mlp, grad_g_mamba, grad_conv_bc, grad_conv_bc_bias = unpack(row[width_a:], sums)

    return (
        result,
        d_hidden,
        d_embeds,
        grad_g_attn,
        adapter_down_gradient,
        grad_w_qkv.astype(f32),
        adapter_up_gradient,
        grad_w_o.astype(f32),
        grad_g_mlp,
        grad_w_gu.astype(f32),
        grad_w_down.astype(f32),
        grad_g_mamba,
        grad_w_zx.astype(f32),
        grad_w_bc,
        grad_w_dt,
        grad_conv_x,
        grad_conv_x_bias,
        grad_conv_bc,
        grad_conv_bc_bias,
        grad_dt_bias,
        grad_a_log,
        grad_d_skip,
        grad_g_gate,
        grad_w_out.astype(f32),
    )


def solution(mesh):
    placed = (
        P(("fsdp", "ctx"), None),
        P(("fsdp", "ctx"), None),
        P(("fsdp", "ctx"), None),
        P("fsdp", None),
        P(),
        P(),
        P(None, ("fsdp", "ctx"), "tp"),
        P(None, None, "tp"),
        P("tp", ("fsdp", "ctx")),
        P(),
        P(None, ("fsdp", "ctx"), "tp"),
        P("tp", ("fsdp", "ctx")),
        P(),
        P(None, ("fsdp", "ctx"), "tp"),
        P(),
        P(None, "tp"),
        P(None, "tp"),
        P("tp"),
        P(),
        P(),
        P("tp"),
        P("tp"),
        P("tp"),
        P("tp"),
        P("tp", ("fsdp", "ctx")),
    )
    devices = mesh.shape["fsdp"] * mesh.shape["ctx"] * mesh.shape["tp"]
    one_head_each = devices == AHEADS and mesh.shape["ctx"] == 2 and mesh.shape["tp"] == 4
    return jax.shard_map(
        per_device_split if one_head_each else per_device,
        mesh=mesh,
        in_specs=placed,
        out_specs=(
            P(("fsdp", "ctx"), None),
            P(("fsdp", "ctx"), None),
            P(("fsdp", "ctx"), None),
            P(),
            P(),
            P(None, ("fsdp", "ctx"), "tp"),
            P(None, None, "tp"),
            P("tp", ("fsdp", "ctx")),
            P(),
            P(None, ("fsdp", "ctx"), "tp"),
            P("tp", ("fsdp", "ctx")),
            P(),
            P(None, ("fsdp", "ctx"), "tp"),
            P(),
            P(None, "tp"),
            P(None, "tp"),
            P("tp"),
            P(),
            P(),
            P("tp"),
            P("tp"),
            P("tp"),
            P("tp"),
            P("tp", ("fsdp", "ctx")),
        ),
        check_vma=False,
    )
```

```python
import functools

import jax
import jax.numpy as jnp
from jax import lax
from jax.experimental import pallas as pl
from jax.experimental.pallas import tpu as pltpu
from jax.sharding import PartitionSpec as P

MODEL_WIDTH = 2048
AHEADS = 32
AHD = 128
INNER = 4096
MIXER_HEAD_SIZE = 64
STATE = 128
SPAN = 128


highest = lax.Precision.HIGHEST
epsilon = 1e-05


def matrix_product(left, right):
    return jnp.dot(left, right, preferred_element_type=jnp.float32)


def matrix_product_transposed(left, right):
    return lax.dot_general(
        left, right, (((1,), (1,)), ((), ())), preferred_element_type=jnp.float32
    )


def outer_product_sum(left, right):
    return lax.dot_general(
        left, right, (((0,), (0,)), ((), ())), preferred_element_type=jnp.float32
    )


def rms_scale(values, gain):
    return values * lax.rsqrt(jnp.mean(values * values, axis=-1, keepdims=True) + epsilon) * gain


def gated_gelu(gate_in, up_in):
    return jax.nn.gelu(gate_in, approximate=True) * up_in


def layout(lengths_row, total_rows):
    ends = jnp.cumsum(lengths_row)
    slot_index = jnp.arange(total_rows, dtype=jnp.int32)
    passed = (slot_index[:, None] >= ends[None, :]).astype(jnp.int32)
    segment = jnp.sum(passed, axis=1)
    position = slot_index - jnp.sum(passed * lengths_row[None, :], axis=1)
    return (segment, position, slot_index)


def causal_conv(values, kernel, bias, position):
    total_rows = values.shape[0]
    total = values * kernel[0][None, :] + bias[None, :]
    for lag in range(1, kernel.shape[0]):
        shifted = jnp.concatenate(
            [jnp.zeros((lag, values.shape[1]), values.dtype), values[: total_rows - lag]], axis=0
        )
        keep = (position >= lag).astype(values.dtype)[:, None]
        total = total + shifted * keep * kernel[lag][None, :]
    return jax.nn.silu(total)


def rotate(values, position):
    half_dim = values.shape[-1] // 2
    inverse = 10000.0 ** (-jnp.arange(half_dim, dtype=jnp.float32) / half_dim)
    angle = position.astype(jnp.float32)[:, None] * inverse[None, :]
    cosine = jnp.cos(angle)[:, None, :]
    sine_part = jnp.sin(angle)[:, None, :]
    first_half = values[..., :half_dim]
    second_half = values[..., half_dim:]
    return jnp.concatenate(
        [
            first_half * cosine - second_half * sine_part,
            second_half * cosine + first_half * sine_part,
        ],
        axis=-1,
    )


def attend_core(pair_data, values, segment, slot_index, position, block_rows):
    group_row_block = values.shape[0]
    count_of_heads = values.shape[1] // AHD
    paired = pair_data.reshape(group_row_block, count_of_heads, 2, AHD)
    queries = rotate(paired[:, :, 0], position).astype(jnp.bfloat16)
    keys_all = rotate(paired[:, :, 1], position).astype(jnp.bfloat16)
    vals_all = values.reshape(group_row_block, count_of_heads, AHD).astype(jnp.bfloat16)
    scaling = AHD ** (-0.5)
    block_count = group_row_block // block_rows

    def one_block(inputs):
        query_part, query_seg, query_slot = inputs
        scores = (
            jnp.einsum("qhd,khd->hqk", query_part, keys_all, preferred_element_type=jnp.float32)
            * scaling
        )
        allowed = (query_seg[:, None] == segment[None, :]) & (
            query_slot[:, None] >= slot_index[None, :]
        )
        scores = jnp.where(allowed[None], scores, -1e30)
        weights = jnp.exp(scores)
        weights_low = (weights / jnp.sum(weights, axis=-1, keepdims=True)).astype(jnp.bfloat16)
        return jnp.einsum("hqk,khd->qhd", weights_low, vals_all, preferred_element_type=jnp.float32)

    mapped = lax.map(
        jax.checkpoint(one_block),
        (
            queries.reshape(block_count, block_rows, count_of_heads, AHD),
            segment.reshape(block_count, block_rows),
            slot_index.reshape(block_count, block_rows),
        ),
    )
    return mapped.reshape(group_row_block, count_of_heads * AHD)


def state_scan(inputs_x, step_size, b_mat, c_mat, decay_rate, segment):
    total_rows, count_of_heads, head_dim = inputs_x.shape
    spans = total_rows // SPAN
    log_decay = step_size * decay_rate[None, :]
    weighted = inputs_x * step_size[:, :, None]
    causal = jnp.arange(SPAN)[:, None] >= jnp.arange(SPAN)[None, :]

    def advance(carried_in, inputs):
        memory, last_segment = carried_in
        decay_part, weighted_part, b_part, c_part, seg_part = inputs
        running = jnp.cumsum(decay_part, axis=0)
        same_seq = (seg_part[:, None] == seg_part[None, :]) & causal
        intersection = jnp.dot(c_part, b_part.T, precision=highest)
        log_gap = jnp.where(same_seq[:, :, None], running[:, None, :] - running[None, :, :], 0.0)
        mixing = jnp.where(same_seq[:, :, None], jnp.exp(log_gap), 0.0) * intersection[:, :, None]
        output = jnp.einsum("tsh,shp->thp", mixing, weighted_part, precision=highest)
        carried = (seg_part == last_segment).astype(jnp.float32)
        reach_back = jnp.exp(running) * carried[:, None]
        output = (
            output
            + jnp.einsum("tn,hpn->thp", c_part, memory, precision=highest) * reach_back[:, :, None]
        )
        tail_seg = seg_part[-1]
        toward = (
            jnp.exp(running[-1][None, :] - running)
            * (seg_part == tail_seg).astype(jnp.float32)[:, None]
        )
        next_state = jnp.einsum("sh,shp,sn->hpn", toward, weighted_part, b_part, precision=highest)
        keep_all = jnp.exp(running[-1]) * (tail_seg == last_segment).astype(jnp.float32)
        next_state = next_state + memory * keep_all[:, None, None]
        return ((next_state, tail_seg), output)

    initial = (jnp.zeros((count_of_heads, head_dim, b_mat.shape[1]), jnp.float32), jnp.int32(-1))
    pieces = (
        log_decay.reshape(spans, SPAN, count_of_heads),
        weighted.reshape(spans, SPAN, count_of_heads, head_dim),
        b_mat.reshape(spans, SPAN, -1),
        c_mat.reshape(spans, SPAN, -1),
        segment.reshape(spans, SPAN),
    )
    last_state, outputs = lax.scan(jax.checkpoint(advance), initial, pieces)
    return outputs.reshape(total_rows, count_of_heads, head_dim)


def mamba_core(
    inner_in,
    step_in,
    bc_post,
    bias_in,
    decay_in,
    skip_weight_input,
    kernel_in,
    conv_bias_in,
    position,
    segment,
):
    group_row_block = inner_in.shape[0]
    count_of_heads = step_in.shape[1]
    mixer_result = causal_conv(inner_in, kernel_in, conv_bias_in, position)
    reshaped_tensor = mixer_result.reshape(group_row_block, count_of_heads, MIXER_HEAD_SIZE)
    step_size = jax.nn.softplus(step_in + bias_in[None, :])
    scan_result = state_scan(
        reshaped_tensor,
        step_size,
        bc_post[:, :STATE],
        bc_post[:, STATE:],
        -jnp.exp(decay_in),
        segment,
    )
    return (scan_result + skip_weight_input[None, :, None] * reshaped_tensor).reshape(
        group_row_block, count_of_heads * MIXER_HEAD_SIZE
    )


def collect(first_part, second_part):
    return (
        lax.all_gather(first_part, ("fsdp", "ctx"), axis=1, tiled=True),
        lax.all_gather(second_part, ("fsdp", "ctx"), axis=1, tiled=True),
    )


def collect_again(first_part, second_part):
    return (
        lax.all_gather(first_part, ("fsdp", "ctx"), axis=1, tiled=True),
        lax.all_gather(second_part, ("fsdp", "ctx"), axis=1, tiled=True),
    )


def tensor_sum(partial_sum):
    return lax.psum(partial_sum, "tp")


def tensor_pair(first_part, second_part):
    return (
        lax.psum(first_part.astype(jnp.bfloat16), "tp").astype(jnp.float32),
        lax.psum(second_part.astype(jnp.bfloat16), "tp").astype(jnp.float32),
    )


def heads_pair(first_part, second_part):
    return (
        lax.all_to_all(first_part, "ctx", split_axis=1, concat_axis=0, tiled=True),
        lax.all_to_all(second_part, "ctx", split_axis=1, concat_axis=0, tiled=True),
    )


def heads_one(values):
    return lax.all_to_all(values, "ctx", split_axis=1, concat_axis=0, tiled=True)


def tokens_pair(first_part, second_part):
    return (
        lax.all_to_all(first_part, "ctx", split_axis=0, concat_axis=1, tiled=True),
        lax.all_to_all(second_part, "ctx", split_axis=0, concat_axis=1, tiled=True),
    )


def tokens_one(values):
    return lax.all_to_all(values, "ctx", split_axis=0, concat_axis=1, tiled=True)


def per_device(
    hidden,
    embeds,
    cotangent,
    lengths,
    attention_norm_gain,
    adapter_down_maps,
    query_key_value_weight,
    adapter_up_maps,
    attention_output_weight,
    feedforward_norm_gain,
    gate_up_weight,
    down_weight,
    mixer_norm_gain,
    mixer_gate_input_weight,
    state_map_weight,
    step_size_weight,
    mixer_input_taps,
    mixer_input_tap_bias,
    state_map_taps,
    state_map_tap_bias,
    step_size_bias,
    log_decay_rate,
    head_skip_weight,
    gated_norm_gain,
    mixer_output_weight,
):
    tok_rows = hidden.shape[0]
    ctx_size = lax.axis_size("ctx")
    ctx_index = lax.axis_index("ctx")
    group_row_block = tok_rows * ctx_size
    block_rows = group_row_block // max(1, group_row_block // 1024)
    segment, position, slot_index = layout(lengths[0], group_row_block)
    hidden_f = hidden.astype(jnp.float32)
    embeds_f = embeds.astype(jnp.float32)
    attention_block_full, attn_out = collect(query_key_value_weight, attention_output_weight)
    joined = jnp.concatenate([hidden_f, embeds_f], axis=1)
    normed_a, norm_a_back = jax.vjp(rms_scale, joined, attention_norm_gain)
    attention_input_reduced = normed_a.astype(jnp.bfloat16)
    middle_reduced_precision = [
        matrix_product(attention_input_reduced, adapter_down_maps[group_member]).astype(
            jnp.bfloat16
        )
        for group_member in range(3)
    ]
    projected_input = [
        (
            matrix_product(attention_input_reduced, attention_block_full[group_member])
            + matrix_product(middle_reduced_precision[group_member], adapter_up_maps[group_member])
        ).astype(jnp.bfloat16)
        for group_member in range(3)
    ]
    tp_heads = projected_input[0].shape[1] // AHD
    pair_data = jnp.stack(
        [
            projected_input[0].reshape(tok_rows, tp_heads, AHD),
            projected_input[1].reshape(tok_rows, tp_heads, AHD),
        ],
        axis=2,
    ).reshape(tok_rows, tp_heads * 2 * AHD)
    pair_heads, value_heads = heads_pair(pair_data, projected_input[2])
    attn_core, attn_pull = jax.vjp(
        lambda pairs_in, values_in: attend_core(
            pairs_in, values_in, segment, slot_index, position, block_rows
        ),
        pair_heads.astype(jnp.float32),
        value_heads.astype(jnp.float32),
    )
    attn_tokens = tokens_one(attn_core.astype(jnp.bfloat16))
    after_attn = hidden_f + tensor_sum(matrix_product(attn_tokens, attn_out))
    mlp_big, mlp_down = collect(gate_up_weight, down_weight)
    normed_m, norm_m_back = jax.vjp(rms_scale, after_attn, feedforward_norm_gain)
    xm_low = normed_m.astype(jnp.bfloat16)
    gate_pre = matrix_product(xm_low, mlp_big[0])
    up_pre = matrix_product(xm_low, mlp_big[1])
    activated, act_back = jax.vjp(gated_gelu, gate_pre, up_pre)
    hid_low = activated.astype(jnp.bfloat16)
    after_mlp = after_attn + tensor_sum(matrix_product(hid_low, mlp_down))
    mamba_big, mamba_out = collect(mixer_gate_input_weight, mixer_output_weight)
    normed_n, norm_n_back = jax.vjp(rms_scale, after_mlp, mixer_norm_gain)
    xn_low = normed_n.astype(jnp.bfloat16)
    gate_z = matrix_product(xn_low, mamba_big[0])
    inner_x = matrix_product(xn_low, mamba_big[1]).astype(jnp.bfloat16)
    step_raw = matrix_product(xn_low, step_size_weight).astype(jnp.bfloat16)
    bc_low = matrix_product(xn_low, state_map_weight).astype(jnp.bfloat16)
    x_heads, step_heads = heads_pair(inner_x, step_raw)
    bc_group = lax.all_gather(bc_low, "ctx", axis=0, tiled=True)
    bc_post, bc_conv_pull = jax.vjp(
        lambda values_in, kernel_in, conv_bias_in: causal_conv(
            values_in, kernel_in, conv_bias_in, position
        ),
        bc_group.astype(jnp.float32),
        state_map_taps,
        state_map_tap_bias,
    )
    heads_on_device_share = step_heads.shape[1]
    start_offset = ctx_index * heads_on_device_share
    channel_count_here = heads_on_device_share * MIXER_HEAD_SIZE
    channel_offset_begin = start_offset * MIXER_HEAD_SIZE
    bias_local = lax.dynamic_slice_in_dim(step_size_bias, start_offset, heads_on_device_share)
    decay_local = lax.dynamic_slice_in_dim(log_decay_rate, start_offset, heads_on_device_share)
    skip_local = lax.dynamic_slice_in_dim(head_skip_weight, start_offset, heads_on_device_share)
    kernel_local = lax.dynamic_slice_in_dim(
        mixer_input_taps, channel_offset_begin, channel_count_here, 1
    )
    conv_bias_local = lax.dynamic_slice_in_dim(
        mixer_input_tap_bias, channel_offset_begin, channel_count_here, 0
    )
    scan_out, scan_pull = jax.vjp(
        lambda xs_in, step_in, bcp_in, bias_in, decay_in, skip_weight_input, kernel_in, conv_bias_in: mamba_core(
            xs_in,
            step_in,
            bcp_in,
            bias_in,
            decay_in,
            skip_weight_input,
            kernel_in,
            conv_bias_in,
            position,
            segment,
        ),
        x_heads.astype(jnp.float32),
        step_heads.astype(jnp.float32),
        bc_post,
        bias_local,
        decay_local,
        skip_local,
        kernel_local,
        conv_bias_local,
    )
    y_tokens = tokens_one(scan_out.astype(jnp.bfloat16)).astype(jnp.float32)
    silu_z = jax.nn.silu(gate_z)
    gated = y_tokens * silu_z
    total_sq = tensor_sum(jnp.sum(gated * gated, axis=1))
    inverse = lax.rsqrt(total_sq / INNER + epsilon)[:, None]
    yn_low = (gated * inverse * gated_norm_gain).astype(jnp.bfloat16)
    after_mamba = after_mlp + tensor_sum(matrix_product(yn_low, mamba_out))
    result = after_mamba.astype(jnp.bfloat16)
    grad_out = cotangent.astype(jnp.float32)
    mamba_big, mamba_out = collect_again(mixer_gate_input_weight, mixer_output_weight)
    d_yn = matrix_product_transposed(cotangent, mamba_out)
    grad_w_out = outer_product_sum(yn_low, cotangent)
    gain_part = d_yn * gated_norm_gain
    cross = tensor_sum(jnp.sum(gain_part * gated, axis=1))
    grad_g_gate = jnp.sum(d_yn * gated * inverse, axis=0)
    d_gated = gain_part * inverse - gated * inverse**3 * (cross / INNER)[:, None]
    d_y = (d_gated * silu_z).astype(jnp.bfloat16)
    sigmoid_z = jax.nn.sigmoid(gate_z)
    d_z = (d_gated * y_tokens * sigmoid_z * (1.0 + gate_z * (1.0 - sigmoid_z))).astype(jnp.bfloat16)
    dy_heads = heads_one(d_y)
    (
        d_xs,
        d_step,
        d_bc_post,
        grad_bias_local,
        grad_decay_local,
        grad_skip_local,
        grad_kernel_local,
        grad_conv_bias_local,
    ) = scan_pull(dy_heads.astype(jnp.float32))
    d_xs_tok, d_step_tok = tokens_pair(d_xs.astype(jnp.bfloat16), d_step.astype(jnp.bfloat16))
    d_bc_ctx = lax.psum(d_bc_post.astype(jnp.bfloat16), "ctx").astype(jnp.float32)
    dxn_part = (
        matrix_product_transposed(d_z, mamba_big[0])
        + matrix_product_transposed(d_xs_tok, mamba_big[1])
        + matrix_product_transposed(d_step_tok, step_size_weight)
    )
    grad_w_zx = jnp.stack([outer_product_sum(xn_low, d_z), outer_product_sum(xn_low, d_xs_tok)])
    grad_w_dt = outer_product_sum(xn_low, d_step_tok)
    dxn_sum, d_bc_full = tensor_pair(dxn_part, d_bc_ctx)
    d_bc_pre = bc_conv_pull(d_bc_full)[0]
    d_bc_mine = lax.dynamic_slice_in_dim(d_bc_pre, ctx_index * tok_rows, tok_rows, 0)
    own_rows = (slot_index // tok_rows == ctx_index).astype(jnp.float32)[:, None]
    ignored_part, grad_conv_bc, grad_conv_bc_bias = bc_conv_pull(d_bc_full * own_rows)
    d_bc_low = d_bc_mine.astype(jnp.bfloat16)
    dxn_total = dxn_sum + matrix_product_transposed(d_bc_low, state_map_weight)
    grad_w_bc = outer_product_sum(xn_low, d_bc_low)
    d_norm_n, grad_g_mamba = norm_n_back(dxn_total)
    d_after_mlp = grad_out + d_norm_n
    shard_heads = step_size_bias.shape[0]
    zero_heads = jnp.zeros((shard_heads,), jnp.float32)
    grad_dt_bias = lax.dynamic_update_slice_in_dim(zero_heads, grad_bias_local, start_offset, 0)
    grad_a_log = lax.dynamic_update_slice_in_dim(zero_heads, grad_decay_local, start_offset, 0)
    grad_d_skip = lax.dynamic_update_slice_in_dim(zero_heads, grad_skip_local, start_offset, 0)
    grad_conv_x = lax.dynamic_update_slice_in_dim(
        jnp.zeros(mixer_input_taps.shape, jnp.float32), grad_kernel_local, channel_offset_begin, 1
    )
    grad_conv_x_bias = lax.dynamic_update_slice_in_dim(
        jnp.zeros(mixer_input_tap_bias.shape, jnp.float32),
        grad_conv_bias_local,
        channel_offset_begin,
        0,
    )
    mlp_big, mlp_down = collect_again(gate_up_weight, down_weight)
    d_mlp_low = d_after_mlp.astype(jnp.bfloat16)
    d_hid = matrix_product_transposed(d_mlp_low, mlp_down)
    grad_w_down = outer_product_sum(hid_low, d_mlp_low)
    d_gate, d_up = act_back(d_hid)
    d_gate_low = d_gate.astype(jnp.bfloat16)
    d_up_low = d_up.astype(jnp.bfloat16)
    d_xm = tensor_sum(
        matrix_product_transposed(d_gate_low, mlp_big[0])
        + matrix_product_transposed(d_up_low, mlp_big[1])
    )
    grad_w_gu = jnp.stack(
        [outer_product_sum(xm_low, d_gate_low), outer_product_sum(xm_low, d_up_low)]
    )
    d_norm_m, grad_g_mlp = norm_m_back(d_xm)
    d_after_attn = d_after_mlp + d_norm_m
    attention_block_full, attn_out = collect_again(query_key_value_weight, attention_output_weight)
    d_attn_low = d_after_attn.astype(jnp.bfloat16)
    d_tokens = matrix_product_transposed(d_attn_low, attn_out).astype(jnp.bfloat16)
    grad_w_o = outer_product_sum(attn_tokens, d_attn_low)
    d_core = heads_one(d_tokens)
    d_pairs, d_values = attn_pull(d_core.astype(jnp.float32))
    d_pair_tok, d_value_tok = tokens_pair(
        d_pairs.astype(jnp.bfloat16), d_values.astype(jnp.bfloat16)
    )
    d_paired = d_pair_tok.reshape(tok_rows, tp_heads, 2, AHD)
    projection_gradient = [
        d_paired[:, :, 0].reshape(tok_rows, tp_heads * AHD),
        d_paired[:, :, 1].reshape(tok_rows, tp_heads * AHD),
        d_value_tok,
    ]
    dxa_part = (
        matrix_product_transposed(projection_gradient[0], attention_block_full[0])
        + matrix_product_transposed(projection_gradient[1], attention_block_full[1])
        + matrix_product_transposed(projection_gradient[2], attention_block_full[2])
    )
    dmid_part = jnp.concatenate(
        [
            matrix_product_transposed(
                projection_gradient[group_member], adapter_up_maps[group_member]
            )
            for group_member in range(3)
        ],
        axis=1,
    )
    grad_w_qkv = jnp.stack(
        [
            outer_product_sum(attention_input_reduced, projection_gradient[group_member])
            for group_member in range(3)
        ]
    )
    adapter_up_gradient = jnp.stack(
        [
            outer_product_sum(
                middle_reduced_precision[group_member], projection_gradient[group_member]
            )
            for group_member in range(3)
        ]
    )
    dxa_sum, dmid_sum = tensor_pair(dxa_part, dmid_part)
    dmid_low = dmid_sum.astype(jnp.bfloat16)
    rank_column_block = adapter_down_maps.shape[2]
    middle_gradient_pieces = [
        dmid_low[:, group_member * rank_column_block : (group_member + 1) * rank_column_block]
        for group_member in range(3)
    ]
    dxa_total = (
        dxa_sum
        + matrix_product_transposed(middle_gradient_pieces[0], adapter_down_maps[0])
        + matrix_product_transposed(middle_gradient_pieces[1], adapter_down_maps[1])
        + matrix_product_transposed(middle_gradient_pieces[2], adapter_down_maps[2])
    )
    adapter_down_gradient = jnp.stack(
        [
            outer_product_sum(attention_input_reduced, middle_gradient_pieces[group_member])
            for group_member in range(3)
        ]
    )
    d_joined, grad_g_attn = norm_a_back(dxa_total)
    d_hidden = d_after_attn + d_joined[:, :MODEL_WIDTH]
    d_embeds = d_joined[:, MODEL_WIDTH:]
    grad_w_qkv, grad_w_o, grad_w_gu, grad_w_down, grad_w_zx, grad_w_out = (
        lax.psum_scatter(
            grad_w_qkv.astype(jnp.bfloat16), ("fsdp", "ctx"), scatter_dimension=1, tiled=True
        ).astype(jnp.float32),
        lax.psum_scatter(
            grad_w_o.astype(jnp.bfloat16), ("fsdp", "ctx"), scatter_dimension=1, tiled=True
        ).astype(jnp.float32),
        lax.psum_scatter(
            grad_w_gu.astype(jnp.bfloat16), ("fsdp", "ctx"), scatter_dimension=1, tiled=True
        ).astype(jnp.float32),
        lax.psum_scatter(
            grad_w_down.astype(jnp.bfloat16), ("fsdp", "ctx"), scatter_dimension=1, tiled=True
        ).astype(jnp.float32),
        lax.psum_scatter(
            grad_w_zx.astype(jnp.bfloat16), ("fsdp", "ctx"), scatter_dimension=1, tiled=True
        ).astype(jnp.float32),
        lax.psum_scatter(
            grad_w_out.astype(jnp.bfloat16), ("fsdp", "ctx"), scatter_dimension=1, tiled=True
        ).astype(jnp.float32),
    )
    (
        grad_g_attn,
        adapter_down_gradient,
        adapter_up_gradient,
        grad_g_mlp,
        grad_g_mamba,
        grad_w_bc,
        grad_w_dt,
        grad_conv_x,
        grad_conv_x_bias,
        grad_conv_bc,
        grad_conv_bc_bias,
        grad_dt_bias,
        grad_a_log,
        grad_d_skip,
        grad_g_gate,
    ) = (
        lax.psum(grad_g_attn.astype(jnp.bfloat16), ("fsdp", "ctx")).astype(jnp.float32),
        lax.psum(adapter_down_gradient.astype(jnp.bfloat16), ("fsdp", "ctx")).astype(jnp.float32),
        lax.psum(adapter_up_gradient.astype(jnp.bfloat16), ("fsdp", "ctx")).astype(jnp.float32),
        lax.psum(grad_g_mlp.astype(jnp.bfloat16), ("fsdp", "ctx")).astype(jnp.float32),
        lax.psum(grad_g_mamba.astype(jnp.bfloat16), ("fsdp", "ctx")).astype(jnp.float32),
        lax.psum(grad_w_bc.astype(jnp.bfloat16), ("fsdp", "ctx")).astype(jnp.float32),
        lax.psum(grad_w_dt.astype(jnp.bfloat16), ("fsdp", "ctx")).astype(jnp.float32),
        lax.psum(grad_conv_x.astype(jnp.bfloat16), ("fsdp", "ctx")).astype(jnp.float32),
        lax.psum(grad_conv_x_bias.astype(jnp.bfloat16), ("fsdp", "ctx")).astype(jnp.float32),
        lax.psum(grad_conv_bc.astype(jnp.bfloat16), ("fsdp", "ctx")).astype(jnp.float32),
        lax.psum(grad_conv_bc_bias.astype(jnp.bfloat16), ("fsdp", "ctx")).astype(jnp.float32),
        lax.psum(grad_dt_bias.astype(jnp.bfloat16), ("fsdp", "ctx")).astype(jnp.float32),
        lax.psum(grad_a_log.astype(jnp.bfloat16), ("fsdp", "ctx")).astype(jnp.float32),
        lax.psum(grad_d_skip.astype(jnp.bfloat16), ("fsdp", "ctx")).astype(jnp.float32),
        lax.psum(grad_g_gate.astype(jnp.bfloat16), ("fsdp", "ctx")).astype(jnp.float32),
    )
    return (
        result,
        d_hidden,
        d_embeds,
        grad_g_attn,
        adapter_down_gradient,
        grad_w_qkv,
        adapter_up_gradient,
        grad_w_o,
        grad_g_mlp,
        grad_w_gu,
        grad_w_down,
        grad_g_mamba,
        grad_w_zx,
        grad_w_bc,
        grad_w_dt,
        grad_conv_x,
        grad_conv_x_bias,
        grad_conv_bc,
        grad_conv_bc_bias,
        grad_dt_bias,
        grad_a_log,
        grad_d_skip,
        grad_g_gate,
        grad_w_out,
    )


PLANE = ("fsdp", "ctx")
EVERY = ("fsdp", "ctx", "tp")


MESH = pl.DeviceIdType.MESH
IN_VMEM = pl.BlockSpec(memory_space=pltpu.VMEM)
IN_HBM = pl.BlockSpec(memory_space=pltpu.HBM)
IN_SMEM = pl.BlockSpec(memory_space=pltpu.SMEM)
DMA = pltpu.SemaphoreType.DMA
GATHER_SHARES = (2,) * 8
SUM_SHARES = (2,) * 8
GATHER_LAGS = (0, 2, 4)
SUM_LAGS = (0, 1, 3, 5, 7)


class Place:
    def __init__(self, sizes):
        self.groups, self.ctx, self.tp = sizes
        g, c, t = (lax.axis_index(name) for name in EVERY)
        y, k = t // 2, lax.rem(t, 2)
        self.g, self.c, self.t, self.y, self.k = g, c, t, y, k
        self.core = (g, c, y * 2 + 1 - k)
        self.side_y = (g, c, (1 - y) * 2 + k)
        self.side_x = (g, 1 - c, t)
        self.line = [(lax.rem(g + d, self.groups), c, t) for d in range(1, self.groups)]
        self.plane = self.groups * self.ctx
        self.index = g * self.ctx + c

    def plane_peer(self, d):
        other = lax.rem(self.index + d, self.plane)
        return other, (other // self.ctx, lax.rem(other, self.ctx), self.t)

    def plane_source(self, d):
        return lax.rem(self.index + self.plane - d, self.plane)


def greet(devices):
    barrier = pltpu.get_barrier_semaphore()
    for device in devices:
        pl.semaphore_signal(barrier, inc=1, device_id=device, device_id_type=MESH)
    pl.semaphore_wait(barrier, len(devices))


def remote(src, dst, send_sem, recv_sem, device):
    return pltpu.make_async_remote_copy(
        src_ref=src,
        dst_ref=dst,
        send_sem=send_sem,
        recv_sem=recv_sem,
        device_id=device,
        device_id_type=MESH,
    )


def cut(ref, axis, index, width):
    if axis is None:
        return ref
    at = [slice(None)] * len(ref.shape)
    start = index * width
    if width % 128 == 0:
        start = pl.multiple_of(start, 128)
    at[axis] = pl.ds(start, width)
    return ref.at[tuple(at)]


class Moves:
    def __init__(self, place, specs, sources, targets, stages, send, recv, local):
        self.sent = []
        self.place, self.specs = place, specs
        self.sources, self.targets = sources, targets
        self.stages, self.send, self.recv, self.local = stages, send, recv, local

    def part(self, i, to, origin):
        split, join = self.specs[i]
        src, dst = self.sources[i], self.targets[i]
        n = self.place.plane
        if split is None:
            return src, cut(dst, join, origin, src.shape[join])
        return (
            cut(src, split, to, src.shape[split] // n),
            cut(dst, join, origin, dst.shape[join] // n),
        )

    def start(self, first=0):
        place = self.place
        self.loads, self.queue = [], []
        for i in range(len(self.specs)):
            self.queue += [(i, d) for d in range(1, place.plane)]
            src, _ = self.part(i, place.index, place.index)
            load = pltpu.make_async_copy(src, self.stages[i], self.local.at[i, 0])
            load.start()
            self.loads.append(load)
        self.queue.sort(key=lambda one: one[1] % place.ctx != first)

    def issue(self, count):
        for i, d in self.queue[:count]:
            other, device = self.place.plane_peer(d)
            src, dst = self.part(i, other, self.place.index)
            copy = remote(src, dst, self.send.at[i, d], self.recv.at[i, d], device)
            copy.start()
            self.sent.append(copy)
        self.queue = self.queue[count:]

    def settle(self):
        self.stores = []
        for i, load in enumerate(self.loads):
            load.wait()
            _, dst = self.part(i, self.place.index, self.place.index)
            store = pltpu.make_async_copy(self.stages[i], dst, self.local.at[i, 1])
            store.start()
            self.stores.append(store)

    def finish(self):
        place = self.place
        for i in range(len(self.specs)):
            for d in range(1, place.plane):
                _, device = place.plane_peer(d)
                src, dst = self.part(i, place.index, place.plane_source(d))
                remote(src, dst, self.send.at[i, d], self.recv.at[i, d], device).wait_recv()
        for copy in self.sent:
            copy.wait_send()
        for store in self.stores:
            store.wait()


def moves_setup(moves, plane):
    outs, scratch = [], []
    for array, split, join in moves:
        shape = list(array.shape)
        part = list(array.shape)
        if split is not None:
            part[split] //= plane
            shape[split] //= plane
        shape[join] *= plane
        outs.append(jax.ShapeDtypeStruct(tuple(shape), array.dtype))
        scratch.append(pltpu.VMEM(tuple(part), array.dtype))
    n = len(moves)
    if n:
        scratch += [DMA((n, plane)), DMA((n, plane)), DMA((n, 2))]
    return outs, scratch


class Gather:
    def __init__(self, place, x, o, pieces, sems):
        self.place, self.x, self.o, self.pieces, self.sems = place, x, o, pieces, sems
        self.n = len(pieces)
        self.first, self.second = [], [None] * self.n
        self.third, self.fourth = [None] * self.n, [None] * self.n

    def line_copy(self, q, d, owner):
        place, cols = self.place, pl.ds(*self.pieces[q])
        return remote(
            self.x.at[:, cols],
            self.o.at[owner, place.c, place.y, place.k, :, cols],
            self.sems[0].at[q, d],
            self.sems[1].at[q, d],
            place.line[d],
        )

    def begin(self):
        place = self.place
        own_at = self.o.at[place.g, place.c, place.y, place.k]
        own = pltpu.make_async_copy(self.x, own_at, self.sems[8])
        own.start()
        for q in range(self.n):
            for d in range(place.groups - 1):
                copy = self.line_copy(q, d, place.g)
                copy.start()
                self.first.append(copy)
        own.wait()

    def to_side(self, q):
        place = self.place
        for d in range(place.groups - 1):
            source = lax.rem(place.g + place.groups - d - 1, place.groups)
            self.line_copy(q, d, source).wait_recv()
        part = self.o.at[:, place.c, place.y, place.k, :, pl.ds(*self.pieces[q])]
        device = place.side_y if q % 2 == 0 else place.side_x
        self.second[q] = remote(part, part, self.sems[2].at[q], self.sems[3].at[q], device)
        self.second[q].start()

    def to_other_side(self, q):
        place, cols = self.place, pl.ds(*self.pieces[q])
        self.second[q].wait_recv()
        if q % 2 == 0:
            part, device = self.o.at[:, place.c, :, place.k, :, cols], place.side_x
        else:
            part, device = self.o.at[:, :, place.y, place.k, :, cols], place.side_y
        self.third[q] = remote(part, part, self.sems[4].at[q], self.sems[5].at[q], device)
        self.third[q].start()

    def to_core(self, q):
        place = self.place
        self.third[q].wait_recv()
        part = self.o.at[:, :, :, place.k, :, pl.ds(*self.pieces[q])]
        self.fourth[q] = remote(part, part, self.sems[6].at[q], self.sems[7].at[q], place.core)
        self.fourth[q].start()

    def steps(self):
        return pipelined(self.n, (self.to_side, self.to_other_side, self.to_core), GATHER_LAGS)

    def end(self):
        for copy in self.fourth:
            copy.wait_recv()
        for copy in self.first + self.second + self.third + self.fourth:
            copy.wait_send()


def pipelined(count, stages, lags):
    def step(at):
        for stage, lag in zip(stages, lags):
            if 0 <= at - lag < count:
                stage(at - lag)

    return [functools.partial(step, at) for at in range(count + max(lags))]


def gather_sems(n, groups):
    return [DMA((n, groups - 1)), DMA((n, groups - 1))] + [DMA((n,))] * 6 + [DMA]


class Scatter:
    def __init__(self, place, make, pieces, bufs, acc, sems):
        self.place, self.make, self.pieces, self.bufs, self.acc = place, make, pieces, bufs, acc
        self.sems = sems
        n = len(pieces)
        self.n = n
        self.c1, self.c2, self.c3, self.c4 = [None] * n, [None] * n, [None] * n, [None] * n

    def to_core(self, q):
        theirs, mine, b1 = self.bufs[:3]
        cols, k = pl.ds(*self.pieces[q]), self.place.k
        self.make(q, theirs, 1 - k)
        self.c1[q] = remote(
            theirs.at[..., cols],
            b1.at[..., cols],
            self.sems[0].at[q],
            self.sems[1].at[q],
            self.place.core,
        )
        self.c1[q].start()
        self.make(q, mine, k)

    def to_side(self, q):
        _, mine, b1, b2, _, _ = self.bufs
        place, cols = self.place, pl.ds(*self.pieces[q])
        f32 = jnp.float32
        self.c1[q].wait_recv()
        b1[..., cols] = (b1[..., cols].astype(f32) + mine[..., cols].astype(f32)).astype(b1.dtype)
        if q % 2 == 0:
            part, device = b1.at[:, :, 1 - place.y, :, cols], place.side_y
        else:
            part, device = b1.at[:, 1 - place.c, :, :, cols], place.side_x
        self.c2[q] = remote(
            part, b2.at[:, :, :, cols], self.sems[2].at[q], self.sems[3].at[q], device
        )
        self.c2[q].start()

    def to_other_side(self, q):
        _, _, b1, b2, b3, _ = self.bufs
        place, cols = self.place, pl.ds(*self.pieces[q])
        f32 = jnp.float32
        self.c2[q].wait_recv()
        own = b1[:, :, place.y, :, cols] if q % 2 == 0 else b1[:, place.c, :, :, cols]
        b2[:, :, :, cols] = (b2[:, :, :, cols].astype(f32) + own.astype(f32)).astype(b2.dtype)
        if q % 2 == 0:
            part, device = b2.at[:, 1 - place.c, :, cols], place.side_x
        else:
            part, device = b2.at[:, 1 - place.y, :, cols], place.side_y
        self.c3[q] = remote(part, b3.at[:, :, cols], self.sems[4].at[q], self.sems[5].at[q], device)
        self.c3[q].start()

    def along_line(self, q):
        _, _, _, b2, b3, b4 = self.bufs
        place, cols = self.place, pl.ds(*self.pieces[q])
        f32 = jnp.float32
        self.c3[q].wait_recv()
        own = b2[:, place.c, :, cols] if q % 2 == 0 else b2[:, place.y, :, cols]
        b3[:, :, cols] = (b3[:, :, cols].astype(f32) + own.astype(f32)).astype(b3.dtype)
        self.c4[q] = []
        for d in range(place.groups - 1):
            to = lax.rem(place.g + d + 1, place.groups)
            copy = remote(
                b3.at[to, :, cols],
                b4.at[d, :, cols],
                self.sems[6].at[q, d],
                self.sems[7].at[q, d],
                place.line[d],
            )
            copy.start()
            self.c4[q].append(copy)

    def land(self, q):
        b3, b4 = self.bufs[4:]
        cols = pl.ds(*self.pieces[q])
        total = b3[self.place.g, :, cols].astype(jnp.float32)
        for d in range(self.place.groups - 1):
            self.c4[q][d].wait_recv()
            total = total + b4[d, :, cols].astype(jnp.float32)
        self.acc[:, cols] = total

    def steps(self):
        stages = (self.to_core, self.to_side, self.to_other_side, self.along_line, self.land)
        return pipelined(self.n, stages, SUM_LAGS)

    def end(self):
        for q in range(self.n):
            for copy in [self.c1[q], self.c2[q], self.c3[q]] + self.c4[q]:
                copy.wait_send()


class SmallSum:
    def __init__(self, place, x, o, zbuf, buf, zs, zr, ss, rs):
        self.place, self.x, self.o, self.zbuf, self.buf = place, x, o, zbuf, buf
        self.zs, self.zr, self.ss, self.rs = zs, zr, ss, rs

    def begin(self):
        self.copies = []
        for d, device in enumerate(self.place.line):
            copy = remote(self.x, self.zbuf.at[d], self.zs.at[d], self.zr.at[d], device)
            copy.start()
            self.copies.append(copy)

    def line(self):
        place, groups = self.place, self.place.groups
        for copy in self.copies:
            copy.wait_recv()
        total = None
        for owner in range(groups):
            part = self.x[...]
            for d in range(groups - 1):
                source = lax.rem(place.g + groups - d - 1, groups)
                part = jnp.where(source == owner, self.zbuf[d], part)
            total = part if total is None else total + part
        self.o[...] = total
        self.send(0)

    def send(self, i):
        device = (self.place.side_x, self.place.side_y, self.place.core)[i]
        self.copy = remote(self.o, self.buf.at[i], self.ss.at[i], self.rs.at[i], device)
        self.copy.start()

    def add(self, i):
        self.copy.wait_recv()
        self.copy.wait_send()
        self.o[...] = self.o[...] + self.buf[i]
        if i < 2:
            self.send(i + 1)

    def steps(self):
        return [self.line] + [functools.partial(self.add, i) for i in range(3)]

    def end(self):
        for copy in self.copies:
            copy.wait_send()


def small_scratch(shape, groups):
    f32 = jnp.float32
    return [
        pltpu.VMEM((groups - 1, *shape), f32),
        pltpu.VMEM((3, *shape), f32),
        DMA((groups - 1,)),
        DMA((groups - 1,)),
        DMA((3,)),
        DMA((3,)),
    ]


def weave(*streams):
    found = []
    rounds = max((start + len(steps) for start, steps in streams), default=0)
    for at in range(rounds):
        for start, steps in streams:
            if 0 <= at - start < len(steps):
                found.append(steps[at - start])
    return found


def scatter_scratch(n, groups, rows, width):
    bf16 = jnp.bfloat16
    bufs = [
        pltpu.VMEM((groups, 2, 2, rows, width), bf16),
        pltpu.VMEM((groups, 2, 2, rows, width), bf16),
        pltpu.VMEM((groups, 2, 2, rows, width), bf16),
        pltpu.VMEM((groups, 2, rows, width), bf16),
        pltpu.VMEM((groups, rows, width), bf16),
        pltpu.VMEM((groups - 1, rows, width), bf16),
        pltpu.VMEM((rows, width), jnp.float32),
    ]
    sems = [DMA((n,))] * 6 + [DMA((n, groups - 1))] * 2
    return bufs, sems


def rms_rows(x, gain):
    return x * lax.rsqrt(jnp.mean(x * x, axis=-1, keepdims=True) + epsilon) * gain


def rms_back(x, gain, grad):
    inverse = lax.rsqrt(jnp.mean(x * x, axis=-1, keepdims=True) + epsilon)
    scaled = grad * gain
    along = jnp.mean(scaled * x, axis=-1, keepdims=True)
    d_gain = jnp.sum(grad * x * inverse, axis=0, keepdims=True)
    return scaled * inverse - x * inverse**3 * along, d_gain


NT = (((1,), (1,)), ((), ()))
NN = (((1,), (0,)), ((), ()))


class Summed:
    def __init__(self, sizes, products, extra=None, pieces=SUM_SHARES):
        self.sizes, self.products, self.extra = sizes, products, extra
        self.rows = products[0][0].shape[0] // (sizes[0] * sizes[1] * sizes[2])
        self.width = products[0][1].shape[-2 if products[0][3] else -1]
        self.more = 0 if extra is None else extra.shape[1]
        self.rights, self.places = [], []
        for _, right, _, _ in products:
            found = [i for i, other in enumerate(self.rights) if other is right]
            self.places.append(found[0] if found else len(self.rights))
            if not found:
                self.rights.append(right)
        at, self.pieces = 0, []
        for share in pieces:
            self.pieces.append((at, self.width * share // 16))
            at += self.width * share // 16
        if self.more:
            self.pieces.append((self.width, self.more))
        self.bufs, self.sems = scatter_scratch(
            len(self.pieces), sizes[0], self.rows, self.width + self.more
        )

    def operands(self):
        groups, ctx, tp = self.sizes
        split = (groups, ctx, tp // 2, 2, self.rows)
        found = [product[0].reshape(*split, product[0].shape[1]) for product in self.products]
        found += self.rights
        if self.more:
            found.append(self.extra.reshape(*split, self.more))
        return found

    def stage(self, place, inputs, scratch):
        count = len(self.products)
        lefts, rights = inputs[:count], inputs[count : count + len(self.rights)]
        bufs, sems = scratch[: len(self.bufs)], scratch[len(self.bufs) :]
        groups, ctx, tp = self.sizes

        def make(q, into, core):
            at, size = self.pieces[q]
            if at >= self.width:
                into[..., pl.ds(at, size)] = inputs[-1][:, :, :, core]
                return

            def block(i, _):
                total = None
                for left, where, (_, _, lead, transposed) in zip(
                    lefts, self.places, self.products
                ):
                    right = rights[where] if lead is None else rights[where].at[lead]
                    a = left[i, :, :, core]
                    a = a.reshape(-1, a.shape[-1])
                    some = right[pl.ds(at, size), :] if transposed else right[:, pl.ds(at, size)]
                    part = lax.dot_general(
                        a, some, NT if transposed else NN, preferred_element_type=jnp.float32
                    )
                    total = part if total is None else total + part
                into[i, :, :, :, pl.ds(at, size)] = total.astype(into.dtype).reshape(
                    ctx, tp // 2, self.rows, size
                )
                return 0

            lax.fori_loop(0, groups, block, 0)

        return Scatter(place, make, self.pieces, bufs[:-1], bufs[-1], sems)


def exchange(
    sizes,
    number,
    summed,
    finish,
    finish_args,
    finish_outs,
    gathered,
    moves,
    plan=(3,),
    start_also=5,
    start_second=10,
    also_gather=None,
    also_sum=None,
    tail=0,
    small=0,
):
    groups, ctx, tp = sizes
    f32, bf16 = jnp.float32, jnp.bfloat16
    rows = summed.rows
    out_pieces = gather_pieces(gathered)
    move_outs, move_scratch = moves_setup(moves, groups * ctx)
    n_moves = len(moves)
    move_specs = [(split, join) for _, split, join in moves]
    S = jax.ShapeDtypeStruct

    operands, in_specs, out_shape, out_specs, scratch = [], [], [], [], []

    def add_in(arrays, spec=IN_VMEM):
        at = len(operands)
        operands.extend(arrays)
        in_specs.extend([spec] * len(arrays))
        return slice(at, len(operands))

    def add_out(shapes, spec=IN_VMEM):
        at = len(out_shape)
        out_shape.extend(shapes)
        out_specs.extend([spec] * len(shapes))
        return slice(at, len(out_shape))

    def add_scratch(shapes):
        at = len(scratch)
        scratch.extend(shapes)
        return slice(at, len(scratch))

    in_sum = add_in(summed.operands())
    in_args = add_in(list(finish_args))
    o_main = add_out([S((groups, ctx, tp // 2, 2, rows, gathered), bf16)])
    o_finish = add_out([S(shape, f32) for shape in finish_outs])
    s_sum = add_scratch(summed.bufs + summed.sems)
    s_main = add_scratch(
        [pltpu.VMEM((rows, gathered), bf16)] + gather_sems(len(out_pieces), groups)
    )
    if also_gather is not None:
        also_pieces = gather_pieces(also_gather.shape[1])
        in_also = add_in([also_gather])
        o_also = add_out([S((groups, ctx, tp // 2, 2, rows, also_gather.shape[1]), bf16)])
        s_also = add_scratch(gather_sems(len(also_pieces), groups))
    if also_sum is not None:
        second, second_finish, second_args, second_out = also_sum
        in_second, in_second_args = add_in(second.operands()), add_in(second_args)
        o_second = add_out([second_out])
        s_second = add_scratch(second.bufs + second.sems)
    if tail:
        o_tail = add_out([S((tp // 2, 2, rows, tail), bf16)])
        s_tail = add_scratch([pltpu.VMEM((rows, tail), bf16)] + [DMA] * 5)
    if small:
        o_small = add_out([S((1, small), f32)])
        s_small = add_scratch([pltpu.VMEM((1, small), f32)] + small_scratch((1, small), groups))
    in_moves = add_in([array for array, _, _ in moves], IN_HBM)
    o_moves = add_out(move_outs, IN_HBM)
    s_moves = add_scratch(move_scratch)

    def kernel(*refs):
        ins = refs[: len(operands)]
        outs = refs[len(operands) : len(operands) + len(out_shape)]
        scr = refs[len(operands) + len(out_shape) :]
        place = Place(sizes)
        devices = [place.core, place.side_y]
        if n_moves:
            devices += [place.plane_peer(d)[1] for d in range(1, place.plane)]
        else:
            devices += [place.side_x] + place.line
        greet(devices)
        carried = None
        if n_moves:
            parts = scr[s_moves]
            carried = Moves(
                place, move_specs, ins[in_moves], outs[o_moves], parts[:n_moves], *parts[n_moves:]
            )
            carried.start()
        main_sum = summed.stage(place, ins[in_sum], scr[s_sum])
        low, *main_sems = scr[s_main]
        main_gather = Gather(place, low, outs[o_main][0], out_pieces, main_sems)
        streams = [(0, main_sum.steps())]
        ends = [main_sum, main_gather]
        if also_gather is not None:
            side_gather = Gather(place, ins[in_also][0], outs[o_also][0], also_pieces, scr[s_also])
            side_gather.begin()
            streams.append((start_also, side_gather.steps()))
            ends.append(side_gather)
        later = []
        if also_sum is not None:
            side_sum = second.stage(place, ins[in_second], scr[s_second])
            side_steps = side_sum.steps()
            ready = max(0, min(len(side_steps), len(summed.pieces) + SUM_LAGS[-1] - start_second))
            streams.append((start_second, side_steps[:ready]))
            later.append((0, side_steps[ready:]))
            ends.append(side_sum)
        total = n_moves * (groups * ctx - 1)
        steps = weave(*streams)
        for i, step in enumerate(steps):
            if carried is not None and i < len(plan):
                carried.issue(plan[i])
            step()
        if carried is not None:
            carried.settle()
        low_tail = scr[s_tail][0] if tail else None
        low_small = scr[s_small][0] if small else None
        finish(place, main_sum.acc, ins[in_args], outs[o_finish], low, low_tail, low_small)
        main_gather.begin()
        if small:
            small_sum = SmallSum(place, low_small, outs[o_small][0], *scr[s_small][1:])
            small_sum.begin()
            later.append((1, small_sum.steps()))
            ends.append(small_sum)
        if tail:
            ys, yr, ks, kr, own_sem = scr[s_tail][1:]
            y, k, spot = place.y, place.k, outs[o_tail][0]
            own = pltpu.make_async_copy(low_tail, spot.at[y, k], own_sem)
            own.start()
            to_y = remote(low_tail, spot.at[y, k], ys, yr, place.side_y)
            to_y.start()
            own.wait()
        steps = weave((0, main_gather.steps()), *later)
        if carried is not None:
            carried.issue(total)
        for step in steps:
            step()
        if tail:
            to_y.wait_recv()
            part = spot.at[:, k]
            to_k = remote(part, part, ks, kr, place.core)
            to_k.start()
            to_k.wait_recv()
            to_y.wait_send()
            to_k.wait_send()
        if also_sum is not None:
            second_finish(side_sum.acc, ins[in_second_args], outs[o_second][0])
        for stage in ends:
            stage.end()
        if carried is not None:
            carried.finish()

    results = pl.pallas_call(
        kernel,
        out_shape=out_shape,
        in_specs=in_specs,
        out_specs=out_specs,
        scratch_shapes=scratch,
        name=f"exchange_{number}",
        compiler_params=pltpu.CompilerParams(
            collective_id=number, has_side_effects=True, vmem_limit_bytes=62 * 2**20
        ),
    )(*operands)
    found = {"gathered": results[0].reshape(-1, gathered), "finish": results[o_finish]}
    if also_gather is not None:
        found["also"] = results[o_also][0].reshape(-1, also_gather.shape[1])
    if also_sum is not None:
        found["second"] = results[o_second][0]
    if tail:
        found["tail"] = results[o_tail][0].reshape(-1, tail)
    if small:
        found["small"] = results[o_small][0]
    found["moves"] = results[o_moves]
    return found


def gather_pieces(width):
    if width < 1024:
        return [(0, width)]
    whole = width // 2048 * 2048
    at, found = 0, []
    for share in GATHER_SHARES:
        found.append((at, whole * share // 16))
        at += whole * share // 16
    if width > whole:
        found.append((whole, width - whole))
    return found


def opening(sizes, number, hidden, embeds, cotangent, lengths, gain, down_maps, shard, moves):
    groups, ctx, tp = sizes
    f32, bf16 = jnp.float32, jnp.bfloat16
    rows = hidden.shape[0] // tp
    half = hidden.shape[1]
    rank = down_maps.shape[2]
    mids = down_maps.shape[0] * rank
    rest = 3 * half
    width = rest + mids + 128
    out_pieces = gather_pieces(width)
    move_outs, move_scratch = moves_setup(moves, groups * ctx)
    move_specs = [(split, join) for _, split, join in moves]
    n_moves = len(moves)

    def kernel(*refs):
        hid, emb, cot, lens, gain_ref, down_ref = refs[:6]
        up_ref, step_ref, taps_ref, bias_ref, norm_ref, *head_refs = refs[6:14]
        refs = list(refs[14:])
        sources = refs[:n_moves]
        o, up_o, step_o, small_o = refs[n_moves : n_moves + 4]
        targets = refs[n_moves + 4 : 2 * n_moves + 4]
        own = refs[2 * n_moves + 4 :]
        low, gs = own[0], own[1:10]
        stages = own[10 : 10 + n_moves]
        send, recv, local = own[10 + n_moves :]
        place = Place(sizes)
        greet(
            [place.core, place.side_y]
            + [place.plane_peer(d)[1] for d in range(1, place.plane)]
        )
        carried = Moves(place, move_specs, sources, targets, stages, send, recv, local)
        carried.start(1)
        mine = pl.ds(pl.multiple_of(place.t * rows, 16), rows)
        a, b = hid[mine, :].astype(f32), emb[mine, :].astype(f32)
        squares = jnp.sum(a * a, axis=1, keepdims=True) + jnp.sum(b * b, axis=1, keepdims=True)
        inverse = lax.rsqrt(squares / (2 * half) + epsilon)
        low[:, :half] = (a * inverse * gain_ref[:, :half]).astype(bf16)
        low[:, half : 2 * half] = (b * inverse * gain_ref[:, half:]).astype(bf16)
        for j in range(down_maps.shape[0]):
            at = rest + j * rank
            low[:, at : at + rank] = lax.dot_general(
                low[:, : 2 * half], down_ref[j], NN, preferred_element_type=f32
            ).astype(bf16)
        slot = lax.broadcasted_iota(jnp.int32, (rows, 128), 0)
        slot = slot + (place.c * tp + place.t) * rows
        lane = lax.broadcasted_iota(jnp.int32, (rows, 128), 1)
        segment, position, end = jnp.zeros_like(slot), slot, 0
        for i in range(lengths.shape[1]):
            length = lens[0, i]
            end = end + length
            passed = (slot >= end).astype(jnp.int32)
            segment = segment + passed
            position = position - passed * length
        marks = jnp.where(lane == 0, segment, position)
        low[:, 2 * half : rest] = cot[mine, :]
        low[:, rest + mids :] = marks.astype(f32).astype(bf16)
        gather = Gather(place, low, o, out_pieces, gs)
        gather.begin()
        carried.issue(len(carried.queue))
        lanes = pl.ds(pl.multiple_of(place.index * 128, 128), 128)
        for j in range(up_o.shape[0]):
            up_o[j] = up_ref[j, :, lanes]
        heads = step_ref.shape[1]
        few = heads // place.plane
        row = lax.broadcasted_iota(jnp.int32, (heads, 128), 0) - place.index * few
        col = lax.broadcasted_iota(jnp.int32, (heads, 128), 1)
        pick = (row == col) & (col < few)
        wide = row == col // (128 // few)
        step_o[...] = lax.dot_general(
            step_ref[...], pick.astype(bf16), NN, preferred_element_type=f32
        ).astype(bf16)
        small_o[...] = jnp.zeros_like(small_o)
        small_o[0:4, :] = taps_ref[:, lanes]
        small_o[4:5, :] = bias_ref[:, lanes]
        small_o[6:7, :] = norm_ref[:, lanes]
        for at, head_ref, chosen in zip((5, 8, 9), head_refs, (wide, pick, pick)):
            small_o[at : at + 1, :] = lax.dot_general(
                jnp.broadcast_to(head_ref[...], (8, heads)),
                chosen.astype(f32),
                NN,
                precision=highest,
                preferred_element_type=f32,
            )[0:1]
        for step in gather.steps():
            step()
        carried.settle()
        gather.end()
        carried.finish()

    S = jax.ShapeDtypeStruct
    results = pl.pallas_call(
        kernel,
        out_shape=[
            S((groups, ctx, tp // 2, 2, rows, width), bf16),
            S((*shard[0].shape[:2], 128), bf16),
            S((shard[1].shape[0], 128), bf16),
            S((16, 128), f32),
        ]
        + move_outs,
        in_specs=[IN_VMEM] * 3 + [IN_SMEM] + [IN_VMEM] * 10 + [IN_HBM] * n_moves,
        out_specs=[IN_VMEM] * 4 + [IN_HBM] * n_moves,
        scratch_shapes=[pltpu.VMEM((rows, width), bf16)]
        + gather_sems(len(out_pieces), groups)
        + move_scratch,
        name=f"opening_{number}",
        compiler_params=pltpu.CompilerParams(
            collective_id=number, has_side_effects=True, vmem_limit_bytes=62 * 2**20
        ),
    )(
        *(hidden, embeds, cotangent, lengths, gain.reshape(1, -1), down_maps),
        *shard,
        *[array for array, _, _ in moves],
    )
    return [results[0].reshape(-1, width)] + list(results[1:])


def sum_small(sizes, number, values):
    def kernel(x, o, *scratch):
        place = Place(sizes)
        greet([place.core, place.side_y, place.side_x] + place.line)
        summing = SmallSum(place, x, o, *scratch)
        summing.begin()
        for step in summing.steps():
            step()
        summing.end()

    return pl.pallas_call(
        kernel,
        out_shape=jax.ShapeDtypeStruct(values.shape, jnp.float32),
        in_specs=[IN_VMEM],
        out_specs=IN_VMEM,
        scratch_shapes=small_scratch(values.shape, sizes[0]),
        name=f"sum_small_{number}",
        compiler_params=pltpu.CompilerParams(collective_id=number, has_side_effects=True),
    )(values)


def own_of(place, ref, rows):
    if ref.shape[0] == rows:
        return ref[...].astype(jnp.float32)
    return ref[pl.ds(pl.multiple_of(place.t * rows, 16), rows), :].astype(jnp.float32)


def finish_forward(place, acc, args, outs, low, low_tail, low_small):
    rest, gain = args
    outs[0][...] = own_of(place, rest, acc.shape[0]) + acc[...]
    low[...] = rms_rows(outs[0][...], gain[...]).astype(jnp.bfloat16)


def finish_mixer_back(place, acc, args, outs, low, low_tail, low_small):
    after_mlp, gain, cot, state_map = args
    width = after_mlp.shape[1]
    low[:, width:] = acc[:, width:].astype(jnp.bfloat16)
    d_normed = acc[:, :width] + lax.dot_general(
        low[:, width:], state_map[...], NT, preferred_element_type=jnp.float32
    )
    d_rows, d_gain = rms_back(after_mlp[...], gain[...], d_normed)
    outs[1][...] = d_gain
    d_rows = cot[...].astype(jnp.float32) + d_rows
    outs[0][...] = d_rows
    low[:, :width] = d_rows.astype(jnp.bfloat16)


def finish_mlp_back(place, acc, args, outs, low, low_tail, low_small):
    after_attn, gain, d_after_mlp = args
    d_rows, d_gain = rms_back(after_attn[...], gain[...], acc[...])
    outs[1][...] = d_gain
    d_rows = d_after_mlp[...] + d_rows
    outs[0][...] = d_rows
    low[...] = d_rows.astype(jnp.bfloat16)


def finish_attention_back(place, acc, args, outs, low, low_tail, low_small):
    hidden, embeds, gain, d_after_attn, down_maps, out_mine, row = args
    half = hidden.shape[1]
    bf16, f32 = jnp.bfloat16, jnp.float32
    low[...] = acc[:, 2 * half :].astype(bf16)
    inputs = [own_of(place, part, acc.shape[0]) for part in (hidden, embeds)]
    squares = sum(jnp.sum(part * part, axis=1, keepdims=True) for part in inputs)
    inverse = lax.rsqrt(squares / (2 * half) + epsilon)
    along = jnp.zeros_like(squares)
    for i, part in enumerate(inputs):
        cols = slice(i * half, (i + 1) * half)
        grad = acc[:, cols]
        for j in range(down_maps.shape[0]):
            rank = down_maps.shape[2]
            grad = grad + lax.dot_general(
                low[:, j * rank : (j + 1) * rank],
                down_maps[j, cols, :],
                NT,
                preferred_element_type=f32,
            )
        acc[:, cols] = grad
        along = along + jnp.sum(grad * gain[:, cols] * part, axis=1, keepdims=True)
    along = along / (2 * half)
    low_tail[:, :half] = out_mine[...]
    low_small[:, 2 * half :] = row[...]
    for i, part in enumerate(inputs):
        cols = slice(i * half, (i + 1) * half)
        grad = acc[:, cols]
        low_small[:, cols] = jnp.sum(grad * part * inverse, axis=0, keepdims=True)
        d_rows = grad * gain[:, cols] * inverse - part * inverse**3 * along
        if i == 0:
            d_rows = d_rows + d_after_attn[...]
        low_tail[:, (i + 1) * half : (i + 2) * half] = d_rows.astype(bf16)


def finish_out(acc, args, out):
    out[...] = (args[0][...] + acc[...]).astype(out.dtype)


def adapter_products(xa, dmid, width):
    block, rank = 1024, dmid.shape[1] // 3

    def kernel(a, b, o, b_t):
        @pl.when(pl.program_id(0) == 0)
        def _():
            b_t[...] = b[...].T

        both = quick(b_t[...], a[...], NN)
        for j in range(3):
            o[j] = both[j * rank : (j + 1) * rank].T

    return pl.pallas_call(
        kernel,
        out_shape=jax.ShapeDtypeStruct((3, width, rank), jnp.float32),
        grid=(width // block,),
        in_specs=[
            pl.BlockSpec((xa.shape[0], block), lambda i: (0, i)),
            pl.BlockSpec(dmid.shape, lambda i: (0, 0)),
        ],
        out_specs=pl.BlockSpec((3, block, rank), lambda i: (0, i, 0)),
        scratch_shapes=[pltpu.VMEM(dmid.shape[::-1], dmid.dtype)],
        compiler_params=pltpu.CompilerParams(vmem_limit_bytes=60 * 2**20),
        name="adapter_products",
    )(xa, dmid)


def unpack(packed, parts):
    flat, at, found = packed.reshape(-1), 0, []
    for part in parts:
        found.append(flat[at : at + part.size].reshape(part.shape))
        at += part.size
    return found


TN = (((0,), (0,)), ((), ()))


def exact(left, right, dims):
    return lax.dot_general(left, right, dims, precision=highest, preferred_element_type=jnp.float32)


def quick(left, right, dims):
    return lax.dot_general(left, right, dims, preferred_element_type=jnp.float32)


def down_rows(values, by):
    return pltpu.roll(values, by, 0)


def up_rows(values, by):
    return pltpu.roll(values, values.shape[0] - by, 0)


def taps_forward(values, taps, bias, position):
    total = values * taps[0:1, :] + bias
    for lag in range(1, taps.shape[0]):
        kept = jnp.where(position >= lag, down_rows(values, lag), 0.0)
        total = total + kept * taps[lag : lag + 1, :]
    return total


def taps_backward(d_total, values, taps, position):
    d_values = d_total * taps[0:1, :]
    rows = [jnp.sum(d_total * values, axis=0, keepdims=True)]
    for lag in range(1, taps.shape[0]):
        kept = jnp.where(position >= lag, d_total, 0.0)
        rows.append(jnp.sum(kept * down_rows(values, lag), axis=0, keepdims=True))
        d_values = d_values + up_rows(kept, lag) * taps[lag : lag + 1, :]
    return d_values, rows + [jnp.sum(d_total, axis=0, keepdims=True)]


def silu_slope(values):
    sigmoid = jax.nn.sigmoid(values)
    return sigmoid * (1.0 + values * (1.0 - sigmoid))


class Scan:
    def __init__(self, xs, raw, bc, marks, taps, bias, bc_taps, bc_bias, heads):
        f32 = jnp.float32
        rows, lanes = xs.shape
        self.rows, self.half = rows, lanes // 2
        self.position = marks[:, 1:2].astype(f32)
        self.lane = lax.broadcasted_iota(jnp.int32, (rows, lanes), 1)
        self.xs, self.bc = xs.astype(f32), bc.astype(f32)
        self.pre_x = taps_forward(self.xs, taps, bias, self.position)
        self.pre_bc = taps_forward(self.bc, bc_taps, bc_bias, self.position)
        self.xc, bcc = jax.nn.silu(self.pre_x), jax.nn.silu(self.pre_bc)
        self.b_mat, self.c_mat = bcc[:, :STATE], bcc[:, STATE:]
        self.step_in = raw.astype(f32) + heads[0:1, :]
        self.dt = jax.nn.softplus(self.step_in)
        self.rate = -jnp.exp(heads[1:2, :])
        self.log_decay = self.dt * self.rate
        running, by = self.log_decay, 1
        while by < rows:
            running = running + jnp.where(self.position >= by, down_rows(running, by), 0.0)
            by *= 2
        self.running = running
        self.across = running.T
        row = lax.broadcasted_iota(jnp.int32, (rows, rows), 0)
        col = lax.broadcasted_iota(jnp.int32, (rows, rows), 1)
        first = row.astype(f32) - self.position
        self.same = (col <= row) & (col.astype(f32) >= first)
        self.meet = exact(self.c_mat, self.b_mat, NT)
        self.dt_wide = self.by_head([self.dt[:, h : h + 1] for h in range(2)])
        self.weighted = self.xc * self.dt_wide

    def by_head(self, values):
        return jnp.where(self.lane < self.half, values[0], values[1])

    def in_lane(self, values):
        return jnp.where(self.lane == 0, values[0], jnp.where(self.lane == 1, values[1], 0.0))

    def decay(self, h):
        gap = self.running[:, h : h + 1] - self.across[h : h + 1, :]
        return jnp.where(self.same, jnp.exp(jnp.where(self.same, gap, 0.0)), 0.0)

    def forward(self, skip):
        outs = [exact(self.decay(h) * self.meet, self.weighted, NN) for h in range(2)]
        return self.by_head(outs) + skip * self.xc

    def to_ends(self, values):
        rows = values.shape[0]
        row = lax.broadcasted_iota(jnp.int32, values.shape, 0)
        wide = jnp.broadcast_to(self.position, values.shape)
        by = 1
        while by < rows:
            inside = (up_rows(wide, by) >= by) & (row < rows - by)
            values = values + jnp.where(inside, up_rows(values, by), 0.0)
            by *= 2
        return values


def mixer_forward(xn, marked, mark_block, w_zx, w_step, state_map, w_out, small, bc_taps, bc_bias, groups):
    f32, bf16 = jnp.float32, jnp.bfloat16
    total, width = xn.shape
    rows, lanes = total // groups, w_zx.shape[2]
    state2 = state_map.shape[1]

    def kernel(xn_r, cot_r, marks_r, zx_r, st_r, sm_r, wo_r, sml, bt_r, bb_r, z_o, xs_o, raw_o, bc_o, y_o, dyn_o, sums_o):
        x = xn_r[...]
        z = quick(x, zx_r[0], NN)
        xs = quick(x, zx_r[1], NN).astype(bf16)
        raw = quick(x, st_r[...], NN).astype(bf16)
        bc = quick(x, sm_r[...], NN).astype(bf16)
        z_o[...], xs_o[...], raw_o[...], bc_o[...] = z, xs, raw, bc
        scan = Scan(
            xs, raw, bc, marks_r[...].astype(f32), sml[0:4, :], sml[4:5, :], bt_r[...], bb_r[...], sml[8:10, :]
        )
        y = scan.forward(sml[5:6, :]).astype(bf16)
        y_o[...] = y
        gated = y.astype(f32) * jax.nn.silu(z)
        d_yn = quick(cot_r[...], wo_r[...], NT)
        dyn_o[...] = d_yn
        ones = jnp.ones((8, lanes), f32)
        sums_o[0, 0:1] = exact(ones, gated * gated, NT)[0:1]
        sums_o[0, 1:2] = exact(ones, d_yn * sml[6:7, :] * gated, NT)[0:1]

    def by_group(columns):
        return pl.BlockSpec((rows, columns), lambda g: (g, 0))

    def whole(array):
        return pl.BlockSpec(array.shape, lambda g: (0,) * array.ndim)

    S = jax.ShapeDtypeStruct
    return pl.pallas_call(
        kernel,
        grid=(groups,),
        in_specs=[by_group(width), pl.BlockSpec((rows, width), lambda g: (g, 2))]
        + [pl.BlockSpec((rows, 128), lambda g: (g, mark_block))]
        + [whole(array) for array in (w_zx, w_step, state_map, w_out, small, bc_taps, bc_bias)],
        out_specs=[by_group(lanes)] * 3
        + [by_group(state2), by_group(lanes), by_group(lanes), pl.BlockSpec((1, 2, rows), lambda g: (g, 0, 0))],
        out_shape=[
            S((total, lanes), f32),
            S((total, lanes), bf16),
            S((total, lanes), bf16),
            S((total, state2), bf16),
            S((total, lanes), bf16),
            S((total, lanes), f32),
            S((groups, 2, rows), f32),
        ],
        compiler_params=pltpu.CompilerParams(vmem_limit_bytes=60 * 2**20),
        name="mixer_forward",
    )(xn, marked, marked, w_zx, w_step, state_map, w_out, small, bc_taps, bc_bias)


def mixer_backward(xn, marked, mark_block, kept, sums, small, bc_taps, bc_bias, groups):
    f32, bf16 = jnp.float32, jnp.bfloat16
    z, xs, raw, bc, y, d_yn = kept
    total, width = xn.shape
    rows, lanes, state2 = total // groups, z.shape[1], bc.shape[1]

    def kernel(
        xn_r, cot_r, marks_r, z_r, xs_r, raw_r, bc_r, y_r, dyn_r, sums_r, sml, bt_r, bb_r,
        dz_o, dxs_o, draw_o, dbc_o, yn_o, gzx_o, gst_o, gout_o, gsm_o, gbc_o, acc_in, acc_out,
    ):
        group = pl.program_id(0)
        scan = Scan(
            xs_r[...], raw_r[...], bc_r[...], marks_r[...].astype(f32),
            sml[0:4, :], sml[4:5, :], bt_r[...], bb_r[...], sml[8:10, :],
        )
        skip, gain = sml[5:6, :], sml[6:7, :]
        sums_wide = [jnp.broadcast_to(sums_r[0, i : i + 1], (128, rows)).T for i in range(2)]
        inverse = lax.rsqrt(sums_wide[0] / INNER + epsilon)
        cross = sums_wide[1] / INNER
        gate, out, d_normed = z_r[...], y_r[...].astype(f32), dyn_r[...]
        silu_z = jax.nn.silu(gate)
        gated = out * silu_z
        yn = (gated * inverse * gain).astype(bf16)
        yn_o[...] = yn
        g_gate = jnp.sum(d_normed * gated * inverse, axis=0, keepdims=True)
        d_gated = d_normed * gain * inverse - gated * inverse**3 * cross
        d_y = (d_gated * silu_z).astype(bf16).astype(f32)
        d_z = (d_gated * out * silu_slope(gate)).astype(bf16)
        dz_o[...] = d_z
        g_skip = jnp.sum(d_y * scan.xc, axis=0, keepdims=True)
        d_weighted, d_meet = jnp.zeros_like(d_y), jnp.zeros_like(scan.meet)
        by_row, by_col = [], []
        for h in range(2):
            mine = (scan.lane < scan.half) if h == 0 else (scan.lane >= scan.half)
            d_head = jnp.where(mine, d_y, 0.0)
            decay = scan.decay(h)
            mixing = decay * scan.meet
            d_mixing = exact(d_head, scan.weighted, NT)
            d_weighted = d_weighted + exact(mixing, d_head, TN)
            d_meet = d_meet + d_mixing * decay
            moved = d_mixing * mixing
            by_row.append(jnp.sum(moved, axis=1, keepdims=True))
            by_col.append(jnp.sum(moved, axis=0, keepdims=True))
        columns = [jnp.broadcast_to(by_col[h], (128, rows)).T for h in range(2)]
        d_running = scan.in_lane([by_row[h] - columns[h] for h in range(2)])
        d_log = scan.to_ends(d_running)
        shared = d_weighted * scan.xc
        d_dt = scan.in_lane(
            [
                jnp.sum(jnp.where(scan.lane < scan.half, shared, 0.0), axis=1, keepdims=True),
                jnp.sum(jnp.where(scan.lane >= scan.half, shared, 0.0), axis=1, keepdims=True),
            ]
        )
        d_step = (d_dt + d_log * scan.rate) * jax.nn.sigmoid(scan.step_in)
        g_bias = jnp.sum(d_step, axis=0, keepdims=True)
        g_decay = jnp.sum(d_log * scan.log_decay, axis=0, keepdims=True)
        d_raw = d_step.astype(bf16)
        draw_o[...] = d_raw
        d_xc = skip * d_y + d_weighted * scan.dt_wide
        d_xs, g_taps = taps_backward(
            d_xc * silu_slope(scan.pre_x), scan.xs, sml[0:4, :], scan.position
        )
        d_xs = d_xs.astype(bf16)
        dxs_o[...] = d_xs
        d_bcc = jnp.concatenate(
            [exact(d_meet, scan.c_mat, TN), exact(d_meet, scan.b_mat, NN)], axis=1
        )
        d_bc, g_bc_taps = taps_backward(
            d_bcc * silu_slope(scan.pre_bc), scan.bc, bt_r[...], scan.position
        )
        dbc_o[...] = d_bc.astype(bf16)
        in_part = quick(jnp.concatenate([d_z, d_xs, d_raw], axis=1), xn_r[...], TN)
        out_part = quick(yn, cot_r[...], TN)
        blank = jnp.zeros((1, lanes), f32)
        few = jnp.concatenate(
            g_taps + [g_gate, g_bias, g_decay, g_skip] + [blank] * 7, axis=0
        )
        few_bc = jnp.concatenate(g_bc_taps + [jnp.zeros((3, state2), f32)], axis=0)

        @pl.when(group == 0)
        def _():
            acc_in[...], acc_out[...] = in_part, out_part
            gsm_o[...], gbc_o[...] = few, few_bc

        @pl.when(group > 0)
        def _():
            acc_in[...] += in_part
            acc_out[...] += out_part
            gsm_o[...] += few
            gbc_o[...] += few_bc

        @pl.when(group == groups - 1)
        def _():
            for i in range(2):
                gzx_o[i] = acc_in[i * lanes : (i + 1) * lanes, :].T.astype(bf16)
            gst_o[...] = acc_in[2 * lanes : 2 * lanes + 8, :]
            gout_o[...] = acc_out[...].astype(bf16)

    def by_group(columns):
        return pl.BlockSpec((rows, columns), lambda g: (g, 0))

    def whole(shape):
        return pl.BlockSpec(shape, lambda g: (0,) * len(shape))

    S = jax.ShapeDtypeStruct
    return pl.pallas_call(
        kernel,
        grid=(groups,),
        in_specs=[by_group(width), pl.BlockSpec((rows, width), lambda g: (g, 2))]
        + [pl.BlockSpec((rows, 128), lambda g: (g, mark_block))]
        + [by_group(array.shape[1]) for array in kept]
        + [pl.BlockSpec((1, 2, rows), lambda g: (g, 0, 0)), whole(small.shape), whole(bc_taps.shape), whole(bc_bias.shape)],
        out_specs=[by_group(lanes)] * 3
        + [by_group(state2), by_group(lanes)]
        + [
            whole((2, width, lanes)),
            whole((8, width)),
            whole((lanes, width)),
            whole((16, lanes)),
            whole((8, state2)),
        ],
        out_shape=[
            S((total, lanes), bf16),
            S((total, lanes), bf16),
            S((total, lanes), bf16),
            S((total, state2), bf16),
            S((total, lanes), bf16),
            S((2, width, lanes), bf16),
            S((8, width), f32),
            S((lanes, width), bf16),
            S((16, lanes), f32),
            S((8, state2), f32),
        ],
        scratch_shapes=[pltpu.VMEM((3 * lanes, width), f32), pltpu.VMEM((lanes, width), f32)],
        compiler_params=pltpu.CompilerParams(vmem_limit_bytes=60 * 2**20),
        name="mixer_backward",
    )(xn, marked, marked, z, xs, raw, bc, y, d_yn, sums, small, bc_taps, bc_bias)


def swap_halves(values):
    return pltpu.roll(values, values.shape[1] // 2, 1)


def attend_weights(qr, kr, marks, rows):
    f32 = jnp.float32
    row = lax.broadcasted_iota(jnp.int32, (rows, rows), 0)
    col = lax.broadcasted_iota(jnp.int32, (rows, rows), 1)
    first = row.astype(f32) - marks[:, 1:2]
    allowed = (col <= row) & (col.astype(f32) >= first)
    weights = jnp.exp(jnp.where(allowed, quick(qr, kr, NT) * AHD ** (-0.5), -1e30))
    return weights / jnp.sum(weights, axis=-1, keepdims=True)


def attention_forward(xa, width, w_qkv, up_maps, frequencies, groups):
    f32, bf16 = jnp.float32, jnp.bfloat16
    total, columns = xa.shape
    rows, rank = total // groups, up_maps.shape[1]
    side = columns - (3 * width) // 2
    side_block = pl.BlockSpec((rows, side), lambda g: (g, columns // side - 1))

    def kernel(xa_r, side_r, w_r, up_r, freq_r, ao_o, q_o, k_o, v_o, cos_o, sin_o, w_all):
        @pl.when(pl.program_id(0) == 0)
        def _():
            for j in range(3):
                w_all[:, j * AHD : (j + 1) * AHD] = w_r[j]

        marks = side_r[:, 3 * rank :].astype(f32)
        wide = quick(xa_r[...], w_all[...], NN)
        proj = []
        for j in range(3):
            mid = side_r[:, j * rank : (j + 1) * rank]
            proj.append((wide[:, j * AHD : (j + 1) * AHD] + quick(mid, up_r[j], NN)).astype(bf16))
        angle = marks[:, 1:2] * freq_r[...]
        lane = lax.broadcasted_iota(jnp.int32, angle.shape, 1)
        cosine, sine = jnp.cos(angle), jnp.sin(angle)
        sine = jnp.where(lane < AHD // 2, -sine, sine)
        cos_o[...], sin_o[...] = cosine, sine
        qr, kr = [
            (piece * cosine + swap_halves(piece) * sine).astype(bf16)
            for piece in (proj[0].astype(f32), proj[1].astype(f32))
        ]
        q_o[...], k_o[...], v_o[...] = qr, kr, proj[2]
        low = attend_weights(qr, kr, marks, rows).astype(bf16)
        ao_o[...] = quick(low, proj[2], NN).astype(bf16)

    def by_group(size):
        return pl.BlockSpec((rows, size), lambda g: (g, 0))

    def whole(array):
        return pl.BlockSpec(array.shape, lambda g: (0,) * array.ndim)

    S = jax.ShapeDtypeStruct
    return pl.pallas_call(
        kernel,
        grid=(groups,),
        in_specs=[by_group(width), side_block, whole(w_qkv), whole(up_maps), whole(frequencies)],
        out_specs=[by_group(AHD)] * 6,
        out_shape=[S((total, AHD), bf16)] * 4 + [S((total, AHD), f32)] * 2,
        scratch_shapes=[pltpu.VMEM((width, 3 * AHD), bf16)],
        compiler_params=pltpu.CompilerParams(vmem_limit_bytes=60 * 2**20),
        name="attention_forward",
    )(xa, xa, w_qkv, up_maps, frequencies)


def attention_backward(d_attn, xa, width, w_o, up_maps, kept, groups):
    f32, bf16 = jnp.float32, jnp.bfloat16
    total, columns = xa.shape
    rows, rank = total // groups, up_maps.shape[1]
    side = columns - (3 * width) // 2
    side_block = pl.BlockSpec((rows, side), lambda g: (g, columns // side - 1))
    model = d_attn.shape[1]

    def kernel(
        da_r, xa_r, side_r, wo_r, up_r, ao_r, q_r, k_r, v_r, cos_r, sin_r,
        dq_o, dk_o, dv_o, dmid_o, gw_o, go_o, gup_o, acc_w, acc_o,
    ):
        group = pl.program_id(0)
        d_rows = da_r[...]
        marks = side_r[:, 3 * rank :].astype(f32)
        d_ao = quick(d_rows, wo_r[...], NT).astype(bf16)
        qr, kr, vals = q_r[...], k_r[...], v_r[...]
        weights = attend_weights(qr, kr, marks, rows)
        d_vals = quick(weights.astype(bf16), d_ao, TN)
        d_weights = quick(d_ao, vals, NT).astype(bf16).astype(f32)
        along = jnp.sum(d_weights * weights, axis=-1, keepdims=True)
        d_scores = (weights * (d_weights - along) * AHD ** (-0.5)).astype(bf16)
        cosine, sine = cos_r[...], sin_r[...]
        pieces = []
        for d_turned in (quick(d_scores, kr, NN), quick(d_scores, qr, TN)):
            d_turned = d_turned.astype(bf16).astype(f32)
            pieces.append((d_turned * cosine + swap_halves(d_turned * sine)).astype(bf16))
        pieces.append(d_vals.astype(bf16))
        for j, out in enumerate((dq_o, dk_o, dv_o)):
            out[...] = pieces[j]
            dmid_o[:, j * rank : (j + 1) * rank] = quick(pieces[j], up_r[j], NT).astype(bf16)
        part = quick(jnp.concatenate(pieces, axis=1), xa_r[...], TN)
        part_o = quick(ao_r[...], d_rows, TN)
        parts_up = [
            quick(side_r[:, j * rank : (j + 1) * rank], pieces[j], TN)
            for j in range(3)
        ]

        @pl.when(group == 0)
        def _():
            acc_w[...], acc_o[...] = part, part_o
            for j in range(3):
                gup_o[j] = parts_up[j]

        @pl.when(group > 0)
        def _():
            acc_w[...] += part
            acc_o[...] += part_o
            for j in range(3):
                gup_o[j] += parts_up[j]

        @pl.when(group == groups - 1)
        def _():
            for j in range(3):
                gw_o[j] = acc_w[j * AHD : (j + 1) * AHD, :].T.astype(bf16)
            go_o[...] = acc_o[...].astype(bf16)

    def by_group(size):
        return pl.BlockSpec((rows, size), lambda g: (g, 0))

    def whole(shape):
        return pl.BlockSpec(shape, lambda g: (0,) * len(shape))

    S = jax.ShapeDtypeStruct
    return pl.pallas_call(
        kernel,
        grid=(groups,),
        in_specs=[by_group(model), by_group(width), side_block, whole(w_o.shape), whole(up_maps.shape)]
        + [by_group(AHD)] * 6,
        out_specs=[by_group(AHD)] * 3
        + [by_group(3 * rank)]
        + [whole((3, width, AHD)), whole((AHD, model)), whole((3, rank, AHD))],
        out_shape=[S((total, AHD), bf16)] * 3
        + [
            S((total, 3 * rank), bf16),
            S((3, width, AHD), bf16),
            S((AHD, model), bf16),
            S((3, rank, AHD), f32),
        ],
        scratch_shapes=[pltpu.VMEM((3 * AHD, width), f32), pltpu.VMEM((AHD, model), f32)],
        compiler_params=pltpu.CompilerParams(vmem_limit_bytes=60 * 2**20),
        name="attention_backward",
    )(d_attn, xa, xa, w_o, up_maps, *kept)


def per_device_split(
    hidden,
    embeds,
    cotangent,
    lengths,
    attention_norm_gain,
    adapter_down_maps,
    query_key_value_weight,
    adapter_up_maps,
    attention_output_weight,
    feedforward_norm_gain,
    gate_up_weight,
    down_weight,
    mixer_norm_gain,
    mixer_gate_input_weight,
    state_map_weight,
    step_size_weight,
    mixer_input_taps,
    mixer_input_tap_bias,
    state_map_taps,
    state_map_tap_bias,
    step_size_bias,
    log_decay_rate,
    head_skip_weight,
    gated_norm_gain,
    mixer_output_weight,
):
    bf16, f32 = jnp.bfloat16, jnp.float32
    tp_size, ctx_size, groups = (lax.axis_size(name) for name in ("tp", "ctx", "fsdp"))
    tp_index, ctx_index = lax.axis_index("tp"), lax.axis_index("ctx")
    plane_index = lax.axis_index("fsdp") * ctx_size + ctx_index
    plane_size = groups * ctx_size
    tok_rows = hidden.shape[0]
    mine = tok_rows // tp_size
    group_rows = tok_rows * ctx_size
    start = tp_index * mine

    sizes = (groups, ctx_size, tp_size)

    def own_rows(values):
        return lax.dynamic_slice_in_dim(values, start, mine, 0)

    width = hidden.shape[1]
    own_shape = (mine, width)
    cot_low = own_rows(cotangent)

    rank = adapter_down_maps.shape[2]
    width_a = adapter_down_maps.shape[1]
    xa_wide, up_maps, w_step, small, w_o, w_qkv = opening(
        sizes,
        1,
        hidden,
        embeds,
        cotangent,
        lengths,
        attention_norm_gain,
        adapter_down_maps,
        [
            adapter_up_maps,
            step_size_weight,
            mixer_input_taps,
            mixer_input_tap_bias[None],
            gated_norm_gain[None],
            head_skip_weight[None],
            step_size_bias[None],
            log_decay_rate[None],
        ],
        [(attention_output_weight, 0, 1), (query_key_value_weight, 2, 1)],
    )
    half = AHD // 2
    frequencies = 10000.0 ** (-jnp.arange(half, dtype=f32) / half)
    frequencies = jnp.concatenate([frequencies, frequencies])[None]
    kept_a = attention_forward(xa_wide, width_a, w_qkv, up_maps, frequencies, groups)
    ao_low = kept_a[0]

    gain_m = feedforward_norm_gain.reshape(1, -1)
    found = exchange(
        sizes,
        2,
        Summed(sizes, [(ao_low, w_o, None, False)]),
        finish_forward,
        [hidden, gain_m],
        [own_shape],
        width,
        [(gate_up_weight, 2, 1), (down_weight, 0, 1)],
    )
    xm, (after_attn,), (w_gu, w_down) = found["gathered"], found["finish"], found["moves"]
    gate_pre, up_pre = matrix_product(xm, w_gu[0]), matrix_product(xm, w_gu[1])
    activated, act_back = jax.vjp(gated_gelu, gate_pre, up_pre)
    hid_low = activated.astype(bf16)

    gain_n = mixer_norm_gain.reshape(1, -1)
    found = exchange(
        sizes,
        3,
        Summed(sizes, [(hid_low, w_down, None, False)]),
        finish_forward,
        [after_attn, gain_n],
        [own_shape],
        width,
        [(mixer_gate_input_weight, 2, 1), (mixer_output_weight, 0, 1)],
        plan=(6,),
    )
    xn, (after_mlp,) = found["gathered"], found["finish"]
    w_zx, w_out = found["moves"]
    few = step_size_weight.shape[1] // plane_size
    bc_bias = state_map_tap_bias[None]
    mark_block = (3 * width + 3 * rank) // 128
    *kept, sums = mixer_forward(
        xn, xa_wide, mark_block, w_zx, w_step, state_map_weight, w_out, small, state_map_taps, bc_bias, groups
    )
    sums = sum_small(sizes, 4, sums)
    d_z, d_xs, d_step, d_bc_part, yn_low, grad_w_zx, grad_w_dt, grad_w_out, few_x, few_bc = (
        mixer_backward(xn, xa_wide, mark_block, kept, sums, small, state_map_taps, bc_bias, groups)
    )
    grad_conv_bc, grad_conv_bc_bias = few_bc[:4], few_bc[4]
    found = exchange(
        sizes,
        5,
        Summed(
            sizes,
            [
                (d_z, w_zx, 0, True),
                (d_xs, w_zx, 1, True),
                (d_step, w_step, None, True),
            ],
            d_bc_part,
        ),
        finish_mixer_back,
        [after_mlp, gain_n, cot_low, state_map_weight],
        [own_shape, gain_n.shape],
        width + d_bc_part.shape[1],
        [(grad_w_zx, 1, 2), (grad_w_out, 1, 0)],
        plan=(6,),
        also_sum=(
            Summed(sizes, [(yn_low, w_out, None, False)]),
            finish_out,
            [after_mlp],
            jax.ShapeDtypeStruct(own_shape, bf16),
        ),
    )
    gathered, (d_after_mlp, grad_g_mamba) = found["gathered"], found["finish"]
    out_mine, (grad_w_zx, grad_w_out) = found["second"], found["moves"]

    d_mlp, d_bc = gathered[:, :width], gathered[:, width:]
    grad_w_bc = outer_product_sum(xn, d_bc)
    grad_w_down = outer_product_sum(hid_low, d_mlp)
    d_gate, d_up = act_back(matrix_product_transposed(d_mlp, w_down))
    d_gate, d_up = d_gate.astype(bf16), d_up.astype(bf16)
    grad_w_gu = jnp.stack(
        [outer_product_sum(xm, d_gate).astype(bf16), outer_product_sum(xm, d_up).astype(bf16)]
    )

    found = exchange(
        sizes,
        6,
        Summed(sizes, [(d_gate, w_gu, 0, True), (d_up, w_gu, 1, True)]),
        finish_mlp_back,
        [after_attn, gain_m, d_after_mlp],
        [own_shape, gain_m.shape],
        width,
        [(grad_w_gu, 1, 2), (grad_w_down.astype(bf16), 1, 0)],
    )
    d_attn, (d_after_attn, grad_g_mlp) = found["gathered"], found["finish"]
    grad_w_gu, grad_w_down = found["moves"]
    *d_proj, dmid_part, grad_w_qkv, grad_w_o, adapter_up_gradient = attention_backward(
        d_attn, xa_wide, width_a, w_o, up_maps, kept_a, groups
    )
    shares = jnp.concatenate([few_x, grad_w_dt[:few].reshape(-1, 128)]).astype(bf16)
    sums = [grad_g_mlp[0], grad_g_mamba[0], grad_conv_bc, grad_conv_bc_bias]
    row = jnp.concatenate([part.reshape(-1) for part in sums])[None]
    found = exchange(
        sizes,
        7,
        Summed(sizes, [(d_proj[j], w_qkv, j, True) for j in range(3)], dmid_part),
        finish_attention_back,
        [
            hidden,
            embeds,
            attention_norm_gain.reshape(1, -1),
            d_after_attn,
            adapter_down_maps,
            out_mine,
            row,
        ],
        [],
        3 * rank,
        [
            (grad_w_qkv, 1, 2),
            (grad_w_o, 1, 0),
            (adapter_up_gradient.astype(bf16), None, 2),
            (shares, None, 1),
        ],
        plan=(5,),
        tail=3 * width,
        small=width_a + row.shape[1],
    )
    dmid, back, row = found["gathered"], found["tail"], found["small"][0]
    grad_w_qkv, grad_w_o, adapter_up_gradient, shared = found["moves"]
    adapter_down_gradient = adapter_products(xa_wide, dmid, width_a)
    result = back[:, :width]
    d_hidden = back[:, width : 2 * width].astype(f32)
    d_embeds = back[:, 2 * width :].astype(f32)
    adapter_up_gradient = adapter_up_gradient.astype(f32)
    shared = shared.astype(f32)
    grad_conv_x, grad_conv_x_bias, grad_g_gate = shared[:4], shared[4], shared[5]
    heads = shared.reshape(-1, plane_size, 128)
    grad_dt_bias = heads[6, :, :few].reshape(-1)
    grad_a_log = heads[7, :, :few].reshape(-1)
    grad_d_skip = heads[8].reshape(plane_size, few, MIXER_HEAD_SIZE).sum(axis=2).reshape(-1)
    grad_w_dt = shared[16:].reshape(few, -1, plane_size, 128).transpose(1, 3, 2, 0)
    grad_w_dt = grad_w_dt.reshape(-1, plane_size * few)
    grad_g_attn = row[:width_a]
    grad_g_mlp, grad_g_mamba, grad_conv_bc, grad_conv_bc_bias = unpack(row[width_a:], sums)

    return (
        result,
        d_hidden,
        d_embeds,
        grad_g_attn,
        adapter_down_gradient,
        grad_w_qkv.astype(f32),
        adapter_up_gradient,
        grad_w_o.astype(f32),
        grad_g_mlp,
        grad_w_gu.astype(f32),
        grad_w_down.astype(f32),
        grad_g_mamba,
        grad_w_zx.astype(f32),
        grad_w_bc,
        grad_w_dt,
        grad_conv_x,
        grad_conv_x_bias,
        grad_conv_bc,
        grad_conv_bc_bias,
        grad_dt_bias,
        grad_a_log,
        grad_d_skip,
        grad_g_gate,
        grad_w_out.astype(f32),
    )


def solution(mesh):
    placed = (
        P(("fsdp", "ctx"), None),
        P(("fsdp", "ctx"), None),
        P(("fsdp", "ctx"), None),
        P("fsdp", None),
        P(),
        P(),
        P(None, ("fsdp", "ctx"), "tp"),
        P(None, None, "tp"),
        P("tp", ("fsdp", "ctx")),
        P(),
        P(None, ("fsdp", "ctx"), "tp"),
        P("tp", ("fsdp", "ctx")),
        P(),
        P(None, ("fsdp", "ctx"), "tp"),
        P(),
        P(None, "tp"),
        P(None, "tp"),
        P("tp"),
        P(),
        P(),
        P("tp"),
        P("tp"),
        P("tp"),
        P("tp"),
        P("tp", ("fsdp", "ctx")),
    )
    devices = mesh.shape["fsdp"] * mesh.shape["ctx"] * mesh.shape["tp"]
    one_head_each = devices == AHEADS and mesh.shape["ctx"] == 2 and mesh.shape["tp"] == 4
    return jax.shard_map(
        per_device_split if one_head_each else per_device,
        mesh=mesh,
        in_specs=placed,
        out_specs=(
            P(("fsdp", "ctx"), None),
            P(("fsdp", "ctx"), None),
            P(("fsdp", "ctx"), None),
            P(),
            P(),
            P(None, ("fsdp", "ctx"), "tp"),
            P(None, None, "tp"),
            P("tp", ("fsdp", "ctx")),
            P(),
            P(None, ("fsdp", "ctx"), "tp"),
            P("tp", ("fsdp", "ctx")),
            P(),
            P(None, ("fsdp", "ctx"), "tp"),
            P(),
            P(None, "tp"),
            P(None, "tp"),
            P("tp"),
            P(),
            P(),
            P("tp"),
            P("tp"),
            P("tp"),
            P("tp"),
            P("tp", ("fsdp", "ctx")),
        ),
        check_vma=False,
    )
```

```python
import functools

import jax
import jax.numpy as jnp
from jax import lax
from jax.experimental import pallas as pl
from jax.experimental.pallas import tpu as pltpu
from jax.sharding import PartitionSpec as P

MODEL_WIDTH = 2048
AHEADS = 32
AHD = 128
INNER = 4096
MIXER_HEAD_SIZE = 64
STATE = 128
SPAN = 128


highest = lax.Precision.HIGHEST
epsilon = 1e-05


def matrix_product(left, right):
    return jnp.dot(left, right, preferred_element_type=jnp.float32)


def matrix_product_transposed(left, right):
    return lax.dot_general(
        left, right, (((1,), (1,)), ((), ())), preferred_element_type=jnp.float32
    )


def outer_product_sum(left, right):
    return lax.dot_general(
        left, right, (((0,), (0,)), ((), ())), preferred_element_type=jnp.float32
    )


def rms_scale(values, gain):
    return values * lax.rsqrt(jnp.mean(values * values, axis=-1, keepdims=True) + epsilon) * gain


def gated_gelu(gate_in, up_in):
    return jax.nn.gelu(gate_in, approximate=True) * up_in


def layout(lengths_row, total_rows):
    ends = jnp.cumsum(lengths_row)
    slot_index = jnp.arange(total_rows, dtype=jnp.int32)
    passed = (slot_index[:, None] >= ends[None, :]).astype(jnp.int32)
    segment = jnp.sum(passed, axis=1)
    position = slot_index - jnp.sum(passed * lengths_row[None, :], axis=1)
    return (segment, position, slot_index)


def causal_conv(values, kernel, bias, position):
    total_rows = values.shape[0]
    total = values * kernel[0][None, :] + bias[None, :]
    for lag in range(1, kernel.shape[0]):
        shifted = jnp.concatenate(
            [jnp.zeros((lag, values.shape[1]), values.dtype), values[: total_rows - lag]], axis=0
        )
        keep = (position >= lag).astype(values.dtype)[:, None]
        total = total + shifted * keep * kernel[lag][None, :]
    return jax.nn.silu(total)


def rotate(values, position):
    half_dim = values.shape[-1] // 2
    inverse = 10000.0 ** (-jnp.arange(half_dim, dtype=jnp.float32) / half_dim)
    angle = position.astype(jnp.float32)[:, None] * inverse[None, :]
    cosine = jnp.cos(angle)[:, None, :]
    sine_part = jnp.sin(angle)[:, None, :]
    first_half = values[..., :half_dim]
    second_half = values[..., half_dim:]
    return jnp.concatenate(
        [
            first_half * cosine - second_half * sine_part,
            second_half * cosine + first_half * sine_part,
        ],
        axis=-1,
    )


def attend_core(pair_data, values, segment, slot_index, position, block_rows):
    group_row_block = values.shape[0]
    count_of_heads = values.shape[1] // AHD
    paired = pair_data.reshape(group_row_block, count_of_heads, 2, AHD)
    queries = rotate(paired[:, :, 0], position).astype(jnp.bfloat16)
    keys_all = rotate(paired[:, :, 1], position).astype(jnp.bfloat16)
    vals_all = values.reshape(group_row_block, count_of_heads, AHD).astype(jnp.bfloat16)
    scaling = AHD ** (-0.5)
    block_count = group_row_block // block_rows

    def one_block(inputs):
        query_part, query_seg, query_slot = inputs
        scores = (
            jnp.einsum("qhd,khd->hqk", query_part, keys_all, preferred_element_type=jnp.float32)
            * scaling
        )
        allowed = (query_seg[:, None] == segment[None, :]) & (
            query_slot[:, None] >= slot_index[None, :]
        )
        scores = jnp.where(allowed[None], scores, -1e30)
        weights = jnp.exp(scores)
        weights_low = (weights / jnp.sum(weights, axis=-1, keepdims=True)).astype(jnp.bfloat16)
        return jnp.einsum("hqk,khd->qhd", weights_low, vals_all, preferred_element_type=jnp.float32)

    mapped = lax.map(
        jax.checkpoint(one_block),
        (
            queries.reshape(block_count, block_rows, count_of_heads, AHD),
            segment.reshape(block_count, block_rows),
            slot_index.reshape(block_count, block_rows),
        ),
    )
    return mapped.reshape(group_row_block, count_of_heads * AHD)


def state_scan(inputs_x, step_size, b_mat, c_mat, decay_rate, segment):
    total_rows, count_of_heads, head_dim = inputs_x.shape
    spans = total_rows // SPAN
    log_decay = step_size * decay_rate[None, :]
    weighted = inputs_x * step_size[:, :, None]
    causal = jnp.arange(SPAN)[:, None] >= jnp.arange(SPAN)[None, :]

    def advance(carried_in, inputs):
        memory, last_segment = carried_in
        decay_part, weighted_part, b_part, c_part, seg_part = inputs
        running = jnp.cumsum(decay_part, axis=0)
        same_seq = (seg_part[:, None] == seg_part[None, :]) & causal
        intersection = jnp.dot(c_part, b_part.T, precision=highest)
        log_gap = jnp.where(same_seq[:, :, None], running[:, None, :] - running[None, :, :], 0.0)
        mixing = jnp.where(same_seq[:, :, None], jnp.exp(log_gap), 0.0) * intersection[:, :, None]
        output = jnp.einsum("tsh,shp->thp", mixing, weighted_part, precision=highest)
        carried = (seg_part == last_segment).astype(jnp.float32)
        reach_back = jnp.exp(running) * carried[:, None]
        output = (
            output
            + jnp.einsum("tn,hpn->thp", c_part, memory, precision=highest) * reach_back[:, :, None]
        )
        tail_seg = seg_part[-1]
        toward = (
            jnp.exp(running[-1][None, :] - running)
            * (seg_part == tail_seg).astype(jnp.float32)[:, None]
        )
        next_state = jnp.einsum("sh,shp,sn->hpn", toward, weighted_part, b_part, precision=highest)
        keep_all = jnp.exp(running[-1]) * (tail_seg == last_segment).astype(jnp.float32)
        next_state = next_state + memory * keep_all[:, None, None]
        return ((next_state, tail_seg), output)

    initial = (jnp.zeros((count_of_heads, head_dim, b_mat.shape[1]), jnp.float32), jnp.int32(-1))
    pieces = (
        log_decay.reshape(spans, SPAN, count_of_heads),
        weighted.reshape(spans, SPAN, count_of_heads, head_dim),
        b_mat.reshape(spans, SPAN, -1),
        c_mat.reshape(spans, SPAN, -1),
        segment.reshape(spans, SPAN),
    )
    last_state, outputs = lax.scan(jax.checkpoint(advance), initial, pieces)
    return outputs.reshape(total_rows, count_of_heads, head_dim)


def mamba_core(
    inner_in,
    step_in,
    bc_post,
    bias_in,
    decay_in,
    skip_weight_input,
    kernel_in,
    conv_bias_in,
    position,
    segment,
):
    group_row_block = inner_in.shape[0]
    count_of_heads = step_in.shape[1]
    mixer_result = causal_conv(inner_in, kernel_in, conv_bias_in, position)
    reshaped_tensor = mixer_result.reshape(group_row_block, count_of_heads, MIXER_HEAD_SIZE)
    step_size = jax.nn.softplus(step_in + bias_in[None, :])
    scan_result = state_scan(
        reshaped_tensor,
        step_size,
        bc_post[:, :STATE],
        bc_post[:, STATE:],
        -jnp.exp(decay_in),
        segment,
    )
    return (scan_result + skip_weight_input[None, :, None] * reshaped_tensor).reshape(
        group_row_block, count_of_heads * MIXER_HEAD_SIZE
    )


def collect(first_part, second_part):
    return (
        lax.all_gather(first_part, ("fsdp", "ctx"), axis=1, tiled=True),
        lax.all_gather(second_part, ("fsdp", "ctx"), axis=1, tiled=True),
    )


def collect_again(first_part, second_part):
    return (
        lax.all_gather(first_part, ("fsdp", "ctx"), axis=1, tiled=True),
        lax.all_gather(second_part, ("fsdp", "ctx"), axis=1, tiled=True),
    )


def tensor_sum(partial_sum):
    return lax.psum(partial_sum, "tp")


def tensor_pair(first_part, second_part):
    return (
        lax.psum(first_part.astype(jnp.bfloat16), "tp").astype(jnp.float32),
        lax.psum(second_part.astype(jnp.bfloat16), "tp").astype(jnp.float32),
    )


def heads_pair(first_part, second_part):
    return (
        lax.all_to_all(first_part, "ctx", split_axis=1, concat_axis=0, tiled=True),
        lax.all_to_all(second_part, "ctx", split_axis=1, concat_axis=0, tiled=True),
    )


def heads_one(values):
    return lax.all_to_all(values, "ctx", split_axis=1, concat_axis=0, tiled=True)


def tokens_pair(first_part, second_part):
    return (
        lax.all_to_all(first_part, "ctx", split_axis=0, concat_axis=1, tiled=True),
        lax.all_to_all(second_part, "ctx", split_axis=0, concat_axis=1, tiled=True),
    )


def tokens_one(values):
    return lax.all_to_all(values, "ctx", split_axis=0, concat_axis=1, tiled=True)


def per_device(
    hidden,
    embeds,
    cotangent,
    lengths,
    attention_norm_gain,
    adapter_down_maps,
    query_key_value_weight,
    adapter_up_maps,
    attention_output_weight,
    feedforward_norm_gain,
    gate_up_weight,
    down_weight,
    mixer_norm_gain,
    mixer_gate_input_weight,
    state_map_weight,
    step_size_weight,
    mixer_input_taps,
    mixer_input_tap_bias,
    state_map_taps,
    state_map_tap_bias,
    step_size_bias,
    log_decay_rate,
    head_skip_weight,
    gated_norm_gain,
    mixer_output_weight,
):
    tok_rows = hidden.shape[0]
    ctx_size = lax.axis_size("ctx")
    ctx_index = lax.axis_index("ctx")
    group_row_block = tok_rows * ctx_size
    block_rows = group_row_block // max(1, group_row_block // 1024)
    segment, position, slot_index = layout(lengths[0], group_row_block)
    hidden_f = hidden.astype(jnp.float32)
    embeds_f = embeds.astype(jnp.float32)
    attention_block_full, attn_out = collect(query_key_value_weight, attention_output_weight)
    joined = jnp.concatenate([hidden_f, embeds_f], axis=1)
    normed_a, norm_a_back = jax.vjp(rms_scale, joined, attention_norm_gain)
    attention_input_reduced = normed_a.astype(jnp.bfloat16)
    middle_reduced_precision = [
        matrix_product(attention_input_reduced, adapter_down_maps[group_member]).astype(
            jnp.bfloat16
        )
        for group_member in range(3)
    ]
    projected_input = [
        (
            matrix_product(attention_input_reduced, attention_block_full[group_member])
            + matrix_product(middle_reduced_precision[group_member], adapter_up_maps[group_member])
        ).astype(jnp.bfloat16)
        for group_member in range(3)
    ]
    tp_heads = projected_input[0].shape[1] // AHD
    pair_data = jnp.stack(
        [
            projected_input[0].reshape(tok_rows, tp_heads, AHD),
            projected_input[1].reshape(tok_rows, tp_heads, AHD),
        ],
        axis=2,
    ).reshape(tok_rows, tp_heads * 2 * AHD)
    pair_heads, value_heads = heads_pair(pair_data, projected_input[2])
    attn_core, attn_pull = jax.vjp(
        lambda pairs_in, values_in: attend_core(
            pairs_in, values_in, segment, slot_index, position, block_rows
        ),
        pair_heads.astype(jnp.float32),
        value_heads.astype(jnp.float32),
    )
    attn_tokens = tokens_one(attn_core.astype(jnp.bfloat16))
    after_attn = hidden_f + tensor_sum(matrix_product(attn_tokens, attn_out))
    mlp_big, mlp_down = collect(gate_up_weight, down_weight)
    normed_m, norm_m_back = jax.vjp(rms_scale, after_attn, feedforward_norm_gain)
    xm_low = normed_m.astype(jnp.bfloat16)
    gate_pre = matrix_product(xm_low, mlp_big[0])
    up_pre = matrix_product(xm_low, mlp_big[1])
    activated, act_back = jax.vjp(gated_gelu, gate_pre, up_pre)
    hid_low = activated.astype(jnp.bfloat16)
    after_mlp = after_attn + tensor_sum(matrix_product(hid_low, mlp_down))
    mamba_big, mamba_out = collect(mixer_gate_input_weight, mixer_output_weight)
    normed_n, norm_n_back = jax.vjp(rms_scale, after_mlp, mixer_norm_gain)
    xn_low = normed_n.astype(jnp.bfloat16)
    gate_z = matrix_product(xn_low, mamba_big[0])
    inner_x = matrix_product(xn_low, mamba_big[1]).astype(jnp.bfloat16)
    step_raw = matrix_product(xn_low, step_size_weight).astype(jnp.bfloat16)
    bc_low = matrix_product(xn_low, state_map_weight).astype(jnp.bfloat16)
    x_heads, step_heads = heads_pair(inner_x, step_raw)
    bc_group = lax.all_gather(bc_low, "ctx", axis=0, tiled=True)
    bc_post, bc_conv_pull = jax.vjp(
        lambda values_in, kernel_in, conv_bias_in: causal_conv(
            values_in, kernel_in, conv_bias_in, position
        ),
        bc_group.astype(jnp.float32),
        state_map_taps,
        state_map_tap_bias,
    )
    heads_on_device_share = step_heads.shape[1]
    start_offset = ctx_index * heads_on_device_share
    channel_count_here = heads_on_device_share * MIXER_HEAD_SIZE
    channel_offset_begin = start_offset * MIXER_HEAD_SIZE
    bias_local = lax.dynamic_slice_in_dim(step_size_bias, start_offset, heads_on_device_share)
    decay_local = lax.dynamic_slice_in_dim(log_decay_rate, start_offset, heads_on_device_share)
    skip_local = lax.dynamic_slice_in_dim(head_skip_weight, start_offset, heads_on_device_share)
    kernel_local = lax.dynamic_slice_in_dim(
        mixer_input_taps, channel_offset_begin, channel_count_here, 1
    )
    conv_bias_local = lax.dynamic_slice_in_dim(
        mixer_input_tap_bias, channel_offset_begin, channel_count_here, 0
    )
    scan_out, scan_pull = jax.vjp(
        lambda xs_in, step_in, bcp_in, bias_in, decay_in, skip_weight_input, kernel_in, conv_bias_in: mamba_core(
            xs_in,
            step_in,
            bcp_in,
            bias_in,
            decay_in,
            skip_weight_input,
            kernel_in,
            conv_bias_in,
            position,
            segment,
        ),
        x_heads.astype(jnp.float32),
        step_heads.astype(jnp.float32),
        bc_post,
        bias_local,
        decay_local,
        skip_local,
        kernel_local,
        conv_bias_local,
    )
    y_tokens = tokens_one(scan_out.astype(jnp.bfloat16)).astype(jnp.float32)
    silu_z = jax.nn.silu(gate_z)
    gated = y_tokens * silu_z
    total_sq = tensor_sum(jnp.sum(gated * gated, axis=1))
    inverse = lax.rsqrt(total_sq / INNER + epsilon)[:, None]
    yn_low = (gated * inverse * gated_norm_gain).astype(jnp.bfloat16)
    after_mamba = after_mlp + tensor_sum(matrix_product(yn_low, mamba_out))
    result = after_mamba.astype(jnp.bfloat16)
    grad_out = cotangent.astype(jnp.float32)
    mamba_big, mamba_out = collect_again(mixer_gate_input_weight, mixer_output_weight)
    d_yn = matrix_product_transposed(cotangent, mamba_out)
    grad_w_out = outer_product_sum(yn_low, cotangent)
    gain_part = d_yn * gated_norm_gain
    cross = tensor_sum(jnp.sum(gain_part * gated, axis=1))
    grad_g_gate = jnp.sum(d_yn * gated * inverse, axis=0)
    d_gated = gain_part * inverse - gated * inverse**3 * (cross / INNER)[:, None]
    d_y = (d_gated * silu_z).astype(jnp.bfloat16)
    sigmoid_z = jax.nn.sigmoid(gate_z)
    d_z = (d_gated * y_tokens * sigmoid_z * (1.0 + gate_z * (1.0 - sigmoid_z))).astype(jnp.bfloat16)
    dy_heads = heads_one(d_y)
    (
        d_xs,
        d_step,
        d_bc_post,
        grad_bias_local,
        grad_decay_local,
        grad_skip_local,
        grad_kernel_local,
        grad_conv_bias_local,
    ) = scan_pull(dy_heads.astype(jnp.float32))
    d_xs_tok, d_step_tok = tokens_pair(d_xs.astype(jnp.bfloat16), d_step.astype(jnp.bfloat16))
    d_bc_ctx = lax.psum(d_bc_post.astype(jnp.bfloat16), "ctx").astype(jnp.float32)
    dxn_part = (
        matrix_product_transposed(d_z, mamba_big[0])
        + matrix_product_transposed(d_xs_tok, mamba_big[1])
        + matrix_product_transposed(d_step_tok, step_size_weight)
    )
    grad_w_zx = jnp.stack([outer_product_sum(xn_low, d_z), outer_product_sum(xn_low, d_xs_tok)])
    grad_w_dt = outer_product_sum(xn_low, d_step_tok)
    dxn_sum, d_bc_full = tensor_pair(dxn_part, d_bc_ctx)
    d_bc_pre = bc_conv_pull(d_bc_full)[0]
    d_bc_mine = lax.dynamic_slice_in_dim(d_bc_pre, ctx_index * tok_rows, tok_rows, 0)
    own_rows = (slot_index // tok_rows == ctx_index).astype(jnp.float32)[:, None]
    ignored_part, grad_conv_bc, grad_conv_bc_bias = bc_conv_pull(d_bc_full * own_rows)
    d_bc_low = d_bc_mine.astype(jnp.bfloat16)
    dxn_total = dxn_sum + matrix_product_transposed(d_bc_low, state_map_weight)
    grad_w_bc = outer_product_sum(xn_low, d_bc_low)
    d_norm_n, grad_g_mamba = norm_n_back(dxn_total)
    d_after_mlp = grad_out + d_norm_n
    shard_heads = step_size_bias.shape[0]
    zero_heads = jnp.zeros((shard_heads,), jnp.float32)
    grad_dt_bias = lax.dynamic_update_slice_in_dim(zero_heads, grad_bias_local, start_offset, 0)
    grad_a_log = lax.dynamic_update_slice_in_dim(zero_heads, grad_decay_local, start_offset, 0)
    grad_d_skip = lax.dynamic_update_slice_in_dim(zero_heads, grad_skip_local, start_offset, 0)
    grad_conv_x = lax.dynamic_update_slice_in_dim(
        jnp.zeros(mixer_input_taps.shape, jnp.float32), grad_kernel_local, channel_offset_begin, 1
    )
    grad_conv_x_bias = lax.dynamic_update_slice_in_dim(
        jnp.zeros(mixer_input_tap_bias.shape, jnp.float32),
        grad_conv_bias_local,
        channel_offset_begin,
        0,
    )
    mlp_big, mlp_down = collect_again(gate_up_weight, down_weight)
    d_mlp_low = d_after_mlp.astype(jnp.bfloat16)
    d_hid = matrix_product_transposed(d_mlp_low, mlp_down)
    grad_w_down = outer_product_sum(hid_low, d_mlp_low)
    d_gate, d_up = act_back(d_hid)
    d_gate_low = d_gate.astype(jnp.bfloat16)
    d_up_low = d_up.astype(jnp.bfloat16)
    d_xm = tensor_sum(
        matrix_product_transposed(d_gate_low, mlp_big[0])
        + matrix_product_transposed(d_up_low, mlp_big[1])
    )
    grad_w_gu = jnp.stack(
        [outer_product_sum(xm_low, d_gate_low), outer_product_sum(xm_low, d_up_low)]
    )
    d_norm_m, grad_g_mlp = norm_m_back(d_xm)
    d_after_attn = d_after_mlp + d_norm_m
    attention_block_full, attn_out = collect_again(query_key_value_weight, attention_output_weight)
    d_attn_low = d_after_attn.astype(jnp.bfloat16)
    d_tokens = matrix_product_transposed(d_attn_low, attn_out).astype(jnp.bfloat16)
    grad_w_o = outer_product_sum(attn_tokens, d_attn_low)
    d_core = heads_one(d_tokens)
    d_pairs, d_values = attn_pull(d_core.astype(jnp.float32))
    d_pair_tok, d_value_tok = tokens_pair(
        d_pairs.astype(jnp.bfloat16), d_values.astype(jnp.bfloat16)
    )
    d_paired = d_pair_tok.reshape(tok_rows, tp_heads, 2, AHD)
    projection_gradient = [
        d_paired[:, :, 0].reshape(tok_rows, tp_heads * AHD),
        d_paired[:, :, 1].reshape(tok_rows, tp_heads * AHD),
        d_value_tok,
    ]
    dxa_part = (
        matrix_product_transposed(projection_gradient[0], attention_block_full[0])
        + matrix_product_transposed(projection_gradient[1], attention_block_full[1])
        + matrix_product_transposed(projection_gradient[2], attention_block_full[2])
    )
    dmid_part = jnp.concatenate(
        [
            matrix_product_transposed(
                projection_gradient[group_member], adapter_up_maps[group_member]
            )
            for group_member in range(3)
        ],
        axis=1,
    )
    grad_w_qkv = jnp.stack(
        [
            outer_product_sum(attention_input_reduced, projection_gradient[group_member])
            for group_member in range(3)
        ]
    )
    adapter_up_gradient = jnp.stack(
        [
            outer_product_sum(
                middle_reduced_precision[group_member], projection_gradient[group_member]
            )
            for group_member in range(3)
        ]
    )
    dxa_sum, dmid_sum = tensor_pair(dxa_part, dmid_part)
    dmid_low = dmid_sum.astype(jnp.bfloat16)
    rank_column_block = adapter_down_maps.shape[2]
    middle_gradient_pieces = [
        dmid_low[:, group_member * rank_column_block : (group_member + 1) * rank_column_block]
        for group_member in range(3)
    ]
    dxa_total = (
        dxa_sum
        + matrix_product_transposed(middle_gradient_pieces[0], adapter_down_maps[0])
        + matrix_product_transposed(middle_gradient_pieces[1], adapter_down_maps[1])
        + matrix_product_transposed(middle_gradient_pieces[2], adapter_down_maps[2])
    )
    adapter_down_gradient = jnp.stack(
        [
            outer_product_sum(attention_input_reduced, middle_gradient_pieces[group_member])
            for group_member in range(3)
        ]
    )
    d_joined, grad_g_attn = norm_a_back(dxa_total)
    d_hidden = d_after_attn + d_joined[:, :MODEL_WIDTH]
    d_embeds = d_joined[:, MODEL_WIDTH:]
    grad_w_qkv, grad_w_o, grad_w_gu, grad_w_down, grad_w_zx, grad_w_out = (
        lax.psum_scatter(
            grad_w_qkv.astype(jnp.bfloat16), ("fsdp", "ctx"), scatter_dimension=1, tiled=True
        ).astype(jnp.float32),
        lax.psum_scatter(
            grad_w_o.astype(jnp.bfloat16), ("fsdp", "ctx"), scatter_dimension=1, tiled=True
        ).astype(jnp.float32),
        lax.psum_scatter(
            grad_w_gu.astype(jnp.bfloat16), ("fsdp", "ctx"), scatter_dimension=1, tiled=True
        ).astype(jnp.float32),
        lax.psum_scatter(
            grad_w_down.astype(jnp.bfloat16), ("fsdp", "ctx"), scatter_dimension=1, tiled=True
        ).astype(jnp.float32),
        lax.psum_scatter(
            grad_w_zx.astype(jnp.bfloat16), ("fsdp", "ctx"), scatter_dimension=1, tiled=True
        ).astype(jnp.float32),
        lax.psum_scatter(
            grad_w_out.astype(jnp.bfloat16), ("fsdp", "ctx"), scatter_dimension=1, tiled=True
        ).astype(jnp.float32),
    )
    (
        grad_g_attn,
        adapter_down_gradient,
        adapter_up_gradient,
        grad_g_mlp,
        grad_g_mamba,
        grad_w_bc,
        grad_w_dt,
        grad_conv_x,
        grad_conv_x_bias,
        grad_conv_bc,
        grad_conv_bc_bias,
        grad_dt_bias,
        grad_a_log,
        grad_d_skip,
        grad_g_gate,
    ) = (
        lax.psum(grad_g_attn.astype(jnp.bfloat16), ("fsdp", "ctx")).astype(jnp.float32),
        lax.psum(adapter_down_gradient.astype(jnp.bfloat16), ("fsdp", "ctx")).astype(jnp.float32),
        lax.psum(adapter_up_gradient.astype(jnp.bfloat16), ("fsdp", "ctx")).astype(jnp.float32),
        lax.psum(grad_g_mlp.astype(jnp.bfloat16), ("fsdp", "ctx")).astype(jnp.float32),
        lax.psum(grad_g_mamba.astype(jnp.bfloat16), ("fsdp", "ctx")).astype(jnp.float32),
        lax.psum(grad_w_bc.astype(jnp.bfloat16), ("fsdp", "ctx")).astype(jnp.float32),
        lax.psum(grad_w_dt.astype(jnp.bfloat16), ("fsdp", "ctx")).astype(jnp.float32),
        lax.psum(grad_conv_x.astype(jnp.bfloat16), ("fsdp", "ctx")).astype(jnp.float32),
        lax.psum(grad_conv_x_bias.astype(jnp.bfloat16), ("fsdp", "ctx")).astype(jnp.float32),
        lax.psum(grad_conv_bc.astype(jnp.bfloat16), ("fsdp", "ctx")).astype(jnp.float32),
        lax.psum(grad_conv_bc_bias.astype(jnp.bfloat16), ("fsdp", "ctx")).astype(jnp.float32),
        lax.psum(grad_dt_bias.astype(jnp.bfloat16), ("fsdp", "ctx")).astype(jnp.float32),
        lax.psum(grad_a_log.astype(jnp.bfloat16), ("fsdp", "ctx")).astype(jnp.float32),
        lax.psum(grad_d_skip.astype(jnp.bfloat16), ("fsdp", "ctx")).astype(jnp.float32),
        lax.psum(grad_g_gate.astype(jnp.bfloat16), ("fsdp", "ctx")).astype(jnp.float32),
    )
    return (
        result,
        d_hidden,
        d_embeds,
        grad_g_attn,
        adapter_down_gradient,
        grad_w_qkv,
        adapter_up_gradient,
        grad_w_o,
        grad_g_mlp,
        grad_w_gu,
        grad_w_down,
        grad_g_mamba,
        grad_w_zx,
        grad_w_bc,
        grad_w_dt,
        grad_conv_x,
        grad_conv_x_bias,
        grad_conv_bc,
        grad_conv_bc_bias,
        grad_dt_bias,
        grad_a_log,
        grad_d_skip,
        grad_g_gate,
        grad_w_out,
    )


PLANE = ("fsdp", "ctx")
EVERY = ("fsdp", "ctx", "tp")


MESH = pl.DeviceIdType.MESH
IN_VMEM = pl.BlockSpec(memory_space=pltpu.VMEM)
IN_HBM = pl.BlockSpec(memory_space=pltpu.HBM)
IN_SMEM = pl.BlockSpec(memory_space=pltpu.SMEM)
DMA = pltpu.SemaphoreType.DMA
GATHER_SHARES = (2,) * 8
SUM_SHARES = (2,) * 8
GATHER_LAGS = (0, 2, 4)
SUM_LAGS = (0, 1, 3, 5, 7)


class Place:
    def __init__(self, sizes):
        self.groups, self.ctx, self.tp = sizes
        g, c, t = (lax.axis_index(name) for name in EVERY)
        y, k = t // 2, lax.rem(t, 2)
        self.g, self.c, self.t, self.y, self.k = g, c, t, y, k
        self.core = (g, c, y * 2 + 1 - k)
        self.side_y = (g, c, (1 - y) * 2 + k)
        self.side_x = (g, 1 - c, t)
        self.line = [(lax.rem(g + d, self.groups), c, t) for d in range(1, self.groups)]
        self.plane = self.groups * self.ctx
        self.index = g * self.ctx + c

    def plane_peer(self, d):
        other = lax.rem(self.index + d, self.plane)
        return other, (other // self.ctx, lax.rem(other, self.ctx), self.t)

    def plane_source(self, d):
        return lax.rem(self.index + self.plane - d, self.plane)


def greet(devices):
    barrier = pltpu.get_barrier_semaphore()
    for device in devices:
        pl.semaphore_signal(barrier, inc=1, device_id=device, device_id_type=MESH)
    pl.semaphore_wait(barrier, len(devices))


def remote(src, dst, send_sem, recv_sem, device):
    return pltpu.make_async_remote_copy(
        src_ref=src,
        dst_ref=dst,
        send_sem=send_sem,
        recv_sem=recv_sem,
        device_id=device,
        device_id_type=MESH,
    )


def cut(ref, axis, index, width):
    if axis is None:
        return ref
    at = [slice(None)] * len(ref.shape)
    start = index * width
    if width % 128 == 0:
        start = pl.multiple_of(start, 128)
    at[axis] = pl.ds(start, width)
    return ref.at[tuple(at)]


class Moves:
    def __init__(self, place, specs, sources, targets, stages, send, recv, local):
        self.sent = []
        self.place, self.specs = place, specs
        self.sources, self.targets = sources, targets
        self.stages, self.send, self.recv, self.local = stages, send, recv, local

    def part(self, i, to, origin):
        split, join = self.specs[i]
        src, dst = self.sources[i], self.targets[i]
        n = self.place.plane
        if split is None:
            return src, cut(dst, join, origin, src.shape[join])
        return (
            cut(src, split, to, src.shape[split] // n),
            cut(dst, join, origin, dst.shape[join] // n),
        )

    def start(self, first=0):
        place = self.place
        self.loads, self.queue = [], []
        for i in range(len(self.specs)):
            self.queue += [(i, d) for d in range(1, place.plane)]
            src, _ = self.part(i, place.index, place.index)
            load = pltpu.make_async_copy(src, self.stages[i], self.local.at[i, 0])
            load.start()
            self.loads.append(load)
        self.queue.sort(key=lambda one: one[1] % place.ctx != first)

    def issue(self, count):
        for i, d in self.queue[:count]:
            other, device = self.place.plane_peer(d)
            src, dst = self.part(i, other, self.place.index)
            copy = remote(src, dst, self.send.at[i, d], self.recv.at[i, d], device)
            copy.start()
            self.sent.append(copy)
        self.queue = self.queue[count:]

    def settle(self):
        self.stores = []
        for i, load in enumerate(self.loads):
            load.wait()
            _, dst = self.part(i, self.place.index, self.place.index)
            store = pltpu.make_async_copy(self.stages[i], dst, self.local.at[i, 1])
            store.start()
            self.stores.append(store)

    def finish(self):
        place = self.place
        for i in range(len(self.specs)):
            for d in range(1, place.plane):
                _, device = place.plane_peer(d)
                src, dst = self.part(i, place.index, place.plane_source(d))
                remote(src, dst, self.send.at[i, d], self.recv.at[i, d], device).wait_recv()
        for copy in self.sent:
            copy.wait_send()
        for store in self.stores:
            store.wait()


def moves_setup(moves, plane):
    outs, scratch = [], []
    for array, split, join in moves:
        shape = list(array.shape)
        part = list(array.shape)
        if split is not None:
            part[split] //= plane
            shape[split] //= plane
        shape[join] *= plane
        outs.append(jax.ShapeDtypeStruct(tuple(shape), array.dtype))
        scratch.append(pltpu.VMEM(tuple(part), array.dtype))
    n = len(moves)
    if n:
        scratch += [DMA((n, plane)), DMA((n, plane)), DMA((n, 2))]
    return outs, scratch


class Gather:
    def __init__(self, place, x, o, pieces, sems):
        self.place, self.x, self.o, self.pieces, self.sems = place, x, o, pieces, sems
        self.n = len(pieces)
        self.first, self.second = [], [None] * self.n
        self.third, self.fourth = [None] * self.n, [None] * self.n

    def line_copy(self, q, d, owner):
        place, cols = self.place, pl.ds(*self.pieces[q])
        return remote(
            self.x.at[:, cols],
            self.o.at[owner, place.c, place.y, place.k, :, cols],
            self.sems[0].at[q, d],
            self.sems[1].at[q, d],
            place.line[d],
        )

    def begin(self):
        place = self.place
        own_at = self.o.at[place.g, place.c, place.y, place.k]
        own = pltpu.make_async_copy(self.x, own_at, self.sems[8])
        own.start()
        for q in range(self.n):
            for d in range(place.groups - 1):
                copy = self.line_copy(q, d, place.g)
                copy.start()
                self.first.append(copy)
        own.wait()

    def to_side(self, q):
        place = self.place
        for d in range(place.groups - 1):
            source = lax.rem(place.g + place.groups - d - 1, place.groups)
            self.line_copy(q, d, source).wait_recv()
        part = self.o.at[:, place.c, place.y, place.k, :, pl.ds(*self.pieces[q])]
        device = place.side_y if q % 2 == 0 else place.side_x
        self.second[q] = remote(part, part, self.sems[2].at[q], self.sems[3].at[q], device)
        self.second[q].start()

    def to_other_side(self, q):
        place, cols = self.place, pl.ds(*self.pieces[q])
        self.second[q].wait_recv()
        if q % 2 == 0:
            part, device = self.o.at[:, place.c, :, place.k, :, cols], place.side_x
        else:
            part, device = self.o.at[:, :, place.y, place.k, :, cols], place.side_y
        self.third[q] = remote(part, part, self.sems[4].at[q], self.sems[5].at[q], device)
        self.third[q].start()

    def to_core(self, q):
        place = self.place
        self.third[q].wait_recv()
        part = self.o.at[:, :, :, place.k, :, pl.ds(*self.pieces[q])]
        self.fourth[q] = remote(part, part, self.sems[6].at[q], self.sems[7].at[q], place.core)
        self.fourth[q].start()

    def steps(self):
        return pipelined(self.n, (self.to_side, self.to_other_side, self.to_core), GATHER_LAGS)

    def end(self):
        for copy in self.fourth:
            copy.wait_recv()
        for copy in self.first + self.second + self.third + self.fourth:
            copy.wait_send()


class PlaneGather:
    def __init__(self, place, x, o, zs, zr, ss, sr, own_sem):
        self.place, self.x, self.o, self.zs, self.zr = place, x, o, zs, zr
        self.ss, self.sr, self.own_sem = ss, sr, own_sem

    def line_copy(self, d, owner):
        place = self.place
        to = self.o.at[owner, place.c]
        return remote(self.x, to, self.zs.at[d], self.zr.at[d], place.line[d])

    def begin(self):
        place = self.place
        self.own = pltpu.make_async_copy(self.x, self.o.at[place.g, place.c], self.own_sem)
        self.own.start()
        for d in range(place.groups - 1):
            self.line_copy(d, place.g).start()

    def step(self):
        place = self.place
        self.own.wait()
        for d in range(place.groups - 1):
            self.line_copy(d, lax.rem(place.g + place.groups - d - 1, place.groups)).wait_recv()
        part = self.o.at[:, place.c]
        self.onward = remote(part, part, self.ss, self.sr, place.side_x)
        self.onward.start()

    def end(self):
        self.onward.wait_recv()
        self.onward.wait_send()
        for d in range(self.place.groups - 1):
            self.line_copy(d, self.place.g).wait_send()


def pipelined(count, stages, lags):
    def step(at):
        for stage, lag in zip(stages, lags):
            if 0 <= at - lag < count:
                stage(at - lag)

    return [functools.partial(step, at) for at in range(count + max(lags))]


def gather_sems(n, groups):
    return [DMA((n, groups - 1)), DMA((n, groups - 1))] + [DMA((n,))] * 6 + [DMA]


class Scatter:
    def __init__(self, place, make, pieces, bufs, acc, sems):
        self.place, self.make, self.pieces, self.bufs, self.acc = place, make, pieces, bufs, acc
        self.sems = sems
        n = len(pieces)
        self.n = n
        self.c1, self.c2, self.c3, self.c4 = [None] * n, [None] * n, [None] * n, [None] * n

    def to_core(self, q):
        theirs, mine, b1 = self.bufs[:3]
        cols, k = pl.ds(*self.pieces[q]), self.place.k
        self.make(q, theirs, 1 - k)
        self.c1[q] = remote(
            theirs.at[..., cols],
            b1.at[..., cols],
            self.sems[0].at[q],
            self.sems[1].at[q],
            self.place.core,
        )
        self.c1[q].start()
        self.make(q, mine, k)

    def to_side(self, q):
        _, mine, b1, b2, _, _ = self.bufs
        place, cols = self.place, pl.ds(*self.pieces[q])
        f32 = jnp.float32
        self.c1[q].wait_recv()
        b1[..., cols] = (b1[..., cols].astype(f32) + mine[..., cols].astype(f32)).astype(b1.dtype)
        if q % 2 == 0:
            part, device = b1.at[:, :, 1 - place.y, :, cols], place.side_y
        else:
            part, device = b1.at[:, 1 - place.c, :, :, cols], place.side_x
        self.c2[q] = remote(
            part, b2.at[:, :, :, cols], self.sems[2].at[q], self.sems[3].at[q], device
        )
        self.c2[q].start()

    def to_other_side(self, q):
        _, _, b1, b2, b3, _ = self.bufs
        place, cols = self.place, pl.ds(*self.pieces[q])
        f32 = jnp.float32
        self.c2[q].wait_recv()
        own = b1[:, :, place.y, :, cols] if q % 2 == 0 else b1[:, place.c, :, :, cols]
        b2[:, :, :, cols] = (b2[:, :, :, cols].astype(f32) + own.astype(f32)).astype(b2.dtype)
        if q % 2 == 0:
            part, device = b2.at[:, 1 - place.c, :, cols], place.side_x
        else:
            part, device = b2.at[:, 1 - place.y, :, cols], place.side_y
        self.c3[q] = remote(part, b3.at[:, :, cols], self.sems[4].at[q], self.sems[5].at[q], device)
        self.c3[q].start()

    def along_line(self, q):
        _, _, _, b2, b3, b4 = self.bufs
        place, cols = self.place, pl.ds(*self.pieces[q])
        f32 = jnp.float32
        self.c3[q].wait_recv()
        own = b2[:, place.c, :, cols] if q % 2 == 0 else b2[:, place.y, :, cols]
        b3[:, :, cols] = (b3[:, :, cols].astype(f32) + own.astype(f32)).astype(b3.dtype)
        self.c4[q] = []
        for d in range(place.groups - 1):
            to = lax.rem(place.g + d + 1, place.groups)
            copy = remote(
                b3.at[to, :, cols],
                b4.at[d, :, cols],
                self.sems[6].at[q, d],
                self.sems[7].at[q, d],
                place.line[d],
            )
            copy.start()
            self.c4[q].append(copy)

    def land(self, q):
        b3, b4 = self.bufs[4:]
        cols = pl.ds(*self.pieces[q])
        total = b3[self.place.g, :, cols].astype(jnp.float32)
        for d in range(self.place.groups - 1):
            self.c4[q][d].wait_recv()
            total = total + b4[d, :, cols].astype(jnp.float32)
        self.acc[:, cols] = total

    def steps(self):
        stages = (self.to_core, self.to_side, self.to_other_side, self.along_line, self.land)
        return pipelined(self.n, stages, SUM_LAGS)

    def end(self):
        for q in range(self.n):
            for copy in [self.c1[q], self.c2[q], self.c3[q]] + self.c4[q]:
                copy.wait_send()


class SmallSum:
    def __init__(self, place, x, o, zbuf, buf, zs, zr, ss, rs):
        self.place, self.x, self.o, self.zbuf, self.buf = place, x, o, zbuf, buf
        self.zs, self.zr, self.ss, self.rs = zs, zr, ss, rs

    def begin(self):
        self.copies = []
        for d, device in enumerate(self.place.line):
            copy = remote(self.x, self.zbuf.at[d], self.zs.at[d], self.zr.at[d], device)
            copy.start()
            self.copies.append(copy)

    def line(self):
        place, groups = self.place, self.place.groups
        for copy in self.copies:
            copy.wait_recv()
        total = None
        for owner in range(groups):
            part = self.x[...]
            for d in range(groups - 1):
                source = lax.rem(place.g + groups - d - 1, groups)
                part = jnp.where(source == owner, self.zbuf[d], part)
            total = part if total is None else total + part
        self.o[...] = total
        self.send(0)

    def send(self, i):
        device = (self.place.side_x, self.place.side_y, self.place.core)[i]
        self.copy = remote(self.o, self.buf.at[i], self.ss.at[i], self.rs.at[i], device)
        self.copy.start()

    def add(self, i):
        self.copy.wait_recv()
        self.copy.wait_send()
        self.o[...] = self.o[...] + self.buf[i]
        if i < 2:
            self.send(i + 1)

    def steps(self):
        return [self.line] + [functools.partial(self.add, i) for i in range(3)]

    def end(self):
        for copy in self.copies:
            copy.wait_send()


def small_scratch(shape, groups):
    f32 = jnp.float32
    return [
        pltpu.VMEM((groups - 1, *shape), f32),
        pltpu.VMEM((3, *shape), f32),
        DMA((groups - 1,)),
        DMA((groups - 1,)),
        DMA((3,)),
        DMA((3,)),
    ]


def weave(*streams):
    found = []
    rounds = max((start + len(steps) for start, steps in streams), default=0)
    for at in range(rounds):
        for start, steps in streams:
            if 0 <= at - start < len(steps):
                found.append(steps[at - start])
    return found


def scatter_scratch(n, groups, rows, width):
    bf16 = jnp.bfloat16
    bufs = [
        pltpu.VMEM((groups, 2, 2, rows, width), bf16),
        pltpu.VMEM((groups, 2, 2, rows, width), bf16),
        pltpu.VMEM((groups, 2, 2, rows, width), bf16),
        pltpu.VMEM((groups, 2, rows, width), bf16),
        pltpu.VMEM((groups, rows, width), bf16),
        pltpu.VMEM((groups - 1, rows, width), bf16),
        pltpu.VMEM((rows, width), jnp.float32),
    ]
    sems = [DMA((n,))] * 6 + [DMA((n, groups - 1))] * 2
    return bufs, sems


def rms_rows(x, gain):
    return x * lax.rsqrt(jnp.mean(x * x, axis=-1, keepdims=True) + epsilon) * gain


def rms_back(x, gain, grad):
    inverse = lax.rsqrt(jnp.mean(x * x, axis=-1, keepdims=True) + epsilon)
    scaled = grad * gain
    along = jnp.mean(scaled * x, axis=-1, keepdims=True)
    d_gain = jnp.sum(grad * x * inverse, axis=0, keepdims=True)
    return scaled * inverse - x * inverse**3 * along, d_gain


NT = (((1,), (1,)), ((), ()))
NN = (((1,), (0,)), ((), ()))


class Summed:
    def __init__(self, sizes, products, extra=None, pieces=SUM_SHARES):
        self.sizes, self.products, self.extra = sizes, products, extra
        self.rows = products[0][0].shape[0] // (sizes[0] * sizes[1] * sizes[2])
        self.width = products[0][1].shape[-2 if products[0][3] else -1]
        self.more = 0 if extra is None else extra.shape[1]
        self.rights, self.places = [], []
        for _, right, _, _ in products:
            found = [i for i, other in enumerate(self.rights) if other is right]
            self.places.append(found[0] if found else len(self.rights))
            if not found:
                self.rights.append(right)
        at, self.pieces = 0, []
        for share in pieces:
            self.pieces.append((at, self.width * share // 16))
            at += self.width * share // 16
        if self.more:
            self.pieces.append((self.width, self.more))
        self.bufs, self.sems = scatter_scratch(
            len(self.pieces), sizes[0], self.rows, self.width + self.more
        )

    def operands(self):
        groups, ctx, tp = self.sizes
        split = (groups, ctx, tp // 2, 2, self.rows)
        found = [product[0].reshape(*split, product[0].shape[1]) for product in self.products]
        found += self.rights
        if self.more:
            found.append(self.extra.reshape(*split, self.more))
        return found

    def stage(self, place, inputs, scratch):
        count = len(self.products)
        lefts, rights = inputs[:count], inputs[count : count + len(self.rights)]
        bufs, sems = scratch[: len(self.bufs)], scratch[len(self.bufs) :]
        groups, ctx, tp = self.sizes

        def make(q, into, core):
            at, size = self.pieces[q]
            if at >= self.width:
                into[..., pl.ds(at, size)] = inputs[-1][:, :, :, core]
                return

            def block(i, _):
                total = None
                for left, where, (_, _, lead, transposed) in zip(
                    lefts, self.places, self.products
                ):
                    right = rights[where] if lead is None else rights[where].at[lead]
                    a = left[i, :, :, core]
                    a = a.reshape(-1, a.shape[-1])
                    some = right[pl.ds(at, size), :] if transposed else right[:, pl.ds(at, size)]
                    part = lax.dot_general(
                        a, some, NT if transposed else NN, preferred_element_type=jnp.float32
                    )
                    total = part if total is None else total + part
                into[i, :, :, :, pl.ds(at, size)] = total.astype(into.dtype).reshape(
                    ctx, tp // 2, self.rows, size
                )
                return 0

            lax.fori_loop(0, groups, block, 0)

        return Scatter(place, make, self.pieces, bufs[:-1], bufs[-1], sems)


def exchange(
    sizes,
    number,
    summed,
    finish,
    finish_args,
    finish_outs,
    gathered,
    moves,
    plan=(3,),
    start_also=5,
    start_second=10,
    also_gather=None,
    also_sum=None,
    tail=0,
    small=0,
    spread=None,
):
    groups, ctx, tp = sizes
    f32, bf16 = jnp.float32, jnp.bfloat16
    rows = summed.rows
    out_pieces = gather_pieces(gathered)
    move_outs, move_scratch = moves_setup(moves, groups * ctx)
    n_moves = len(moves)
    move_specs = [(split, join) for _, split, join in moves]
    S = jax.ShapeDtypeStruct

    operands, in_specs, out_shape, out_specs, scratch = [], [], [], [], []

    def add_in(arrays, spec=IN_VMEM):
        at = len(operands)
        operands.extend(arrays)
        in_specs.extend([spec] * len(arrays))
        return slice(at, len(operands))

    def add_out(shapes, spec=IN_VMEM):
        at = len(out_shape)
        out_shape.extend(shapes)
        out_specs.extend([spec] * len(shapes))
        return slice(at, len(out_shape))

    def add_scratch(shapes):
        at = len(scratch)
        scratch.extend(shapes)
        return slice(at, len(scratch))

    in_sum = add_in(summed.operands())
    in_args = add_in(list(finish_args))
    o_main = add_out([S((groups, ctx, tp // 2, 2, rows, gathered), bf16)])
    o_finish = add_out([S(shape, f32) for shape in finish_outs])
    s_sum = add_scratch(summed.bufs + summed.sems)
    s_main = add_scratch(
        [pltpu.VMEM((rows, gathered), bf16)] + gather_sems(len(out_pieces), groups)
    )
    if also_gather is not None:
        also_pieces = gather_pieces(also_gather.shape[1])
        in_also = add_in([also_gather])
        o_also = add_out([S((groups, ctx, tp // 2, 2, rows, also_gather.shape[1]), bf16)])
        s_also = add_scratch(gather_sems(len(also_pieces), groups))
    if also_sum is not None:
        second, second_finish, second_args, second_out = also_sum
        in_second, in_second_args = add_in(second.operands()), add_in(second_args)
        o_second = add_out([second_out])
        s_second = add_scratch(second.bufs + second.sems)
    if tail:
        o_tail = add_out([S((tp // 2, 2, rows, tail), bf16)])
        s_tail = add_scratch([pltpu.VMEM((rows, tail), bf16)] + [DMA] * 5)
    if small:
        o_small = add_out([S((1, small), f32)])
        s_small = add_scratch([pltpu.VMEM((1, small), f32)] + small_scratch((1, small), groups))
    if spread is not None:
        in_spread = add_in([spread])
        o_spread = add_out([S((groups, ctx, *spread.shape), spread.dtype)])
        s_spread = add_scratch([DMA((groups - 1,)), DMA((groups - 1,)), DMA, DMA, DMA])
    in_moves = add_in([array for array, _, _ in moves], IN_HBM)
    o_moves = add_out(move_outs, IN_HBM)
    s_moves = add_scratch(move_scratch)

    def kernel(*refs):
        ins = refs[: len(operands)]
        outs = refs[len(operands) : len(operands) + len(out_shape)]
        scr = refs[len(operands) + len(out_shape) :]
        place = Place(sizes)
        devices = [place.core, place.side_y]
        if n_moves:
            devices += [place.plane_peer(d)[1] for d in range(1, place.plane)]
        else:
            devices += [place.side_x] + place.line
        greet(devices)
        carried = None
        if n_moves:
            parts = scr[s_moves]
            carried = Moves(
                place, move_specs, ins[in_moves], outs[o_moves], parts[:n_moves], *parts[n_moves:]
            )
            carried.start()
        main_sum = summed.stage(place, ins[in_sum], scr[s_sum])
        low, *main_sems = scr[s_main]
        main_gather = Gather(place, low, outs[o_main][0], out_pieces, main_sems)
        streams = [(0, main_sum.steps())]
        ends = [main_sum, main_gather]
        if also_gather is not None:
            side_gather = Gather(place, ins[in_also][0], outs[o_also][0], also_pieces, scr[s_also])
            side_gather.begin()
            streams.append((start_also, side_gather.steps()))
            ends.append(side_gather)
        if spread is not None:
            plane = PlaneGather(place, ins[in_spread][0], outs[o_spread][0], *scr[s_spread])
            plane.begin()
            streams.append((6, [plane.step]))
            ends.append(plane)
        later = []
        if also_sum is not None:
            side_sum = second.stage(place, ins[in_second], scr[s_second])
            side_steps = side_sum.steps()
            ready = max(0, min(len(side_steps), len(summed.pieces) + SUM_LAGS[-1] - start_second))
            streams.append((start_second, side_steps[:ready]))
            later.append((0, side_steps[ready:]))
            ends.append(side_sum)
        total = n_moves * (groups * ctx - 1)
        steps = weave(*streams)
        for i, step in enumerate(steps):
            if carried is not None and i < len(plan):
                carried.issue(plan[i])
            step()
        if carried is not None:
            carried.settle()
        low_tail = scr[s_tail][0] if tail else None
        low_small = scr[s_small][0] if small else None
        finish(place, main_sum.acc, ins[in_args], outs[o_finish], low, low_tail, low_small)
        main_gather.begin()
        if small:
            small_sum = SmallSum(place, low_small, outs[o_small][0], *scr[s_small][1:])
            small_sum.begin()
            later.append((1, small_sum.steps()))
            ends.append(small_sum)
        if tail:
            ys, yr, ks, kr, own_sem = scr[s_tail][1:]
            y, k, spot = place.y, place.k, outs[o_tail][0]
            own = pltpu.make_async_copy(low_tail, spot.at[y, k], own_sem)
            own.start()
            to_y = remote(low_tail, spot.at[y, k], ys, yr, place.side_y)
            to_y.start()
            own.wait()
        steps = weave((0, main_gather.steps()), *later)
        if carried is not None:
            carried.issue(total)
        for step in steps:
            step()
        if tail:
            to_y.wait_recv()
            part = spot.at[:, k]
            to_k = remote(part, part, ks, kr, place.core)
            to_k.start()
            to_k.wait_recv()
            to_y.wait_send()
            to_k.wait_send()
        if also_sum is not None:
            second_finish(side_sum.acc, ins[in_second_args], outs[o_second][0])
        for stage in ends:
            stage.end()
        if carried is not None:
            carried.finish()

    results = pl.pallas_call(
        kernel,
        out_shape=out_shape,
        in_specs=in_specs,
        out_specs=out_specs,
        scratch_shapes=scratch,
        name=f"exchange_{number}",
        compiler_params=pltpu.CompilerParams(
            collective_id=number, has_side_effects=True, vmem_limit_bytes=62 * 2**20
        ),
    )(*operands)
    found = {"gathered": results[0].reshape(-1, gathered), "finish": results[o_finish]}
    if also_gather is not None:
        found["also"] = results[o_also][0].reshape(-1, also_gather.shape[1])
    if also_sum is not None:
        found["second"] = results[o_second][0]
    if tail:
        found["tail"] = results[o_tail][0].reshape(-1, tail)
    if small:
        found["small"] = results[o_small][0]
    if spread is not None:
        found["spread"] = results[o_spread][0]
    found["moves"] = results[o_moves]
    return found


def gather_pieces(width):
    if width < 1024:
        return [(0, width)]
    whole = width // 2048 * 2048
    at, found = 0, []
    for share in GATHER_SHARES:
        found.append((at, whole * share // 16))
        at += whole * share // 16
    if width > whole:
        found.append((whole, width - whole))
    return found


def opening(sizes, number, hidden, embeds, cotangent, lengths, gain, down_maps, shard, moves):
    groups, ctx, tp = sizes
    f32, bf16 = jnp.float32, jnp.bfloat16
    rows = hidden.shape[0] // tp
    half = hidden.shape[1]
    rank = down_maps.shape[2]
    mids = down_maps.shape[0] * rank
    rest = 3 * half
    width = rest + mids + 128
    out_pieces = gather_pieces(width)
    move_outs, move_scratch = moves_setup(moves, groups * ctx)
    move_specs = [(split, join) for _, split, join in moves]
    n_moves = len(moves)

    def kernel(*refs):
        hid, emb, cot, lens, gain_ref, down_ref = refs[:6]
        up_ref, step_ref, taps_ref, bias_ref, norm_ref, *head_refs = refs[6:14]
        refs = list(refs[14:])
        sources = refs[:n_moves]
        o, up_o, step_o, small_o = refs[n_moves : n_moves + 4]
        targets = refs[n_moves + 4 : 2 * n_moves + 4]
        own = refs[2 * n_moves + 4 :]
        low, gs = own[0], own[1:10]
        stages = own[10 : 10 + n_moves]
        send, recv, local = own[10 + n_moves :]
        place = Place(sizes)
        greet(
            [place.core, place.side_y]
            + [place.plane_peer(d)[1] for d in range(1, place.plane)]
        )
        carried = Moves(place, move_specs, sources, targets, stages, send, recv, local)
        carried.start(1)
        mine = pl.ds(pl.multiple_of(place.t * rows, 16), rows)
        a, b = hid[mine, :].astype(f32), emb[mine, :].astype(f32)
        squares = jnp.sum(a * a, axis=1, keepdims=True) + jnp.sum(b * b, axis=1, keepdims=True)
        inverse = lax.rsqrt(squares / (2 * half) + epsilon)
        low[:, :half] = (a * inverse * gain_ref[:, :half]).astype(bf16)
        low[:, half : 2 * half] = (b * inverse * gain_ref[:, half:]).astype(bf16)
        for j in range(down_maps.shape[0]):
            at = rest + j * rank
            low[:, at : at + rank] = lax.dot_general(
                low[:, : 2 * half], down_ref[j], NN, preferred_element_type=f32
            ).astype(bf16)
        slot = lax.broadcasted_iota(jnp.int32, (rows, 128), 0)
        slot = slot + (place.c * tp + place.t) * rows
        lane = lax.broadcasted_iota(jnp.int32, (rows, 128), 1)
        segment, position, end = jnp.zeros_like(slot), slot, 0
        for i in range(lengths.shape[1]):
            length = lens[0, i]
            end = end + length
            passed = (slot >= end).astype(jnp.int32)
            segment = segment + passed
            position = position - passed * length
        marks = jnp.where(lane == 0, segment, position)
        low[:, 2 * half : rest] = cot[mine, :]
        low[:, rest + mids :] = marks.astype(f32).astype(bf16)
        gather = Gather(place, low, o, out_pieces, gs)
        gather.begin()
        carried.issue(len(carried.queue))
        lanes = pl.ds(pl.multiple_of(place.index * 128, 128), 128)
        for j in range(up_o.shape[0]):
            up_o[j] = up_ref[j, :, lanes]
        heads = step_ref.shape[1]
        few = heads // place.plane
        row = lax.broadcasted_iota(jnp.int32, (heads, 128), 0) - place.index * few
        col = lax.broadcasted_iota(jnp.int32, (heads, 128), 1)
        pick = (row == col) & (col < few)
        wide = row == col // (128 // few)
        step_o[...] = lax.dot_general(
            step_ref[...], pick.astype(bf16), NN, preferred_element_type=f32
        ).astype(bf16)
        small_o[...] = jnp.zeros_like(small_o)
        small_o[0:4, :] = taps_ref[:, lanes]
        small_o[4:5, :] = bias_ref[:, lanes]
        small_o[6:7, :] = norm_ref[:, lanes]
        for at, head_ref, chosen in zip((5, 8, 9), head_refs, (wide, pick, pick)):
            small_o[at : at + 1, :] = lax.dot_general(
                jnp.broadcast_to(head_ref[...], (8, heads)),
                chosen.astype(f32),
                NN,
                precision=highest,
                preferred_element_type=f32,
            )[0:1]
        for step in gather.steps():
            step()
        carried.settle()
        gather.end()
        carried.finish()

    S = jax.ShapeDtypeStruct
    results = pl.pallas_call(
        kernel,
        out_shape=[
            S((groups, ctx, tp // 2, 2, rows, width), bf16),
            S((*shard[0].shape[:2], 128), bf16),
            S((shard[1].shape[0], 128), bf16),
            S((16, 128), f32),
        ]
        + move_outs,
        in_specs=[IN_VMEM] * 3 + [IN_SMEM] + [IN_VMEM] * 10 + [IN_HBM] * n_moves,
        out_specs=[IN_VMEM] * 4 + [IN_HBM] * n_moves,
        scratch_shapes=[pltpu.VMEM((rows, width), bf16)]
        + gather_sems(len(out_pieces), groups)
        + move_scratch,
        name=f"opening_{number}",
        compiler_params=pltpu.CompilerParams(
            collective_id=number, has_side_effects=True, vmem_limit_bytes=62 * 2**20
        ),
    )(
        *(hidden, embeds, cotangent, lengths, gain.reshape(1, -1), down_maps),
        *shard,
        *[array for array, _, _ in moves],
    )
    return [results[0].reshape(-1, width)] + list(results[1:])


def sum_small(sizes, number, values):
    def kernel(x, o, *scratch):
        place = Place(sizes)
        greet([place.core, place.side_y, place.side_x] + place.line)
        summing = SmallSum(place, x, o, *scratch)
        summing.begin()
        for step in summing.steps():
            step()
        summing.end()

    return pl.pallas_call(
        kernel,
        out_shape=jax.ShapeDtypeStruct(values.shape, jnp.float32),
        in_specs=[IN_VMEM],
        out_specs=IN_VMEM,
        scratch_shapes=small_scratch(values.shape, sizes[0]),
        name=f"sum_small_{number}",
        compiler_params=pltpu.CompilerParams(collective_id=number, has_side_effects=True),
    )(values)


def own_of(place, ref, rows):
    if ref.shape[0] == rows:
        return ref[...].astype(jnp.float32)
    return ref[pl.ds(pl.multiple_of(place.t * rows, 16), rows), :].astype(jnp.float32)


def finish_forward(place, acc, args, outs, low, low_tail, low_small):
    rest, gain = args
    outs[0][...] = own_of(place, rest, acc.shape[0]) + acc[...]
    low[...] = rms_rows(outs[0][...], gain[...]).astype(jnp.bfloat16)


def finish_mixer_back(place, acc, args, outs, low, low_tail, low_small):
    after_mlp, gain, cot, state_map = args
    width = after_mlp.shape[1]
    low[:, width:] = acc[:, width:].astype(jnp.bfloat16)
    d_normed = acc[:, :width] + lax.dot_general(
        low[:, width:], state_map[...], NT, preferred_element_type=jnp.float32
    )
    d_rows, d_gain = rms_back(after_mlp[...], gain[...], d_normed)
    outs[1][...] = d_gain
    d_rows = cot[...].astype(jnp.float32) + d_rows
    outs[0][...] = d_rows
    low[:, :width] = d_rows.astype(jnp.bfloat16)


def finish_mlp_back(place, acc, args, outs, low, low_tail, low_small):
    after_attn, gain, d_after_mlp = args
    d_rows, d_gain = rms_back(after_attn[...], gain[...], acc[...])
    outs[1][...] = d_gain
    d_rows = d_after_mlp[...] + d_rows
    outs[0][...] = d_rows
    low[...] = d_rows.astype(jnp.bfloat16)


def finish_attention_back(place, acc, args, outs, low, low_tail, low_small):
    hidden, embeds, gain, d_after_attn, down_maps, out_mine, row = args
    half = hidden.shape[1]
    bf16, f32 = jnp.bfloat16, jnp.float32
    low[...] = acc[:, 2 * half :].astype(bf16)
    inputs = [own_of(place, part, acc.shape[0]) for part in (hidden, embeds)]
    squares = sum(jnp.sum(part * part, axis=1, keepdims=True) for part in inputs)
    inverse = lax.rsqrt(squares / (2 * half) + epsilon)
    along = jnp.zeros_like(squares)
    for i, part in enumerate(inputs):
        cols = slice(i * half, (i + 1) * half)
        grad = acc[:, cols]
        for j in range(down_maps.shape[0]):
            rank = down_maps.shape[2]
            grad = grad + lax.dot_general(
                low[:, j * rank : (j + 1) * rank],
                down_maps[j, cols, :],
                NT,
                preferred_element_type=f32,
            )
        acc[:, cols] = grad
        along = along + jnp.sum(grad * gain[:, cols] * part, axis=1, keepdims=True)
    along = along / (2 * half)
    low_tail[:, :half] = out_mine[...]
    low_small[:, 2 * half :] = row[...]
    for i, part in enumerate(inputs):
        cols = slice(i * half, (i + 1) * half)
        grad = acc[:, cols]
        low_small[:, cols] = jnp.sum(grad * part * inverse, axis=0, keepdims=True)
        d_rows = grad * gain[:, cols] * inverse - part * inverse**3 * along
        if i == 0:
            d_rows = d_rows + d_after_attn[...]
        low_tail[:, (i + 1) * half : (i + 2) * half] = d_rows.astype(bf16)


def finish_out(acc, args, out):
    out[...] = (args[0][...] + acc[...]).astype(out.dtype)


def adapter_products(xa, dmid, width):
    block, rank = 1024, dmid.shape[1] // 3

    def kernel(a, b, o, b_t):
        @pl.when(pl.program_id(0) == 0)
        def _():
            b_t[...] = b[...].T

        both = quick(b_t[...], a[...], NN)
        for j in range(3):
            o[j] = both[j * rank : (j + 1) * rank].T

    return pl.pallas_call(
        kernel,
        out_shape=jax.ShapeDtypeStruct((3, width, rank), jnp.float32),
        grid=(width // block,),
        in_specs=[
            pl.BlockSpec((xa.shape[0], block), lambda i: (0, i)),
            pl.BlockSpec(dmid.shape, lambda i: (0, 0)),
        ],
        out_specs=pl.BlockSpec((3, block, rank), lambda i: (0, i, 0)),
        scratch_shapes=[pltpu.VMEM(dmid.shape[::-1], dmid.dtype)],
        compiler_params=pltpu.CompilerParams(vmem_limit_bytes=60 * 2**20),
        name="adapter_products",
    )(xa, dmid)


def unpack(packed, parts):
    flat, at, found = packed.reshape(-1), 0, []
    for part in parts:
        found.append(flat[at : at + part.size].reshape(part.shape))
        at += part.size
    return found


TN = (((0,), (0,)), ((), ()))


def exact(left, right, dims):
    return lax.dot_general(left, right, dims, precision=highest, preferred_element_type=jnp.float32)


def quick(left, right, dims):
    return lax.dot_general(left, right, dims, preferred_element_type=jnp.float32)


def down_rows(values, by):
    return pltpu.roll(values, by, 0)


def up_rows(values, by):
    return pltpu.roll(values, values.shape[0] - by, 0)


def taps_forward(values, taps, bias, position):
    total = values * taps[0:1, :] + bias
    for lag in range(1, taps.shape[0]):
        kept = jnp.where(position >= lag, down_rows(values, lag), 0.0)
        total = total + kept * taps[lag : lag + 1, :]
    return total


def taps_backward(d_total, values, taps, position):
    d_values = d_total * taps[0:1, :]
    rows = [jnp.sum(d_total * values, axis=0, keepdims=True)]
    for lag in range(1, taps.shape[0]):
        kept = jnp.where(position >= lag, d_total, 0.0)
        rows.append(jnp.sum(kept * down_rows(values, lag), axis=0, keepdims=True))
        d_values = d_values + up_rows(kept, lag) * taps[lag : lag + 1, :]
    return d_values, rows + [jnp.sum(d_total, axis=0, keepdims=True)]


def silu_slope(values):
    sigmoid = jax.nn.sigmoid(values)
    return sigmoid * (1.0 + values * (1.0 - sigmoid))


class Scan:
    def __init__(self, xs, raw, bc, marks, taps, bias, bc_taps, bc_bias, heads):
        f32 = jnp.float32
        rows, lanes = xs.shape
        self.rows, self.half = rows, lanes // 2
        self.position = marks[:, 1:2].astype(f32)
        self.lane = lax.broadcasted_iota(jnp.int32, (rows, lanes), 1)
        self.xs, self.bc = xs.astype(f32), bc.astype(f32)
        self.pre_x = taps_forward(self.xs, taps, bias, self.position)
        self.pre_bc = taps_forward(self.bc, bc_taps, bc_bias, self.position)
        self.xc, bcc = jax.nn.silu(self.pre_x), jax.nn.silu(self.pre_bc)
        self.b_mat, self.c_mat = bcc[:, :STATE], bcc[:, STATE:]
        self.step_in = raw.astype(f32) + heads[0:1, :]
        self.dt = jax.nn.softplus(self.step_in)
        self.rate = -jnp.exp(heads[1:2, :])
        self.log_decay = self.dt * self.rate
        running, by = self.log_decay, 1
        while by < rows:
            running = running + jnp.where(self.position >= by, down_rows(running, by), 0.0)
            by *= 2
        self.running = running
        self.across = running.T
        row = lax.broadcasted_iota(jnp.int32, (rows, rows), 0)
        col = lax.broadcasted_iota(jnp.int32, (rows, rows), 1)
        first = row.astype(f32) - self.position
        self.same = (col <= row) & (col.astype(f32) >= first)
        self.meet = exact(self.c_mat, self.b_mat, NT)
        self.dt_wide = self.by_head([self.dt[:, h : h + 1] for h in range(2)])
        self.weighted = self.xc * self.dt_wide

    def by_head(self, values):
        return jnp.where(self.lane < self.half, values[0], values[1])

    def in_lane(self, values):
        return jnp.where(self.lane == 0, values[0], jnp.where(self.lane == 1, values[1], 0.0))

    def decay(self, h):
        gap = self.running[:, h : h + 1] - self.across[h : h + 1, :]
        return jnp.where(self.same, jnp.exp(jnp.where(self.same, gap, 0.0)), 0.0)

    def forward(self, skip):
        outs = [exact(self.decay(h) * self.meet, self.weighted, NN) for h in range(2)]
        return self.by_head(outs) + skip * self.xc

    def to_ends(self, values):
        rows = values.shape[0]
        row = lax.broadcasted_iota(jnp.int32, values.shape, 0)
        wide = jnp.broadcast_to(self.position, values.shape)
        by = 1
        while by < rows:
            inside = (up_rows(wide, by) >= by) & (row < rows - by)
            values = values + jnp.where(inside, up_rows(values, by), 0.0)
            by *= 2
        return values


def mixer_forward(xn, marked, mark_block, w_zx, w_step, state_map, w_out, small, bc_taps, bc_bias, groups):
    f32, bf16 = jnp.float32, jnp.bfloat16
    total, width = xn.shape
    rows, lanes = total // groups, w_zx.shape[2]
    state2 = state_map.shape[1]

    def kernel(xn_r, cot_r, marks_r, zx_r, st_r, sm_r, wo_r, sml, bt_r, bb_r, z_o, xs_o, raw_o, bc_o, y_o, dyn_o, sums_o):
        x = xn_r[...]
        z = quick(x, zx_r[0], NN)
        xs = quick(x, zx_r[1], NN).astype(bf16)
        raw = quick(x, st_r[...], NN).astype(bf16)
        bc = quick(x, sm_r[...], NN).astype(bf16)
        z_o[...], xs_o[...], raw_o[...], bc_o[...] = z, xs, raw, bc
        scan = Scan(
            xs, raw, bc, marks_r[...].astype(f32), sml[0:4, :], sml[4:5, :], bt_r[...], bb_r[...], sml[8:10, :]
        )
        y = scan.forward(sml[5:6, :]).astype(bf16)
        y_o[...] = y
        gated = y.astype(f32) * jax.nn.silu(z)
        d_yn = quick(cot_r[...], wo_r[...], NT)
        dyn_o[...] = d_yn
        ones = jnp.ones((8, lanes), f32)
        sums_o[0, 0:1] = exact(ones, gated * gated, NT)[0:1]
        sums_o[0, 1:2] = exact(ones, d_yn * sml[6:7, :] * gated, NT)[0:1]

    def by_group(columns):
        return pl.BlockSpec((rows, columns), lambda g: (g, 0))

    def whole(array):
        return pl.BlockSpec(array.shape, lambda g: (0,) * array.ndim)

    S = jax.ShapeDtypeStruct
    return pl.pallas_call(
        kernel,
        grid=(groups,),
        in_specs=[by_group(width), pl.BlockSpec((rows, width), lambda g: (g, 2))]
        + [pl.BlockSpec((rows, 128), lambda g: (g, mark_block))]
        + [whole(array) for array in (w_zx, w_step, state_map, w_out, small, bc_taps, bc_bias)],
        out_specs=[by_group(lanes)] * 3
        + [by_group(state2), by_group(lanes), by_group(lanes), pl.BlockSpec((1, 2, rows), lambda g: (g, 0, 0))],
        out_shape=[
            S((total, lanes), f32),
            S((total, lanes), bf16),
            S((total, lanes), bf16),
            S((total, state2), bf16),
            S((total, lanes), bf16),
            S((total, lanes), f32),
            S((groups, 2, rows), f32),
        ],
        compiler_params=pltpu.CompilerParams(vmem_limit_bytes=60 * 2**20),
        name="mixer_forward",
    )(xn, marked, marked, w_zx, w_step, state_map, w_out, small, bc_taps, bc_bias)


def mixer_backward(xn, marked, mark_block, kept, sums, small, bc_taps, bc_bias, groups):
    f32, bf16 = jnp.float32, jnp.bfloat16
    z, xs, raw, bc, y, d_yn = kept
    total, width = xn.shape
    rows, lanes, state2 = total // groups, z.shape[1], bc.shape[1]

    def kernel(
        xn_r, cot_r, marks_r, z_r, xs_r, raw_r, bc_r, y_r, dyn_r, sums_r, sml, bt_r, bb_r,
        dz_o, dxs_o, draw_o, dbc_o, yn_o, gzx_o, gst_o, gout_o, gsm_o, gbc_o, acc_in, acc_out,
    ):
        group = pl.program_id(0)
        scan = Scan(
            xs_r[...], raw_r[...], bc_r[...], marks_r[...].astype(f32),
            sml[0:4, :], sml[4:5, :], bt_r[...], bb_r[...], sml[8:10, :],
        )
        skip, gain = sml[5:6, :], sml[6:7, :]
        sums_wide = [jnp.broadcast_to(sums_r[0, i : i + 1], (128, rows)).T for i in range(2)]
        inverse = lax.rsqrt(sums_wide[0] / INNER + epsilon)
        cross = sums_wide[1] / INNER
        gate, out, d_normed = z_r[...], y_r[...].astype(f32), dyn_r[...]
        silu_z = jax.nn.silu(gate)
        gated = out * silu_z
        yn = (gated * inverse * gain).astype(bf16)
        yn_o[...] = yn
        g_gate = jnp.sum(d_normed * gated * inverse, axis=0, keepdims=True)
        d_gated = d_normed * gain * inverse - gated * inverse**3 * cross
        d_y = (d_gated * silu_z).astype(bf16).astype(f32)
        d_z = (d_gated * out * silu_slope(gate)).astype(bf16)
        dz_o[...] = d_z
        g_skip = jnp.sum(d_y * scan.xc, axis=0, keepdims=True)
        d_weighted, d_meet = jnp.zeros_like(d_y), jnp.zeros_like(scan.meet)
        by_row, by_col = [], []
        for h in range(2):
            mine = (scan.lane < scan.half) if h == 0 else (scan.lane >= scan.half)
            d_head = jnp.where(mine, d_y, 0.0)
            decay = scan.decay(h)
            mixing = decay * scan.meet
            d_mixing = exact(d_head, scan.weighted, NT)
            d_weighted = d_weighted + exact(mixing, d_head, TN)
            d_meet = d_meet + d_mixing * decay
            moved = d_mixing * mixing
            by_row.append(jnp.sum(moved, axis=1, keepdims=True))
            by_col.append(jnp.sum(moved, axis=0, keepdims=True))
        columns = [jnp.broadcast_to(by_col[h], (128, rows)).T for h in range(2)]
        d_running = scan.in_lane([by_row[h] - columns[h] for h in range(2)])
        d_log = scan.to_ends(d_running)
        shared = d_weighted * scan.xc
        d_dt = scan.in_lane(
            [
                jnp.sum(jnp.where(scan.lane < scan.half, shared, 0.0), axis=1, keepdims=True),
                jnp.sum(jnp.where(scan.lane >= scan.half, shared, 0.0), axis=1, keepdims=True),
            ]
        )
        d_step = (d_dt + d_log * scan.rate) * jax.nn.sigmoid(scan.step_in)
        g_bias = jnp.sum(d_step, axis=0, keepdims=True)
        g_decay = jnp.sum(d_log * scan.log_decay, axis=0, keepdims=True)
        d_raw = d_step.astype(bf16)
        draw_o[...] = d_raw
        d_xc = skip * d_y + d_weighted * scan.dt_wide
        d_xs, g_taps = taps_backward(
            d_xc * silu_slope(scan.pre_x), scan.xs, sml[0:4, :], scan.position
        )
        d_xs = d_xs.astype(bf16)
        dxs_o[...] = d_xs
        d_bcc = jnp.concatenate(
            [exact(d_meet, scan.c_mat, TN), exact(d_meet, scan.b_mat, NN)], axis=1
        )
        d_bc, g_bc_taps = taps_backward(
            d_bcc * silu_slope(scan.pre_bc), scan.bc, bt_r[...], scan.position
        )
        dbc_o[...] = d_bc.astype(bf16)
        in_part = quick(jnp.concatenate([d_z, d_xs, d_raw], axis=1), xn_r[...], TN)
        out_part = quick(yn, cot_r[...], TN)
        blank = jnp.zeros((1, lanes), f32)
        few = jnp.concatenate(
            g_taps + [g_gate, g_bias, g_decay, g_skip] + [blank] * 7, axis=0
        )
        few_bc = jnp.concatenate(g_bc_taps + [jnp.zeros((3, state2), f32)], axis=0)

        @pl.when(group == 0)
        def _():
            acc_in[...], acc_out[...] = in_part, out_part
            gsm_o[...], gbc_o[...] = few, few_bc

        @pl.when(group > 0)
        def _():
            acc_in[...] += in_part
            acc_out[...] += out_part
            gsm_o[...] += few
            gbc_o[...] += few_bc

        @pl.when(group == groups - 1)
        def _():
            for i in range(2):
                gzx_o[i] = acc_in[i * lanes : (i + 1) * lanes, :].T.astype(bf16)
            gst_o[...] = acc_in[2 * lanes : 2 * lanes + 8, :]
            gout_o[...] = acc_out[...].astype(bf16)

    def by_group(columns):
        return pl.BlockSpec((rows, columns), lambda g: (g, 0))

    def whole(shape):
        return pl.BlockSpec(shape, lambda g: (0,) * len(shape))

    S = jax.ShapeDtypeStruct
    return pl.pallas_call(
        kernel,
        grid=(groups,),
        in_specs=[by_group(width), pl.BlockSpec((rows, width), lambda g: (g, 2))]
        + [pl.BlockSpec((rows, 128), lambda g: (g, mark_block))]
        + [by_group(array.shape[1]) for array in kept]
        + [pl.BlockSpec((1, 2, rows), lambda g: (g, 0, 0)), whole(small.shape), whole(bc_taps.shape), whole(bc_bias.shape)],
        out_specs=[by_group(lanes)] * 3
        + [by_group(state2), by_group(lanes)]
        + [
            whole((2, width, lanes)),
            whole((8, width)),
            whole((lanes, width)),
            whole((16, lanes)),
            whole((8, state2)),
        ],
        out_shape=[
            S((total, lanes), bf16),
            S((total, lanes), bf16),
            S((total, lanes), bf16),
            S((total, state2), bf16),
            S((total, lanes), bf16),
            S((2, width, lanes), bf16),
            S((8, width), f32),
            S((lanes, width), bf16),
            S((16, lanes), f32),
            S((8, state2), f32),
        ],
        scratch_shapes=[pltpu.VMEM((3 * lanes, width), f32), pltpu.VMEM((lanes, width), f32)],
        compiler_params=pltpu.CompilerParams(vmem_limit_bytes=60 * 2**20),
        name="mixer_backward",
    )(xn, marked, marked, z, xs, raw, bc, y, d_yn, sums, small, bc_taps, bc_bias)


def swap_halves(values):
    return pltpu.roll(values, values.shape[1] // 2, 1)


def attend_weights(qr, kr, marks, rows):
    f32 = jnp.float32
    row = lax.broadcasted_iota(jnp.int32, (rows, rows), 0)
    col = lax.broadcasted_iota(jnp.int32, (rows, rows), 1)
    first = row.astype(f32) - marks[:, 1:2]
    allowed = (col <= row) & (col.astype(f32) >= first)
    weights = jnp.exp(jnp.where(allowed, quick(qr, kr, NT) * AHD ** (-0.5), -1e30))
    return weights / jnp.sum(weights, axis=-1, keepdims=True)


def attention_forward(xa, width, w_qkv, up_maps, frequencies, groups):
    f32, bf16 = jnp.float32, jnp.bfloat16
    total, columns = xa.shape
    rows, rank = total // groups, up_maps.shape[1]
    side = columns - (3 * width) // 2
    side_block = pl.BlockSpec((rows, side), lambda g: (g, columns // side - 1))

    def kernel(xa_r, side_r, w_r, up_r, freq_r, ao_o, q_o, k_o, v_o, cos_o, sin_o, w_all):
        @pl.when(pl.program_id(0) == 0)
        def _():
            for j in range(3):
                w_all[:, j * AHD : (j + 1) * AHD] = w_r[j]

        marks = side_r[:, 3 * rank :].astype(f32)
        wide = quick(xa_r[...], w_all[...], NN)
        proj = []
        for j in range(3):
            mid = side_r[:, j * rank : (j + 1) * rank]
            proj.append((wide[:, j * AHD : (j + 1) * AHD] + quick(mid, up_r[j], NN)).astype(bf16))
        angle = marks[:, 1:2] * freq_r[...]
        lane = lax.broadcasted_iota(jnp.int32, angle.shape, 1)
        cosine, sine = jnp.cos(angle), jnp.sin(angle)
        sine = jnp.where(lane < AHD // 2, -sine, sine)
        cos_o[...], sin_o[...] = cosine, sine
        qr, kr = [
            (piece * cosine + swap_halves(piece) * sine).astype(bf16)
            for piece in (proj[0].astype(f32), proj[1].astype(f32))
        ]
        q_o[...], k_o[...], v_o[...] = qr, kr, proj[2]
        low = attend_weights(qr, kr, marks, rows).astype(bf16)
        ao_o[...] = quick(low, proj[2], NN).astype(bf16)

    def by_group(size):
        return pl.BlockSpec((rows, size), lambda g: (g, 0))

    def whole(array):
        return pl.BlockSpec(array.shape, lambda g: (0,) * array.ndim)

    S = jax.ShapeDtypeStruct
    return pl.pallas_call(
        kernel,
        grid=(groups,),
        in_specs=[by_group(width), side_block, whole(w_qkv), whole(up_maps), whole(frequencies)],
        out_specs=[by_group(AHD)] * 6,
        out_shape=[S((total, AHD), bf16)] * 4 + [S((total, AHD), f32)] * 2,
        scratch_shapes=[pltpu.VMEM((width, 3 * AHD), bf16)],
        compiler_params=pltpu.CompilerParams(vmem_limit_bytes=60 * 2**20),
        name="attention_forward",
    )(xa, xa, w_qkv, up_maps, frequencies)


def attention_backward(d_attn, xa, width, w_o, up_maps, kept, groups):
    f32, bf16 = jnp.float32, jnp.bfloat16
    total, columns = xa.shape
    rows, rank = total // groups, up_maps.shape[1]
    side = columns - (3 * width) // 2
    side_block = pl.BlockSpec((rows, side), lambda g: (g, columns // side - 1))
    model = d_attn.shape[1]

    def kernel(
        da_r, xa_r, side_r, wo_r, up_r, ao_r, q_r, k_r, v_r, cos_r, sin_r,
        dq_o, dk_o, dv_o, dmid_o, gw_o, go_o, gup_o, acc_w, acc_o,
    ):
        group = pl.program_id(0)
        d_rows = da_r[...]
        marks = side_r[:, 3 * rank :].astype(f32)
        d_ao = quick(d_rows, wo_r[...], NT).astype(bf16)
        qr, kr, vals = q_r[...], k_r[...], v_r[...]
        weights = attend_weights(qr, kr, marks, rows)
        d_vals = quick(weights.astype(bf16), d_ao, TN)
        d_weights = quick(d_ao, vals, NT).astype(bf16).astype(f32)
        along = jnp.sum(d_weights * weights, axis=-1, keepdims=True)
        d_scores = (weights * (d_weights - along) * AHD ** (-0.5)).astype(bf16)
        cosine, sine = cos_r[...], sin_r[...]
        pieces = []
        for d_turned in (quick(d_scores, kr, NN), quick(d_scores, qr, TN)):
            d_turned = d_turned.astype(bf16).astype(f32)
            pieces.append((d_turned * cosine + swap_halves(d_turned * sine)).astype(bf16))
        pieces.append(d_vals.astype(bf16))
        for j, out in enumerate((dq_o, dk_o, dv_o)):
            out[...] = pieces[j]
            dmid_o[:, j * rank : (j + 1) * rank] = quick(pieces[j], up_r[j], NT).astype(bf16)
        part = quick(jnp.concatenate(pieces, axis=1), xa_r[...], TN)
        part_o = quick(ao_r[...], d_rows, TN)
        parts_up = [
            quick(side_r[:, j * rank : (j + 1) * rank], pieces[j], TN)
            for j in range(3)
        ]

        @pl.when(group == 0)
        def _():
            acc_w[...], acc_o[...] = part, part_o
            for j in range(3):
                gup_o[j] = parts_up[j]

        @pl.when(group > 0)
        def _():
            acc_w[...] += part
            acc_o[...] += part_o
            for j in range(3):
                gup_o[j] += parts_up[j]

        @pl.when(group == groups - 1)
        def _():
            for j in range(3):
                gw_o[j] = acc_w[j * AHD : (j + 1) * AHD, :].T.astype(bf16)
            go_o[...] = acc_o[...].astype(bf16)

    def by_group(size):
        return pl.BlockSpec((rows, size), lambda g: (g, 0))

    def whole(shape):
        return pl.BlockSpec(shape, lambda g: (0,) * len(shape))

    S = jax.ShapeDtypeStruct
    return pl.pallas_call(
        kernel,
        grid=(groups,),
        in_specs=[by_group(model), by_group(width), side_block, whole(w_o.shape), whole(up_maps.shape)]
        + [by_group(AHD)] * 6,
        out_specs=[by_group(AHD)] * 3
        + [by_group(3 * rank)]
        + [whole((3, width, AHD)), whole((AHD, model)), whole((3, rank, AHD))],
        out_shape=[S((total, AHD), bf16)] * 3
        + [
            S((total, 3 * rank), bf16),
            S((3, width, AHD), bf16),
            S((AHD, model), bf16),
            S((3, rank, AHD), f32),
        ],
        scratch_shapes=[pltpu.VMEM((3 * AHD, width), f32), pltpu.VMEM((AHD, model), f32)],
        compiler_params=pltpu.CompilerParams(vmem_limit_bytes=60 * 2**20),
        name="attention_backward",
    )(d_attn, xa, xa, w_o, up_maps, *kept)


def per_device_split(
    hidden,
    embeds,
    cotangent,
    lengths,
    attention_norm_gain,
    adapter_down_maps,
    query_key_value_weight,
    adapter_up_maps,
    attention_output_weight,
    feedforward_norm_gain,
    gate_up_weight,
    down_weight,
    mixer_norm_gain,
    mixer_gate_input_weight,
    state_map_weight,
    step_size_weight,
    mixer_input_taps,
    mixer_input_tap_bias,
    state_map_taps,
    state_map_tap_bias,
    step_size_bias,
    log_decay_rate,
    head_skip_weight,
    gated_norm_gain,
    mixer_output_weight,
):
    bf16, f32 = jnp.bfloat16, jnp.float32
    tp_size, ctx_size, groups = (lax.axis_size(name) for name in ("tp", "ctx", "fsdp"))
    tp_index, ctx_index = lax.axis_index("tp"), lax.axis_index("ctx")
    plane_index = lax.axis_index("fsdp") * ctx_size + ctx_index
    plane_size = groups * ctx_size
    tok_rows = hidden.shape[0]
    mine = tok_rows // tp_size
    group_rows = tok_rows * ctx_size
    start = tp_index * mine

    sizes = (groups, ctx_size, tp_size)

    def own_rows(values):
        return lax.dynamic_slice_in_dim(values, start, mine, 0)

    width = hidden.shape[1]
    own_shape = (mine, width)
    cot_low = own_rows(cotangent)

    rank = adapter_down_maps.shape[2]
    width_a = adapter_down_maps.shape[1]
    xa_wide, up_maps, w_step, small, w_o, w_qkv = opening(
        sizes,
        1,
        hidden,
        embeds,
        cotangent,
        lengths,
        attention_norm_gain,
        adapter_down_maps,
        [
            adapter_up_maps,
            step_size_weight,
            mixer_input_taps,
            mixer_input_tap_bias[None],
            gated_norm_gain[None],
            head_skip_weight[None],
            step_size_bias[None],
            log_decay_rate[None],
        ],
        [(attention_output_weight, 0, 1), (query_key_value_weight, 2, 1)],
    )
    half = AHD // 2
    frequencies = 10000.0 ** (-jnp.arange(half, dtype=f32) / half)
    frequencies = jnp.concatenate([frequencies, frequencies])[None]
    kept_a = attention_forward(xa_wide, width_a, w_qkv, up_maps, frequencies, groups)
    ao_low = kept_a[0]

    gain_m = feedforward_norm_gain.reshape(1, -1)
    found = exchange(
        sizes,
        2,
        Summed(sizes, [(ao_low, w_o, None, False)]),
        finish_forward,
        [hidden, gain_m],
        [own_shape],
        width,
        [(gate_up_weight, 2, 1), (down_weight, 0, 1)],
    )
    xm, (after_attn,), (w_gu, w_down) = found["gathered"], found["finish"], found["moves"]
    gate_pre, up_pre = matrix_product(xm, w_gu[0]), matrix_product(xm, w_gu[1])
    activated, act_back = jax.vjp(gated_gelu, gate_pre, up_pre)
    hid_low = activated.astype(bf16)

    gain_n = mixer_norm_gain.reshape(1, -1)
    found = exchange(
        sizes,
        3,
        Summed(sizes, [(hid_low, w_down, None, False)]),
        finish_forward,
        [after_attn, gain_n],
        [own_shape],
        width,
        [(mixer_gate_input_weight, 2, 1), (mixer_output_weight, 0, 1)],
        plan=(6,),
    )
    xn, (after_mlp,) = found["gathered"], found["finish"]
    w_zx, w_out = found["moves"]
    few = step_size_weight.shape[1] // plane_size
    bc_bias = state_map_tap_bias[None]
    mark_block = (3 * width + 3 * rank) // 128
    *kept, sums = mixer_forward(
        xn, xa_wide, mark_block, w_zx, w_step, state_map_weight, w_out, small, state_map_taps, bc_bias, groups
    )
    sums = sum_small(sizes, 4, sums)
    d_z, d_xs, d_step, d_bc_part, yn_low, grad_w_zx, grad_w_dt, grad_w_out, few_x, few_bc = (
        mixer_backward(xn, xa_wide, mark_block, kept, sums, small, state_map_taps, bc_bias, groups)
    )
    grad_conv_bc, grad_conv_bc_bias = few_bc[:4], few_bc[4]
    found = exchange(
        sizes,
        5,
        Summed(
            sizes,
            [
                (d_z, w_zx, 0, True),
                (d_xs, w_zx, 1, True),
                (d_step, w_step, None, True),
            ],
            d_bc_part,
        ),
        finish_mixer_back,
        [after_mlp, gain_n, cot_low, state_map_weight],
        [own_shape, gain_n.shape],
        width + d_bc_part.shape[1],
        [(grad_w_zx, 1, 2), (grad_w_out, 1, 0)],
        plan=(6,),
        also_sum=(
            Summed(sizes, [(yn_low, w_out, None, False)]),
            finish_out,
            [after_mlp],
            jax.ShapeDtypeStruct(own_shape, bf16),
        ),
    )
    gathered, (d_after_mlp, grad_g_mamba) = found["gathered"], found["finish"]
    out_mine, (grad_w_zx, grad_w_out) = found["second"], found["moves"]

    d_mlp, d_bc = gathered[:, :width], gathered[:, width:]
    grad_w_bc = outer_product_sum(xn, d_bc)
    grad_w_down = outer_product_sum(hid_low, d_mlp)
    d_gate, d_up = act_back(matrix_product_transposed(d_mlp, w_down))
    d_gate, d_up = d_gate.astype(bf16), d_up.astype(bf16)
    grad_w_gu = jnp.stack(
        [outer_product_sum(xm, d_gate).astype(bf16), outer_product_sum(xm, d_up).astype(bf16)]
    )

    found = exchange(
        sizes,
        6,
        Summed(sizes, [(d_gate, w_gu, 0, True), (d_up, w_gu, 1, True)]),
        finish_mlp_back,
        [after_attn, gain_m, d_after_mlp],
        [own_shape, gain_m.shape],
        width,
        [(grad_w_gu, 1, 2), (grad_w_down.astype(bf16), 1, 0)],
    )
    d_attn, (d_after_attn, grad_g_mlp) = found["gathered"], found["finish"]
    grad_w_gu, grad_w_down = found["moves"]
    *d_proj, dmid_part, grad_w_qkv, grad_w_o, adapter_up_gradient = attention_backward(
        d_attn, xa_wide, width_a, w_o, up_maps, kept_a, groups
    )
    shares = jnp.concatenate([few_x, grad_w_dt[:few].reshape(-1, 128)]).astype(bf16)
    sums = [grad_g_mlp[0], grad_g_mamba[0], grad_conv_bc, grad_conv_bc_bias]
    row = jnp.concatenate([part.reshape(-1) for part in sums])[None]
    found = exchange(
        sizes,
        7,
        Summed(sizes, [(d_proj[j], w_qkv, j, True) for j in range(3)], dmid_part),
        finish_attention_back,
        [
            hidden,
            embeds,
            attention_norm_gain.reshape(1, -1),
            d_after_attn,
            adapter_down_maps,
            out_mine,
            row,
        ],
        [],
        3 * rank,
        [
            (grad_w_qkv, 1, 2),
            (grad_w_o, 1, 0),
        ],
        plan=(5,),
        tail=3 * width,
        small=width_a + row.shape[1],
        spread=jnp.concatenate([adapter_up_gradient.reshape(-1, 128).astype(bf16), shares]),
    )
    dmid, back, row = found["gathered"], found["tail"], found["small"][0]
    grad_w_qkv, grad_w_o = found["moves"]
    shared = found["spread"].reshape(plane_size, -1, 128)
    adapter_up_gradient = shared[:, : 3 * rank].reshape(plane_size, 3, rank, 128)
    adapter_up_gradient = adapter_up_gradient.transpose(1, 2, 0, 3).reshape(3, rank, -1)
    shared = shared[:, 3 * rank :].transpose(1, 0, 2).reshape(-1, plane_size * 128)
    adapter_down_gradient = adapter_products(xa_wide, dmid, width_a)
    result = back[:, :width]
    d_hidden = back[:, width : 2 * width].astype(f32)
    d_embeds = back[:, 2 * width :].astype(f32)
    adapter_up_gradient = adapter_up_gradient.astype(f32)
    shared = shared.astype(f32)
    grad_conv_x, grad_conv_x_bias, grad_g_gate = shared[:4], shared[4], shared[5]
    heads = shared.reshape(-1, plane_size, 128)
    grad_dt_bias = heads[6, :, :few].reshape(-1)
    grad_a_log = heads[7, :, :few].reshape(-1)
    grad_d_skip = heads[8].reshape(plane_size, few, MIXER_HEAD_SIZE).sum(axis=2).reshape(-1)
    grad_w_dt = shared[16:].reshape(few, -1, plane_size, 128).transpose(1, 3, 2, 0)
    grad_w_dt = grad_w_dt.reshape(-1, plane_size * few)
    grad_g_attn = row[:width_a]
    grad_g_mlp, grad_g_mamba, grad_conv_bc, grad_conv_bc_bias = unpack(row[width_a:], sums)

    return (
        result,
        d_hidden,
        d_embeds,
        grad_g_attn,
        adapter_down_gradient,
        grad_w_qkv.astype(f32),
        adapter_up_gradient,
        grad_w_o.astype(f32),
        grad_g_mlp,
        grad_w_gu.astype(f32),
        grad_w_down.astype(f32),
        grad_g_mamba,
        grad_w_zx.astype(f32),
        grad_w_bc,
        grad_w_dt,
        grad_conv_x,
        grad_conv_x_bias,
        grad_conv_bc,
        grad_conv_bc_bias,
        grad_dt_bias,
        grad_a_log,
        grad_d_skip,
        grad_g_gate,
        grad_w_out.astype(f32),
    )


def solution(mesh):
    placed = (
        P(("fsdp", "ctx"), None),
        P(("fsdp", "ctx"), None),
        P(("fsdp", "ctx"), None),
        P("fsdp", None),
        P(),
        P(),
        P(None, ("fsdp", "ctx"), "tp"),
        P(None, None, "tp"),
        P("tp", ("fsdp", "ctx")),
        P(),
        P(None, ("fsdp", "ctx"), "tp"),
        P("tp", ("fsdp", "ctx")),
        P(),
        P(None, ("fsdp", "ctx"), "tp"),
        P(),
        P(None, "tp"),
        P(None, "tp"),
        P("tp"),
        P(),
        P(),
        P("tp"),
        P("tp"),
        P("tp"),
        P("tp"),
        P("tp", ("fsdp", "ctx")),
    )
    devices = mesh.shape["fsdp"] * mesh.shape["ctx"] * mesh.shape["tp"]
    one_head_each = devices == AHEADS and mesh.shape["ctx"] == 2 and mesh.shape["tp"] == 4
    return jax.shard_map(
        per_device_split if one_head_each else per_device,
        mesh=mesh,
        in_specs=placed,
        out_specs=(
            P(("fsdp", "ctx"), None),
            P(("fsdp", "ctx"), None),
            P(("fsdp", "ctx"), None),
            P(),
            P(),
            P(None, ("fsdp", "ctx"), "tp"),
            P(None, None, "tp"),
            P("tp", ("fsdp", "ctx")),
            P(),
            P(None, ("fsdp", "ctx"), "tp"),
            P("tp", ("fsdp", "ctx")),
            P(),
            P(None, ("fsdp", "ctx"), "tp"),
            P(),
            P(None, "tp"),
            P(None, "tp"),
            P("tp"),
            P(),
            P(),
            P("tp"),
            P("tp"),
            P("tp"),
            P("tp"),
            P("tp", ("fsdp", "ctx")),
        ),
        check_vma=False,
    )
```

```python
import functools

import jax
import jax.numpy as jnp
from jax import lax
from jax.experimental import pallas as pl
from jax.experimental.pallas import tpu as pltpu
from jax.sharding import PartitionSpec as P

MODEL_WIDTH = 2048
AHEADS = 32
AHD = 128
INNER = 4096
MIXER_HEAD_SIZE = 64
STATE = 128
SPAN = 128


highest = lax.Precision.HIGHEST
epsilon = 1e-05


def matrix_product(left, right):
    return jnp.dot(left, right, preferred_element_type=jnp.float32)


def matrix_product_transposed(left, right):
    return lax.dot_general(
        left, right, (((1,), (1,)), ((), ())), preferred_element_type=jnp.float32
    )


def outer_product_sum(left, right):
    return lax.dot_general(
        left, right, (((0,), (0,)), ((), ())), preferred_element_type=jnp.float32
    )


def rms_scale(values, gain):
    return values * lax.rsqrt(jnp.mean(values * values, axis=-1, keepdims=True) + epsilon) * gain


def gated_gelu(gate_in, up_in):
    return jax.nn.gelu(gate_in, approximate=True) * up_in


def layout(lengths_row, total_rows):
    ends = jnp.cumsum(lengths_row)
    slot_index = jnp.arange(total_rows, dtype=jnp.int32)
    passed = (slot_index[:, None] >= ends[None, :]).astype(jnp.int32)
    segment = jnp.sum(passed, axis=1)
    position = slot_index - jnp.sum(passed * lengths_row[None, :], axis=1)
    return (segment, position, slot_index)


def causal_conv(values, kernel, bias, position):
    total_rows = values.shape[0]
    total = values * kernel[0][None, :] + bias[None, :]
    for lag in range(1, kernel.shape[0]):
        shifted = jnp.concatenate(
            [jnp.zeros((lag, values.shape[1]), values.dtype), values[: total_rows - lag]], axis=0
        )
        keep = (position >= lag).astype(values.dtype)[:, None]
        total = total + shifted * keep * kernel[lag][None, :]
    return jax.nn.silu(total)


def rotate(values, position):
    half_dim = values.shape[-1] // 2
    inverse = 10000.0 ** (-jnp.arange(half_dim, dtype=jnp.float32) / half_dim)
    angle = position.astype(jnp.float32)[:, None] * inverse[None, :]
    cosine = jnp.cos(angle)[:, None, :]
    sine_part = jnp.sin(angle)[:, None, :]
    first_half = values[..., :half_dim]
    second_half = values[..., half_dim:]
    return jnp.concatenate(
        [
            first_half * cosine - second_half * sine_part,
            second_half * cosine + first_half * sine_part,
        ],
        axis=-1,
    )


def attend_core(pair_data, values, segment, slot_index, position, block_rows):
    group_row_block = values.shape[0]
    count_of_heads = values.shape[1] // AHD
    paired = pair_data.reshape(group_row_block, count_of_heads, 2, AHD)
    queries = rotate(paired[:, :, 0], position).astype(jnp.bfloat16)
    keys_all = rotate(paired[:, :, 1], position).astype(jnp.bfloat16)
    vals_all = values.reshape(group_row_block, count_of_heads, AHD).astype(jnp.bfloat16)
    scaling = AHD ** (-0.5)
    block_count = group_row_block // block_rows

    def one_block(inputs):
        query_part, query_seg, query_slot = inputs
        scores = (
            jnp.einsum("qhd,khd->hqk", query_part, keys_all, preferred_element_type=jnp.float32)
            * scaling
        )
        allowed = (query_seg[:, None] == segment[None, :]) & (
            query_slot[:, None] >= slot_index[None, :]
        )
        scores = jnp.where(allowed[None], scores, -1e30)
        weights = jnp.exp(scores)
        weights_low = (weights / jnp.sum(weights, axis=-1, keepdims=True)).astype(jnp.bfloat16)
        return jnp.einsum("hqk,khd->qhd", weights_low, vals_all, preferred_element_type=jnp.float32)

    mapped = lax.map(
        jax.checkpoint(one_block),
        (
            queries.reshape(block_count, block_rows, count_of_heads, AHD),
            segment.reshape(block_count, block_rows),
            slot_index.reshape(block_count, block_rows),
        ),
    )
    return mapped.reshape(group_row_block, count_of_heads * AHD)


def state_scan(inputs_x, step_size, b_mat, c_mat, decay_rate, segment):
    total_rows, count_of_heads, head_dim = inputs_x.shape
    spans = total_rows // SPAN
    log_decay = step_size * decay_rate[None, :]
    weighted = inputs_x * step_size[:, :, None]
    causal = jnp.arange(SPAN)[:, None] >= jnp.arange(SPAN)[None, :]

    def advance(carried_in, inputs):
        memory, last_segment = carried_in
        decay_part, weighted_part, b_part, c_part, seg_part = inputs
        running = jnp.cumsum(decay_part, axis=0)
        same_seq = (seg_part[:, None] == seg_part[None, :]) & causal
        intersection = jnp.dot(c_part, b_part.T, precision=highest)
        log_gap = jnp.where(same_seq[:, :, None], running[:, None, :] - running[None, :, :], 0.0)
        mixing = jnp.where(same_seq[:, :, None], jnp.exp(log_gap), 0.0) * intersection[:, :, None]
        output = jnp.einsum("tsh,shp->thp", mixing, weighted_part, precision=highest)
        carried = (seg_part == last_segment).astype(jnp.float32)
        reach_back = jnp.exp(running) * carried[:, None]
        output = (
            output
            + jnp.einsum("tn,hpn->thp", c_part, memory, precision=highest) * reach_back[:, :, None]
        )
        tail_seg = seg_part[-1]
        toward = (
            jnp.exp(running[-1][None, :] - running)
            * (seg_part == tail_seg).astype(jnp.float32)[:, None]
        )
        next_state = jnp.einsum("sh,shp,sn->hpn", toward, weighted_part, b_part, precision=highest)
        keep_all = jnp.exp(running[-1]) * (tail_seg == last_segment).astype(jnp.float32)
        next_state = next_state + memory * keep_all[:, None, None]
        return ((next_state, tail_seg), output)

    initial = (jnp.zeros((count_of_heads, head_dim, b_mat.shape[1]), jnp.float32), jnp.int32(-1))
    pieces = (
        log_decay.reshape(spans, SPAN, count_of_heads),
        weighted.reshape(spans, SPAN, count_of_heads, head_dim),
        b_mat.reshape(spans, SPAN, -1),
        c_mat.reshape(spans, SPAN, -1),
        segment.reshape(spans, SPAN),
    )
    last_state, outputs = lax.scan(jax.checkpoint(advance), initial, pieces)
    return outputs.reshape(total_rows, count_of_heads, head_dim)


def mamba_core(
    inner_in,
    step_in,
    bc_post,
    bias_in,
    decay_in,
    skip_weight_input,
    kernel_in,
    conv_bias_in,
    position,
    segment,
):
    group_row_block = inner_in.shape[0]
    count_of_heads = step_in.shape[1]
    mixer_result = causal_conv(inner_in, kernel_in, conv_bias_in, position)
    reshaped_tensor = mixer_result.reshape(group_row_block, count_of_heads, MIXER_HEAD_SIZE)
    step_size = jax.nn.softplus(step_in + bias_in[None, :])
    scan_result = state_scan(
        reshaped_tensor,
        step_size,
        bc_post[:, :STATE],
        bc_post[:, STATE:],
        -jnp.exp(decay_in),
        segment,
    )
    return (scan_result + skip_weight_input[None, :, None] * reshaped_tensor).reshape(
        group_row_block, count_of_heads * MIXER_HEAD_SIZE
    )


def collect(first_part, second_part):
    return (
        lax.all_gather(first_part, ("fsdp", "ctx"), axis=1, tiled=True),
        lax.all_gather(second_part, ("fsdp", "ctx"), axis=1, tiled=True),
    )


def collect_again(first_part, second_part):
    return (
        lax.all_gather(first_part, ("fsdp", "ctx"), axis=1, tiled=True),
        lax.all_gather(second_part, ("fsdp", "ctx"), axis=1, tiled=True),
    )


def tensor_sum(partial_sum):
    return lax.psum(partial_sum, "tp")


def tensor_pair(first_part, second_part):
    return (
        lax.psum(first_part.astype(jnp.bfloat16), "tp").astype(jnp.float32),
        lax.psum(second_part.astype(jnp.bfloat16), "tp").astype(jnp.float32),
    )


def heads_pair(first_part, second_part):
    return (
        lax.all_to_all(first_part, "ctx", split_axis=1, concat_axis=0, tiled=True),
        lax.all_to_all(second_part, "ctx", split_axis=1, concat_axis=0, tiled=True),
    )


def heads_one(values):
    return lax.all_to_all(values, "ctx", split_axis=1, concat_axis=0, tiled=True)


def tokens_pair(first_part, second_part):
    return (
        lax.all_to_all(first_part, "ctx", split_axis=0, concat_axis=1, tiled=True),
        lax.all_to_all(second_part, "ctx", split_axis=0, concat_axis=1, tiled=True),
    )


def tokens_one(values):
    return lax.all_to_all(values, "ctx", split_axis=0, concat_axis=1, tiled=True)


def per_device(
    hidden,
    embeds,
    cotangent,
    lengths,
    attention_norm_gain,
    adapter_down_maps,
    query_key_value_weight,
    adapter_up_maps,
    attention_output_weight,
    feedforward_norm_gain,
    gate_up_weight,
    down_weight,
    mixer_norm_gain,
    mixer_gate_input_weight,
    state_map_weight,
    step_size_weight,
    mixer_input_taps,
    mixer_input_tap_bias,
    state_map_taps,
    state_map_tap_bias,
    step_size_bias,
    log_decay_rate,
    head_skip_weight,
    gated_norm_gain,
    mixer_output_weight,
):
    tok_rows = hidden.shape[0]
    ctx_size = lax.axis_size("ctx")
    ctx_index = lax.axis_index("ctx")
    group_row_block = tok_rows * ctx_size
    block_rows = group_row_block // max(1, group_row_block // 1024)
    segment, position, slot_index = layout(lengths[0], group_row_block)
    hidden_f = hidden.astype(jnp.float32)
    embeds_f = embeds.astype(jnp.float32)
    attention_block_full, attn_out = collect(query_key_value_weight, attention_output_weight)
    joined = jnp.concatenate([hidden_f, embeds_f], axis=1)
    normed_a, norm_a_back = jax.vjp(rms_scale, joined, attention_norm_gain)
    attention_input_reduced = normed_a.astype(jnp.bfloat16)
    middle_reduced_precision = [
        matrix_product(attention_input_reduced, adapter_down_maps[group_member]).astype(
            jnp.bfloat16
        )
        for group_member in range(3)
    ]
    projected_input = [
        (
            matrix_product(attention_input_reduced, attention_block_full[group_member])
            + matrix_product(middle_reduced_precision[group_member], adapter_up_maps[group_member])
        ).astype(jnp.bfloat16)
        for group_member in range(3)
    ]
    tp_heads = projected_input[0].shape[1] // AHD
    pair_data = jnp.stack(
        [
            projected_input[0].reshape(tok_rows, tp_heads, AHD),
            projected_input[1].reshape(tok_rows, tp_heads, AHD),
        ],
        axis=2,
    ).reshape(tok_rows, tp_heads * 2 * AHD)
    pair_heads, value_heads = heads_pair(pair_data, projected_input[2])
    attn_core, attn_pull = jax.vjp(
        lambda pairs_in, values_in: attend_core(
            pairs_in, values_in, segment, slot_index, position, block_rows
        ),
        pair_heads.astype(jnp.float32),
        value_heads.astype(jnp.float32),
    )
    attn_tokens = tokens_one(attn_core.astype(jnp.bfloat16))
    after_attn = hidden_f + tensor_sum(matrix_product(attn_tokens, attn_out))
    mlp_big, mlp_down = collect(gate_up_weight, down_weight)
    normed_m, norm_m_back = jax.vjp(rms_scale, after_attn, feedforward_norm_gain)
    xm_low = normed_m.astype(jnp.bfloat16)
    gate_pre = matrix_product(xm_low, mlp_big[0])
    up_pre = matrix_product(xm_low, mlp_big[1])
    activated, act_back = jax.vjp(gated_gelu, gate_pre, up_pre)
    hid_low = activated.astype(jnp.bfloat16)
    after_mlp = after_attn + tensor_sum(matrix_product(hid_low, mlp_down))
    mamba_big, mamba_out = collect(mixer_gate_input_weight, mixer_output_weight)
    normed_n, norm_n_back = jax.vjp(rms_scale, after_mlp, mixer_norm_gain)
    xn_low = normed_n.astype(jnp.bfloat16)
    gate_z = matrix_product(xn_low, mamba_big[0])
    inner_x = matrix_product(xn_low, mamba_big[1]).astype(jnp.bfloat16)
    step_raw = matrix_product(xn_low, step_size_weight).astype(jnp.bfloat16)
    bc_low = matrix_product(xn_low, state_map_weight).astype(jnp.bfloat16)
    x_heads, step_heads = heads_pair(inner_x, step_raw)
    bc_group = lax.all_gather(bc_low, "ctx", axis=0, tiled=True)
    bc_post, bc_conv_pull = jax.vjp(
        lambda values_in, kernel_in, conv_bias_in: causal_conv(
            values_in, kernel_in, conv_bias_in, position
        ),
        bc_group.astype(jnp.float32),
        state_map_taps,
        state_map_tap_bias,
    )
    heads_on_device_share = step_heads.shape[1]
    start_offset = ctx_index * heads_on_device_share
    channel_count_here = heads_on_device_share * MIXER_HEAD_SIZE
    channel_offset_begin = start_offset * MIXER_HEAD_SIZE
    bias_local = lax.dynamic_slice_in_dim(step_size_bias, start_offset, heads_on_device_share)
    decay_local = lax.dynamic_slice_in_dim(log_decay_rate, start_offset, heads_on_device_share)
    skip_local = lax.dynamic_slice_in_dim(head_skip_weight, start_offset, heads_on_device_share)
    kernel_local = lax.dynamic_slice_in_dim(
        mixer_input_taps, channel_offset_begin, channel_count_here, 1
    )
    conv_bias_local = lax.dynamic_slice_in_dim(
        mixer_input_tap_bias, channel_offset_begin, channel_count_here, 0
    )
    scan_out, scan_pull = jax.vjp(
        lambda xs_in, step_in, bcp_in, bias_in, decay_in, skip_weight_input, kernel_in, conv_bias_in: mamba_core(
            xs_in,
            step_in,
            bcp_in,
            bias_in,
            decay_in,
            skip_weight_input,
            kernel_in,
            conv_bias_in,
            position,
            segment,
        ),
        x_heads.astype(jnp.float32),
        step_heads.astype(jnp.float32),
        bc_post,
        bias_local,
        decay_local,
        skip_local,
        kernel_local,
        conv_bias_local,
    )
    y_tokens = tokens_one(scan_out.astype(jnp.bfloat16)).astype(jnp.float32)
    silu_z = jax.nn.silu(gate_z)
    gated = y_tokens * silu_z
    total_sq = tensor_sum(jnp.sum(gated * gated, axis=1))
    inverse = lax.rsqrt(total_sq / INNER + epsilon)[:, None]
    yn_low = (gated * inverse * gated_norm_gain).astype(jnp.bfloat16)
    after_mamba = after_mlp + tensor_sum(matrix_product(yn_low, mamba_out))
    result = after_mamba.astype(jnp.bfloat16)
    grad_out = cotangent.astype(jnp.float32)
    mamba_big, mamba_out = collect_again(mixer_gate_input_weight, mixer_output_weight)
    d_yn = matrix_product_transposed(cotangent, mamba_out)
    grad_w_out = outer_product_sum(yn_low, cotangent)
    gain_part = d_yn * gated_norm_gain
    cross = tensor_sum(jnp.sum(gain_part * gated, axis=1))
    grad_g_gate = jnp.sum(d_yn * gated * inverse, axis=0)
    d_gated = gain_part * inverse - gated * inverse**3 * (cross / INNER)[:, None]
    d_y = (d_gated * silu_z).astype(jnp.bfloat16)
    sigmoid_z = jax.nn.sigmoid(gate_z)
    d_z = (d_gated * y_tokens * sigmoid_z * (1.0 + gate_z * (1.0 - sigmoid_z))).astype(jnp.bfloat16)
    dy_heads = heads_one(d_y)
    (
        d_xs,
        d_step,
        d_bc_post,
        grad_bias_local,
        grad_decay_local,
        grad_skip_local,
        grad_kernel_local,
        grad_conv_bias_local,
    ) = scan_pull(dy_heads.astype(jnp.float32))
    d_xs_tok, d_step_tok = tokens_pair(d_xs.astype(jnp.bfloat16), d_step.astype(jnp.bfloat16))
    d_bc_ctx = lax.psum(d_bc_post.astype(jnp.bfloat16), "ctx").astype(jnp.float32)
    dxn_part = (
        matrix_product_transposed(d_z, mamba_big[0])
        + matrix_product_transposed(d_xs_tok, mamba_big[1])
        + matrix_product_transposed(d_step_tok, step_size_weight)
    )
    grad_w_zx = jnp.stack([outer_product_sum(xn_low, d_z), outer_product_sum(xn_low, d_xs_tok)])
    grad_w_dt = outer_product_sum(xn_low, d_step_tok)
    dxn_sum, d_bc_full = tensor_pair(dxn_part, d_bc_ctx)
    d_bc_pre = bc_conv_pull(d_bc_full)[0]
    d_bc_mine = lax.dynamic_slice_in_dim(d_bc_pre, ctx_index * tok_rows, tok_rows, 0)
    own_rows = (slot_index // tok_rows == ctx_index).astype(jnp.float32)[:, None]
    ignored_part, grad_conv_bc, grad_conv_bc_bias = bc_conv_pull(d_bc_full * own_rows)
    d_bc_low = d_bc_mine.astype(jnp.bfloat16)
    dxn_total = dxn_sum + matrix_product_transposed(d_bc_low, state_map_weight)
    grad_w_bc = outer_product_sum(xn_low, d_bc_low)
    d_norm_n, grad_g_mamba = norm_n_back(dxn_total)
    d_after_mlp = grad_out + d_norm_n
    shard_heads = step_size_bias.shape[0]
    zero_heads = jnp.zeros((shard_heads,), jnp.float32)
    grad_dt_bias = lax.dynamic_update_slice_in_dim(zero_heads, grad_bias_local, start_offset, 0)
    grad_a_log = lax.dynamic_update_slice_in_dim(zero_heads, grad_decay_local, start_offset, 0)
    grad_d_skip = lax.dynamic_update_slice_in_dim(zero_heads, grad_skip_local, start_offset, 0)
    grad_conv_x = lax.dynamic_update_slice_in_dim(
        jnp.zeros(mixer_input_taps.shape, jnp.float32), grad_kernel_local, channel_offset_begin, 1
    )
    grad_conv_x_bias = lax.dynamic_update_slice_in_dim(
        jnp.zeros(mixer_input_tap_bias.shape, jnp.float32),
        grad_conv_bias_local,
        channel_offset_begin,
        0,
    )
    mlp_big, mlp_down = collect_again(gate_up_weight, down_weight)
    d_mlp_low = d_after_mlp.astype(jnp.bfloat16)
    d_hid = matrix_product_transposed(d_mlp_low, mlp_down)
    grad_w_down = outer_product_sum(hid_low, d_mlp_low)
    d_gate, d_up = act_back(d_hid)
    d_gate_low = d_gate.astype(jnp.bfloat16)
    d_up_low = d_up.astype(jnp.bfloat16)
    d_xm = tensor_sum(
        matrix_product_transposed(d_gate_low, mlp_big[0])
        + matrix_product_transposed(d_up_low, mlp_big[1])
    )
    grad_w_gu = jnp.stack(
        [outer_product_sum(xm_low, d_gate_low), outer_product_sum(xm_low, d_up_low)]
    )
    d_norm_m, grad_g_mlp = norm_m_back(d_xm)
    d_after_attn = d_after_mlp + d_norm_m
    attention_block_full, attn_out = collect_again(query_key_value_weight, attention_output_weight)
    d_attn_low = d_after_attn.astype(jnp.bfloat16)
    d_tokens = matrix_product_transposed(d_attn_low, attn_out).astype(jnp.bfloat16)
    grad_w_o = outer_product_sum(attn_tokens, d_attn_low)
    d_core = heads_one(d_tokens)
    d_pairs, d_values = attn_pull(d_core.astype(jnp.float32))
    d_pair_tok, d_value_tok = tokens_pair(
        d_pairs.astype(jnp.bfloat16), d_values.astype(jnp.bfloat16)
    )
    d_paired = d_pair_tok.reshape(tok_rows, tp_heads, 2, AHD)
    projection_gradient = [
        d_paired[:, :, 0].reshape(tok_rows, tp_heads * AHD),
        d_paired[:, :, 1].reshape(tok_rows, tp_heads * AHD),
        d_value_tok,
    ]
    dxa_part = (
        matrix_product_transposed(projection_gradient[0], attention_block_full[0])
        + matrix_product_transposed(projection_gradient[1], attention_block_full[1])
        + matrix_product_transposed(projection_gradient[2], attention_block_full[2])
    )
    dmid_part = jnp.concatenate(
        [
            matrix_product_transposed(
                projection_gradient[group_member], adapter_up_maps[group_member]
            )
            for group_member in range(3)
        ],
        axis=1,
    )
    grad_w_qkv = jnp.stack(
        [
            outer_product_sum(attention_input_reduced, projection_gradient[group_member])
            for group_member in range(3)
        ]
    )
    adapter_up_gradient = jnp.stack(
        [
            outer_product_sum(
                middle_reduced_precision[group_member], projection_gradient[group_member]
            )
            for group_member in range(3)
        ]
    )
    dxa_sum, dmid_sum = tensor_pair(dxa_part, dmid_part)
    dmid_low = dmid_sum.astype(jnp.bfloat16)
    rank_column_block = adapter_down_maps.shape[2]
    middle_gradient_pieces = [
        dmid_low[:, group_member * rank_column_block : (group_member + 1) * rank_column_block]
        for group_member in range(3)
    ]
    dxa_total = (
        dxa_sum
        + matrix_product_transposed(middle_gradient_pieces[0], adapter_down_maps[0])
        + matrix_product_transposed(middle_gradient_pieces[1], adapter_down_maps[1])
        + matrix_product_transposed(middle_gradient_pieces[2], adapter_down_maps[2])
    )
    adapter_down_gradient = jnp.stack(
        [
            outer_product_sum(attention_input_reduced, middle_gradient_pieces[group_member])
            for group_member in range(3)
        ]
    )
    d_joined, grad_g_attn = norm_a_back(dxa_total)
    d_hidden = d_after_attn + d_joined[:, :MODEL_WIDTH]
    d_embeds = d_joined[:, MODEL_WIDTH:]
    grad_w_qkv, grad_w_o, grad_w_gu, grad_w_down, grad_w_zx, grad_w_out = (
        lax.psum_scatter(
            grad_w_qkv.astype(jnp.bfloat16), ("fsdp", "ctx"), scatter_dimension=1, tiled=True
        ).astype(jnp.float32),
        lax.psum_scatter(
            grad_w_o.astype(jnp.bfloat16), ("fsdp", "ctx"), scatter_dimension=1, tiled=True
        ).astype(jnp.float32),
        lax.psum_scatter(
            grad_w_gu.astype(jnp.bfloat16), ("fsdp", "ctx"), scatter_dimension=1, tiled=True
        ).astype(jnp.float32),
        lax.psum_scatter(
            grad_w_down.astype(jnp.bfloat16), ("fsdp", "ctx"), scatter_dimension=1, tiled=True
        ).astype(jnp.float32),
        lax.psum_scatter(
            grad_w_zx.astype(jnp.bfloat16), ("fsdp", "ctx"), scatter_dimension=1, tiled=True
        ).astype(jnp.float32),
        lax.psum_scatter(
            grad_w_out.astype(jnp.bfloat16), ("fsdp", "ctx"), scatter_dimension=1, tiled=True
        ).astype(jnp.float32),
    )
    (
        grad_g_attn,
        adapter_down_gradient,
        adapter_up_gradient,
        grad_g_mlp,
        grad_g_mamba,
        grad_w_bc,
        grad_w_dt,
        grad_conv_x,
        grad_conv_x_bias,
        grad_conv_bc,
        grad_conv_bc_bias,
        grad_dt_bias,
        grad_a_log,
        grad_d_skip,
        grad_g_gate,
    ) = (
        lax.psum(grad_g_attn.astype(jnp.bfloat16), ("fsdp", "ctx")).astype(jnp.float32),
        lax.psum(adapter_down_gradient.astype(jnp.bfloat16), ("fsdp", "ctx")).astype(jnp.float32),
        lax.psum(adapter_up_gradient.astype(jnp.bfloat16), ("fsdp", "ctx")).astype(jnp.float32),
        lax.psum(grad_g_mlp.astype(jnp.bfloat16), ("fsdp", "ctx")).astype(jnp.float32),
        lax.psum(grad_g_mamba.astype(jnp.bfloat16), ("fsdp", "ctx")).astype(jnp.float32),
        lax.psum(grad_w_bc.astype(jnp.bfloat16), ("fsdp", "ctx")).astype(jnp.float32),
        lax.psum(grad_w_dt.astype(jnp.bfloat16), ("fsdp", "ctx")).astype(jnp.float32),
        lax.psum(grad_conv_x.astype(jnp.bfloat16), ("fsdp", "ctx")).astype(jnp.float32),
        lax.psum(grad_conv_x_bias.astype(jnp.bfloat16), ("fsdp", "ctx")).astype(jnp.float32),
        lax.psum(grad_conv_bc.astype(jnp.bfloat16), ("fsdp", "ctx")).astype(jnp.float32),
        lax.psum(grad_conv_bc_bias.astype(jnp.bfloat16), ("fsdp", "ctx")).astype(jnp.float32),
        lax.psum(grad_dt_bias.astype(jnp.bfloat16), ("fsdp", "ctx")).astype(jnp.float32),
        lax.psum(grad_a_log.astype(jnp.bfloat16), ("fsdp", "ctx")).astype(jnp.float32),
        lax.psum(grad_d_skip.astype(jnp.bfloat16), ("fsdp", "ctx")).astype(jnp.float32),
        lax.psum(grad_g_gate.astype(jnp.bfloat16), ("fsdp", "ctx")).astype(jnp.float32),
    )
    return (
        result,
        d_hidden,
        d_embeds,
        grad_g_attn,
        adapter_down_gradient,
        grad_w_qkv,
        adapter_up_gradient,
        grad_w_o,
        grad_g_mlp,
        grad_w_gu,
        grad_w_down,
        grad_g_mamba,
        grad_w_zx,
        grad_w_bc,
        grad_w_dt,
        grad_conv_x,
        grad_conv_x_bias,
        grad_conv_bc,
        grad_conv_bc_bias,
        grad_dt_bias,
        grad_a_log,
        grad_d_skip,
        grad_g_gate,
        grad_w_out,
    )


PLANE = ("fsdp", "ctx")
EVERY = ("fsdp", "ctx", "tp")


MESH = pl.DeviceIdType.MESH
IN_VMEM = pl.BlockSpec(memory_space=pltpu.VMEM)
IN_HBM = pl.BlockSpec(memory_space=pltpu.HBM)
IN_SMEM = pl.BlockSpec(memory_space=pltpu.SMEM)
DMA = pltpu.SemaphoreType.DMA
GATHER_SHARES = (2,) * 8
SUM_SHARES = (2,) * 8
GATHER_LAGS = (0, 2, 4)
SUM_LAGS = (0, 1, 3, 5, 7)


class Place:
    def __init__(self, sizes):
        self.groups, self.ctx, self.tp = sizes
        g, c, t = (lax.axis_index(name) for name in EVERY)
        y, k = t // 2, lax.rem(t, 2)
        self.g, self.c, self.t, self.y, self.k = g, c, t, y, k
        self.core = (g, c, y * 2 + 1 - k)
        self.side_y = (g, c, (1 - y) * 2 + k)
        self.side_x = (g, 1 - c, t)
        self.line = [(lax.rem(g + d, self.groups), c, t) for d in range(1, self.groups)]
        self.plane = self.groups * self.ctx
        self.index = g * self.ctx + c

    def plane_peer(self, d):
        other = lax.rem(self.index + d, self.plane)
        return other, (other // self.ctx, lax.rem(other, self.ctx), self.t)

    def plane_source(self, d):
        return lax.rem(self.index + self.plane - d, self.plane)


def greet(devices):
    barrier = pltpu.get_barrier_semaphore()
    for device in devices:
        pl.semaphore_signal(barrier, inc=1, device_id=device, device_id_type=MESH)
    pl.semaphore_wait(barrier, len(devices))


def remote(src, dst, send_sem, recv_sem, device):
    return pltpu.make_async_remote_copy(
        src_ref=src,
        dst_ref=dst,
        send_sem=send_sem,
        recv_sem=recv_sem,
        device_id=device,
        device_id_type=MESH,
    )


def cut(ref, axis, index, width):
    if axis is None:
        return ref
    at = [slice(None)] * len(ref.shape)
    start = index * width
    if width % 128 == 0:
        start = pl.multiple_of(start, 128)
    at[axis] = pl.ds(start, width)
    return ref.at[tuple(at)]


class Moves:
    def __init__(self, place, specs, sources, targets, stages, send, recv, local):
        self.sent = []
        self.place, self.specs = place, specs
        self.sources, self.targets = sources, targets
        self.stages, self.send, self.recv, self.local = stages, send, recv, local

    def part(self, i, to, origin):
        split, join = self.specs[i]
        src, dst = self.sources[i], self.targets[i]
        n = self.place.plane
        if split is None:
            return src, cut(dst, join, origin, src.shape[join])
        return (
            cut(src, split, to, src.shape[split] // n),
            cut(dst, join, origin, dst.shape[join] // n),
        )

    def start(self, first=0):
        place = self.place
        self.loads, self.queue = [], []
        for i in range(len(self.specs)):
            self.queue += [(i, d) for d in range(1, place.plane)]
            src, _ = self.part(i, place.index, place.index)
            load = pltpu.make_async_copy(src, self.stages[i], self.local.at[i, 0])
            load.start()
            self.loads.append(load)
        self.queue.sort(key=lambda one: one[1] % place.ctx != first)

    def issue(self, count):
        for i, d in self.queue[:count]:
            other, device = self.place.plane_peer(d)
            src, dst = self.part(i, other, self.place.index)
            copy = remote(src, dst, self.send.at[i, d], self.recv.at[i, d], device)
            copy.start()
            self.sent.append(copy)
        self.queue = self.queue[count:]

    def settle(self):
        self.stores = []
        for i, load in enumerate(self.loads):
            load.wait()
            _, dst = self.part(i, self.place.index, self.place.index)
            store = pltpu.make_async_copy(self.stages[i], dst, self.local.at[i, 1])
            store.start()
            self.stores.append(store)

    def finish(self):
        place = self.place
        for i in range(len(self.specs)):
            for d in range(1, place.plane):
                _, device = place.plane_peer(d)
                src, dst = self.part(i, place.index, place.plane_source(d))
                remote(src, dst, self.send.at[i, d], self.recv.at[i, d], device).wait_recv()
        for copy in self.sent:
            copy.wait_send()
        for store in self.stores:
            store.wait()


def moves_setup(moves, plane):
    outs, scratch = [], []
    for array, split, join in moves:
        shape = list(array.shape)
        part = list(array.shape)
        if split is not None:
            part[split] //= plane
            shape[split] //= plane
        shape[join] *= plane
        outs.append(jax.ShapeDtypeStruct(tuple(shape), array.dtype))
        scratch.append(pltpu.VMEM(tuple(part), array.dtype))
    n = len(moves)
    if n:
        scratch += [DMA((n, plane)), DMA((n, plane)), DMA((n, 2))]
    return outs, scratch


class Gather:
    def __init__(self, place, x, o, pieces, sems):
        self.place, self.x, self.o, self.pieces, self.sems = place, x, o, pieces, sems
        self.n = len(pieces)
        self.first, self.second = [], [None] * self.n
        self.third, self.fourth = [None] * self.n, [None] * self.n

    def line_copy(self, q, d, owner):
        place, cols = self.place, pl.ds(*self.pieces[q])
        return remote(
            self.x.at[:, cols],
            self.o.at[owner, place.c, place.y, place.k, :, cols],
            self.sems[0].at[q, d],
            self.sems[1].at[q, d],
            place.line[d],
        )

    def begin(self):
        place = self.place
        own_at = self.o.at[place.g, place.c, place.y, place.k]
        own = pltpu.make_async_copy(self.x, own_at, self.sems[8])
        own.start()
        for q in range(self.n):
            for d in range(place.groups - 1):
                copy = self.line_copy(q, d, place.g)
                copy.start()
                self.first.append(copy)
        own.wait()

    def to_side(self, q):
        place = self.place
        for d in range(place.groups - 1):
            source = lax.rem(place.g + place.groups - d - 1, place.groups)
            self.line_copy(q, d, source).wait_recv()
        part = self.o.at[:, place.c, place.y, place.k, :, pl.ds(*self.pieces[q])]
        device = place.side_y if q % 2 == 0 else place.side_x
        self.second[q] = remote(part, part, self.sems[2].at[q], self.sems[3].at[q], device)
        self.second[q].start()

    def to_other_side(self, q):
        place, cols = self.place, pl.ds(*self.pieces[q])
        self.second[q].wait_recv()
        if q % 2 == 0:
            part, device = self.o.at[:, place.c, :, place.k, :, cols], place.side_x
        else:
            part, device = self.o.at[:, :, place.y, place.k, :, cols], place.side_y
        self.third[q] = remote(part, part, self.sems[4].at[q], self.sems[5].at[q], device)
        self.third[q].start()

    def to_core(self, q):
        place = self.place
        self.third[q].wait_recv()
        part = self.o.at[:, :, :, place.k, :, pl.ds(*self.pieces[q])]
        self.fourth[q] = remote(part, part, self.sems[6].at[q], self.sems[7].at[q], place.core)
        self.fourth[q].start()

    def steps(self):
        return pipelined(self.n, (self.to_side, self.to_other_side, self.to_core), GATHER_LAGS)

    def end(self):
        for copy in self.fourth:
            copy.wait_recv()
        for copy in self.first + self.second + self.third + self.fourth:
            copy.wait_send()


class PlaneGather:
    def __init__(self, place, x, o, zs, zr, ss, sr, own_sem):
        self.place, self.x, self.o, self.zs, self.zr = place, x, o, zs, zr
        self.ss, self.sr, self.own_sem = ss, sr, own_sem

    def line_copy(self, d, owner):
        place = self.place
        to = self.o.at[owner, place.c]
        return remote(self.x, to, self.zs.at[d], self.zr.at[d], place.line[d])

    def begin(self):
        place = self.place
        self.own = pltpu.make_async_copy(self.x, self.o.at[place.g, place.c], self.own_sem)
        self.own.start()
        for d in range(place.groups - 1):
            self.line_copy(d, place.g).start()

    def step(self):
        place = self.place
        self.own.wait()
        for d in range(place.groups - 1):
            self.line_copy(d, lax.rem(place.g + place.groups - d - 1, place.groups)).wait_recv()
        part = self.o.at[:, place.c]
        self.onward = remote(part, part, self.ss, self.sr, place.side_x)
        self.onward.start()

    def end(self):
        self.onward.wait_recv()
        self.onward.wait_send()
        for d in range(self.place.groups - 1):
            self.line_copy(d, self.place.g).wait_send()


def pipelined(count, stages, lags):
    def step(at):
        for stage, lag in zip(stages, lags):
            if 0 <= at - lag < count:
                stage(at - lag)

    return [functools.partial(step, at) for at in range(count + max(lags))]


def gather_sems(n, groups):
    return [DMA((n, groups - 1)), DMA((n, groups - 1))] + [DMA((n,))] * 6 + [DMA]


class Scatter:
    def __init__(self, place, make, pieces, bufs, acc, sems):
        self.place, self.make, self.pieces, self.bufs, self.acc = place, make, pieces, bufs, acc
        self.sems = sems
        n = len(pieces)
        self.n = n
        self.c1, self.c2, self.c3, self.c4 = [None] * n, [None] * n, [None] * n, [None] * n

    def to_core(self, q):
        theirs, mine, b1 = self.bufs[:3]
        cols, k = pl.ds(*self.pieces[q]), self.place.k
        self.make(q, theirs, 1 - k)
        self.c1[q] = remote(
            theirs.at[..., cols],
            b1.at[..., cols],
            self.sems[0].at[q],
            self.sems[1].at[q],
            self.place.core,
        )
        self.c1[q].start()
        self.make(q, mine, k)

    def to_side(self, q):
        _, mine, b1, b2, _, _ = self.bufs
        place, cols = self.place, pl.ds(*self.pieces[q])
        f32 = jnp.float32
        self.c1[q].wait_recv()
        b1[..., cols] = (b1[..., cols].astype(f32) + mine[..., cols].astype(f32)).astype(b1.dtype)
        if q % 2 == 0:
            part, device = b1.at[:, :, 1 - place.y, :, cols], place.side_y
        else:
            part, device = b1.at[:, 1 - place.c, :, :, cols], place.side_x
        self.c2[q] = remote(
            part, b2.at[:, :, :, cols], self.sems[2].at[q], self.sems[3].at[q], device
        )
        self.c2[q].start()

    def to_other_side(self, q):
        _, _, b1, b2, b3, _ = self.bufs
        place, cols = self.place, pl.ds(*self.pieces[q])
        f32 = jnp.float32
        self.c2[q].wait_recv()
        own = b1[:, :, place.y, :, cols] if q % 2 == 0 else b1[:, place.c, :, :, cols]
        b2[:, :, :, cols] = (b2[:, :, :, cols].astype(f32) + own.astype(f32)).astype(b2.dtype)
        if q % 2 == 0:
            part, device = b2.at[:, 1 - place.c, :, cols], place.side_x
        else:
            part, device = b2.at[:, 1 - place.y, :, cols], place.side_y
        self.c3[q] = remote(part, b3.at[:, :, cols], self.sems[4].at[q], self.sems[5].at[q], device)
        self.c3[q].start()

    def along_line(self, q):
        _, _, _, b2, b3, b4 = self.bufs
        place, cols = self.place, pl.ds(*self.pieces[q])
        f32 = jnp.float32
        self.c3[q].wait_recv()
        own = b2[:, place.c, :, cols] if q % 2 == 0 else b2[:, place.y, :, cols]
        b3[:, :, cols] = (b3[:, :, cols].astype(f32) + own.astype(f32)).astype(b3.dtype)
        self.c4[q] = []
        for d in range(place.groups - 1):
            to = lax.rem(place.g + d + 1, place.groups)
            copy = remote(
                b3.at[to, :, cols],
                b4.at[d, :, cols],
                self.sems[6].at[q, d],
                self.sems[7].at[q, d],
                place.line[d],
            )
            copy.start()
            self.c4[q].append(copy)

    def land(self, q):
        b3, b4 = self.bufs[4:]
        cols = pl.ds(*self.pieces[q])
        total = b3[self.place.g, :, cols].astype(jnp.float32)
        for d in range(self.place.groups - 1):
            self.c4[q][d].wait_recv()
            total = total + b4[d, :, cols].astype(jnp.float32)
        self.acc[:, cols] = total

    def steps(self):
        stages = (self.to_core, self.to_side, self.to_other_side, self.along_line, self.land)
        return pipelined(self.n, stages, SUM_LAGS)

    def end(self):
        for q in range(self.n):
            for copy in [self.c1[q], self.c2[q], self.c3[q]] + self.c4[q]:
                copy.wait_send()


class SmallSum:
    def __init__(self, place, x, o, zbuf, buf, zs, zr, ss, rs):
        self.place, self.x, self.o, self.zbuf, self.buf = place, x, o, zbuf, buf
        self.zs, self.zr, self.ss, self.rs = zs, zr, ss, rs

    def begin(self):
        self.copies = []
        for d, device in enumerate(self.place.line):
            copy = remote(self.x, self.zbuf.at[d], self.zs.at[d], self.zr.at[d], device)
            copy.start()
            self.copies.append(copy)

    def line(self):
        place, groups = self.place, self.place.groups
        for copy in self.copies:
            copy.wait_recv()
        total = None
        for owner in range(groups):
            part = self.x[...]
            for d in range(groups - 1):
                source = lax.rem(place.g + groups - d - 1, groups)
                part = jnp.where(source == owner, self.zbuf[d], part)
            total = part if total is None else total + part
        self.o[...] = total
        self.send(0)

    def send(self, i):
        device = (self.place.side_x, self.place.side_y, self.place.core)[i]
        self.copy = remote(self.o, self.buf.at[i], self.ss.at[i], self.rs.at[i], device)
        self.copy.start()

    def add(self, i):
        self.copy.wait_recv()
        self.copy.wait_send()
        self.o[...] = self.o[...] + self.buf[i]
        if i < 2:
            self.send(i + 1)

    def steps(self):
        return [self.line] + [functools.partial(self.add, i) for i in range(3)]

    def end(self):
        for copy in self.copies:
            copy.wait_send()


def small_scratch(shape, groups):
    f32 = jnp.float32
    return [
        pltpu.VMEM((groups - 1, *shape), f32),
        pltpu.VMEM((3, *shape), f32),
        DMA((groups - 1,)),
        DMA((groups - 1,)),
        DMA((3,)),
        DMA((3,)),
    ]


def weave(*streams):
    found = []
    rounds = max((start + len(steps) for start, steps in streams), default=0)
    for at in range(rounds):
        for start, steps in streams:
            if 0 <= at - start < len(steps):
                found.append(steps[at - start])
    return found


def scatter_scratch(n, groups, rows, width):
    bf16 = jnp.bfloat16
    bufs = [
        pltpu.VMEM((groups, 2, 2, rows, width), bf16),
        pltpu.VMEM((groups, 2, 2, rows, width), bf16),
        pltpu.VMEM((groups, 2, 2, rows, width), bf16),
        pltpu.VMEM((groups, 2, rows, width), bf16),
        pltpu.VMEM((groups, rows, width), bf16),
        pltpu.VMEM((groups - 1, rows, width), bf16),
        pltpu.VMEM((rows, width), jnp.float32),
    ]
    sems = [DMA((n,))] * 6 + [DMA((n, groups - 1))] * 2
    return bufs, sems


def rms_rows(x, gain):
    return x * lax.rsqrt(jnp.mean(x * x, axis=-1, keepdims=True) + epsilon) * gain


def rms_back(x, gain, grad):
    inverse = lax.rsqrt(jnp.mean(x * x, axis=-1, keepdims=True) + epsilon)
    scaled = grad * gain
    along = jnp.mean(scaled * x, axis=-1, keepdims=True)
    d_gain = jnp.sum(grad * x * inverse, axis=0, keepdims=True)
    return scaled * inverse - x * inverse**3 * along, d_gain


NT = (((1,), (1,)), ((), ()))
NN = (((1,), (0,)), ((), ()))


class Summed:
    def __init__(self, sizes, products, extra=None, pieces=SUM_SHARES):
        self.sizes, self.products, self.extra = sizes, products, extra
        self.rows = products[0][0].shape[0] // (sizes[0] * sizes[1] * sizes[2])
        self.width = products[0][1].shape[-2 if products[0][3] else -1]
        self.more = 0 if extra is None else extra.shape[1]
        self.rights, self.places = [], []
        for _, right, _, _ in products:
            found = [i for i, other in enumerate(self.rights) if other is right]
            self.places.append(found[0] if found else len(self.rights))
            if not found:
                self.rights.append(right)
        at, self.pieces = 0, []
        for share in pieces:
            self.pieces.append((at, self.width * share // 16))
            at += self.width * share // 16
        if self.more:
            self.pieces.append((self.width, self.more))
        self.bufs, self.sems = scatter_scratch(
            len(self.pieces), sizes[0], self.rows, self.width + self.more
        )

    def operands(self):
        groups, ctx, tp = self.sizes
        split = (groups, ctx, tp // 2, 2, self.rows)
        found = [product[0].reshape(*split, product[0].shape[1]) for product in self.products]
        found += self.rights
        if self.more:
            found.append(self.extra.reshape(*split, self.more))
        return found

    def stage(self, place, inputs, scratch):
        count = len(self.products)
        lefts, rights = inputs[:count], inputs[count : count + len(self.rights)]
        bufs, sems = scratch[: len(self.bufs)], scratch[len(self.bufs) :]
        groups, ctx, tp = self.sizes

        def make(q, into, core):
            at, size = self.pieces[q]
            if at >= self.width:
                into[..., pl.ds(at, size)] = inputs[-1][:, :, :, core]
                return

            def block(i, _):
                total = None
                for left, where, (_, _, lead, transposed) in zip(
                    lefts, self.places, self.products
                ):
                    right = rights[where] if lead is None else rights[where].at[lead]
                    a = left[i, :, :, core]
                    a = a.reshape(-1, a.shape[-1])
                    some = right[pl.ds(at, size), :] if transposed else right[:, pl.ds(at, size)]
                    part = lax.dot_general(
                        a, some, NT if transposed else NN, preferred_element_type=jnp.float32
                    )
                    total = part if total is None else total + part
                into[i, :, :, :, pl.ds(at, size)] = total.astype(into.dtype).reshape(
                    ctx, tp // 2, self.rows, size
                )
                return 0

            lax.fori_loop(0, groups, block, 0)

        return Scatter(place, make, self.pieces, bufs[:-1], bufs[-1], sems)


def exchange(
    sizes,
    number,
    summed,
    finish,
    finish_args,
    finish_outs,
    gathered,
    moves,
    plan=(3,),
    start_also=5,
    start_second=10,
    also_gather=None,
    also_sum=None,
    tail=0,
    small=0,
    spread=None,
):
    groups, ctx, tp = sizes
    f32, bf16 = jnp.float32, jnp.bfloat16
    rows = summed.rows
    out_pieces = gather_pieces(gathered)
    move_outs, move_scratch = moves_setup(moves, groups * ctx)
    n_moves = len(moves)
    move_specs = [(split, join) for _, split, join in moves]
    S = jax.ShapeDtypeStruct

    operands, in_specs, out_shape, out_specs, scratch = [], [], [], [], []

    def add_in(arrays, spec=IN_VMEM):
        at = len(operands)
        operands.extend(arrays)
        in_specs.extend([spec] * len(arrays))
        return slice(at, len(operands))

    def add_out(shapes, spec=IN_VMEM):
        at = len(out_shape)
        out_shape.extend(shapes)
        out_specs.extend([spec] * len(shapes))
        return slice(at, len(out_shape))

    def add_scratch(shapes):
        at = len(scratch)
        scratch.extend(shapes)
        return slice(at, len(scratch))

    in_sum = add_in(summed.operands())
    in_args = add_in(list(finish_args))
    o_main = add_out([S((groups, ctx, tp // 2, 2, rows, gathered), bf16)])
    o_finish = add_out([S(shape, f32) for shape in finish_outs])
    s_sum = add_scratch(summed.bufs + summed.sems)
    s_main = add_scratch(
        [pltpu.VMEM((rows, gathered), bf16)] + gather_sems(len(out_pieces), groups)
    )
    if also_gather is not None:
        also_pieces = gather_pieces(also_gather.shape[1])
        in_also = add_in([also_gather])
        o_also = add_out([S((groups, ctx, tp // 2, 2, rows, also_gather.shape[1]), bf16)])
        s_also = add_scratch(gather_sems(len(also_pieces), groups))
    if also_sum is not None:
        second, second_finish, second_args, second_out = also_sum
        in_second, in_second_args = add_in(second.operands()), add_in(second_args)
        o_second = add_out([second_out])
        s_second = add_scratch(second.bufs + second.sems)
    if tail:
        o_tail = add_out([S((tp // 2, 2, rows, tail), bf16)])
        s_tail = add_scratch([pltpu.VMEM((rows, tail), bf16)] + [DMA] * 5)
    if small:
        o_small = add_out([S((1, small), f32)])
        s_small = add_scratch([pltpu.VMEM((1, small), f32)] + small_scratch((1, small), groups))
    if spread is not None:
        in_spread = add_in([spread])
        o_spread = add_out([S((groups, ctx, *spread.shape), spread.dtype)])
        s_spread = add_scratch([DMA((groups - 1,)), DMA((groups - 1,)), DMA, DMA, DMA])
    in_moves = add_in([array for array, _, _ in moves], IN_HBM)
    o_moves = add_out(move_outs, IN_HBM)
    s_moves = add_scratch(move_scratch)

    def kernel(*refs):
        ins = refs[: len(operands)]
        outs = refs[len(operands) : len(operands) + len(out_shape)]
        scr = refs[len(operands) + len(out_shape) :]
        place = Place(sizes)
        devices = [place.core, place.side_y]
        if n_moves:
            devices += [place.plane_peer(d)[1] for d in range(1, place.plane)]
        else:
            devices += [place.side_x] + place.line
        greet(devices)
        carried = None
        if n_moves:
            parts = scr[s_moves]
            carried = Moves(
                place, move_specs, ins[in_moves], outs[o_moves], parts[:n_moves], *parts[n_moves:]
            )
            carried.start()
        main_sum = summed.stage(place, ins[in_sum], scr[s_sum])
        low, *main_sems = scr[s_main]
        main_gather = Gather(place, low, outs[o_main][0], out_pieces, main_sems)
        streams = [(0, main_sum.steps())]
        ends = [main_sum, main_gather]
        if also_gather is not None:
            side_gather = Gather(place, ins[in_also][0], outs[o_also][0], also_pieces, scr[s_also])
            side_gather.begin()
            streams.append((start_also, side_gather.steps()))
            ends.append(side_gather)
        if spread is not None:
            plane = PlaneGather(place, ins[in_spread][0], outs[o_spread][0], *scr[s_spread])
            plane.begin()
            streams.append((6, [plane.step]))
            ends.append(plane)
        later = []
        if also_sum is not None:
            side_sum = second.stage(place, ins[in_second], scr[s_second])
            side_steps = side_sum.steps()
            ready = max(0, min(len(side_steps), len(summed.pieces) + SUM_LAGS[-1] - start_second))
            streams.append((start_second, side_steps[:ready]))
            later.append((0, side_steps[ready:]))
            ends.append(side_sum)
        total = n_moves * (groups * ctx - 1)
        steps = weave(*streams)
        for i, step in enumerate(steps):
            if carried is not None and i < len(plan):
                carried.issue(plan[i])
            step()
        if carried is not None:
            carried.settle()
        low_tail = scr[s_tail][0] if tail else None
        low_small = scr[s_small][0] if small else None
        finish(place, main_sum.acc, ins[in_args], outs[o_finish], low, low_tail, low_small)
        main_gather.begin()
        if small:
            small_sum = SmallSum(place, low_small, outs[o_small][0], *scr[s_small][1:])
            small_sum.begin()
            later.append((1, small_sum.steps()))
            ends.append(small_sum)
        if tail:
            ys, yr, ks, kr, own_sem = scr[s_tail][1:]
            y, k, spot = place.y, place.k, outs[o_tail][0]
            own = pltpu.make_async_copy(low_tail, spot.at[y, k], own_sem)
            own.start()
            to_y = remote(low_tail, spot.at[y, k], ys, yr, place.side_y)
            to_y.start()
            own.wait()
        steps = weave((0, main_gather.steps()), *later)
        if carried is not None:
            carried.issue(total)
        for step in steps:
            step()
        if tail:
            to_y.wait_recv()
            part = spot.at[:, k]
            to_k = remote(part, part, ks, kr, place.core)
            to_k.start()
            to_k.wait_recv()
            to_y.wait_send()
            to_k.wait_send()
        if also_sum is not None:
            second_finish(side_sum.acc, ins[in_second_args], outs[o_second][0])
        for stage in ends:
            stage.end()
        if carried is not None:
            carried.finish()

    results = pl.pallas_call(
        kernel,
        out_shape=out_shape,
        in_specs=in_specs,
        out_specs=out_specs,
        scratch_shapes=scratch,
        name=f"exchange_{number}",
        compiler_params=pltpu.CompilerParams(
            collective_id=number, has_side_effects=True, vmem_limit_bytes=62 * 2**20
        ),
    )(*operands)
    found = {"gathered": results[0].reshape(-1, gathered), "finish": results[o_finish]}
    if also_gather is not None:
        found["also"] = results[o_also][0].reshape(-1, also_gather.shape[1])
    if also_sum is not None:
        found["second"] = results[o_second][0]
    if tail:
        found["tail"] = results[o_tail][0].reshape(-1, tail)
    if small:
        found["small"] = results[o_small][0]
    if spread is not None:
        found["spread"] = results[o_spread][0]
    found["moves"] = results[o_moves]
    return found


def gather_pieces(width):
    if width < 1024:
        return [(0, width)]
    whole = width // 2048 * 2048
    at, found = 0, []
    for share in GATHER_SHARES:
        found.append((at, whole * share // 16))
        at += whole * share // 16
    if width > whole:
        found.append((whole, width - whole))
    return found


def opening(sizes, number, hidden, embeds, cotangent, lengths, gain, down_maps, shard, moves):
    groups, ctx, tp = sizes
    f32, bf16 = jnp.float32, jnp.bfloat16
    rows = hidden.shape[0] // tp
    half = hidden.shape[1]
    rank = down_maps.shape[2]
    mids = down_maps.shape[0] * rank
    rest = 3 * half
    width = rest + mids + 128
    out_pieces = gather_pieces(width)
    move_outs, move_scratch = moves_setup(moves, groups * ctx)
    move_specs = [(split, join) for _, split, join in moves]
    n_moves = len(moves)

    def kernel(*refs):
        hid, emb, cot, lens, gain_ref, down_ref = refs[:6]
        up_ref, step_ref, taps_ref, bias_ref, norm_ref, *head_refs = refs[6:14]
        refs = list(refs[14:])
        sources = refs[:n_moves]
        o, up_o, step_o, small_o = refs[n_moves : n_moves + 4]
        targets = refs[n_moves + 4 : 2 * n_moves + 4]
        own = refs[2 * n_moves + 4 :]
        low, gs = own[0], own[1:10]
        stages = own[10 : 10 + n_moves]
        send, recv, local = own[10 + n_moves :]
        place = Place(sizes)
        greet(
            [place.core, place.side_y]
            + [place.plane_peer(d)[1] for d in range(1, place.plane)]
        )
        carried = Moves(place, move_specs, sources, targets, stages, send, recv, local)
        carried.start(1)
        mine = pl.ds(pl.multiple_of(place.t * rows, 16), rows)
        a, b = hid[mine, :].astype(f32), emb[mine, :].astype(f32)
        squares = jnp.sum(a * a, axis=1, keepdims=True) + jnp.sum(b * b, axis=1, keepdims=True)
        inverse = lax.rsqrt(squares / (2 * half) + epsilon)
        low[:, :half] = (a * inverse * gain_ref[:, :half]).astype(bf16)
        low[:, half : 2 * half] = (b * inverse * gain_ref[:, half:]).astype(bf16)
        for j in range(down_maps.shape[0]):
            at = rest + j * rank
            low[:, at : at + rank] = lax.dot_general(
                low[:, : 2 * half], down_ref[j], NN, preferred_element_type=f32
            ).astype(bf16)
        slot = lax.broadcasted_iota(jnp.int32, (rows, 128), 0)
        slot = slot + (place.c * tp + place.t) * rows
        lane = lax.broadcasted_iota(jnp.int32, (rows, 128), 1)
        segment, position, end = jnp.zeros_like(slot), slot, 0
        for i in range(lengths.shape[1]):
            length = lens[0, i]
            end = end + length
            passed = (slot >= end).astype(jnp.int32)
            segment = segment + passed
            position = position - passed * length
        marks = jnp.where(lane == 0, segment, position)
        low[:, 2 * half : rest] = cot[mine, :]
        low[:, rest + mids :] = marks.astype(f32).astype(bf16)
        gather = Gather(place, low, o, out_pieces, gs)
        gather.begin()
        carried.issue(len(carried.queue))
        lanes = pl.ds(pl.multiple_of(place.index * 128, 128), 128)
        for j in range(up_o.shape[0]):
            up_o[j] = up_ref[j, :, lanes]
        heads = step_ref.shape[0]
        few = heads // place.plane
        row = lax.broadcasted_iota(jnp.int32, (heads, 128), 0) - place.index * few
        col = lax.broadcasted_iota(jnp.int32, (heads, 128), 1)
        pick = (row == col) & (col < few)
        wide = row == col // (128 // few)
        step_o[...] = lax.dot_general(
            step_ref[...], pick.astype(bf16), TN, preferred_element_type=f32
        ).astype(bf16)
        small_o[...] = jnp.zeros_like(small_o)
        small_o[0:4, :] = taps_ref[:, lanes]
        small_o[4:5, :] = bias_ref[:, lanes]
        small_o[6:7, :] = norm_ref[:, lanes]
        for at, head_ref, chosen in zip((5, 8, 9), head_refs, (wide, pick, pick)):
            small_o[at : at + 1, :] = lax.dot_general(
                jnp.broadcast_to(head_ref[...], (8, heads)),
                chosen.astype(f32),
                NN,
                precision=highest,
                preferred_element_type=f32,
            )[0:1]
        for step in gather.steps():
            step()
        carried.settle()
        gather.end()
        carried.finish()

    S = jax.ShapeDtypeStruct
    results = pl.pallas_call(
        kernel,
        out_shape=[
            S((groups, ctx, tp // 2, 2, rows, width), bf16),
            S((*shard[0].shape[:2], 128), bf16),
            S((shard[1].shape[1], 128), bf16),
            S((16, 128), f32),
        ]
        + move_outs,
        in_specs=[IN_VMEM] * 3 + [IN_SMEM] + [IN_VMEM] * 10 + [IN_HBM] * n_moves,
        out_specs=[IN_VMEM] * 4 + [IN_HBM] * n_moves,
        scratch_shapes=[pltpu.VMEM((rows, width), bf16)]
        + gather_sems(len(out_pieces), groups)
        + move_scratch,
        name=f"opening_{number}",
        compiler_params=pltpu.CompilerParams(
            collective_id=number, has_side_effects=True, vmem_limit_bytes=62 * 2**20
        ),
    )(
        *(hidden, embeds, cotangent, lengths, gain.reshape(1, -1), down_maps),
        *shard,
        *[array for array, _, _ in moves],
    )
    return [results[0].reshape(-1, width)] + list(results[1:])


def sum_small(sizes, number, values):
    def kernel(x, o, *scratch):
        place = Place(sizes)
        greet([place.core, place.side_y, place.side_x] + place.line)
        summing = SmallSum(place, x, o, *scratch)
        summing.begin()
        for step in summing.steps():
            step()
        summing.end()

    return pl.pallas_call(
        kernel,
        out_shape=jax.ShapeDtypeStruct(values.shape, jnp.float32),
        in_specs=[IN_VMEM],
        out_specs=IN_VMEM,
        scratch_shapes=small_scratch(values.shape, sizes[0]),
        name=f"sum_small_{number}",
        compiler_params=pltpu.CompilerParams(collective_id=number, has_side_effects=True),
    )(values)


def own_of(place, ref, rows):
    if ref.shape[0] == rows:
        return ref[...].astype(jnp.float32)
    return ref[pl.ds(pl.multiple_of(place.t * rows, 16), rows), :].astype(jnp.float32)


def finish_forward(place, acc, args, outs, low, low_tail, low_small):
    rest, gain = args
    outs[0][...] = own_of(place, rest, acc.shape[0]) + acc[...]
    low[...] = rms_rows(outs[0][...], gain[...]).astype(jnp.bfloat16)


def finish_mixer_back(place, acc, args, outs, low, low_tail, low_small):
    after_mlp, gain, cot, state_map = args
    width = after_mlp.shape[1]
    low[:, width:] = acc[:, width:].astype(jnp.bfloat16)
    d_normed = acc[:, :width] + lax.dot_general(
        low[:, width:], state_map[...], NT, preferred_element_type=jnp.float32
    )
    d_rows, d_gain = rms_back(after_mlp[...], gain[...], d_normed)
    outs[1][...] = d_gain
    d_rows = cot[...].astype(jnp.float32) + d_rows
    outs[0][...] = d_rows
    low[:, :width] = d_rows.astype(jnp.bfloat16)


def finish_mlp_back(place, acc, args, outs, low, low_tail, low_small):
    after_attn, gain, d_after_mlp = args
    d_rows, d_gain = rms_back(after_attn[...], gain[...], acc[...])
    outs[1][...] = d_gain
    d_rows = d_after_mlp[...] + d_rows
    outs[0][...] = d_rows
    low[...] = d_rows.astype(jnp.bfloat16)


def finish_attention_back(place, acc, args, outs, low, low_tail, low_small):
    hidden, embeds, gain, d_after_attn, down_maps, out_mine, row = args
    half = hidden.shape[1]
    bf16, f32 = jnp.bfloat16, jnp.float32
    low[...] = acc[:, 2 * half :].astype(bf16)
    inputs = [own_of(place, part, acc.shape[0]) for part in (hidden, embeds)]
    squares = sum(jnp.sum(part * part, axis=1, keepdims=True) for part in inputs)
    inverse = lax.rsqrt(squares / (2 * half) + epsilon)
    along = jnp.zeros_like(squares)
    for i, part in enumerate(inputs):
        cols = slice(i * half, (i + 1) * half)
        grad = acc[:, cols]
        for j in range(down_maps.shape[0]):
            rank = down_maps.shape[2]
            grad = grad + lax.dot_general(
                low[:, j * rank : (j + 1) * rank],
                down_maps[j, cols, :],
                NT,
                preferred_element_type=f32,
            )
        acc[:, cols] = grad
        along = along + jnp.sum(grad * gain[:, cols] * part, axis=1, keepdims=True)
    along = along / (2 * half)
    low_tail[:, :half] = out_mine[...]
    low_small[:, 2 * half :] = row[...]
    for i, part in enumerate(inputs):
        cols = slice(i * half, (i + 1) * half)
        grad = acc[:, cols]
        low_small[:, cols] = jnp.sum(grad * part * inverse, axis=0, keepdims=True)
        d_rows = grad * gain[:, cols] * inverse - part * inverse**3 * along
        if i == 0:
            d_rows = d_rows + d_after_attn[...]
        low_tail[:, (i + 1) * half : (i + 2) * half] = d_rows.astype(bf16)


def finish_out(acc, args, out):
    out[...] = (args[0][...] + acc[...]).astype(out.dtype)


def adapter_products(xa, dmid, width):
    block, rank = 1024, dmid.shape[1] // 3

    def kernel(a, b, o, b_t):
        @pl.when(pl.program_id(0) == 0)
        def _():
            b_t[...] = b[...].T

        both = quick(b_t[...], a[...], NN)
        for j in range(3):
            o[j] = both[j * rank : (j + 1) * rank].T

    return pl.pallas_call(
        kernel,
        out_shape=jax.ShapeDtypeStruct((3, width, rank), jnp.float32),
        grid=(width // block,),
        in_specs=[
            pl.BlockSpec((xa.shape[0], block), lambda i: (0, i)),
            pl.BlockSpec(dmid.shape, lambda i: (0, 0)),
        ],
        out_specs=pl.BlockSpec((3, block, rank), lambda i: (0, i, 0)),
        scratch_shapes=[pltpu.VMEM(dmid.shape[::-1], dmid.dtype)],
        compiler_params=pltpu.CompilerParams(vmem_limit_bytes=60 * 2**20),
        name="adapter_products",
    )(xa, dmid)


def unpack(packed, parts):
    flat, at, found = packed.reshape(-1), 0, []
    for part in parts:
        found.append(flat[at : at + part.size].reshape(part.shape))
        at += part.size
    return found


TN = (((0,), (0,)), ((), ()))


def exact(left, right, dims):
    return lax.dot_general(left, right, dims, precision=highest, preferred_element_type=jnp.float32)


def quick(left, right, dims):
    return lax.dot_general(left, right, dims, preferred_element_type=jnp.float32)


def down_rows(values, by):
    return pltpu.roll(values, by, 0)


def up_rows(values, by):
    return pltpu.roll(values, values.shape[0] - by, 0)


def taps_forward(values, taps, bias, position):
    total = values * taps[0:1, :] + bias
    for lag in range(1, taps.shape[0]):
        kept = jnp.where(position >= lag, down_rows(values, lag), 0.0)
        total = total + kept * taps[lag : lag + 1, :]
    return total


def taps_backward(d_total, values, taps, position):
    d_values = d_total * taps[0:1, :]
    rows = [jnp.sum(d_total * values, axis=0, keepdims=True)]
    for lag in range(1, taps.shape[0]):
        kept = jnp.where(position >= lag, d_total, 0.0)
        rows.append(jnp.sum(kept * down_rows(values, lag), axis=0, keepdims=True))
        d_values = d_values + up_rows(kept, lag) * taps[lag : lag + 1, :]
    return d_values, rows + [jnp.sum(d_total, axis=0, keepdims=True)]


def silu_slope(values):
    sigmoid = jax.nn.sigmoid(values)
    return sigmoid * (1.0 + values * (1.0 - sigmoid))


class Scan:
    def __init__(self, xs, raw, bc, marks, taps, bias, bc_taps, bc_bias, heads):
        f32 = jnp.float32
        rows, lanes = xs.shape
        self.rows, self.half = rows, lanes // 2
        self.position = marks[:, 1:2].astype(f32)
        self.lane = lax.broadcasted_iota(jnp.int32, (rows, lanes), 1)
        self.xs, self.bc = xs.astype(f32), bc.astype(f32)
        self.pre_x = taps_forward(self.xs, taps, bias, self.position)
        self.pre_bc = taps_forward(self.bc, bc_taps, bc_bias, self.position)
        self.xc, bcc = jax.nn.silu(self.pre_x), jax.nn.silu(self.pre_bc)
        self.b_mat, self.c_mat = bcc[:, :STATE], bcc[:, STATE:]
        self.step_in = raw.astype(f32) + heads[0:1, :]
        self.dt = jax.nn.softplus(self.step_in)
        self.rate = -jnp.exp(heads[1:2, :])
        self.log_decay = self.dt * self.rate
        running, by = self.log_decay, 1
        while by < rows:
            running = running + jnp.where(self.position >= by, down_rows(running, by), 0.0)
            by *= 2
        self.running = running
        self.across = running.T
        row = lax.broadcasted_iota(jnp.int32, (rows, rows), 0)
        col = lax.broadcasted_iota(jnp.int32, (rows, rows), 1)
        first = row.astype(f32) - self.position
        self.same = (col <= row) & (col.astype(f32) >= first)
        self.meet = exact(self.c_mat, self.b_mat, NT)
        self.dt_wide = self.by_head([self.dt[:, h : h + 1] for h in range(2)])
        self.weighted = self.xc * self.dt_wide

    def by_head(self, values):
        return jnp.where(self.lane < self.half, values[0], values[1])

    def in_lane(self, values):
        return jnp.where(self.lane == 0, values[0], jnp.where(self.lane == 1, values[1], 0.0))

    def decay(self, h):
        gap = self.running[:, h : h + 1] - self.across[h : h + 1, :]
        return jnp.where(self.same, jnp.exp(jnp.where(self.same, gap, 0.0)), 0.0)

    def forward(self, skip):
        outs = [exact(self.decay(h) * self.meet, self.weighted, NN) for h in range(2)]
        return self.by_head(outs) + skip * self.xc

    def to_ends(self, values):
        rows = values.shape[0]
        row = lax.broadcasted_iota(jnp.int32, values.shape, 0)
        wide = jnp.broadcast_to(self.position, values.shape)
        by = 1
        while by < rows:
            inside = (up_rows(wide, by) >= by) & (row < rows - by)
            values = values + jnp.where(inside, up_rows(values, by), 0.0)
            by *= 2
        return values


def mixer_forward(xn, marked, mark_block, w_zx, w_step, state_map, w_out, small, bc_taps, bc_bias, groups):
    f32, bf16 = jnp.float32, jnp.bfloat16
    total, width = xn.shape
    rows, lanes = total // groups, w_zx.shape[2]
    state2 = state_map.shape[1]

    def kernel(xn_r, cot_r, marks_r, zx_r, st_r, sm_r, wo_r, sml, bt_r, bb_r, z_o, xs_o, raw_o, bc_o, y_o, dyn_o, sums_o):
        x = xn_r[...]
        z = quick(x, zx_r[0], NN)
        xs = quick(x, zx_r[1], NN).astype(bf16)
        raw = quick(x, st_r[...], NN).astype(bf16)
        bc = quick(x, sm_r[...], NN).astype(bf16)
        z_o[...], xs_o[...], raw_o[...], bc_o[...] = z, xs, raw, bc
        scan = Scan(
            xs, raw, bc, marks_r[...].astype(f32), sml[0:4, :], sml[4:5, :], bt_r[...], bb_r[...], sml[8:10, :]
        )
        y = scan.forward(sml[5:6, :]).astype(bf16)
        y_o[...] = y
        gated = y.astype(f32) * jax.nn.silu(z)
        d_yn = quick(cot_r[...], wo_r[...], NT)
        dyn_o[...] = d_yn
        ones = jnp.ones((8, lanes), f32)
        sums_o[0, 0:1] = exact(ones, gated * gated, NT)[0:1]
        sums_o[0, 1:2] = exact(ones, d_yn * sml[6:7, :] * gated, NT)[0:1]

    def by_group(columns):
        return pl.BlockSpec((rows, columns), lambda g: (g, 0))

    def whole(array):
        return pl.BlockSpec(array.shape, lambda g: (0,) * array.ndim)

    S = jax.ShapeDtypeStruct
    return pl.pallas_call(
        kernel,
        grid=(groups,),
        in_specs=[by_group(width), pl.BlockSpec((rows, width), lambda g: (g, 2))]
        + [pl.BlockSpec((rows, 128), lambda g: (g, mark_block))]
        + [whole(array) for array in (w_zx, w_step, state_map, w_out, small, bc_taps, bc_bias)],
        out_specs=[by_group(lanes)] * 3
        + [by_group(state2), by_group(lanes), by_group(lanes), pl.BlockSpec((1, 2, rows), lambda g: (g, 0, 0))],
        out_shape=[
            S((total, lanes), f32),
            S((total, lanes), bf16),
            S((total, lanes), bf16),
            S((total, state2), bf16),
            S((total, lanes), bf16),
            S((total, lanes), f32),
            S((groups, 2, rows), f32),
        ],
        compiler_params=pltpu.CompilerParams(vmem_limit_bytes=60 * 2**20),
        name="mixer_forward",
    )(xn, marked, marked, w_zx, w_step, state_map, w_out, small, bc_taps, bc_bias)


def mixer_backward(xn, marked, mark_block, kept, sums, small, bc_taps, bc_bias, groups):
    f32, bf16 = jnp.float32, jnp.bfloat16
    z, xs, raw, bc, y, d_yn = kept
    total, width = xn.shape
    rows, lanes, state2 = total // groups, z.shape[1], bc.shape[1]

    def kernel(
        xn_r, cot_r, marks_r, z_r, xs_r, raw_r, bc_r, y_r, dyn_r, sums_r, sml, bt_r, bb_r,
        dz_o, dxs_o, draw_o, dbc_o, yn_o, gzx_o, gst_o, gout_o, gsm_o, gbc_o, acc_in, acc_out,
    ):
        group = pl.program_id(0)
        scan = Scan(
            xs_r[...], raw_r[...], bc_r[...], marks_r[...].astype(f32),
            sml[0:4, :], sml[4:5, :], bt_r[...], bb_r[...], sml[8:10, :],
        )
        skip, gain = sml[5:6, :], sml[6:7, :]
        sums_wide = [jnp.broadcast_to(sums_r[0, i : i + 1], (128, rows)).T for i in range(2)]
        inverse = lax.rsqrt(sums_wide[0] / INNER + epsilon)
        cross = sums_wide[1] / INNER
        gate, out, d_normed = z_r[...], y_r[...].astype(f32), dyn_r[...]
        silu_z = jax.nn.silu(gate)
        gated = out * silu_z
        yn = (gated * inverse * gain).astype(bf16)
        yn_o[...] = yn
        g_gate = jnp.sum(d_normed * gated * inverse, axis=0, keepdims=True)
        d_gated = d_normed * gain * inverse - gated * inverse**3 * cross
        d_y = (d_gated * silu_z).astype(bf16).astype(f32)
        d_z = (d_gated * out * silu_slope(gate)).astype(bf16)
        dz_o[...] = d_z
        g_skip = jnp.sum(d_y * scan.xc, axis=0, keepdims=True)
        d_weighted, d_meet = jnp.zeros_like(d_y), jnp.zeros_like(scan.meet)
        by_row, by_col = [], []
        for h in range(2):
            mine = (scan.lane < scan.half) if h == 0 else (scan.lane >= scan.half)
            d_head = jnp.where(mine, d_y, 0.0)
            decay = scan.decay(h)
            mixing = decay * scan.meet
            d_mixing = exact(d_head, scan.weighted, NT)
            d_weighted = d_weighted + exact(mixing, d_head, TN)
            d_meet = d_meet + d_mixing * decay
            moved = d_mixing * mixing
            by_row.append(jnp.sum(moved, axis=1, keepdims=True))
            by_col.append(jnp.sum(moved, axis=0, keepdims=True))
        columns = [jnp.broadcast_to(by_col[h], (128, rows)).T for h in range(2)]
        d_running = scan.in_lane([by_row[h] - columns[h] for h in range(2)])
        d_log = scan.to_ends(d_running)
        shared = d_weighted * scan.xc
        d_dt = scan.in_lane(
            [
                jnp.sum(jnp.where(scan.lane < scan.half, shared, 0.0), axis=1, keepdims=True),
                jnp.sum(jnp.where(scan.lane >= scan.half, shared, 0.0), axis=1, keepdims=True),
            ]
        )
        d_step = (d_dt + d_log * scan.rate) * jax.nn.sigmoid(scan.step_in)
        g_bias = jnp.sum(d_step, axis=0, keepdims=True)
        g_decay = jnp.sum(d_log * scan.log_decay, axis=0, keepdims=True)
        d_raw = d_step.astype(bf16)
        draw_o[...] = d_raw
        d_xc = skip * d_y + d_weighted * scan.dt_wide
        d_xs, g_taps = taps_backward(
            d_xc * silu_slope(scan.pre_x), scan.xs, sml[0:4, :], scan.position
        )
        d_xs = d_xs.astype(bf16)
        dxs_o[...] = d_xs
        d_bcc = jnp.concatenate(
            [exact(d_meet, scan.c_mat, TN), exact(d_meet, scan.b_mat, NN)], axis=1
        )
        d_bc, g_bc_taps = taps_backward(
            d_bcc * silu_slope(scan.pre_bc), scan.bc, bt_r[...], scan.position
        )
        dbc_o[...] = d_bc.astype(bf16)
        in_part = quick(jnp.concatenate([d_z, d_xs, d_raw], axis=1), xn_r[...], TN)
        out_part = quick(yn, cot_r[...], TN)
        blank = jnp.zeros((1, lanes), f32)
        few = jnp.concatenate(
            g_taps + [g_gate, g_bias, g_decay, g_skip] + [blank] * 7, axis=0
        )
        few_bc = jnp.concatenate(g_bc_taps + [jnp.zeros((3, state2), f32)], axis=0)

        @pl.when(group == 0)
        def _():
            acc_in[...], acc_out[...] = in_part, out_part
            gsm_o[...], gbc_o[...] = few, few_bc

        @pl.when(group > 0)
        def _():
            acc_in[...] += in_part
            acc_out[...] += out_part
            gsm_o[...] += few
            gbc_o[...] += few_bc

        @pl.when(group == groups - 1)
        def _():
            for i in range(2):
                gzx_o[i] = acc_in[i * lanes : (i + 1) * lanes, :].T.astype(bf16)
            gst_o[...] = acc_in[2 * lanes : 2 * lanes + 8, :]
            gout_o[...] = acc_out[...].astype(bf16)

    def by_group(columns):
        return pl.BlockSpec((rows, columns), lambda g: (g, 0))

    def whole(shape):
        return pl.BlockSpec(shape, lambda g: (0,) * len(shape))

    S = jax.ShapeDtypeStruct
    return pl.pallas_call(
        kernel,
        grid=(groups,),
        in_specs=[by_group(width), pl.BlockSpec((rows, width), lambda g: (g, 2))]
        + [pl.BlockSpec((rows, 128), lambda g: (g, mark_block))]
        + [by_group(array.shape[1]) for array in kept]
        + [pl.BlockSpec((1, 2, rows), lambda g: (g, 0, 0)), whole(small.shape), whole(bc_taps.shape), whole(bc_bias.shape)],
        out_specs=[by_group(lanes)] * 3
        + [by_group(state2), by_group(lanes)]
        + [
            whole((2, width, lanes)),
            whole((8, width)),
            whole((lanes, width)),
            whole((16, lanes)),
            whole((8, state2)),
        ],
        out_shape=[
            S((total, lanes), bf16),
            S((total, lanes), bf16),
            S((total, lanes), bf16),
            S((total, state2), bf16),
            S((total, lanes), bf16),
            S((2, width, lanes), bf16),
            S((8, width), f32),
            S((lanes, width), bf16),
            S((16, lanes), f32),
            S((8, state2), f32),
        ],
        scratch_shapes=[pltpu.VMEM((3 * lanes, width), f32), pltpu.VMEM((lanes, width), f32)],
        compiler_params=pltpu.CompilerParams(vmem_limit_bytes=60 * 2**20),
        name="mixer_backward",
    )(xn, marked, marked, z, xs, raw, bc, y, d_yn, sums, small, bc_taps, bc_bias)


def swap_halves(values):
    return pltpu.roll(values, values.shape[1] // 2, 1)


def attend_weights(qr, kr, marks, rows):
    f32 = jnp.float32
    row = lax.broadcasted_iota(jnp.int32, (rows, rows), 0)
    col = lax.broadcasted_iota(jnp.int32, (rows, rows), 1)
    first = row.astype(f32) - marks[:, 1:2]
    allowed = (col <= row) & (col.astype(f32) >= first)
    weights = jnp.exp(jnp.where(allowed, quick(qr, kr, NT) * AHD ** (-0.5), -1e30))
    return weights / jnp.sum(weights, axis=-1, keepdims=True)


def attention_forward(xa, width, w_qkv, up_maps, frequencies, groups):
    f32, bf16 = jnp.float32, jnp.bfloat16
    total, columns = xa.shape
    rows, rank = total // groups, up_maps.shape[1]
    side = columns - (3 * width) // 2
    side_block = pl.BlockSpec((rows, side), lambda g: (g, columns // side - 1))

    def kernel(xa_r, side_r, w_r, up_r, freq_r, ao_o, q_o, k_o, v_o, cos_o, sin_o, w_all):
        @pl.when(pl.program_id(0) == 0)
        def _():
            for j in range(3):
                w_all[:, j * AHD : (j + 1) * AHD] = w_r[j]

        marks = side_r[:, 3 * rank :].astype(f32)
        wide = quick(xa_r[...], w_all[...], NN)
        proj = []
        for j in range(3):
            mid = side_r[:, j * rank : (j + 1) * rank]
            proj.append((wide[:, j * AHD : (j + 1) * AHD] + quick(mid, up_r[j], NN)).astype(bf16))
        angle = marks[:, 1:2] * freq_r[...]
        lane = lax.broadcasted_iota(jnp.int32, angle.shape, 1)
        cosine, sine = jnp.cos(angle), jnp.sin(angle)
        sine = jnp.where(lane < AHD // 2, -sine, sine)
        cos_o[...], sin_o[...] = cosine, sine
        qr, kr = [
            (piece * cosine + swap_halves(piece) * sine).astype(bf16)
            for piece in (proj[0].astype(f32), proj[1].astype(f32))
        ]
        q_o[...], k_o[...], v_o[...] = qr, kr, proj[2]
        low = attend_weights(qr, kr, marks, rows).astype(bf16)
        ao_o[...] = quick(low, proj[2], NN).astype(bf16)

    def by_group(size):
        return pl.BlockSpec((rows, size), lambda g: (g, 0))

    def whole(array):
        return pl.BlockSpec(array.shape, lambda g: (0,) * array.ndim)

    S = jax.ShapeDtypeStruct
    return pl.pallas_call(
        kernel,
        grid=(groups,),
        in_specs=[by_group(width), side_block, whole(w_qkv), whole(up_maps), whole(frequencies)],
        out_specs=[by_group(AHD)] * 6,
        out_shape=[S((total, AHD), bf16)] * 4 + [S((total, AHD), f32)] * 2,
        scratch_shapes=[pltpu.VMEM((width, 3 * AHD), bf16)],
        compiler_params=pltpu.CompilerParams(vmem_limit_bytes=60 * 2**20),
        name="attention_forward",
    )(xa, xa, w_qkv, up_maps, frequencies)


def attention_backward(d_attn, xa, width, w_o, up_maps, kept, groups):
    f32, bf16 = jnp.float32, jnp.bfloat16
    total, columns = xa.shape
    rows, rank = total // groups, up_maps.shape[1]
    side = columns - (3 * width) // 2
    side_block = pl.BlockSpec((rows, side), lambda g: (g, columns // side - 1))
    model = d_attn.shape[1]

    def kernel(
        da_r, xa_r, side_r, wo_r, up_r, ao_r, q_r, k_r, v_r, cos_r, sin_r,
        dq_o, dk_o, dv_o, dmid_o, gw_o, go_o, gup_o, acc_w, acc_o,
    ):
        group = pl.program_id(0)
        d_rows = da_r[...]
        marks = side_r[:, 3 * rank :].astype(f32)
        d_ao = quick(d_rows, wo_r[...], NT).astype(bf16)
        qr, kr, vals = q_r[...], k_r[...], v_r[...]
        weights = attend_weights(qr, kr, marks, rows)
        d_vals = quick(weights.astype(bf16), d_ao, TN)
        d_weights = quick(d_ao, vals, NT).astype(bf16).astype(f32)
        along = jnp.sum(d_weights * weights, axis=-1, keepdims=True)
        d_scores = (weights * (d_weights - along) * AHD ** (-0.5)).astype(bf16)
        cosine, sine = cos_r[...], sin_r[...]
        pieces = []
        for d_turned in (quick(d_scores, kr, NN), quick(d_scores, qr, TN)):
            d_turned = d_turned.astype(bf16).astype(f32)
            pieces.append((d_turned * cosine + swap_halves(d_turned * sine)).astype(bf16))
        pieces.append(d_vals.astype(bf16))
        for j, out in enumerate((dq_o, dk_o, dv_o)):
            out[...] = pieces[j]
            dmid_o[:, j * rank : (j + 1) * rank] = quick(pieces[j], up_r[j], NT).astype(bf16)
        part = quick(jnp.concatenate(pieces, axis=1), xa_r[...], TN)
        part_o = quick(ao_r[...], d_rows, TN)
        parts_up = [
            quick(side_r[:, j * rank : (j + 1) * rank], pieces[j], TN)
            for j in range(3)
        ]

        @pl.when(group == 0)
        def _():
            acc_w[...], acc_o[...] = part, part_o
            for j in range(3):
                gup_o[j] = parts_up[j]

        @pl.when(group > 0)
        def _():
            acc_w[...] += part
            acc_o[...] += part_o
            for j in range(3):
                gup_o[j] += parts_up[j]

        @pl.when(group == groups - 1)
        def _():
            for j in range(3):
                gw_o[j] = acc_w[j * AHD : (j + 1) * AHD, :].T.astype(bf16)
            go_o[...] = acc_o[...].astype(bf16)

    def by_group(size):
        return pl.BlockSpec((rows, size), lambda g: (g, 0))

    def whole(shape):
        return pl.BlockSpec(shape, lambda g: (0,) * len(shape))

    S = jax.ShapeDtypeStruct
    return pl.pallas_call(
        kernel,
        grid=(groups,),
        in_specs=[by_group(model), by_group(width), side_block, whole(w_o.shape), whole(up_maps.shape)]
        + [by_group(AHD)] * 6,
        out_specs=[by_group(AHD)] * 3
        + [by_group(3 * rank)]
        + [whole((3, width, AHD)), whole((AHD, model)), whole((3, rank, AHD))],
        out_shape=[S((total, AHD), bf16)] * 3
        + [
            S((total, 3 * rank), bf16),
            S((3, width, AHD), bf16),
            S((AHD, model), bf16),
            S((3, rank, AHD), f32),
        ],
        scratch_shapes=[pltpu.VMEM((3 * AHD, width), f32), pltpu.VMEM((AHD, model), f32)],
        compiler_params=pltpu.CompilerParams(vmem_limit_bytes=60 * 2**20),
        name="attention_backward",
    )(d_attn, xa, xa, w_o, up_maps, *kept)


def per_device_split(
    hidden,
    embeds,
    cotangent,
    lengths,
    attention_norm_gain,
    adapter_down_maps,
    query_key_value_weight,
    adapter_up_maps,
    attention_output_weight,
    feedforward_norm_gain,
    gate_up_weight,
    down_weight,
    mixer_norm_gain,
    mixer_gate_input_weight,
    state_map_weight,
    step_size_weight,
    mixer_input_taps,
    mixer_input_tap_bias,
    state_map_taps,
    state_map_tap_bias,
    step_size_bias,
    log_decay_rate,
    head_skip_weight,
    gated_norm_gain,
    mixer_output_weight,
):
    bf16, f32 = jnp.bfloat16, jnp.float32
    tp_size, ctx_size, groups = (lax.axis_size(name) for name in ("tp", "ctx", "fsdp"))
    tp_index, ctx_index = lax.axis_index("tp"), lax.axis_index("ctx")
    plane_index = lax.axis_index("fsdp") * ctx_size + ctx_index
    plane_size = groups * ctx_size
    tok_rows = hidden.shape[0]
    mine = tok_rows // tp_size
    group_rows = tok_rows * ctx_size
    start = tp_index * mine

    sizes = (groups, ctx_size, tp_size)

    def own_rows(values):
        return lax.dynamic_slice_in_dim(values, start, mine, 0)

    width = hidden.shape[1]
    own_shape = (mine, width)
    cot_low = own_rows(cotangent)

    rank = adapter_down_maps.shape[2]
    width_a = adapter_down_maps.shape[1]
    xa_wide, up_maps, w_step, small, w_o, w_qkv = opening(
        sizes,
        1,
        hidden,
        embeds,
        cotangent,
        lengths,
        attention_norm_gain,
        adapter_down_maps,
        [
            adapter_up_maps,
            step_size_weight.T,
            mixer_input_taps,
            mixer_input_tap_bias[None],
            gated_norm_gain[None],
            head_skip_weight[None],
            step_size_bias[None],
            log_decay_rate[None],
        ],
        [(attention_output_weight, 0, 1), (query_key_value_weight, 2, 1)],
    )
    half = AHD // 2
    frequencies = 10000.0 ** (-jnp.arange(half, dtype=f32) / half)
    frequencies = jnp.concatenate([frequencies, frequencies])[None]
    kept_a = attention_forward(xa_wide, width_a, w_qkv, up_maps, frequencies, groups)
    ao_low = kept_a[0]

    gain_m = feedforward_norm_gain.reshape(1, -1)
    found = exchange(
        sizes,
        2,
        Summed(sizes, [(ao_low, w_o, None, False)]),
        finish_forward,
        [hidden, gain_m],
        [own_shape],
        width,
        [(gate_up_weight, 2, 1), (down_weight, 0, 1)],
    )
    xm, (after_attn,), (w_gu, w_down) = found["gathered"], found["finish"], found["moves"]
    gate_pre, up_pre = matrix_product(xm, w_gu[0]), matrix_product(xm, w_gu[1])
    activated, act_back = jax.vjp(gated_gelu, gate_pre, up_pre)
    hid_low = activated.astype(bf16)

    gain_n = mixer_norm_gain.reshape(1, -1)
    found = exchange(
        sizes,
        3,
        Summed(sizes, [(hid_low, w_down, None, False)]),
        finish_forward,
        [after_attn, gain_n],
        [own_shape],
        width,
        [(mixer_gate_input_weight, 2, 1), (mixer_output_weight, 0, 1)],
        plan=(6,),
    )
    xn, (after_mlp,) = found["gathered"], found["finish"]
    w_zx, w_out = found["moves"]
    few = step_size_weight.shape[1] // plane_size
    bc_bias = state_map_tap_bias[None]
    mark_block = (3 * width + 3 * rank) // 128
    *kept, sums = mixer_forward(
        xn, xa_wide, mark_block, w_zx, w_step, state_map_weight, w_out, small, state_map_taps, bc_bias, groups
    )
    sums = sum_small(sizes, 4, sums)
    d_z, d_xs, d_step, d_bc_part, yn_low, grad_w_zx, grad_w_dt, grad_w_out, few_x, few_bc = (
        mixer_backward(xn, xa_wide, mark_block, kept, sums, small, state_map_taps, bc_bias, groups)
    )
    grad_conv_bc, grad_conv_bc_bias = few_bc[:4], few_bc[4]
    found = exchange(
        sizes,
        5,
        Summed(
            sizes,
            [
                (d_z, w_zx, 0, True),
                (d_xs, w_zx, 1, True),
                (d_step, w_step, None, True),
            ],
            d_bc_part,
        ),
        finish_mixer_back,
        [after_mlp, gain_n, cot_low, state_map_weight],
        [own_shape, gain_n.shape],
        width + d_bc_part.shape[1],
        [(grad_w_zx, 1, 2), (grad_w_out, 1, 0)],
        plan=(6,),
        also_sum=(
            Summed(sizes, [(yn_low, w_out, None, False)]),
            finish_out,
            [after_mlp],
            jax.ShapeDtypeStruct(own_shape, bf16),
        ),
    )
    gathered, (d_after_mlp, grad_g_mamba) = found["gathered"], found["finish"]
    out_mine, (grad_w_zx, grad_w_out) = found["second"], found["moves"]

    d_mlp, d_bc = gathered[:, :width], gathered[:, width:]
    grad_w_bc = outer_product_sum(xn, d_bc)
    grad_w_down = outer_product_sum(hid_low, d_mlp)
    d_gate, d_up = act_back(matrix_product_transposed(d_mlp, w_down))
    d_gate, d_up = d_gate.astype(bf16), d_up.astype(bf16)
    grad_w_gu = jnp.stack(
        [outer_product_sum(xm, d_gate).astype(bf16), outer_product_sum(xm, d_up).astype(bf16)]
    )

    found = exchange(
        sizes,
        6,
        Summed(sizes, [(d_gate, w_gu, 0, True), (d_up, w_gu, 1, True)]),
        finish_mlp_back,
        [after_attn, gain_m, d_after_mlp],
        [own_shape, gain_m.shape],
        width,
        [(grad_w_gu, 1, 2), (grad_w_down.astype(bf16), 1, 0)],
    )
    d_attn, (d_after_attn, grad_g_mlp) = found["gathered"], found["finish"]
    grad_w_gu, grad_w_down = found["moves"]
    *d_proj, dmid_part, grad_w_qkv, grad_w_o, adapter_up_gradient = attention_backward(
        d_attn, xa_wide, width_a, w_o, up_maps, kept_a, groups
    )
    shares = jnp.concatenate([few_x, grad_w_dt[:few].reshape(-1, 128)]).astype(bf16)
    sums = [grad_g_mlp[0], grad_g_mamba[0], grad_conv_bc, grad_conv_bc_bias]
    row = jnp.concatenate([part.reshape(-1) for part in sums])[None]
    found = exchange(
        sizes,
        7,
        Summed(sizes, [(d_proj[j], w_qkv, j, True) for j in range(3)], dmid_part),
        finish_attention_back,
        [
            hidden,
            embeds,
            attention_norm_gain.reshape(1, -1),
            d_after_attn,
            adapter_down_maps,
            out_mine,
            row,
        ],
        [],
        3 * rank,
        [
            (grad_w_qkv, 1, 2),
            (grad_w_o, 1, 0),
        ],
        plan=(5,),
        tail=3 * width,
        small=width_a + row.shape[1],
        spread=jnp.concatenate([adapter_up_gradient.reshape(-1, 128).astype(bf16), shares]),
    )
    dmid, back, row = found["gathered"], found["tail"], found["small"][0]
    grad_w_qkv, grad_w_o = found["moves"]
    shared = found["spread"].reshape(plane_size, -1, 128)
    adapter_up_gradient = shared[:, : 3 * rank].reshape(plane_size, 3, rank, 128)
    adapter_up_gradient = adapter_up_gradient.transpose(1, 2, 0, 3).reshape(3, rank, -1)
    shared = shared[:, 3 * rank :].transpose(1, 0, 2).reshape(-1, plane_size * 128)
    adapter_down_gradient = adapter_products(xa_wide, dmid, width_a)
    result = back[:, :width]
    d_hidden = back[:, width : 2 * width].astype(f32)
    d_embeds = back[:, 2 * width :].astype(f32)
    adapter_up_gradient = adapter_up_gradient.astype(f32)
    shared = shared.astype(f32)
    grad_conv_x, grad_conv_x_bias, grad_g_gate = shared[:4], shared[4], shared[5]
    heads = shared.reshape(-1, plane_size, 128)
    grad_dt_bias = heads[6, :, :few].reshape(-1)
    grad_a_log = heads[7, :, :few].reshape(-1)
    grad_d_skip = heads[8].reshape(plane_size, few, MIXER_HEAD_SIZE).sum(axis=2).reshape(-1)
    grad_w_dt = shared[16:].reshape(few, -1, plane_size, 128).transpose(1, 3, 2, 0)
    grad_w_dt = grad_w_dt.reshape(-1, plane_size * few)
    grad_g_attn = row[:width_a]
    grad_g_mlp, grad_g_mamba, grad_conv_bc, grad_conv_bc_bias = unpack(row[width_a:], sums)

    return (
        result,
        d_hidden,
        d_embeds,
        grad_g_attn,
        adapter_down_gradient,
        grad_w_qkv.astype(f32),
        adapter_up_gradient,
        grad_w_o.astype(f32),
        grad_g_mlp,
        grad_w_gu.astype(f32),
        grad_w_down.astype(f32),
        grad_g_mamba,
        grad_w_zx.astype(f32),
        grad_w_bc,
        grad_w_dt,
        grad_conv_x,
        grad_conv_x_bias,
        grad_conv_bc,
        grad_conv_bc_bias,
        grad_dt_bias,
        grad_a_log,
        grad_d_skip,
        grad_g_gate,
        grad_w_out.astype(f32),
    )


def solution(mesh):
    placed = (
        P(("fsdp", "ctx"), None),
        P(("fsdp", "ctx"), None),
        P(("fsdp", "ctx"), None),
        P("fsdp", None),
        P(),
        P(),
        P(None, ("fsdp", "ctx"), "tp"),
        P(None, None, "tp"),
        P("tp", ("fsdp", "ctx")),
        P(),
        P(None, ("fsdp", "ctx"), "tp"),
        P("tp", ("fsdp", "ctx")),
        P(),
        P(None, ("fsdp", "ctx"), "tp"),
        P(),
        P(None, "tp"),
        P(None, "tp"),
        P("tp"),
        P(),
        P(),
        P("tp"),
        P("tp"),
        P("tp"),
        P("tp"),
        P("tp", ("fsdp", "ctx")),
    )
    devices = mesh.shape["fsdp"] * mesh.shape["ctx"] * mesh.shape["tp"]
    one_head_each = devices == AHEADS and mesh.shape["ctx"] == 2 and mesh.shape["tp"] == 4
    return jax.shard_map(
        per_device_split if one_head_each else per_device,
        mesh=mesh,
        in_specs=placed,
        out_specs=(
            P(("fsdp", "ctx"), None),
            P(("fsdp", "ctx"), None),
            P(("fsdp", "ctx"), None),
            P(),
            P(),
            P(None, ("fsdp", "ctx"), "tp"),
            P(None, None, "tp"),
            P("tp", ("fsdp", "ctx")),
            P(),
            P(None, ("fsdp", "ctx"), "tp"),
            P("tp", ("fsdp", "ctx")),
            P(),
            P(None, ("fsdp", "ctx"), "tp"),
            P(),
            P(None, "tp"),
            P(None, "tp"),
            P("tp"),
            P(),
            P(),
            P("tp"),
            P("tp"),
            P("tp"),
            P("tp"),
            P("tp", ("fsdp", "ctx")),
        ),
        check_vma=False,
    )
```
